32 devices in a mesh: gx: 4 (over y, x), gy: 2 (over core), gz: 4 (over z).
Axes of the slice: x: 2, y: 2, z: 4, core: 2. Of those that a mesh axis runs over, the one named last changes fastest.
Arguments:
- rhs: float32 [3, 32, 32, 512], P(None, 'gx', 'gy', 'gz'), may hold values from -24 to 24
- conductivity: float32 [8], replicated, may hold values from 0.1 to 10
- fraction: float32 [3, 32, 32, 512], P(None, 'gx', 'gy', 'gz'), may hold values from 0.5 to 2
- region: int32 [32, 32, 512], P('gx', 'gy', 'gz'), may hold values from 0 to 7
- flags: int32 [3, 32, 32, 512], P(None, 'gx', 'gy', 'gz'), may hold values 0 or 1
Outputs:
- preconditioned: float32 [3, 32, 32, 512], P(None, 'gx', 'gy', 'gz')
The draws below stay inside these ranges and needn't reach their ends.
All inputs are finite; a program needn't handle non-finite values. No bound on the sum of `flags` on one device may be relied on, other than what follows from the above.
Results may differ from the reference program's by a relative error of at most 0.00002.
Values sent between devices are 32-bit elements; how exact they have to be, the bound alone decides.
A program may use at most 64 MiB of HBM per device.

```python
import math
import jax
import jax.numpy as jnp

REGIONS = 8
NX = 32
NY = 32
NZ = 512


def place_ends(values, stream_key, low, largest):
    shape = values.shape
    spot = [jax.random.randint(jax.random.fold_in(stream_key, axis), (), 0, shape[axis]) for axis in range(len(shape))]
    values = values.at[tuple(spot)].set(low)
    longest = shape.index(max(shape))
    spot[longest] = (spot[longest] + 1) % shape[longest]
    return values.at[tuple(spot)].set(largest)


def shard_levels(key, extent, split, low, high):
    def one(dim, blocks):
        heights = jax.random.uniform(jax.random.fold_in(jax.random.fold_in(key, 6), dim), (blocks,), jnp.float32, low / len(split), high / len(split))
        return jnp.repeat(jnp.exp(heights), extent[dim] // blocks).reshape((-1,) + (1,) * (len(extent) - dim - 1))

    loudness = one(*split[0])
    for cut in split[1:]:
        loudness = loudness * one(*cut)
    return loudness


def scatter_about(rng, dims, width, limit, shards=(), kind=jnp.bfloat16):
    loudness = shard_levels(rng, dims, shards, -0.22, 0.18) if shards else 1.0
    values = jax.random.normal(rng, dims, jnp.float32) * width * loudness
    return jnp.minimum(jnp.maximum(values, -limit), limit).astype(kind)


def setup_inputs(seed: int = 0) -> dict:
    arg_keys = jax.random.split(jax.random.key(seed), 6)
    rhs = scatter_about(arg_keys[0], (3, NX, NY, NZ), 4.0, 24.0, ((1, 4), (2, 2), (3, 4)), jnp.float32)
    conductivity = jnp.clip(jnp.exp(jax.random.uniform(arg_keys[1], (REGIONS,), jnp.float32, math.log(0.1), math.log(10.0))), 0.1, 10.0)
    fraction = jnp.clip(jnp.exp(math.log(2.0) - 1.3862944 * jax.random.uniform(arg_keys[2], (3, NX, NY, NZ), jnp.float32) ** shard_levels(arg_keys[2], (3, NX, NY, NZ), ((1, 4), (2, 2), (3, 4)), -0.2, 0.2)), 0.5, 2.0)
    region = place_ends(jax.random.randint(arg_keys[3], (NX, NY, NZ), 0, REGIONS), jax.random.fold_in(arg_keys[3], 1), 0, REGIONS - 1).astype(jnp.int32)
    flags = place_ends((jax.random.randint(arg_keys[4], (3, NX, NY, NZ), 0, 8) < 1).astype(jnp.int32), jax.random.fold_in(arg_keys[4], 1), 0, 1)
    return dict(rhs=rhs, conductivity=conductivity, fraction=fraction, region=region, flags=flags)


edge_damping = 0.8
node_damping = 0.8


def upward(field, spatial):
    return jnp.roll(field, -1, axis=spatial)


def downward(field, spatial):
    return jnp.roll(field, 1, axis=spatial)


def forward_diff(field, spatial):
    return upward(field, spatial) - field


def backward_adjoint(field, spatial):
    return downward(field, spatial) - field


def curl_curl(stacked):
    first, second, third = stacked[0], stacked[1], stacked[2]
    face_zero = forward_diff(third, 1) - forward_diff(second, 2)
    face_one = forward_diff(first, 2) - forward_diff(third, 0)
    face_two = forward_diff(second, 0) - forward_diff(first, 1)
    return jnp.stack([backward_adjoint(face_one, 2) - backward_adjoint(face_two, 1),
                      backward_adjoint(face_two, 0) - backward_adjoint(face_zero, 2),
                      backward_adjoint(face_zero, 1) - backward_adjoint(face_one, 0)])


def conductance(conductivity, region):
    total = jnp.zeros(region.shape, conductivity.dtype)
    for number in range(conductivity.shape[0]):
        total = total + jnp.where(region == number, conductivity[number], jnp.zeros((), conductivity.dtype))
    return total


def masked_operator(field, keeping, sigma):
    masked = keeping * field
    return keeping * (curl_curl(masked) + sigma * masked) + (1.0 - keeping) * field


def nodal_operator(stacked):
    result = 7.0 * stacked
    for spatial in range(3):
        result = result - (jnp.roll(stacked, -1, axis=spatial + 1) + jnp.roll(stacked, 1, axis=spatial + 1))
    return result


def nodal_part(masked_res):
    gradient_rhs = backward_adjoint(masked_res[0], 0)
    for spatial in range(1, 3):
        gradient_rhs = gradient_rhs + backward_adjoint(masked_res[spatial], spatial)
    vector_rhs = [(masked_res[spatial] + downward(masked_res[spatial], spatial)) * 0.5 for spatial in range(3)]
    nodal_rhs = jnp.stack([gradient_rhs] + vector_rhs)
    first_node = node_damping * nodal_rhs / 7.0
    second_node = first_node + node_damping * (nodal_rhs - nodal_operator(first_node)) / 7.0
    potential = second_node[0]
    parts = [forward_diff(potential, spatial) + (second_node[spatial + 1] + upward(second_node[spatial + 1], spatial)) * 0.5 for spatial in range(3)]
    return jnp.stack(parts)


def reference(rhs, conductivity, fraction, region, flags):
    sigma = conductance(conductivity, region)[None] * fraction
    keeping = 1.0 - flags.astype(jnp.float32)
    inverse = 1.0 / (keeping * (4.0 + sigma) + (1.0 - keeping))
    first_iter = edge_damping * inverse * rhs
    second_iter = first_iter + edge_damping * inverse * (rhs - masked_operator(first_iter, keeping, sigma))
    residual = rhs - masked_operator(second_iter, keeping, sigma)
    correction = keeping * nodal_part(keeping * residual)
    return second_iter + correction
```

```python
import functools

import jax
import jax.numpy as jnp
from jax import lax
from jax.experimental import pallas as pl
from jax.experimental.pallas import tpu as pltpu
from jax.sharding import PartitionSpec as P

damping = 0.8
c_node = 0.8 / 7.0
MESH = pl.DeviceIdType.MESH
PAD = 4
SEG = 16


def rot(v, shift, axis):
    return pltpu.roll(v, shift % v.shape[axis], axis)


def y_up(v):
    return rot(v, -1, 0)


def y_down(v):
    return rot(v, 1, 0)


def z_up(v):
    return rot(v, -1, 1)


def z_down(v):
    return rot(v, 1, 1)


def face_zero(u1, u2):
    return (y_up(u2) - u2) - (z_up(u1) - u1)


def face_one(u0, u2, u2p):
    return (z_up(u0) - u0) - (u2p - u2)


def face_two(u0, u1, u1p):
    return (u1p - u1) - (y_up(u0) - u0)


def edges(f0, f1, f2, f1m, f2m):
    return (
        (z_down(f1) - f1) - (y_down(f2) - f2),
        (f2m - f2) - (z_down(f0) - f0),
        (y_down(f0) - f0) - (f1m - f1),
    )


def jacobi_scale(ks):
    return damping / jnp.where(ks > 0.0, 4.0 + ks, 1.0)


def start_iter(rhs, ks):
    return jnp.where(ks > 0.0, jacobi_scale(ks) * rhs, 0.0)


def next_iter(rhs, ks, u, cc):
    new = u + jacobi_scale(ks) * (rhs - (cc + ks * u))
    return jnp.where(ks > 0.0, new, 0.0)


def masked_residual(rhs, ks, u, cc):
    return jnp.where(ks > 0.0, rhs - (cc + ks * u), 0.0)


def nodal_rhs(m0, m0m, m1, m2):
    m1m, m2m = y_down(m1), z_down(m2)
    return (
        (m0m - m0) + (m1m - m1) + (m2m - m2),
        (m0 + m0m) * 0.5,
        (m1 + m1m) * 0.5,
        (m2 + m2m) * 0.5,
    )


def nodal_step(r, rm, rp):
    around = (rm + rp) + (y_up(r) + y_down(r)) + (z_up(r) + z_down(r))
    return (1.2 * c_node) * r + (c_node * c_node) * around


def finish(rhs, ks, u, corr):
    fixed = damping * rhs
    fixed = fixed + damping * (rhs - fixed)
    return jnp.where(ks > 0.0, u + corr, fixed)


def kernel(
    sizes, nx, ny, nz, cond_hbm, rhs_hbm, frac_hbm, reg_hbm, flag_hbm, out_ref,
    cond, rhs_ref, frac_ref, reg_ref, flag_ref,
    e, w, wz, kf, ds, dr, ya, yb, yra, yrb, u1, u2, mm, rr, load, send, recv, near,
):
    gx, gy, gz = sizes
    pos = {"gx": lax.axis_index("gx"), "gy": lax.axis_index("gy"), "gz": lax.axis_index("gz")}
    size = {"gx": gx, "gy": gy, "gz": gz}
    tiles = nx * SEG // nz
    planes = nx + 2 * PAD
    per = nz // SEG

    def device(**steps):
        return {axis: lax.rem(pos[axis] + (step + size[axis]), size[axis]) for axis, step in steps.items()}

    partners = [device(gx=1), device(gx=-1), device(gy=1)]
    if gy > 2:
        partners.append(device(gy=-1))
    steps = [(x, z) for z in (1, -1) for x in (0, 1, -1)]
    far = [device(gx=x, gz=z) for x, z in steps]
    alternate = gz % 2 == 0
    early = lax.rem(pos["gz"], 2) == 0
    barrier = pltpu.get_barrier_semaphore()

    def greet(devices):
        for one in devices:
            pl.semaphore_signal(barrier, inc=1, device_id=one, device_id_type=MESH)

    greet(partners)
    if alternate:
        pl.when(early)(lambda: greet(far))
    else:
        greet(far)
    loads = [
        pltpu.make_async_copy(src, dst, load.at[i])
        for i, (src, dst) in enumerate(
            ((cond_hbm, cond), (reg_hbm, reg_ref), (frac_hbm, frac_ref), (flag_hbm, flag_ref), (rhs_hbm, rhs_ref))
        )
    ]
    with jax.named_scope("load"):
        for one in loads:
            one.start()
        for one in loads:
            one.wait()

    lane = lax.broadcasted_iota(jnp.int32, (ny, nz), 1)
    slot = lane // SEG
    half = nz // 2
    low_half = lane < half
    quad = (lane % SEG) // 4
    left = (lane % SEG) < 8

    def end_piece(v, j):
        return rot(v, 8 + SEG * j, 1)

    packs = [[None] * tiles for _ in range(6)]
    outer = {nx - 3: 0, 3: 1}
    for x in range(nx):
        region = reg_ref[x]
        sigma = jnp.zeros((ny, nz), jnp.float32)
        for number in range(cond.shape[0]):
            sigma = jnp.where(region == number, cond[number], sigma)
        t, j = divmod(x, per)
        for k in range(3):
            ks = jnp.where(flag_ref[k, x] == 0, sigma * frac_ref[k, x], 0.0)
            rhs = rhs_ref[k, x]
            for f, v in ((k, rhs), (3 + k, ks)):
                e[f, PAD + x, 0:ny, :] = v
                piece = end_piece(v, j)
                old = packs[f][t]
                packs[f][t] = piece if old is None else jnp.where(slot == j, piece, old)
            if x in outer:
                kf[outer[x], k] = start_iter(rhs, ks)
    for f in range(6):
        for t in range(tiles):
            w[f, t] = packs[f][t]
    for side in range(2):
        mine = (lane >= half) if side == 0 else low_half
        j = (nx - 3) % per if side == 0 else 3
        t = tiles - 1 if side == 0 else 0
        for zside, off in ((0, 8), (1, 4)):
            tile = None
            for f in range(6):
                v = packs[f][t]
                if f < 3:
                    v = jnp.where(slot == j, start_iter(v, packs[3 + f][t]), v)
                moved = rot(v, 4 * (f % 4) - off + (half if f >= 4 else 0), 1)
                where = (quad == f % 4) & (mine if f < 4 else ~mine)
                tile = moved if tile is None else jnp.where(where, moved, tile)
            ds[side, zside] = tile
    with jax.named_scope("barrierwait"):
        if alternate:
            pl.semaphore_wait(barrier, jnp.where(early, len(partners), len(partners) + len(far)))

            @pl.when(jnp.logical_not(early))
            def _():
                for i, (x, z) in enumerate(steps):
                    there = steps.index((-x, -z))
                    pl.semaphore_signal(near.at[there], inc=1, device_id=far[i], device_id_type=MESH)
        else:
            pl.semaphore_wait(barrier, len(partners) + len(far))

    def copy(number, src, dst, where):
        made = pltpu.make_async_remote_copy(
            src_ref=src, dst_ref=dst, send_sem=send.at[number], recv_sem=recv.at[number],
            device_id=where, device_id_type=MESH,
        )
        made.start()
        return made

    own_rows = pl.ds(0, ny)
    x_copies = [
        copy(6, e.at[:, pl.ds(PAD + nx - 2, 2), own_rows], e.at[:, pl.ds(2, 2), own_rows], device(gx=1)),
        copy(7, e.at[:, pl.ds(PAD, 3), own_rows], e.at[:, pl.ds(PAD + nx, 3), own_rows], device(gx=-1)),
        copy(14, kf.at[0], e.at[pl.ds(0, 3), 1, own_rows], device(gx=1)),
        copy(15, kf.at[1, pl.ds(1, 2)], e.at[pl.ds(1, 2), PAD + nx + 3, own_rows], device(gx=-1)),
    ]

    base_a = planes
    base_b = planes + tiles + 1
    row = lax.broadcasted_iota(jnp.int32, (8, nz), 0)

    def y_start(first, which, out, into):
        for f in range(6):
            for i, p in enumerate(which):
                out[f, i] = jnp.where(row < 4, e[f, p, 0:8, :], e[f, p, ny - 8:ny, :])
        if gy == 2:
            return [copy(first, out, into.at[0], device(gy=1))]
        return [
            copy(first, out, into.at[0], device(gy=-1)),
            copy(first + 1, out, into.at[1], device(gy=1)),
        ]

    def y_finish(copies, which, into):
        for one in copies:
            one.wait()
        for f in range(6):
            for i, p in enumerate(which):
                tile = into[0, f, i] if gy == 2 else jnp.where(row < 4, into[0, f, i], into[1, f, i])
                e[f, p, ny:ny + 8, :] = tile

    def curl_sweep(u, lo, hi, emit):
        def faces(p):
            v0, v1, v2 = u[0, p], u[1, p], u[2, p]
            return face_one(v0, v2, u[2, p + 1]), face_two(v0, v1, u[1, p + 1])

        f1m, f2m = faces(lo - 1)
        for p in range(lo, hi):
            f1, f2 = faces(p)
            f0 = face_zero(u[1, p], u[2, p])
            cc = edges(f0, f1, f2, f1m, f2m)
            for k in range(3):
                emit(k, p, cc[k])
            f1m, f2m = f1, f2

    def emit_second(k, p, cc):
        u2[k, p] = next_iter(e[k, p], e[3 + k, p], u1[k, p], cc)

    def emit_masked(k, p, cc):
        mm[k, p] = masked_residual(e[k, p], e[3 + k, p], u2[k, p], cc)

    def node_range(lo, hi):
        for p in range(lo, hi):
            r = nodal_rhs(mm[0, p], mm[0, p - 1], mm[1, p], mm[2, p])
            for q in range(4):
                rr[q, p] = r[q]

    def first_range(which):
        for p in which:
            for k in range(3):
                u1[k, p] = start_iter(e[k, p], e[3 + k, p])

    own = list(range(PAD, PAD + nx))
    with jax.named_scope("y1"):
        y_own = y_start(10, own, ya, yra)
        y_finish(y_own, own, yra)
    with jax.named_scope("inner"):
        first_range(own)
        curl_sweep(u1, PAD + 1, PAD + nx - 1, emit_second)
        curl_sweep(u2, PAD + 2, PAD + nx - 2, emit_masked)
        node_range(PAD + 3, PAD + nx - 2)
    with jax.named_scope("nearwait"):
        if alternate:
            @pl.when(early)
            def _():
                for i in range(len(steps)):
                    pl.semaphore_wait(near.at[i], 1)
    z_copies = [copy(0, w, wz.at[0], device(gz=1)), copy(1, w, wz.at[1], device(gz=-1))]
    corner_copies = [
        copy(2 + 2 * side + zside, ds.at[side, zside], dr.at[side, zside], device(gx=1 - 2 * side, gz=2 * zside - 1))
        for side in range(2) for zside in range(2)
    ]
    with jax.named_scope("zwait"):
        for one in z_copies:
            one.wait()
    for f in range(6):
        for t in range(tiles):
            mid = w[f, t]
            e[f, base_a + t, 0:ny, :] = jnp.where(left, mid, wz[1, f, t])
            e[f, base_b + t, 0:ny, :] = jnp.where(left, wz[0, f, t], mid)
    with jax.named_scope("xwait"):
        for one in x_copies:
            one.wait()
    with jax.named_scope("cornerwait"):
        for one in corner_copies:
            one.wait()
    for f in range(6):
        ends = None
        for i in range(8):
            if i != 4:
                p = PAD + nx + i if i < 4 else i - 4
                piece = end_piece(e[f, p, 0:ny, :], i)
                ends = piece if ends is None else jnp.where(slot == i, piece, ends)
        corner = []
        for zside, off in ((0, 8), (1, 4)):
            plus, minus = dr[1, zside], dr[0, zside]
            if f < 4:
                corner.append(rot(jnp.where(low_half, plus, minus), off - 4 * f, 1))
            else:
                corner.append(rot(jnp.where(low_half, minus, plus), half + off - 4 * (f - 4), 1))
        e[f, base_a + tiles, 0:ny, :] = jnp.where(left, ends, corner[0])
        e[f, base_b + tiles, 0:ny, :] = jnp.where(left, corner[1], ends)
    rest = list(range(1, PAD)) + list(range(PAD + nx, planes)) + list(range(base_a, base_b + tiles + 1))
    with jax.named_scope("yrest"):
        y_rest = y_start(12, rest, yb, yrb)
        y_finish(y_rest, rest, yrb)

    lane24 = lax.broadcasted_iota(jnp.int32, (ny + 8, nz), 1)

    sent = (lane24 // SEG == 3) | (lane24 // SEG == 5)

    def x_up(vs):
        rs = [rot(v, -SEG, 1) for v in vs]
        return [jnp.where(lane24 < nz - SEG, rs[t], rs[(t + 1) % len(rs)]) for t in range(len(rs))]

    def x_down(vs):
        rs = [rot(v, SEG, 1) for v in vs]
        return [jnp.where(lane24 >= SEG, rs[t], rs[t - 1]) for t in range(len(rs))]

    count = tiles + 1

    def strip_curl(u):
        u1p, u2p = x_up(u[1]), x_up(u[2])
        f0 = [face_zero(u[1][t], u[2][t]) for t in range(count)]
        f1 = [face_one(u[0][t], u[2][t], u2p[t]) for t in range(count)]
        f2 = [face_two(u[0][t], u[1][t], u1p[t]) for t in range(count)]
        f1m, f2m = x_down(f1), x_down(f2)
        out = [edges(f0[t], f1[t], f2[t], f1m[t], f2m[t]) for t in range(count)]
        return [[out[t][k] for t in range(count)] for k in range(3)]

    strips = jax.named_scope('strips')
    strips.__enter__()
    ends = []
    for base in (base_a, base_b):
        def sr(k, t):
            return e[k, base + t]

        def sk(k, t):
            return e[3 + k, base + t]

        span = range(count)
        u = [[start_iter(sr(k, t), sk(k, t)) for t in span] for k in range(3)]
        for k in range(3):
            u[k][tiles] = jnp.where(sent, sr(k, tiles), u[k][tiles])
        cc = strip_curl(u)
        u = [[next_iter(sr(k, t), sk(k, t), u[k][t], cc[k][t]) for t in span] for k in range(3)]
        cc = strip_curl(u)
        m = [[masked_residual(sr(k, t), sk(k, t), u[k][t], cc[k][t]) for t in span] for k in range(3)]
        m0m = x_down(m[0])
        r = [nodal_rhs(m[0][t], m0m[t], m[1][t], m[2][t]) for t in span]
        s = []
        for q in range(4):
            rq = [r[t][q] for t in span]
            rm, rp = x_down(rq), x_up(rq)
            s.append([nodal_step(rq[t], rm[t], rp[t]) for t in span])
        s0p, s1p = x_up(s[0]), x_up(s[1])
        result = []
        for t in range(tiles):
            corr = (
                (s0p[t] - s[0][t]) + (s[1][t] + s1p[t]) * 0.5,
                (y_up(s[0][t]) - s[0][t]) + (s[2][t] + y_up(s[2][t])) * 0.5,
                (z_up(s[0][t]) - s[0][t]) + (s[3][t] + z_up(s[3][t])) * 0.5,
            )
            result.append([finish(sr(k, t), sk(k, t), u[k][t], corr[k])[0:ny] for k in range(3)])
        ends.append(result)
    for t in range(tiles):
        for k in range(3):
            w[k, t] = jnp.where(left, ends[0][t][k], ends[1][t][k])

    strips.__exit__(None, None, None)
    outer_x = jax.named_scope('outerx')
    outer_x.__enter__()
    for k in range(3):
        u1[k, 1] = e[k, 1]
        u1[k, planes - 1] = e[k, planes - 1]
    first_range(list(range(2, PAD)) + list(range(PAD + nx, planes - 1)))
    curl_sweep(u1, PAD - 2, PAD + 1, emit_second)
    curl_sweep(u1, PAD + nx - 1, PAD + nx + 3, emit_second)
    curl_sweep(u2, PAD - 1, PAD + 2, emit_masked)
    curl_sweep(u2, PAD + nx - 2, PAD + nx + 2, emit_masked)
    p = PAD - 2
    v0, v1, v2 = u2[0, p], u2[1, p], u2[2, p]
    f1 = face_one(v0, v2, u2[2, p + 1])
    f2 = face_two(v0, v1, u2[1, p + 1])
    emit_masked(0, p, (z_down(f1) - f1) - (y_down(f2) - f2))
    node_range(PAD - 1, PAD + 3)
    node_range(PAD + nx - 2, PAD + nx + 2)

    outer_x.__exit__(None, None, None)
    inner = (lane >= 4) & (lane < nz - 4)
    s_next = [nodal_step(rr[q, PAD], rr[q, PAD - 1], rr[q, PAD + 1]) for q in range(4)]
    for x in range(nx):
        p = PAD + x
        s = s_next
        s_next = [nodal_step(rr[q, p + 1], rr[q, p], rr[q, p + 2]) for q in range(4)] if x < nx - 1 else [
            nodal_step(rr[q, p + 1], rr[q, p], rr[q, p + 2]) for q in range(2)
        ]
        corr = (
            (s_next[0] - s[0]) + (s[1] + s_next[1]) * 0.5,
            (y_up(s[0]) - s[0]) + (s[2] + y_up(s[2])) * 0.5,
            (z_up(s[0]) - s[0]) + (s[3] + z_up(s[3])) * 0.5,
        )
        t, j = divmod(x, per)
        for k in range(3):
            body = finish(e[k, p, 0:ny], e[3 + k, p, 0:ny], u2[k, p, 0:ny], corr[k][0:ny])
            out_ref[k, x] = jnp.where(inner, body, rot(w[k, t], nz - 8 - SEG * j, 1))


def on_device(sizes, rhs, conductivity, fraction, region, flags):
    _, nx, ny, nz = rhs.shape
    tiles = nx * SEG // nz
    planes = nx + 2 * PAD
    total = planes + 2 * (tiles + 1)
    rest = 2 * PAD - 1 + 2 * (tiles + 1)
    rows = ny + 8
    f32 = jnp.float32
    hbm = pl.BlockSpec(memory_space=pl.ANY)
    sides = 1 if sizes[1] == 2 else 2
    return pl.pallas_call(
        functools.partial(kernel, sizes, nx, ny, nz),
        out_shape=pltpu.VMEM(rhs.shape, rhs.dtype),
        in_specs=[hbm] * 5,
        out_specs=pl.BlockSpec(memory_space=pltpu.VMEM),
        scratch_shapes=[
            pltpu.SMEM(conductivity.shape, f32),
            pltpu.VMEM(rhs.shape, f32),
            pltpu.VMEM(rhs.shape, f32),
            pltpu.VMEM(region.shape, jnp.int32),
            pltpu.VMEM(flags.shape, jnp.int32),
            pltpu.VMEM((6, total, rows, nz), f32),
            pltpu.VMEM((6, tiles, ny, nz), f32),
            pltpu.VMEM((2, 6, tiles, ny, nz), f32),
            pltpu.VMEM((2, 3, ny, nz), f32),
            pltpu.VMEM((2, 2, ny, nz), f32),
            pltpu.VMEM((2, 2, ny, nz), f32),
            pltpu.VMEM((6, nx, 8, nz), f32),
            pltpu.VMEM((6, rest, 8, nz), f32),
            pltpu.VMEM((sides, 6, nx, 8, nz), f32),
            pltpu.VMEM((sides, 6, rest, 8, nz), f32),
            pltpu.VMEM((3, planes, rows, nz), f32),
            pltpu.VMEM((3, planes, rows, nz), f32),
            pltpu.VMEM((3, planes, rows, nz), f32),
            pltpu.VMEM((4, planes, rows, nz), f32),
            pltpu.SemaphoreType.DMA((5,)),
            pltpu.SemaphoreType.DMA((16,)),
            pltpu.SemaphoreType.DMA((16,)),
            pltpu.SemaphoreType.REGULAR((6,)),
        ],
        compiler_params=pltpu.CompilerParams(
            collective_id=0, has_side_effects=True, vmem_limit_bytes=60 * 1024 * 1024
        ),
    )(conductivity, rhs, fraction, region, flags)


def solution(mesh):
    sizes = tuple(mesh.shape[name] for name in ("gx", "gy", "gz"))
    return jax.shard_map(
        functools.partial(on_device, sizes),
        mesh=mesh,
        in_specs=(
            P(None, "gx", "gy", "gz"),
            P(),
            P(None, "gx", "gy", "gz"),
            P("gx", "gy", "gz"),
            P(None, "gx", "gy", "gz"),
        ),
        out_specs=P(None, "gx", "gy", "gz"),
        check_vma=False,
    )
```

```python
import functools

import jax
import jax.numpy as jnp
from jax import lax
from jax.experimental import pallas as pl
from jax.experimental.pallas import tpu as pltpu
from jax.sharding import PartitionSpec as P

damping = 0.8
c_node = 0.8 / 7.0
MESH = pl.DeviceIdType.MESH
PAD = 4
SEG = 16


def rot(v, shift, axis):
    return pltpu.roll(v, shift % v.shape[axis], axis)


def y_up(v):
    return rot(v, -1, 0)


def y_down(v):
    return rot(v, 1, 0)


def z_up(v):
    return rot(v, -1, 1)


def z_down(v):
    return rot(v, 1, 1)


def face_zero(u1, u2):
    return (y_up(u2) - u2) - (z_up(u1) - u1)


def face_one(u0, u2, u2p):
    return (z_up(u0) - u0) - (u2p - u2)


def face_two(u0, u1, u1p):
    return (u1p - u1) - (y_up(u0) - u0)


def edges(f0, f1, f2, f1m, f2m):
    return (
        (z_down(f1) - f1) - (y_down(f2) - f2),
        (f2m - f2) - (z_down(f0) - f0),
        (y_down(f0) - f0) - (f1m - f1),
    )


def jacobi_scale(ks):
    return damping / jnp.where(ks > 0.0, 4.0 + ks, 1.0)


def start_iter(rhs, ks):
    return jnp.where(ks > 0.0, jacobi_scale(ks) * rhs, 0.0)


def next_iter(rhs, ks, u, cc):
    new = u + jacobi_scale(ks) * (rhs - (cc + ks * u))
    return jnp.where(ks > 0.0, new, 0.0)


def masked_residual(rhs, ks, u, cc):
    return jnp.where(ks > 0.0, rhs - (cc + ks * u), 0.0)


def nodal_rhs(m0, m0m, m1, m2):
    m1m, m2m = y_down(m1), z_down(m2)
    return (
        (m0m - m0) + (m1m - m1) + (m2m - m2),
        (m0 + m0m) * 0.5,
        (m1 + m1m) * 0.5,
        (m2 + m2m) * 0.5,
    )


def nodal_step(r, rm, rp):
    around = (rm + rp) + (y_up(r) + y_down(r)) + (z_up(r) + z_down(r))
    return (1.2 * c_node) * r + (c_node * c_node) * around


def finish(rhs, ks, u, corr):
    fixed = damping * rhs
    fixed = fixed + damping * (rhs - fixed)
    return jnp.where(ks > 0.0, u + corr, fixed)


def kernel(
    sizes, nx, ny, nz, cond_hbm, rhs_hbm, frac_hbm, reg_hbm, flag_hbm, out_ref,
    cond, rhs_ref, frac_ref, reg_ref, flag_ref,
    e, w, wz, kf, ds, dr, ya, yb, yra, yrb, u1, u2, mm, rr, load, send, recv, near,
):
    gx, gy, gz = sizes
    pos = {"gx": lax.axis_index("gx"), "gy": lax.axis_index("gy"), "gz": lax.axis_index("gz")}
    size = {"gx": gx, "gy": gy, "gz": gz}
    tiles = nx * SEG // nz
    planes = nx + 2 * PAD
    per = nz // SEG

    def device(**steps):
        return {axis: lax.rem(pos[axis] + (step + size[axis]), size[axis]) for axis, step in steps.items()}

    partners = [device(gx=1), device(gx=-1), device(gy=1)]
    if gy > 2:
        partners.append(device(gy=-1))
    steps = [(x, z) for z in (1, -1) for x in (0, 1, -1)]
    far = [device(gx=x, gz=z) for x, z in steps]
    alternate = gz % 2 == 0
    early = lax.rem(pos["gz"], 2) == 0
    barrier = pltpu.get_barrier_semaphore()

    def greet(devices):
        for one in devices:
            pl.semaphore_signal(barrier, inc=1, device_id=one, device_id_type=MESH)

    greet(partners)
    if alternate:
        pl.when(early)(lambda: greet(far))
    else:
        greet(far)
    loads = [
        pltpu.make_async_copy(src, dst, load.at[i])
        for i, (src, dst) in enumerate(
            ((cond_hbm, cond), (reg_hbm, reg_ref), (frac_hbm, frac_ref), (flag_hbm, flag_ref), (rhs_hbm, rhs_ref))
        )
    ]
    with jax.named_scope("load"):
        for one in loads:
            one.start()
        for one in loads:
            one.wait()

    lane = lax.broadcasted_iota(jnp.int32, (ny, nz), 1)
    slot = lane // SEG
    half = nz // 2
    low_half = lane < half
    quad = (lane % SEG) // 4
    left = (lane % SEG) < 8

    def end_piece(v, j):
        return rot(v, 8 + SEG * j, 1)

    packs = [[None] * tiles for _ in range(6)]
    outer = {nx - 3: 0, 3: 1}
    for x in range(nx):
        region = reg_ref[x]
        sigma = jnp.zeros((ny, nz), jnp.float32)
        for number in range(cond.shape[0]):
            sigma = jnp.where(region == number, cond[number], sigma)
        t, j = divmod(x, per)
        for k in range(3):
            ks = jnp.where(flag_ref[k, x] == 0, sigma * frac_ref[k, x], 0.0)
            rhs = rhs_ref[k, x]
            for f, v in ((k, rhs), (3 + k, ks)):
                e[f, PAD + x, 0:ny, :] = v
                piece = end_piece(v, j)
                old = packs[f][t]
                packs[f][t] = piece if old is None else jnp.where(slot == j, piece, old)
            if x in outer:
                kf[outer[x], k] = start_iter(rhs, ks)
    for f in range(6):
        for t in range(tiles):
            w[f, t] = packs[f][t]
    for side in range(2):
        mine = (lane >= half) if side == 0 else low_half
        j = (nx - 3) % per if side == 0 else 3
        t = tiles - 1 if side == 0 else 0
        for zside, off in ((0, 8), (1, 4)):
            tile = None
            for f in range(6):
                v = packs[f][t]
                if f < 3:
                    v = jnp.where(slot == j, start_iter(v, packs[3 + f][t]), v)
                moved = rot(v, 4 * (f % 4) - off + (half if f >= 4 else 0), 1)
                where = (quad == f % 4) & (mine if f < 4 else ~mine)
                tile = moved if tile is None else jnp.where(where, moved, tile)
            ds[side, zside] = tile
    with jax.named_scope("barrierwait"):
        if alternate:
            pl.semaphore_wait(barrier, jnp.where(early, len(partners), len(partners) + len(far)))

            @pl.when(jnp.logical_not(early))
            def _():
                for i, (x, z) in enumerate(steps):
                    there = steps.index((-x, -z))
                    pl.semaphore_signal(near.at[there], inc=1, device_id=far[i], device_id_type=MESH)
        else:
            pl.semaphore_wait(barrier, len(partners) + len(far))

    def copy(number, src, dst, where, start=True):
        made = pltpu.make_async_remote_copy(
            src_ref=src, dst_ref=dst, send_sem=send.at[number], recv_sem=recv.at[number],
            device_id=where, device_id_type=MESH,
        )
        if start:
            made.start()
        return made

    own_rows = pl.ds(0, ny)
    up_copies = [
        copy(6, e.at[:, pl.ds(PAD + nx - 2, 2), own_rows], e.at[:, pl.ds(2, 2), own_rows], device(gx=1), False),
        copy(14, kf.at[0], e.at[pl.ds(0, 3), 1, own_rows], device(gx=1), False),
    ]
    down_copies = [
        copy(7, e.at[:, pl.ds(PAD, 3), own_rows], e.at[:, pl.ds(PAD + nx, 3), own_rows], device(gx=-1), False),
        copy(15, kf.at[1, pl.ds(1, 2)], e.at[pl.ds(1, 2), PAD + nx + 3, own_rows], device(gx=-1), False),
    ]
    x_copies = up_copies + down_copies
    up_first = lax.rem(pos["gx"], 4) == 3
    z_copies = [copy(0, w, wz.at[0], device(gz=1), False), copy(1, w, wz.at[1], device(gz=-1), False)]
    corner_copies = [
        copy(2 + 2 * side + zside, ds.at[side, zside], dr.at[side, zside], device(gx=1 - 2 * side, gz=2 * zside - 1), False)
        for side in range(2) for zside in range(2)
    ]

    def start_far():
        for one in corner_copies + z_copies:
            one.start()

    if alternate:
        pl.when(jnp.logical_not(early))(start_far)
    else:
        start_far()

    @pl.when(up_first)
    def _():
        for one in up_copies + down_copies:
            one.start()

    @pl.when(jnp.logical_not(up_first))
    def _():
        for one in down_copies + up_copies:
            one.start()

    base_a = planes
    base_b = planes + tiles + 1
    row = lax.broadcasted_iota(jnp.int32, (8, nz), 0)

    def y_start(first, which, out, into):
        for f in range(6):
            for i, p in enumerate(which):
                out[f, i] = jnp.where(row < 4, e[f, p, 0:8, :], e[f, p, ny - 8:ny, :])
        if gy == 2:
            return [copy(first, out, into.at[0], device(gy=1))]
        return [
            copy(first, out, into.at[0], device(gy=-1)),
            copy(first + 1, out, into.at[1], device(gy=1)),
        ]

    def y_finish(copies, which, into):
        for one in copies:
            one.wait()
        for f in range(6):
            for i, p in enumerate(which):
                tile = into[0, f, i] if gy == 2 else jnp.where(row < 4, into[0, f, i], into[1, f, i])
                e[f, p, ny:ny + 8, :] = tile

    def curl_sweep(u, lo, hi, emit):
        def faces(p):
            v0, v1, v2 = u[0, p], u[1, p], u[2, p]
            return face_one(v0, v2, u[2, p + 1]), face_two(v0, v1, u[1, p + 1])

        f1m, f2m = faces(lo - 1)
        for p in range(lo, hi):
            f1, f2 = faces(p)
            f0 = face_zero(u[1, p], u[2, p])
            cc = edges(f0, f1, f2, f1m, f2m)
            for k in range(3):
                emit(k, p, cc[k])
            f1m, f2m = f1, f2

    def emit_second(k, p, cc):
        u2[k, p] = next_iter(e[k, p], e[3 + k, p], u1[k, p], cc)

    def emit_masked(k, p, cc):
        mm[k, p] = masked_residual(e[k, p], e[3 + k, p], u2[k, p], cc)

    def node_range(lo, hi):
        for p in range(lo, hi):
            r = nodal_rhs(mm[0, p], mm[0, p - 1], mm[1, p], mm[2, p])
            for q in range(4):
                rr[q, p] = r[q]

    def first_range(which):
        for p in which:
            for k in range(3):
                u1[k, p] = start_iter(e[k, p], e[3 + k, p])

    own = list(range(PAD, PAD + nx))
    with jax.named_scope("y1"):
        y_own = y_start(10, own, ya, yra)
        y_finish(y_own, own, yra)
    with jax.named_scope("inner"):
        first_range(own)
        curl_sweep(u1, PAD + 1, PAD + nx - 1, emit_second)
        curl_sweep(u2, PAD + 2, PAD + nx - 2, emit_masked)
        node_range(PAD + 3, PAD + nx - 2)
    with jax.named_scope("nearwait"):
        if alternate:
            @pl.when(early)
            def _():
                for i in range(len(steps)):
                    pl.semaphore_wait(near.at[i], 1)
                for one in z_copies + corner_copies:
                    one.start()
    with jax.named_scope("zwait"):
        for one in z_copies:
            one.wait_recv()
    for f in range(6):
        for t in range(tiles):
            mid = w[f, t]
            e[f, base_a + t, 0:ny, :] = jnp.where(left, mid, wz[1, f, t])
            e[f, base_b + t, 0:ny, :] = jnp.where(left, wz[0, f, t], mid)
    with jax.named_scope("xwait"):
        for one in x_copies:
            one.wait_recv()
    with jax.named_scope("cornerwait"):
        for one in corner_copies:
            one.wait_recv()
    for f in range(6):
        ends = None
        for i in range(8):
            if i != 4:
                p = PAD + nx + i if i < 4 else i - 4
                piece = end_piece(e[f, p, 0:ny, :], i)
                ends = piece if ends is None else jnp.where(slot == i, piece, ends)
        corner = []
        for zside, off in ((0, 8), (1, 4)):
            plus, minus = dr[1, zside], dr[0, zside]
            if f < 4:
                corner.append(rot(jnp.where(low_half, plus, minus), off - 4 * f, 1))
            else:
                corner.append(rot(jnp.where(low_half, minus, plus), half + off - 4 * (f - 4), 1))
        e[f, base_a + tiles, 0:ny, :] = jnp.where(left, ends, corner[0])
        e[f, base_b + tiles, 0:ny, :] = jnp.where(left, corner[1], ends)
    rest = list(range(1, PAD)) + list(range(PAD + nx, planes)) + list(range(base_a, base_b + tiles + 1))
    with jax.named_scope("yrest"):
        y_rest = y_start(12, rest, yb, yrb)
        y_finish(y_rest, rest, yrb)

    lane24 = lax.broadcasted_iota(jnp.int32, (ny + 8, nz), 1)

    sent = (lane24 // SEG == 3) | (lane24 // SEG == 5)

    def x_up(vs):
        rs = [rot(v, -SEG, 1) for v in vs]
        return [jnp.where(lane24 < nz - SEG, rs[t], rs[(t + 1) % len(rs)]) for t in range(len(rs))]

    def x_down(vs):
        rs = [rot(v, SEG, 1) for v in vs]
        return [jnp.where(lane24 >= SEG, rs[t], rs[t - 1]) for t in range(len(rs))]

    count = tiles + 1

    def strip_curl(u):
        u1p, u2p = x_up(u[1]), x_up(u[2])
        f0 = [face_zero(u[1][t], u[2][t]) for t in range(count)]
        f1 = [face_one(u[0][t], u[2][t], u2p[t]) for t in range(count)]
        f2 = [face_two(u[0][t], u[1][t], u1p[t]) for t in range(count)]
        f1m, f2m = x_down(f1), x_down(f2)
        out = [edges(f0[t], f1[t], f2[t], f1m[t], f2m[t]) for t in range(count)]
        return [[out[t][k] for t in range(count)] for k in range(3)]

    strips = jax.named_scope('strips')
    strips.__enter__()
    ends = []
    for base in (base_a, base_b):
        def sr(k, t):
            return e[k, base + t]

        def sk(k, t):
            return e[3 + k, base + t]

        span = range(count)
        u = [[start_iter(sr(k, t), sk(k, t)) for t in span] for k in range(3)]
        for k in range(3):
            u[k][tiles] = jnp.where(sent, sr(k, tiles), u[k][tiles])
        cc = strip_curl(u)
        u = [[next_iter(sr(k, t), sk(k, t), u[k][t], cc[k][t]) for t in span] for k in range(3)]
        cc = strip_curl(u)
        m = [[masked_residual(sr(k, t), sk(k, t), u[k][t], cc[k][t]) for t in span] for k in range(3)]
        m0m = x_down(m[0])
        r = [nodal_rhs(m[0][t], m0m[t], m[1][t], m[2][t]) for t in span]
        s = []
        for q in range(4):
            rq = [r[t][q] for t in span]
            rm, rp = x_down(rq), x_up(rq)
            s.append([nodal_step(rq[t], rm[t], rp[t]) for t in span])
        s0p, s1p = x_up(s[0]), x_up(s[1])
        result = []
        for t in range(tiles):
            corr = (
                (s0p[t] - s[0][t]) + (s[1][t] + s1p[t]) * 0.5,
                (y_up(s[0][t]) - s[0][t]) + (s[2][t] + y_up(s[2][t])) * 0.5,
                (z_up(s[0][t]) - s[0][t]) + (s[3][t] + z_up(s[3][t])) * 0.5,
            )
            result.append([finish(sr(k, t), sk(k, t), u[k][t], corr[k])[0:ny] for k in range(3)])
        ends.append(result)
    with jax.named_scope("sendwait"):
        for one in x_copies + z_copies + corner_copies:
            one.wait_send()
    for t in range(tiles):
        for k in range(3):
            w[k, t] = jnp.where(left, ends[0][t][k], ends[1][t][k])

    strips.__exit__(None, None, None)
    outer_x = jax.named_scope('outerx')
    outer_x.__enter__()
    for k in range(3):
        u1[k, 1] = e[k, 1]
        u1[k, planes - 1] = e[k, planes - 1]
    first_range(list(range(2, PAD)) + list(range(PAD + nx, planes - 1)))
    curl_sweep(u1, PAD - 2, PAD + 1, emit_second)
    curl_sweep(u1, PAD + nx - 1, PAD + nx + 3, emit_second)
    curl_sweep(u2, PAD - 1, PAD + 2, emit_masked)
    curl_sweep(u2, PAD + nx - 2, PAD + nx + 2, emit_masked)
    p = PAD - 2
    v0, v1, v2 = u2[0, p], u2[1, p], u2[2, p]
    f1 = face_one(v0, v2, u2[2, p + 1])
    f2 = face_two(v0, v1, u2[1, p + 1])
    emit_masked(0, p, (z_down(f1) - f1) - (y_down(f2) - f2))
    node_range(PAD - 1, PAD + 3)
    node_range(PAD + nx - 2, PAD + nx + 2)

    outer_x.__exit__(None, None, None)
    inner = (lane >= 4) & (lane < nz - 4)
    s_next = [nodal_step(rr[q, PAD], rr[q, PAD - 1], rr[q, PAD + 1]) for q in range(4)]
    for x in range(nx):
        p = PAD + x
        s = s_next
        s_next = [nodal_step(rr[q, p + 1], rr[q, p], rr[q, p + 2]) for q in range(4)] if x < nx - 1 else [
            nodal_step(rr[q, p + 1], rr[q, p], rr[q, p + 2]) for q in range(2)
        ]
        corr = (
            (s_next[0] - s[0]) + (s[1] + s_next[1]) * 0.5,
            (y_up(s[0]) - s[0]) + (s[2] + y_up(s[2])) * 0.5,
            (z_up(s[0]) - s[0]) + (s[3] + z_up(s[3])) * 0.5,
        )
        t, j = divmod(x, per)
        for k in range(3):
            body = finish(e[k, p, 0:ny], e[3 + k, p, 0:ny], u2[k, p, 0:ny], corr[k][0:ny])
            out_ref[k, x] = jnp.where(inner, body, rot(w[k, t], nz - 8 - SEG * j, 1))


def on_device(sizes, rhs, conductivity, fraction, region, flags):
    _, nx, ny, nz = rhs.shape
    tiles = nx * SEG // nz
    planes = nx + 2 * PAD
    total = planes + 2 * (tiles + 1)
    rest = 2 * PAD - 1 + 2 * (tiles + 1)
    rows = ny + 8
    f32 = jnp.float32
    hbm = pl.BlockSpec(memory_space=pl.ANY)
    sides = 1 if sizes[1] == 2 else 2
    return pl.pallas_call(
        functools.partial(kernel, sizes, nx, ny, nz),
        out_shape=pltpu.VMEM(rhs.shape, rhs.dtype),
        in_specs=[hbm] * 5,
        out_specs=pl.BlockSpec(memory_space=pltpu.VMEM),
        scratch_shapes=[
            pltpu.SMEM(conductivity.shape, f32),
            pltpu.VMEM(rhs.shape, f32),
            pltpu.VMEM(rhs.shape, f32),
            pltpu.VMEM(region.shape, jnp.int32),
            pltpu.VMEM(flags.shape, jnp.int32),
            pltpu.VMEM((6, total, rows, nz), f32),
            pltpu.VMEM((6, tiles, ny, nz), f32),
            pltpu.VMEM((2, 6, tiles, ny, nz), f32),
            pltpu.VMEM((2, 3, ny, nz), f32),
            pltpu.VMEM((2, 2, ny, nz), f32),
            pltpu.VMEM((2, 2, ny, nz), f32),
            pltpu.VMEM((6, nx, 8, nz), f32),
            pltpu.VMEM((6, rest, 8, nz), f32),
            pltpu.VMEM((sides, 6, nx, 8, nz), f32),
            pltpu.VMEM((sides, 6, rest, 8, nz), f32),
            pltpu.VMEM((3, planes, rows, nz), f32),
            pltpu.VMEM((3, planes, rows, nz), f32),
            pltpu.VMEM((3, planes, rows, nz), f32),
            pltpu.VMEM((4, planes, rows, nz), f32),
            pltpu.SemaphoreType.DMA((5,)),
            pltpu.SemaphoreType.DMA((16,)),
            pltpu.SemaphoreType.DMA((16,)),
            pltpu.SemaphoreType.REGULAR((6,)),
        ],
        compiler_params=pltpu.CompilerParams(
            collective_id=0, has_side_effects=True, vmem_limit_bytes=60 * 1024 * 1024
        ),
    )(conductivity, rhs, fraction, region, flags)


def solution(mesh):
    sizes = tuple(mesh.shape[name] for name in ("gx", "gy", "gz"))
    return jax.shard_map(
        functools.partial(on_device, sizes),
        mesh=mesh,
        in_specs=(
            P(None, "gx", "gy", "gz"),
            P(),
            P(None, "gx", "gy", "gz"),
            P("gx", "gy", "gz"),
            P(None, "gx", "gy", "gz"),
        ),
        out_specs=P(None, "gx", "gy", "gz"),
        check_vma=False,
    )
```

```python
import functools

import jax
import jax.numpy as jnp
from jax import lax
from jax.experimental import pallas as pl
from jax.experimental.pallas import tpu as pltpu
from jax.sharding import PartitionSpec as P

damping = 0.8
c_node = 0.8 / 7.0
MESH = pl.DeviceIdType.MESH
PAD = 2
SEG = 16


def rot(v, shift, axis):
    return pltpu.roll(v, shift % v.shape[axis], axis)


def y_up(v):
    return rot(v, -1, 0)


def y_down(v):
    return rot(v, 1, 0)


def z_up(v):
    return rot(v, -1, 1)


def z_down(v):
    return rot(v, 1, 1)


def face_zero(u1, u2):
    return (y_up(u2) - u2) - (z_up(u1) - u1)


def face_one(u0, u2, u2p):
    return (z_up(u0) - u0) - (u2p - u2)


def face_two(u0, u1, u1p):
    return (u1p - u1) - (y_up(u0) - u0)


def edges(f0, f1, f2, f1m, f2m):
    return (
        (z_down(f1) - f1) - (y_down(f2) - f2),
        (f2m - f2) - (z_down(f0) - f0),
        (y_down(f0) - f0) - (f1m - f1),
    )


def jacobi_scale(ks):
    return damping / jnp.where(ks > 0.0, 4.0 + ks, 1.0)


def start_iter(rhs, ks):
    return jnp.where(ks > 0.0, jacobi_scale(ks) * rhs, 0.0)


def next_iter(rhs, ks, u, cc):
    new = u + jacobi_scale(ks) * (rhs - (cc + ks * u))
    return jnp.where(ks > 0.0, new, 0.0)


def masked_residual(rhs, ks, u, cc):
    return jnp.where(ks > 0.0, rhs - (cc + ks * u), 0.0)


def nodal_rhs(m0, m0m, m1, m2):
    m1m, m2m = y_down(m1), z_down(m2)
    return (
        (m0m - m0) + (m1m - m1) + (m2m - m2),
        (m0 + m0m) * 0.5,
        (m1 + m1m) * 0.5,
        (m2 + m2m) * 0.5,
    )


def nodal_step(r, rm, rp):
    around = (rm + rp) + (y_up(r) + y_down(r)) + (z_up(r) + z_down(r))
    return (1.2 * c_node) * r + (c_node * c_node) * around


def finish(rhs, ks, u, corr):
    fixed = damping * rhs
    fixed = fixed + damping * (rhs - fixed)
    return jnp.where(ks > 0.0, u + corr, fixed)


def kernel(
    sizes, nx, ny, nz, cond_hbm, rhs_hbm, frac_hbm, reg_hbm, flag_hbm, out_ref,
    cond, frac_ref, reg_ref, flag_ref,
    e, st, sw, u1, u2, mm, rr, zs, zr, ds, dr, ends_out, ends_in, lower_out, lower_in, upper_out, upper_in,
    ya_out, ya_in, yb_out, yb_in, yc_out, yc_in, yd_out, yd_in, ye_out, ye_in, yf_out, yf_in,
    load, send, recv, near,
):
    gx, gy, gz = sizes
    pos = {"gx": lax.axis_index("gx"), "gy": lax.axis_index("gy"), "gz": lax.axis_index("gz")}
    size = {"gx": gx, "gy": gy, "gz": gz}
    first, last = PAD, PAD + nx - 1
    scope = jax.named_scope

    def device(**steps):
        return {axis: lax.rem(pos[axis] + (step + size[axis]), size[axis]) for axis, step in steps.items()}

    partners = [device(gx=1), device(gx=-1), device(gy=1)]
    if gy > 2:
        partners.append(device(gy=-1))
    steps = [(x, z) for z in (1, -1) for x in (0, 1, -1)]
    far = [device(gx=x, gz=z) for x, z in steps]
    alternate = gz % 2 == 0
    early = lax.rem(pos["gz"], 2) == 0
    barrier = pltpu.get_barrier_semaphore()

    def greet(devices):
        for one in devices:
            pl.semaphore_signal(barrier, inc=1, device_id=one, device_id_type=MESH)

    greet(partners)
    if alternate:
        pl.when(early)(lambda: greet(far))
    else:
        greet(far)
    own_rows = pl.ds(0, ny)
    loads = [
        pltpu.make_async_copy(src, dst, load.at[i])
        for i, (src, dst) in enumerate(
            (
                (cond_hbm, cond), (reg_hbm, reg_ref), (frac_hbm, frac_ref), (flag_hbm, flag_ref),
                (rhs_hbm, e.at[pl.ds(0, 3), pl.ds(first, nx), own_rows]),
            )
        )
    ]
    with scope("load"):
        for one in loads:
            one.start()
        for one in loads:
            one.wait()

    started = []
    numbers = iter(range(64))

    def copy(src, dst, where, start=True):
        number = next(numbers)
        made = pltpu.make_async_remote_copy(
            src_ref=src, dst_ref=dst, send_sem=send.at[number], recv_sem=recv.at[number],
            device_id=where, device_id_type=MESH,
        )
        started.append(made)
        if start:
            made.start()
        return made

    row = lax.broadcasted_iota(jnp.int32, (8, nz), 0)
    top, bottom, halo = slice(0, 8), slice(ny - 8, ny), slice(ny, ny + 8)

    def y_start(places, out, into):
        for i, (ref, where) in enumerate(places):
            out[i] = jnp.where(row < 4, ref[(*where, top, slice(None))], ref[(*where, bottom, slice(None))])
        if gy == 2:
            return [copy(out, into.at[0], device(gy=1))]
        return [copy(out, into.at[0], device(gy=-1)), copy(out, into.at[1], device(gy=1))]

    def y_finish(copies, places, into):
        for one in copies:
            one.wait_recv()
        for i, (ref, where) in enumerate(places):
            tile = into[0, i] if gy == 2 else jnp.where(row < 4, into[0, i], into[1, i])
            ref[(*where, halo, slice(None))] = tile

    lane = lax.broadcasted_iota(jnp.int32, (ny, nz), 1)
    slot = lane // SEG
    half = nz // 2
    low_half = lane < half
    quad = (lane % SEG) // 4
    left = (lane % SEG) < 8

    def end_piece(v, j):
        return rot(v, 8 + SEG * j, 1)

    def pick(base, where, other):
        return other if base is None else jnp.where(where, other, base)

    packs = [None] * 6
    with scope("pack"):
        for x in range(nx):
            region = reg_ref[x]
            sigma = jnp.zeros((ny, nz), jnp.float32)
            for number in range(cond.shape[0]):
                sigma = jnp.where(region == number, cond[number], sigma)
            for k in range(3):
                ks = jnp.where(flag_ref[k, x] == 0, sigma * frac_ref[k, x], 0.0)
                e[3 + k, first + x, 0:ny, :] = ks
                for f, v in ((k, e[k, first + x, 0:ny, :]), (3 + k, ks)):
                    packs[f] = pick(packs[f], slot == x, end_piece(v, x))
        for side, off in ((0, 8), (1, 4)):
            tiles = [None, None]
            for f in range(6):
                tiles[f // 4] = pick(tiles[f // 4], quad == f % 4, rot(packs[f], 4 * (f % 4) - off, 1))
            for i in range(2):
                zs[side, i] = tiles[i]
            other = rot(tiles[1], half, 1)
            ds[0, side] = jnp.where(low_half, other, tiles[0])
            ds[1, side] = jnp.where(low_half, tiles[0], other)
        starts = [start_iter(packs[k], packs[3 + k]) for k in range(3)]
        moves = (
            [(f, packs[f], 1, 2 * f, 2) for f in range(6)] + [(k, starts[k], 3, 11 + k, 1) for k in (1, 2)],
            [(f, packs[f], nx - 2, 2 * f, 2) for f in range(6)] + [(k, starts[k], nx - 3, 12 + k, 1) for k in range(3)],
        )
        for side in range(2):
            tiles = [None, None]
            for f, v, at, to, wide in moves[side]:
                t, to = divmod(to, 8)
                tiles[t] = pick(tiles[t], (slot >= to) & (slot < to + wide), rot(v, SEG * (to - at), 1))
            for i in range(2):
                ends_out[side, i] = tiles[i]

    with scope("barrierwait"):
        if alternate:
            pl.semaphore_wait(barrier, jnp.where(early, len(partners), len(partners) + len(far)))

            @pl.when(jnp.logical_not(early))
            def _():
                for i, (x, z) in enumerate(steps):
                    there = steps.index((-x, -z))
                    pl.semaphore_signal(near.at[there], inc=1, device_id=far[i], device_id_type=MESH)
        else:
            pl.semaphore_wait(barrier, len(partners) + len(far))

    own = [(e, (f, p)) for f in range(6) for p in range(first, last + 1)]
    y_own = y_start(own, ya_out, ya_in)

    up, down = device(gx=1), device(gx=-1)
    ends_copies = [copy(ends_out.at[0], ends_in.at[0], down, False), copy(ends_out.at[1], ends_in.at[1], up, False)]
    raw_copies = [
        copy(e.at[:, first, own_rows], e.at[:, last + 1, own_rows], down, False),
        copy(e.at[:, last, own_rows], e.at[:, first - 1, own_rows], up, False),
    ]
    late_copies = [
        copy(upper_out, upper_in.at[:, own_rows], down, False),
        copy(lower_out, lower_in.at[:, own_rows], up, False),
    ]
    z_copies = [copy(zs.at[0], zr.at[0], device(gz=-1), False), copy(zs.at[1], zr.at[1], device(gz=1), False)]
    corner_copies = [
        copy(ds.at[side, zside], dr.at[side, zside], device(gx=1 - 2 * side, gz=2 * zside - 1), False)
        for side in range(2) for zside in range(2)
    ]

    def start(*copies):
        for one in copies:
            one.start()

    def start_far():
        start(*corner_copies, *z_copies)

    up_first = lax.rem(pos["gx"], 4) == 3

    def in_order(begin):
        pl.when(up_first)(lambda: begin(1, 0))
        pl.when(jnp.logical_not(up_first))(lambda: begin(0, 1))

    if alternate:
        pl.when(jnp.logical_not(early))(start_far)
    else:
        start_far()
    in_order(lambda a, b: start(ends_copies[a], raw_copies[a], ends_copies[b]))

    def faces(u, p):
        v0, v1, v2 = u[0, p], u[1, p], u[2, p]
        return face_one(v0, v2, u[2, p + 1]), face_two(v0, v1, u[1, p + 1])

    def curl_sweep(u, before, lo, hi, emit, after=None):
        f1m, f2m = before
        for p in range(lo, hi):
            f1, f2 = faces(u, p) if after is None or p < hi - 1 else after
            f0 = face_zero(u[1, p], u[2, p])
            cc = edges(f0, f1, f2, f1m, f2m)
            for k in range(3):
                emit(k, p, cc[k])
            f1m, f2m = f1, f2

    def emit_second(k, p, cc):
        u2[k, p] = next_iter(e[k, p], e[3 + k, p], u1[k, p], cc)

    def emit_masked(k, p, cc):
        mm[k, p] = masked_residual(e[k, p], e[3 + k, p], u2[k, p], cc)

    def emit_rest(k, p, cc):
        if k > 0 or p != first + 1:
            emit_masked(k, p, cc)

    def node_range(lo, hi):
        for p in range(lo, hi):
            r = nodal_rhs(mm[0, p], mm[0, p - 1], mm[1, p], mm[2, p])
            for q in range(4):
                rr[q, p] = r[q]

    def first_range(lo, hi):
        for p in range(lo, hi):
            for k in range(3):
                u1[k, p] = start_iter(e[k, p], e[3 + k, p])

    def below(v, p):
        up0 = v[0, p]
        return (z_up(up0) - up0) + v[2, p], v[1, p] + (y_up(up0) - up0)

    with scope("y1"):
        y_finish(y_own, own, ya_in)
    with scope("inner"):
        first_range(first, last + 1)
        curl_sweep(u1, faces(u1, first), first + 1, last, emit_second)
        p = last - 1
        sent = (*below(u1, p), e[3, p], *below(u2, p), e[0, p] - e[3, p] * u2[0, p])
        for i, v in enumerate(sent):
            lower_out[i] = v[0:ny]
        p = first + 1
        f1, f2 = faces(u2, p)
        cc = edges(face_zero(u2[1, p], u2[2, p]), f1, f2, -u2[2, p], u2[1, p])
        m0, m1, m2 = [masked_residual(e[k, p], e[3 + k, p], u2[k, p], cc[k]) for k in range(3)]
        mm[0, p] = m0
        sent = (u1[1, p], u1[2, p], e[4, p], e[5, p], u2[1, p], u2[2, p], m0, (y_down(m1) - m1) + (z_down(m2) - m2))
        for i, v in enumerate(sent):
            upper_out[i] = v[0:ny]
    in_order(lambda a, b: start(late_copies[a], raw_copies[b], late_copies[b]))
    with scope("inner2"):
        curl_sweep(u2, faces(u2, first + 1), first + 2, last - 1, emit_masked)
        node_range(first + 2, last - 1)

    with scope("nearwait"):
        if alternate:
            @pl.when(early)
            def _():
                for i in range(len(steps)):
                    pl.semaphore_wait(near.at[i], 1)
                start_far()

    def relay(name, copies, places, out, into):
        with scope(name):
            for one in copies:
                one.wait_recv()
            return y_start(places, out, into)

    raw_up = [(e, (f, last + 1)) for f in range(6)]
    raw_low = [(e, (f, first - 1)) for f in range(6)]
    late_up = [(upper_in, (i,)) for i in range(6)]
    late_low = [(lower_in, (i,)) for i in range(6)]
    strip_tiles = [(st, (f, t)) for f in range(6) for t in range(4)]
    y_raw_up = relay("rawup", raw_copies[:1], raw_up, yb_out, yb_in)
    y_late_up = relay("lateup", late_copies[:1], late_up, yc_out, yc_in)

    with scope("endswait"):
        for one in ends_copies + z_copies + corner_copies:
            one.wait_recv()
    with scope("strippack"):
        for f in range(6):
            t, to = divmod(2 * f, 8)
            piece = rot(ends_in[0, t], SEG * (1 - to), 1)
            piece = jnp.where(slot == 0, end_piece(e[f, last + 1, 0:ny, :], 0), piece)
            piece = jnp.where(slot >= nx - 2, rot(ends_in[1, t], SEG * (nx - 2 - to), 1), piece)
            if f < 3:
                piece = jnp.where(slot == 3, rot(ends_in[0, 1], SEG * (3 - (3 + f)), 1), piece)
                piece = jnp.where(slot == nx - 3, rot(ends_in[1, 1], SEG * (nx - 3 - (4 + f)), 1), piece)
            corner = []
            for zside, off in ((0, 8), (1, 4)):
                plus, minus = dr[1, zside], dr[0, zside]
                if f < 4:
                    corner.append(rot(jnp.where(low_half, plus, minus), off - 4 * f, 1))
                else:
                    corner.append(rot(jnp.where(low_half, minus, plus), half + off - 4 * (f - 4), 1))
            mid = packs[f]
            st[f, 0, 0:ny, :] = jnp.where(left, mid, rot(zr[0, f // 4], 8 - 4 * (f % 4), 1))
            st[f, 1, 0:ny, :] = jnp.where(left, piece, corner[0])
            st[f, 2, 0:ny, :] = jnp.where(left, rot(zr[1, f // 4], 4 - 4 * (f % 4), 1), mid)
            st[f, 3, 0:ny, :] = jnp.where(left, corner[1], piece)
        y_strip = y_start(strip_tiles, yd_out, yd_in)

    y_raw_low = relay("rawlow", raw_copies[1:], raw_low, ye_out, ye_in)

    inner = (lane >= 4) & (lane < nz - 4)

    def node_at(p, count=4):
        return [nodal_step(rr[q, p], rr[q, p - 1], rr[q, p + 1]) for q in range(count)]

    def outputs(lo, hi, kept):
        s_next = node_at(lo)
        for p in range(lo, hi):
            s = s_next
            s_next = node_at(p + 1, 4 if p + 1 < hi else 2)
            corr = (
                (s_next[0] - s[0]) + (s[1] + s_next[1]) * 0.5,
                (y_up(s[0]) - s[0]) + (s[2] + y_up(s[2])) * 0.5,
                (z_up(s[0]) - s[0]) + (s[3] + z_up(s[3])) * 0.5,
            )
            for k in range(3):
                body = finish(e[k, p, 0:ny], e[3 + k, p, 0:ny], u2[k, p, 0:ny], corr[k][0:ny])
                ends = rot(sw[k], nz - 8 - SEG * (p - first), 1)
                out_ref[k, p - first] = jnp.where(inner, body, ends)

    lane24 = lax.broadcasted_iota(jnp.int32, (ny + 8, nz), 1)
    slot24 = lane24 // SEG
    left24 = (lane24 % SEG) < 8

    def x_up(vs):
        rs = [rot(v, -SEG, 1) for v in vs]
        return [jnp.where(lane24 < nz - SEG, rs[t], rs[(t + 1) % len(rs)]) for t in range(len(rs))]

    def x_down(vs):
        rs = [rot(v, SEG, 1) for v in vs]
        return [jnp.where(lane24 >= SEG, rs[t], rs[t - 1]) for t in range(len(rs))]

    span = range(2)

    def strip_curl(u):
        u1p, u2p = x_up(u[1]), x_up(u[2])
        f0 = [face_zero(u[1][t], u[2][t]) for t in span]
        f1 = [face_one(u[0][t], u[2][t], u2p[t]) for t in span]
        f2 = [face_two(u[0][t], u[1][t], u1p[t]) for t in span]
        f1m, f2m = x_down(f1), x_down(f2)
        out = [edges(f0[t], f1[t], f2[t], f1m[t], f2m[t]) for t in span]
        return [[out[t][k] for t in span] for k in range(3)]

    def strips():
        results = []
        for base in (0, 2):
            def sr(k, t):
                return st[k, base + t]

            def sk(k, t):
                return st[3 + k, base + t]

            sent = ((slot24 == 3) | (slot24 == nx - 3)) & (left24 if base == 0 else ~left24)
            u = [[start_iter(sr(k, t), sk(k, t)) for t in span] for k in range(3)]
            for k in range(3):
                u[k][1] = jnp.where(sent, sr(k, 1), u[k][1])
            cc = strip_curl(u)
            u = [[next_iter(sr(k, t), sk(k, t), u[k][t], cc[k][t]) for t in span] for k in range(3)]
            cc = strip_curl(u)
            m = [[masked_residual(sr(k, t), sk(k, t), u[k][t], cc[k][t]) for t in span] for k in range(3)]
            m0m = x_down(m[0])
            r = [nodal_rhs(m[0][t], m0m[t], m[1][t], m[2][t]) for t in span]
            s = []
            for q in range(4):
                rq = [r[t][q] for t in span]
                rm, rp = x_down(rq), x_up(rq)
                s.append([nodal_step(rq[t], rm[t], rp[t]) for t in span])
            s0p, s1p = x_up(s[0])[0], x_up(s[1])[0]
            s0, s1, s2, s3 = [s[q][0] for q in range(4)]
            corr = (
                (s0p - s0) + (s1 + s1p) * 0.5,
                (y_up(s0) - s0) + (s2 + y_up(s2)) * 0.5,
                (z_up(s0) - s0) + (s3 + z_up(s3)) * 0.5,
            )
            results.append([finish(sr(k, 0), sk(k, 0), u[k][0], corr[k])[0:ny] for k in range(3)])
        for k in range(3):
            sw[k] = jnp.where(left, results[0][k], results[1][k])

    with scope("yup"):
        y_finish(y_raw_up, raw_up, yb_in)
        y_finish(y_late_up, late_up, yc_in)
    with scope("upper"):
        p = last + 1
        first_range(p, p + 1)
        f1 = face_one(u1[0, p], u1[2, p], upper_in[1])
        f2 = face_two(u1[0, p], u1[1, p], upper_in[0])
        curl_sweep(u1, faces(u1, last - 1), last, p + 1, emit_second, (f1, f2))
        f1 = face_one(u2[0, p], u2[2, p], upper_in[5])
        f2 = face_two(u2[0, p], u2[1, p], upper_in[4])
        curl_sweep(u2, faces(u2, last - 2), last - 1, p + 1, emit_masked, (f1, f2))
        node_range(last - 1, p + 1)
        v0 = u2[0, p]
        q2 = jnp.where(upper_in[2] > 0.0, u2[1, p] + (y_up(v0) - v0), 0.0)
        q1 = jnp.where(upper_in[3] > 0.0, (z_up(v0) - v0) + u2[2, p], 0.0)
        m0, m0p = mm[0, p], upper_in[6]
        rr[0, p + 1] = (m0 - m0p) + (upper_in[7] + (y_down(q2) - q2) + (z_down(q1) - q1))
        rr[1, p + 1] = (m0p + m0) * 0.5

    with scope("ystrip"):
        y_finish(y_strip, strip_tiles, yd_in)
    with scope("strips"):
        strips()
    with scope("outup"):
        outputs(first + 3, last + 1, None)
    y_late_low = relay("latelow", late_copies[1:], late_low, yf_out, yf_in)
    with scope("ylow"):
        y_finish(y_raw_low, raw_low, ye_in)
        y_finish(y_late_low, late_low, yf_in)
    with scope("lower"):
        p = first - 1
        first_range(p, p + 1)
        curl_sweep(u1, (lower_in[0] - u1[2, p], u1[1, p] - lower_in[1]), p, first + 1, emit_second)
        f1, f2 = lower_in[3] - u2[2, p], u2[1, p] - lower_in[4]
        cc = (z_down(f1) - f1) - (y_down(f2) - f2)
        mm[0, p - 1] = jnp.where(lower_in[2] > 0.0, lower_in[5] - cc, 0.0)
        curl_sweep(u2, (f1, f2), p, first + 2, emit_rest)
        node_range(p, first + 2)
    with scope("outlow"):
        outputs(first, first + 3, None)
    with scope("sendwait"):
        for one in started:
            one.wait_send()


def on_device(sizes, rhs, conductivity, fraction, region, flags):
    _, nx, ny, nz = rhs.shape
    planes = nx + 2 * PAD
    rows = ny + 8
    f32 = jnp.float32
    hbm = pl.BlockSpec(memory_space=pl.ANY)
    sides = 1 if sizes[1] == 2 else 2
    relays = []
    for count in (6 * nx, 6, 6, 24, 6, 6):
        relays += [pltpu.VMEM((count, 8, nz), f32), pltpu.VMEM((sides, count, 8, nz), f32)]
    return pl.pallas_call(
        functools.partial(kernel, sizes, nx, ny, nz),
        out_shape=pltpu.VMEM(rhs.shape, rhs.dtype),
        in_specs=[hbm] * 5,
        out_specs=pl.BlockSpec(memory_space=pltpu.VMEM),
        scratch_shapes=[
            pltpu.SMEM(conductivity.shape, f32),
            pltpu.VMEM(rhs.shape, f32),
            pltpu.VMEM(region.shape, jnp.int32),
            pltpu.VMEM(flags.shape, jnp.int32),
            pltpu.VMEM((6, planes, rows, nz), f32),
            pltpu.VMEM((6, 4, rows, nz), f32),
            pltpu.VMEM((3, ny, nz), f32),
            pltpu.VMEM((3, planes, rows, nz), f32),
            pltpu.VMEM((3, planes, rows, nz), f32),
            pltpu.VMEM((3, planes, rows, nz), f32),
            pltpu.VMEM((4, planes, rows, nz), f32),
            pltpu.VMEM((2, 2, ny, nz), f32),
            pltpu.VMEM((2, 2, ny, nz), f32),
            pltpu.VMEM((2, 2, ny, nz), f32),
            pltpu.VMEM((2, 2, ny, nz), f32),
            pltpu.VMEM((2, 2, ny, nz), f32),
            pltpu.VMEM((2, 2, ny, nz), f32),
            pltpu.VMEM((6, ny, nz), f32),
            pltpu.VMEM((6, rows, nz), f32),
            pltpu.VMEM((8, ny, nz), f32),
            pltpu.VMEM((8, rows, nz), f32),
            *relays,
            pltpu.SemaphoreType.DMA((5,)),
            pltpu.SemaphoreType.DMA((26,)),
            pltpu.SemaphoreType.DMA((26,)),
            pltpu.SemaphoreType.REGULAR((6,)),
        ],
        compiler_params=pltpu.CompilerParams(
            collective_id=0, has_side_effects=True, vmem_limit_bytes=60 * 1024 * 1024
        ),
    )(conductivity, rhs, fraction, region, flags)


def solution(mesh):
    sizes = tuple(mesh.shape[name] for name in ("gx", "gy", "gz"))
    return jax.shard_map(
        functools.partial(on_device, sizes),
        mesh=mesh,
        in_specs=(
            P(None, "gx", "gy", "gz"),
            P(),
            P(None, "gx", "gy", "gz"),
            P("gx", "gy", "gz"),
            P(None, "gx", "gy", "gz"),
        ),
        out_specs=P(None, "gx", "gy", "gz"),
        check_vma=False,
    )
```

```python
import functools
import math

import jax
import jax.numpy as jnp
from jax import lax
from jax.experimental import pallas as pl
from jax.experimental.pallas import tpu as pltpu
from jax.sharding import PartitionSpec as P

damping = 0.8
c_node = 0.8 / 7.0
MESH = pl.DeviceIdType.MESH
PAD = 2
SEG = 16


def rot(v, shift, axis):
    return pltpu.roll(v, shift % v.shape[axis], axis)


def y_up(v):
    return rot(v, -1, 0)


def y_down(v):
    return rot(v, 1, 0)


def z_up(v):
    return rot(v, -1, 1)


def z_down(v):
    return rot(v, 1, 1)


def face_zero(u1, u2):
    return (y_up(u2) - u2) - (z_up(u1) - u1)


def face_one(u0, u2, u2p):
    return (z_up(u0) - u0) - (u2p - u2)


def face_two(u0, u1, u1p):
    return (u1p - u1) - (y_up(u0) - u0)


def edges(f0, f1, f2, f1m, f2m):
    return (
        (z_down(f1) - f1) - (y_down(f2) - f2),
        (f2m - f2) - (z_down(f0) - f0),
        (y_down(f0) - f0) - (f1m - f1),
    )


def jacobi_scale(ks):
    return damping / jnp.where(ks > 0.0, 4.0 + ks, 1.0)


def start_iter(rhs, ks):
    return jnp.where(ks > 0.0, jacobi_scale(ks) * rhs, 0.0)


def next_iter(rhs, ks, u, cc):
    new = u + jacobi_scale(ks) * (rhs - (cc + ks * u))
    return jnp.where(ks > 0.0, new, 0.0)


def masked_residual(rhs, ks, u, cc):
    return jnp.where(ks > 0.0, rhs - (cc + ks * u), 0.0)


def nodal_rhs(m0, m0m, m1, m2):
    m1m, m2m = y_down(m1), z_down(m2)
    return (
        (m0m - m0) + (m1m - m1) + (m2m - m2),
        (m0 + m0m) * 0.5,
        (m1 + m1m) * 0.5,
        (m2 + m2m) * 0.5,
    )


def nodal_step(r, rm, rp):
    around = (rm + rp) + (y_up(r) + y_down(r)) + (z_up(r) + z_down(r))
    return (1.2 * c_node) * r + (c_node * c_node) * around


def finish(rhs, ks, u, corr):
    fixed = damping * rhs
    fixed = fixed + damping * (rhs - fixed)
    return jnp.where(ks > 0.0, u + corr, fixed)


def kernel(
    sizes, nx, ny, nz, cond_hbm, rhs_hbm, frac_hbm, reg_hbm, flag_hbm, out_ref,
    cond, frac_ref, reg_ref, flag_ref,
    e, st, sw, u1, u2, mm, rr, zs, zr, ds, dr, ends_out, ends_in, lower_out, lower_in, upper_out, upper_in,
    ya_out, ya_in, yb_out, yb_in, yc_out, yc_in, yd_out, yd_in, ye_out, ye_in, yf_out, yf_in,
    blank, load, send, recv, near,
):
    gx, gy, gz = sizes
    pos = {"gx": lax.axis_index("gx"), "gy": lax.axis_index("gy"), "gz": lax.axis_index("gz")}
    size = {"gx": gx, "gy": gy, "gz": gz}
    first, last = PAD, PAD + nx - 1
    scope = jax.named_scope

    def device(**steps):
        return {axis: lax.rem(pos[axis] + (step + size[axis]), size[axis]) for axis, step in steps.items()}

    partners = [device(gx=1), device(gx=-1), device(gy=1)]
    if gy > 2:
        partners.append(device(gy=-1))
    steps = [(x, z) for z in (1, -1) for x in (0, 1, -1)]
    far = [device(gx=x, gz=z) for x, z in steps]
    alternate = gz % 2 == 0
    early = lax.rem(pos["gz"], 2) == 0
    barrier = pltpu.get_barrier_semaphore()

    def greet(devices):
        for one in devices:
            pl.semaphore_signal(barrier, inc=1, device_id=one, device_id_type=MESH)

    greet(partners)
    if alternate:
        pl.when(early)(lambda: greet(far))
    else:
        greet(far)
    own_rows = pl.ds(0, ny)
    loads = [
        pltpu.make_async_copy(src, dst, load.at[i])
        for src, dst, i in (
            (rhs_hbm, e.at[pl.ds(0, 3), pl.ds(first, nx), own_rows], 0), (reg_hbm, reg_ref, 0),
            (frac_hbm, frac_ref, 0), (flag_hbm, flag_ref, 0), (cond_hbm, cond, 1),
        )
    ]

    def tiles_of(count):
        return blank.at[pl.ds(0, count)]

    def wait_tiles(semaphore, count):
        pltpu.make_async_copy(tiles_of(count), tiles_of(count), semaphore).wait()

    with scope("load"):
        for one in loads:
            one.start()
        loads[4].wait()
        wait_tiles(load.at[0], 10 * nx * ny // 8)

    sent_tiles = []

    def copy(group, src, dst, where, start=True):
        made = pltpu.make_async_remote_copy(
            src_ref=src, dst_ref=dst, send_sem=send.at[0], recv_sem=recv.at[group],
            device_id=where, device_id_type=MESH,
        )
        sent_tiles.append(math.prod(src.shape) // (8 * nz))
        if start:
            made.start()
        return made

    def arrived(group, count):
        wait_tiles(recv.at[group], count)

    row = lax.broadcasted_iota(jnp.int32, (8, nz), 0)
    top, bottom, halo = slice(0, 8), slice(ny - 8, ny), slice(ny, ny + 8)

    def y_start(group, places, out, into):
        for i, (ref, where) in enumerate(places):
            out[i] = jnp.where(row < 4, ref[(*where, top, slice(None))], ref[(*where, bottom, slice(None))])
        if gy == 2:
            copy(group, out, into.at[0], device(gy=1))
        else:
            copy(group, out, into.at[0], device(gy=-1))
            copy(group, out, into.at[1], device(gy=1))

    def y_finish(group, places, into):
        arrived(group, into.shape[0] * len(places))
        for i, (ref, where) in enumerate(places):
            tile = into[0, i] if gy == 2 else jnp.where(row < 4, into[0, i], into[1, i])
            ref[(*where, halo, slice(None))] = tile

    lane = lax.broadcasted_iota(jnp.int32, (ny, nz), 1)
    slot = lane // SEG
    half = nz // 2
    low_half = lane < half
    quad = (lane % SEG) // 4
    left = (lane % SEG) < 8

    def end_piece(v, j):
        return rot(v, 8 + SEG * j, 1)

    def pick(base, where, other):
        return other if base is None else jnp.where(where, other, base)

    packs = [None] * 6
    with scope("pack"):
        for x in range(nx):
            region = reg_ref[x]
            sigma = jnp.zeros((ny, nz), jnp.float32)
            for number in range(cond.shape[0]):
                sigma = jnp.where(region == number, cond[number], sigma)
            for k in range(3):
                ks = jnp.where(flag_ref[k, x] == 0, sigma * frac_ref[k, x], 0.0)
                e[3 + k, first + x, 0:ny, :] = ks
                for f, v in ((k, e[k, first + x, 0:ny, :]), (3 + k, ks)):
                    packs[f] = pick(packs[f], slot == x, end_piece(v, x))
        for side, off in ((0, 8), (1, 4)):
            tiles = [None, None]
            for f in range(6):
                tiles[f // 4] = pick(tiles[f // 4], quad == f % 4, rot(packs[f], 4 * (f % 4) - off, 1))
            for i in range(2):
                zs[side, i] = tiles[i]
            other = rot(tiles[1], half, 1)
            ds[0, side] = jnp.where(low_half, other, tiles[0])
            ds[1, side] = jnp.where(low_half, tiles[0], other)
        starts = [start_iter(packs[k], packs[3 + k]) for k in range(3)]
        moves = (
            [(f, packs[f], 1, 2 * f, 2) for f in range(6)] + [(k, starts[k], 3, 11 + k, 1) for k in (1, 2)],
            [(f, packs[f], nx - 2, 2 * f, 2) for f in range(6)] + [(k, starts[k], nx - 3, 12 + k, 1) for k in range(3)],
        )
        for side in range(2):
            tiles = [None, None]
            for f, v, at, to, wide in moves[side]:
                t, to = divmod(to, 8)
                tiles[t] = pick(tiles[t], (slot >= to) & (slot < to + wide), rot(v, SEG * (to - at), 1))
            for i in range(2):
                ends_out[side, i] = tiles[i]

    with scope("barrierwait"):
        if alternate:
            pl.semaphore_wait(barrier, jnp.where(early, len(partners), len(partners) + len(far)))

            @pl.when(jnp.logical_not(early))
            def _():
                for one, (_, z) in zip(far, steps):
                    pl.semaphore_signal(near.at[int(z < 0)], inc=1, device_id=one, device_id_type=MESH)
        else:
            pl.semaphore_wait(barrier, len(partners) + len(far))

    own = [(e, (f, p)) for f in range(6) for p in range(first, last + 1)]
    y_start(0, own, ya_out, ya_in)

    up, down = device(gx=1), device(gx=-1)
    ends_copies = [copy(1, ends_out.at[0], ends_in.at[0], down, False), copy(1, ends_out.at[1], ends_in.at[1], up, False)]
    raw_copies = [
        copy(2, e.at[:, first, own_rows], e.at[:, last + 1, own_rows], down, False),
        copy(3, e.at[:, last, own_rows], e.at[:, first - 1, own_rows], up, False),
    ]
    late_copies = [
        copy(4, upper_out, upper_in.at[:, own_rows], down, False),
        copy(5, lower_out, lower_in.at[:, own_rows], up, False),
    ]
    z_copies = [copy(1, zs.at[0], zr.at[0], device(gz=-1), False), copy(1, zs.at[1], zr.at[1], device(gz=1), False)]
    corner_copies = [
        copy(1, ds.at[side, zside], dr.at[side, zside], device(gx=1 - 2 * side, gz=2 * zside - 1), False)
        for side in range(2) for zside in range(2)
    ]

    def start(*copies):
        for one in copies:
            one.start()

    def start_far(zside):
        start(corner_copies[zside], corner_copies[2 + zside], z_copies[zside])

    def start_both():
        start_far(1)
        start_far(0)

    up_first = (lax.rem(pos["gx"], 4) == 3) & (pos["gz"] == 0)

    def in_order(begin):
        pl.when(up_first)(lambda: begin(1, 0))
        pl.when(jnp.logical_not(up_first))(lambda: begin(0, 1))

    if alternate:
        pl.when(jnp.logical_not(early))(start_both)
    else:
        start_both()
    in_order(lambda a, b: start(ends_copies[a], raw_copies[a], ends_copies[b]))

    def faces(u, p):
        v0, v1, v2 = u[0, p], u[1, p], u[2, p]
        return face_one(v0, v2, u[2, p + 1]), face_two(v0, v1, u[1, p + 1])

    def curl_sweep(u, before, lo, hi, emit, after=None):
        f1m, f2m = before
        for p in range(lo, hi):
            f1, f2 = faces(u, p) if after is None or p < hi - 1 else after
            f0 = face_zero(u[1, p], u[2, p])
            cc = edges(f0, f1, f2, f1m, f2m)
            for k in range(3):
                emit(k, p, cc[k])
            f1m, f2m = f1, f2

    def emit_second(k, p, cc):
        u2[k, p] = next_iter(e[k, p], e[3 + k, p], u1[k, p], cc)

    def emit_masked(k, p, cc):
        mm[k, p] = masked_residual(e[k, p], e[3 + k, p], u2[k, p], cc)

    def emit_rest(k, p, cc):
        if k > 0 or p != first + 1:
            emit_masked(k, p, cc)

    def node_range(lo, hi):
        for p in range(lo, hi):
            r = nodal_rhs(mm[0, p], mm[0, p - 1], mm[1, p], mm[2, p])
            for q in range(4):
                rr[q, p] = r[q]

    def first_range(lo, hi):
        for p in range(lo, hi):
            for k in range(3):
                u1[k, p] = start_iter(e[k, p], e[3 + k, p])

    def below(v, p):
        up0 = v[0, p]
        return (z_up(up0) - up0) + v[2, p], v[1, p] + (y_up(up0) - up0)

    with scope("y1"):
        y_finish(0, own, ya_in)
    with scope("inner"):
        first_range(first, last + 1)
        curl_sweep(u1, faces(u1, first), first + 1, last, emit_second)
        p = last - 1
        sent = (*below(u1, p), e[3, p], *below(u2, p), e[0, p] - e[3, p] * u2[0, p])
        for i, v in enumerate(sent):
            lower_out[i] = v[0:ny]
        p = first + 1
        f1, f2 = faces(u2, p)
        cc = edges(face_zero(u2[1, p], u2[2, p]), f1, f2, -u2[2, p], u2[1, p])
        m0, m1, m2 = [masked_residual(e[k, p], e[3 + k, p], u2[k, p], cc[k]) for k in range(3)]
        mm[0, p] = m0
        sent = (u1[1, p], u1[2, p], e[4, p], e[5, p], u2[1, p], u2[2, p], m0, (y_down(m1) - m1) + (z_down(m2) - m2))
        for i, v in enumerate(sent):
            upper_out[i] = v[0:ny]
    @pl.when(up_first)
    def _():
        start(raw_copies[0], late_copies[1], late_copies[0])

    @pl.when(jnp.logical_not(up_first))
    def _():
        start(late_copies[0], raw_copies[1], late_copies[1])

    with scope("inner2"):
        curl_sweep(u2, faces(u2, first + 1), first + 2, last - 1, emit_masked)
        node_range(first + 2, last - 1)

    with scope("nearwait"):
        if alternate:
            @pl.when(early)
            def _():
                for zside in (1, 0):
                    pl.semaphore_wait(near.at[zside], len(far) // 2)
                    start_far(zside)

    def relay(name, group, count, places, out, into):
        with scope(name):
            arrived(group, count * ny // 8)
            y_start(4 + group, places, out, into)

    raw_up = [(e, (f, last + 1)) for f in range(6)]
    raw_low = [(e, (f, first - 1)) for f in range(6)]
    late_up = [(upper_in, (i,)) for i in range(6)]
    late_low = [(lower_in, (i,)) for i in range(6)]
    strip_tiles = [(st, (f, t)) for f in range(6) for t in range(4)]
    relay("rawup", 2, 6, raw_up, yb_out, yb_in)
    relay("lateup", 4, 8, late_up, yc_out, yc_in)

    inner = (lane >= 4) & (lane < nz - 4)

    def node_at(p, count=4):
        return [nodal_step(rr[q, p], rr[q, p - 1], rr[q, p + 1]) for q in range(count)]

    def outputs(lo, hi, kept):
        s_next = node_at(lo)
        for p in range(lo, hi):
            s = s_next
            s_next = node_at(p + 1, 4 if p + 1 < hi else 2)
            corr = (
                (s_next[0] - s[0]) + (s[1] + s_next[1]) * 0.5,
                (y_up(s[0]) - s[0]) + (s[2] + y_up(s[2])) * 0.5,
                (z_up(s[0]) - s[0]) + (s[3] + z_up(s[3])) * 0.5,
            )
            for k in range(3):
                body = finish(e[k, p, 0:ny], e[3 + k, p, 0:ny], u2[k, p, 0:ny], corr[k][0:ny])
                ends = rot(sw[k], nz - 8 - SEG * (p - first), 1)
                out_ref[k, p - first] = jnp.where(inner, body, ends)

    lane24 = lax.broadcasted_iota(jnp.int32, (ny + 8, nz), 1)
    slot24 = lane24 // SEG
    left24 = (lane24 % SEG) < 8

    def x_up(vs):
        rs = [rot(v, -SEG, 1) for v in vs]
        return [jnp.where(lane24 < nz - SEG, rs[t], rs[(t + 1) % len(rs)]) for t in range(len(rs))]

    def x_down(vs):
        rs = [rot(v, SEG, 1) for v in vs]
        return [jnp.where(lane24 >= SEG, rs[t], rs[t - 1]) for t in range(len(rs))]

    span = range(2)

    def strip_curl(u):
        u1p, u2p = x_up(u[1]), x_up(u[2])
        f0 = [face_zero(u[1][t], u[2][t]) for t in span]
        f1 = [face_one(u[0][t], u[2][t], u2p[t]) for t in span]
        f2 = [face_two(u[0][t], u[1][t], u1p[t]) for t in span]
        f1m, f2m = x_down(f1), x_down(f2)
        out = [edges(f0[t], f1[t], f2[t], f1m[t], f2m[t]) for t in span]
        return [[out[t][k] for t in span] for k in range(3)]

    def strips():
        results = []
        for base in (0, 2):
            def sr(k, t):
                return st[k, base + t]

            def sk(k, t):
                return st[3 + k, base + t]

            sent = ((slot24 == 3) | (slot24 == nx - 3)) & (left24 if base == 0 else ~left24)
            u = [[start_iter(sr(k, t), sk(k, t)) for t in span] for k in range(3)]
            for k in range(3):
                u[k][1] = jnp.where(sent, sr(k, 1), u[k][1])
            cc = strip_curl(u)
            u = [[next_iter(sr(k, t), sk(k, t), u[k][t], cc[k][t]) for t in span] for k in range(3)]
            cc = strip_curl(u)
            m = [[masked_residual(sr(k, t), sk(k, t), u[k][t], cc[k][t]) for t in span] for k in range(3)]
            m0m = x_down(m[0])
            r = [nodal_rhs(m[0][t], m0m[t], m[1][t], m[2][t]) for t in span]
            s = []
            for q in range(4):
                rq = [r[t][q] for t in span]
                rm, rp = x_down(rq), x_up(rq)
                s.append([nodal_step(rq[t], rm[t], rp[t]) for t in span])
            s0p, s1p = x_up(s[0])[0], x_up(s[1])[0]
            s0, s1, s2, s3 = [s[q][0] for q in range(4)]
            corr = (
                (s0p - s0) + (s1 + s1p) * 0.5,
                (y_up(s0) - s0) + (s2 + y_up(s2)) * 0.5,
                (z_up(s0) - s0) + (s3 + z_up(s3)) * 0.5,
            )
            results.append([finish(sr(k, 0), sk(k, 0), u[k][0], corr[k])[0:ny] for k in range(3)])
        for k in range(3):
            sw[k] = jnp.where(left, results[0][k], results[1][k])

    relay("rawlow", 3, 6, raw_low, ye_out, ye_in)
    with scope("endswait"):
        arrived(1, 12 * ny // 8)
    with scope("strippack"):
        for f in range(6):
            t, to = divmod(2 * f, 8)
            piece = rot(ends_in[0, t], SEG * (1 - to), 1)
            piece = jnp.where(slot == 0, end_piece(e[f, last + 1, 0:ny, :], 0), piece)
            piece = jnp.where(slot >= nx - 2, rot(ends_in[1, t], SEG * (nx - 2 - to), 1), piece)
            if f < 3:
                piece = jnp.where(slot == 3, rot(ends_in[0, 1], SEG * (3 - (3 + f)), 1), piece)
                piece = jnp.where(slot == nx - 3, rot(ends_in[1, 1], SEG * (nx - 3 - (4 + f)), 1), piece)
            corner = []
            for zside, off in ((0, 8), (1, 4)):
                plus, minus = dr[1, zside], dr[0, zside]
                if f < 4:
                    corner.append(rot(jnp.where(low_half, plus, minus), off - 4 * f, 1))
                else:
                    corner.append(rot(jnp.where(low_half, minus, plus), half + off - 4 * (f - 4), 1))
            mid = packs[f]
            st[f, 0, 0:ny, :] = jnp.where(left, mid, rot(zr[0, f // 4], 8 - 4 * (f % 4), 1))
            st[f, 1, 0:ny, :] = jnp.where(left, piece, corner[0])
            st[f, 2, 0:ny, :] = jnp.where(left, rot(zr[1, f // 4], 4 - 4 * (f % 4), 1), mid)
            st[f, 3, 0:ny, :] = jnp.where(left, corner[1], piece)
        y_start(10, strip_tiles, yd_out, yd_in)

    with scope("yup"):
        y_finish(6, raw_up, yb_in)
        y_finish(8, late_up, yc_in)
    with scope("upper"):
        p = last + 1
        first_range(p, p + 1)
        f1 = face_one(u1[0, p], u1[2, p], upper_in[1])
        f2 = face_two(u1[0, p], u1[1, p], upper_in[0])
        curl_sweep(u1, faces(u1, last - 1), last, p + 1, emit_second, (f1, f2))
        f1 = face_one(u2[0, p], u2[2, p], upper_in[5])
        f2 = face_two(u2[0, p], u2[1, p], upper_in[4])
        curl_sweep(u2, faces(u2, last - 2), last - 1, p + 1, emit_masked, (f1, f2))
        node_range(last - 1, p + 1)
        v0 = u2[0, p]
        q2 = jnp.where(upper_in[2] > 0.0, u2[1, p] + (y_up(v0) - v0), 0.0)
        q1 = jnp.where(upper_in[3] > 0.0, (z_up(v0) - v0) + u2[2, p], 0.0)
        m0, m0p = mm[0, p], upper_in[6]
        rr[0, p + 1] = (m0 - m0p) + (upper_in[7] + (y_down(q2) - q2) + (z_down(q1) - q1))
        rr[1, p + 1] = (m0p + m0) * 0.5

    relay("latelow", 5, 6, late_low, yf_out, yf_in)
    with scope("ystrip"):
        y_finish(10, strip_tiles, yd_in)
    with scope("strips"):
        strips()
    with scope("outup"):
        outputs(first + 3, last + 1, None)
    with scope("ylow"):
        y_finish(7, raw_low, ye_in)
        y_finish(9, late_low, yf_in)
    with scope("lower"):
        p = first - 1
        first_range(p, p + 1)
        curl_sweep(u1, (lower_in[0] - u1[2, p], u1[1, p] - lower_in[1]), p, first + 1, emit_second)
        f1, f2 = lower_in[3] - u2[2, p], u2[1, p] - lower_in[4]
        cc = (z_down(f1) - f1) - (y_down(f2) - f2)
        mm[0, p - 1] = jnp.where(lower_in[2] > 0.0, lower_in[5] - cc, 0.0)
        curl_sweep(u2, (f1, f2), p, first + 2, emit_rest)
        node_range(p, first + 2)
    with scope("outlow"):
        outputs(first, first + 3, None)
    with scope("sendwait"):
        wait_tiles(send.at[0], sum(sent_tiles))


def on_device(sizes, rhs, conductivity, fraction, region, flags):
    _, nx, ny, nz = rhs.shape
    planes = nx + 2 * PAD
    rows = ny + 8
    f32 = jnp.float32
    hbm = pl.BlockSpec(memory_space=pl.ANY)
    sides = 1 if sizes[1] == 2 else 2
    relays = []
    for count in (6 * nx, 6, 6, 24, 6, 6):
        relays += [pltpu.VMEM((count, 8, nz), f32), pltpu.VMEM((sides, count, 8, nz), f32)]
    return pl.pallas_call(
        functools.partial(kernel, sizes, nx, ny, nz),
        out_shape=pltpu.VMEM(rhs.shape, rhs.dtype),
        in_specs=[hbm] * 5,
        out_specs=pl.BlockSpec(memory_space=pltpu.VMEM),
        scratch_shapes=[
            pltpu.SMEM(conductivity.shape, f32),
            pltpu.VMEM(rhs.shape, f32),
            pltpu.VMEM(region.shape, jnp.int32),
            pltpu.VMEM(flags.shape, jnp.int32),
            pltpu.VMEM((6, planes, rows, nz), f32),
            pltpu.VMEM((6, 4, rows, nz), f32),
            pltpu.VMEM((3, ny, nz), f32),
            pltpu.VMEM((3, planes, rows, nz), f32),
            pltpu.VMEM((3, planes, rows, nz), f32),
            pltpu.VMEM((3, planes, rows, nz), f32),
            pltpu.VMEM((4, planes, rows, nz), f32),
            pltpu.VMEM((2, 2, ny, nz), f32),
            pltpu.VMEM((2, 2, ny, nz), f32),
            pltpu.VMEM((2, 2, ny, nz), f32),
            pltpu.VMEM((2, 2, ny, nz), f32),
            pltpu.VMEM((2, 2, ny, nz), f32),
            pltpu.VMEM((2, 2, ny, nz), f32),
            pltpu.VMEM((6, ny, nz), f32),
            pltpu.VMEM((6, rows, nz), f32),
            pltpu.VMEM((8, ny, nz), f32),
            pltpu.VMEM((8, rows, nz), f32),
            *relays,
            pltpu.VMEM((320, 8, nz), f32),
            pltpu.SemaphoreType.DMA((2,)),
            pltpu.SemaphoreType.DMA((1,)),
            pltpu.SemaphoreType.DMA((11,)),
            pltpu.SemaphoreType.REGULAR((2,)),
        ],
        compiler_params=pltpu.CompilerParams(
            collective_id=0, has_side_effects=True, vmem_limit_bytes=60 * 1024 * 1024
        ),
    )(conductivity, rhs, fraction, region, flags)


def solution(mesh):
    sizes = tuple(mesh.shape[name] for name in ("gx", "gy", "gz"))
    return jax.shard_map(
        functools.partial(on_device, sizes),
        mesh=mesh,
        in_specs=(
            P(None, "gx", "gy", "gz"),
            P(),
            P(None, "gx", "gy", "gz"),
            P("gx", "gy", "gz"),
            P(None, "gx", "gy", "gz"),
        ),
        out_specs=P(None, "gx", "gy", "gz"),
        check_vma=False,
    )
```

```python
import functools
import math

import jax
import jax.numpy as jnp
from jax import lax
from jax.experimental import pallas as pl
from jax.experimental.pallas import tpu as pltpu
from jax.sharding import PartitionSpec as P

damping = 0.8
c_node = 0.8 / 7.0
MESH = pl.DeviceIdType.MESH
PAD = 2
SEG = 16


def rot(v, shift, axis):
    return pltpu.roll(v, shift % v.shape[axis], axis)


def y_up(v):
    return rot(v, -1, 0)


def y_down(v):
    return rot(v, 1, 0)


def z_up(v):
    return rot(v, -1, 1)


def z_down(v):
    return rot(v, 1, 1)


def face_zero(u1, u2):
    return (y_up(u2) - u2) - (z_up(u1) - u1)


def face_one(u0, u2, u2p):
    return (z_up(u0) - u0) - (u2p - u2)


def face_two(u0, u1, u1p):
    return (u1p - u1) - (y_up(u0) - u0)


def edges(f0, f1, f2, f1m, f2m):
    return (
        (z_down(f1) - f1) - (y_down(f2) - f2),
        (f2m - f2) - (z_down(f0) - f0),
        (y_down(f0) - f0) - (f1m - f1),
    )


def jacobi_scale(ks):
    return damping / jnp.where(ks > 0.0, 4.0 + ks, 1.0)


def start_iter(rhs, ks):
    return jnp.where(ks > 0.0, jacobi_scale(ks) * rhs, 0.0)


def next_iter(rhs, ks, u, cc):
    new = u + jacobi_scale(ks) * (rhs - (cc + ks * u))
    return jnp.where(ks > 0.0, new, 0.0)


def masked_residual(rhs, ks, u, cc):
    return jnp.where(ks > 0.0, rhs - (cc + ks * u), 0.0)


def nodal_rhs(m0, m0m, m1, m2):
    m1m, m2m = y_down(m1), z_down(m2)
    return (
        (m0m - m0) + (m1m - m1) + (m2m - m2),
        (m0 + m0m) * 0.5,
        (m1 + m1m) * 0.5,
        (m2 + m2m) * 0.5,
    )


def nodal_step(r, rm, rp):
    around = (rm + rp) + (y_up(r) + y_down(r)) + (z_up(r) + z_down(r))
    return (1.2 * c_node) * r + (c_node * c_node) * around


def finish(rhs, ks, u, corr):
    fixed = damping * rhs
    fixed = fixed + damping * (rhs - fixed)
    return jnp.where(ks > 0.0, u + corr, fixed)


def kernel(
    sizes, nx, ny, nz, cond_hbm, rhs_hbm, frac_hbm, reg_hbm, flag_hbm, out_ref,
    cond, frac_ref, reg_ref, flag_ref,
    e, st, sw, u1, u2, mm, rr, zs, zr, ds, dr, ends_out, ends_in, lower_out, lower_in, upper_out, upper_in,
    ya_out, ya_in, yb_out, yb_in, yc_out, yc_in, yd_out, yd_in,
    blank, load, send, recv, near,
):
    gx, gy, gz = sizes
    pos = {"gx": lax.axis_index("gx"), "gy": lax.axis_index("gy"), "gz": lax.axis_index("gz")}
    size = {"gx": gx, "gy": gy, "gz": gz}
    first, last = PAD, PAD + nx - 1
    scope = jax.named_scope

    def device(**steps):
        return {axis: lax.rem(pos[axis] + (step + size[axis]), size[axis]) for axis, step in steps.items()}

    steps = [(x, z) for z in (1, -1) for x in (0, 1, -1)]
    paired = gy == 2
    barrier = pltpu.get_barrier_semaphore()

    def greet(*devices):
        for one in devices:
            pl.semaphore_signal(barrier, inc=1, device_id=one, device_id_type=MESH)

    def on(core, **steps):
        return {**device(**steps), "gy": core}

    if paired:
        greet(on(1, gx=1), on(1, gx=-1))
        pl.when(pos["gy"] == 0)(lambda: greet(device(gy=1)))
        greet(*(on(0, gx=x, gz=z) for x, z in steps))
    else:
        greet(device(gx=1), device(gx=-1), device(gy=1), device(gy=-1), *(device(gx=x, gz=z) for x, z in steps))
    own_rows = pl.ds(0, ny)
    loads = [
        pltpu.make_async_copy(src, dst, load.at[i])
        for src, dst, i in (
            (rhs_hbm, e.at[pl.ds(0, 3), pl.ds(first, nx), own_rows], 0), (reg_hbm, reg_ref, 0),
            (frac_hbm, frac_ref, 0), (flag_hbm, flag_ref, 0), (cond_hbm, cond, 1),
        )
    ]

    def tiles_of(count):
        return blank.at[pl.ds(0, count)]

    def wait_tiles(semaphore, count):
        pltpu.make_async_copy(tiles_of(count), tiles_of(count), semaphore).wait()

    with scope("load"):
        for one in loads:
            one.start()
        if paired:
            @pl.when(pos["gy"] == 1)
            def _():
                pl.semaphore_wait(barrier, 5)
                pl.semaphore_signal(near.at[0], inc=1, device_id=device(gy=1), device_id_type=MESH)
        else:
            pl.semaphore_wait(barrier, 4 + len(steps))

        loads[4].wait()
        wait_tiles(load.at[0], 10 * nx * ny // 8)

    sent_tiles = []

    def copy(group, src, dst, where, start=True):
        made = pltpu.make_async_remote_copy(
            src_ref=src, dst_ref=dst, send_sem=send.at[0], recv_sem=recv.at[group],
            device_id=where, device_id_type=MESH,
        )
        sent_tiles.append(math.prod(src.shape) // (8 * nz))
        if start:
            made.start()
        return made

    def arrived(group, count):
        wait_tiles(recv.at[group], count)

    row = lax.broadcasted_iota(jnp.int32, (8, nz), 0)
    top, bottom, halo = slice(0, 8), slice(ny - 8, ny), slice(ny, ny + 8)

    def y_start(group, places, out, into):
        for i, (ref, where) in enumerate(places):
            out[i] = jnp.where(row < 4, ref[(*where, top, slice(None))], ref[(*where, bottom, slice(None))])
        if gy == 2:
            copy(group, out, into.at[0], device(gy=1))
        else:
            copy(group, out, into.at[0], device(gy=-1))
            copy(group, out, into.at[1], device(gy=1))

    def y_finish(group, places, into):
        arrived(group, into.shape[0] * len(places))
        for i, (ref, where) in enumerate(places):
            tile = into[0, i] if gy == 2 else jnp.where(row < 4, into[0, i], into[1, i])
            ref[(*where, halo, slice(None))] = tile

    lane = lax.broadcasted_iota(jnp.int32, (ny, nz), 1)
    slot = lane // SEG
    half = nz // 2
    low_half = lane < half
    quad = (lane % SEG) // 4
    left = (lane % SEG) < 8

    def end_piece(v, j):
        return rot(v, 8 + SEG * j, 1)

    def pick(base, where, other):
        return other if base is None else jnp.where(where, other, base)

    packs = [None] * 6
    with scope("pack"):
        for x in range(nx):
            region = reg_ref[x]
            sigma = jnp.zeros((ny, nz), jnp.float32)
            for number in range(cond.shape[0]):
                sigma = jnp.where(region == number, cond[number], sigma)
            for k in range(3):
                ks = jnp.where(flag_ref[k, x] == 0, sigma * frac_ref[k, x], 0.0)
                e[3 + k, first + x, 0:ny, :] = ks
                for f, v in ((k, e[k, first + x, 0:ny, :]), (3 + k, ks)):
                    packs[f] = pick(packs[f], slot == x, end_piece(v, x))
        for side, off in ((0, 8), (1, 4)):
            tiles = [None, None]
            for f in range(6):
                tiles[f // 4] = pick(tiles[f // 4], quad == f % 4, rot(packs[f], 4 * (f % 4) - off, 1))
            for i in range(2):
                zs[side, i] = tiles[i]
            other = rot(tiles[1], half, 1)
            ds[0, side] = jnp.where(low_half, other, tiles[0])
            ds[1, side] = jnp.where(low_half, tiles[0], other)
        starts = [start_iter(packs[k], packs[3 + k]) for k in range(3)]
        moves = (
            [(f, packs[f], 1, 2 * f, 2) for f in range(6)] + [(k, starts[k], 3, 11 + k, 1) for k in (1, 2)],
            [(f, packs[f], nx - 2, 2 * f, 2) for f in range(6)] + [(k, starts[k], nx - 3, 12 + k, 1) for k in range(3)],
        )
        for side in range(2):
            tiles = [None, None]
            for f, v, at, to, wide in moves[side]:
                t, to = divmod(to, 8)
                tiles[t] = pick(tiles[t], (slot >= to) & (slot < to + wide), rot(v, SEG * (to - at), 1))
            for i in range(2):
                ends_out[side, i] = tiles[i]

    with scope("barrierwait"):
        if paired:
            @pl.when(pos["gy"] == 0)
            def _():
                pl.semaphore_wait(near.at[0], 1)

    def far_wait():
        if not paired:
            return

        @pl.when(pos["gy"] == 0)
        def _():
            pl.semaphore_wait(barrier, 2 * len(steps))
            pl.semaphore_signal(near.at[1], inc=1, device_id=device(gy=1), device_id_type=MESH)

        @pl.when(pos["gy"] == 1)
        def _():
            pl.semaphore_wait(near.at[1], 1)

    own = [(e, (f, p)) for f in range(6) for p in range(first, last + 1)]
    y_start(0, own, ya_out, ya_in)

    up, down = device(gx=1), device(gx=-1)
    ends_copies = [copy(1, ends_out.at[0], ends_in.at[0], down, False), copy(1, ends_out.at[1], ends_in.at[1], up, False)]
    raw_copies = [
        copy(2, e.at[:, first, own_rows], e.at[:, last + 1, own_rows], down, False),
        copy(3, e.at[:, last, own_rows], e.at[:, first - 1, own_rows], up, False),
    ]
    late_copies = [
        copy(4, upper_out, upper_in.at[:, own_rows], down, False),
        copy(5, lower_out, lower_in.at[:, own_rows], up, False),
    ]
    z_copies = [copy(1, zs.at[0], zr.at[0], device(gz=-1), False), copy(1, zs.at[1], zr.at[1], device(gz=1), False)]
    corner_copies = [
        copy(1, ds.at[side, zside], dr.at[side, zside], device(gx=1 - 2 * side, gz=2 * zside - 1), False)
        for side in range(2) for zside in range(2)
    ]

    def start(*copies):
        for one in copies:
            one.start()

    def start_far(zside):
        start(corner_copies[zside], corner_copies[2 + zside], z_copies[zside])

    def start_both():
        start_far(1)
        start_far(0)

    up_first = (lax.rem(pos["gx"], 4) == 3) & (pos["gz"] == 0)

    def in_order(begin):
        pl.when(up_first)(lambda: begin(1, 0))
        pl.when(jnp.logical_not(up_first))(lambda: begin(0, 1))

    late_start = pos["gz"] == 0
    in_order(lambda a, b: start(ends_copies[a], ends_copies[b]))

    in_order(lambda a, b: start(raw_copies[a]))

    @pl.when(jnp.logical_not(late_start))
    def _():
        with scope("nearwait"):
            far_wait()
            start_both()


    def faces(u, p):
        v0, v1, v2 = u[0, p], u[1, p], u[2, p]
        return face_one(v0, v2, u[2, p + 1]), face_two(v0, v1, u[1, p + 1])

    def curl_sweep(u, before, lo, hi, emit, after=None):
        f1m, f2m = before
        for p in range(lo, hi):
            f1, f2 = faces(u, p) if after is None or p < hi - 1 else after
            f0 = face_zero(u[1, p], u[2, p])
            cc = edges(f0, f1, f2, f1m, f2m)
            for k in range(3):
                emit(k, p, cc[k])
            f1m, f2m = f1, f2

    def emit_second(k, p, cc):
        u2[k, p] = next_iter(e[k, p], e[3 + k, p], u1[k, p], cc)

    def emit_masked(k, p, cc):
        mm[k, p] = masked_residual(e[k, p], e[3 + k, p], u2[k, p], cc)

    def emit_rest(k, p, cc):
        if k > 0 or p != first + 1:
            emit_masked(k, p, cc)

    def node_range(lo, hi):
        for p in range(lo, hi):
            r = nodal_rhs(mm[0, p], mm[0, p - 1], mm[1, p], mm[2, p])
            for q in range(4):
                rr[q, p] = r[q]

    def first_range(lo, hi):
        for p in range(lo, hi):
            for k in range(3):
                u1[k, p] = start_iter(e[k, p], e[3 + k, p])

    def below(v, p):
        up0 = v[0, p]
        return (z_up(up0) - up0) + v[2, p], v[1, p] + (y_up(up0) - up0)

    with scope("y1"):
        y_finish(0, own, ya_in)
    with scope("inner"):
        first_range(first, last + 1)
        curl_sweep(u1, faces(u1, first), first + 1, last, emit_second)
        p = last - 1
        sent = (*below(u1, p), e[3, p], *below(u2, p), e[0, p] - e[3, p] * u2[0, p])
        for i, v in enumerate(sent):
            lower_out[i] = v[0:ny]
        p = first + 1
        f1, f2 = faces(u2, p)
        cc = edges(face_zero(u2[1, p], u2[2, p]), f1, f2, -u2[2, p], u2[1, p])
        m0, m1, m2 = [masked_residual(e[k, p], e[3 + k, p], u2[k, p], cc[k]) for k in range(3)]
        mm[0, p] = m0
        sent = (u1[1, p], u1[2, p], e[4, p], e[5, p], u2[1, p], u2[2, p], m0, (y_down(m1) - m1) + (z_down(m2) - m2))
        for i, v in enumerate(sent):
            upper_out[i] = v[0:ny]
    @pl.when(up_first)
    def _():
        start(raw_copies[0], late_copies[1], late_copies[0])

    @pl.when(jnp.logical_not(up_first))
    def _():
        start(late_copies[0], raw_copies[1], late_copies[1])

    with scope("inner2"):
        curl_sweep(u2, faces(u2, first + 1), first + 2, last - 1, emit_masked)
        node_range(first + 2, last - 1)

    @pl.when(late_start)
    def _():
        with scope("nearwait"):
            far_wait()
            start_both()

    def relay(name, groups, places, out, into):
        with scope(name):
            for group, count in groups:
                arrived(group, count * ny // 8)
            y_start(4 + groups[0][0], places, out, into)

    raw_up = [(e, (f, last + 1)) for f in range(6)]
    raw_low = [(e, (f, first - 1)) for f in range(6)]
    late_up = [(upper_in, (i,)) for i in range(6)]
    late_low = [(lower_in, (i,)) for i in range(6)]
    strip_tiles = [(st, (f, t)) for f in range(6) for t in range(4)]
    relay("lateup", ((2, 6), (4, 8)), raw_up + late_up, yb_out, yb_in)

    inner = (lane >= 4) & (lane < nz - 4)

    def node_at(p, count=4):
        return [nodal_step(rr[q, p], rr[q, p - 1], rr[q, p + 1]) for q in range(count)]

    def outputs(lo, hi, kept):
        s_next = node_at(lo)
        for p in range(lo, hi):
            s = s_next
            s_next = node_at(p + 1, 4 if p + 1 < hi else 2)
            corr = (
                (s_next[0] - s[0]) + (s[1] + s_next[1]) * 0.5,
                (y_up(s[0]) - s[0]) + (s[2] + y_up(s[2])) * 0.5,
                (z_up(s[0]) - s[0]) + (s[3] + z_up(s[3])) * 0.5,
            )
            for k in range(3):
                body = finish(e[k, p, 0:ny], e[3 + k, p, 0:ny], u2[k, p, 0:ny], corr[k][0:ny])
                ends = rot(sw[k], nz - 8 - SEG * (p - first), 1)
                out_ref[k, p - first] = jnp.where(inner, body, ends)

    lane24 = lax.broadcasted_iota(jnp.int32, (ny + 8, nz), 1)
    slot24 = lane24 // SEG
    left24 = (lane24 % SEG) < 8

    def x_up(vs):
        rs = [rot(v, -SEG, 1) for v in vs]
        return [jnp.where(lane24 < nz - SEG, rs[t], rs[(t + 1) % len(rs)]) for t in range(len(rs))]

    def x_down(vs):
        rs = [rot(v, SEG, 1) for v in vs]
        return [jnp.where(lane24 >= SEG, rs[t], rs[t - 1]) for t in range(len(rs))]

    span = range(2)

    def strip_curl(u):
        u1p, u2p = x_up(u[1]), x_up(u[2])
        f0 = [face_zero(u[1][t], u[2][t]) for t in span]
        f1 = [face_one(u[0][t], u[2][t], u2p[t]) for t in span]
        f2 = [face_two(u[0][t], u[1][t], u1p[t]) for t in span]
        f1m, f2m = x_down(f1), x_down(f2)
        out = [edges(f0[t], f1[t], f2[t], f1m[t], f2m[t]) for t in span]
        return [[out[t][k] for t in span] for k in range(3)]

    def strips():
        results = []
        for base in (0, 2):
            def sr(k, t):
                return st[k, base + t]

            def sk(k, t):
                return st[3 + k, base + t]

            sent = ((slot24 == 3) | (slot24 == nx - 3)) & (left24 if base == 0 else ~left24)
            u = [[start_iter(sr(k, t), sk(k, t)) for t in span] for k in range(3)]
            for k in range(3):
                u[k][1] = jnp.where(sent, sr(k, 1), u[k][1])
            cc = strip_curl(u)
            u = [[next_iter(sr(k, t), sk(k, t), u[k][t], cc[k][t]) for t in span] for k in range(3)]
            cc = strip_curl(u)
            m = [[masked_residual(sr(k, t), sk(k, t), u[k][t], cc[k][t]) for t in span] for k in range(3)]
            m0m = x_down(m[0])
            r = [nodal_rhs(m[0][t], m0m[t], m[1][t], m[2][t]) for t in span]
            s = []
            for q in range(4):
                rq = [r[t][q] for t in span]
                rm, rp = x_down(rq), x_up(rq)
                s.append([nodal_step(rq[t], rm[t], rp[t]) for t in span])
            s0p, s1p = x_up(s[0])[0], x_up(s[1])[0]
            s0, s1, s2, s3 = [s[q][0] for q in range(4)]
            corr = (
                (s0p - s0) + (s1 + s1p) * 0.5,
                (y_up(s0) - s0) + (s2 + y_up(s2)) * 0.5,
                (z_up(s0) - s0) + (s3 + z_up(s3)) * 0.5,
            )
            results.append([finish(sr(k, 0), sk(k, 0), u[k][0], corr[k])[0:ny] for k in range(3)])
        for k in range(3):
            sw[k] = jnp.where(left, results[0][k], results[1][k])

    with scope("endswait"):
        arrived(1, 12 * ny // 8)
    with scope("strippack"):
        for f in range(6):
            t, to = divmod(2 * f, 8)
            piece = rot(ends_in[0, t], SEG * (1 - to), 1)
            piece = jnp.where(slot == 0, end_piece(e[f, last + 1, 0:ny, :], 0), piece)
            piece = jnp.where(slot >= nx - 2, rot(ends_in[1, t], SEG * (nx - 2 - to), 1), piece)
            if f < 3:
                piece = jnp.where(slot == 3, rot(ends_in[0, 1], SEG * (3 - (3 + f)), 1), piece)
                piece = jnp.where(slot == nx - 3, rot(ends_in[1, 1], SEG * (nx - 3 - (4 + f)), 1), piece)
            corner = []
            for zside, off in ((0, 8), (1, 4)):
                plus, minus = dr[1, zside], dr[0, zside]
                if f < 4:
                    corner.append(rot(jnp.where(low_half, plus, minus), off - 4 * f, 1))
                else:
                    corner.append(rot(jnp.where(low_half, minus, plus), half + off - 4 * (f - 4), 1))
            mid = packs[f]
            st[f, 0, 0:ny, :] = jnp.where(left, mid, rot(zr[0, f // 4], 8 - 4 * (f % 4), 1))
            st[f, 1, 0:ny, :] = jnp.where(left, piece, corner[0])
            st[f, 2, 0:ny, :] = jnp.where(left, rot(zr[1, f // 4], 4 - 4 * (f % 4), 1), mid)
            st[f, 3, 0:ny, :] = jnp.where(left, corner[1], piece)
        y_start(8, strip_tiles, yd_out, yd_in)

    with scope("yup"):
        y_finish(6, raw_up + late_up, yb_in)
    with scope("upper"):
        p = last + 1
        first_range(p, p + 1)
        f1 = face_one(u1[0, p], u1[2, p], upper_in[1])
        f2 = face_two(u1[0, p], u1[1, p], upper_in[0])
        curl_sweep(u1, faces(u1, last - 1), last, p + 1, emit_second, (f1, f2))
        f1 = face_one(u2[0, p], u2[2, p], upper_in[5])
        f2 = face_two(u2[0, p], u2[1, p], upper_in[4])
        curl_sweep(u2, faces(u2, last - 2), last - 1, p + 1, emit_masked, (f1, f2))
        node_range(last - 1, p + 1)
        v0 = u2[0, p]
        q2 = jnp.where(upper_in[2] > 0.0, u2[1, p] + (y_up(v0) - v0), 0.0)
        q1 = jnp.where(upper_in[3] > 0.0, (z_up(v0) - v0) + u2[2, p], 0.0)
        m0, m0p = mm[0, p], upper_in[6]
        rr[0, p + 1] = (m0 - m0p) + (upper_in[7] + (y_down(q2) - q2) + (z_down(q1) - q1))
        rr[1, p + 1] = (m0p + m0) * 0.5

    relay("latelow", ((3, 6), (5, 6)), raw_low + late_low, yc_out, yc_in)
    with scope("ystrip"):
        y_finish(8, strip_tiles, yd_in)
    with scope("strips"):
        strips()
    with scope("outup"):
        outputs(first + 3, last + 1, None)
    with scope("ylow"):
        y_finish(7, raw_low + late_low, yc_in)
    with scope("lower"):
        p = first - 1
        first_range(p, p + 1)
        curl_sweep(u1, (lower_in[0] - u1[2, p], u1[1, p] - lower_in[1]), p, first + 1, emit_second)
        f1, f2 = lower_in[3] - u2[2, p], u2[1, p] - lower_in[4]
        cc = (z_down(f1) - f1) - (y_down(f2) - f2)
        mm[0, p - 1] = jnp.where(lower_in[2] > 0.0, lower_in[5] - cc, 0.0)
        curl_sweep(u2, (f1, f2), p, first + 2, emit_rest)
        node_range(p, first + 2)
    with scope("outlow"):
        outputs(first, first + 3, None)
    with scope("sendwait"):
        wait_tiles(send.at[0], sum(sent_tiles))


def on_device(sizes, rhs, conductivity, fraction, region, flags):
    _, nx, ny, nz = rhs.shape
    planes = nx + 2 * PAD
    rows = ny + 8
    f32 = jnp.float32
    hbm = pl.BlockSpec(memory_space=pl.ANY)
    sides = 1 if sizes[1] == 2 else 2
    relays = []
    for count in (6 * nx, 12, 12, 24):
        relays += [pltpu.VMEM((count, 8, nz), f32), pltpu.VMEM((sides, count, 8, nz), f32)]
    return pl.pallas_call(
        functools.partial(kernel, sizes, nx, ny, nz),
        out_shape=pltpu.VMEM(rhs.shape, rhs.dtype),
        in_specs=[hbm] * 5,
        out_specs=pl.BlockSpec(memory_space=pltpu.VMEM),
        scratch_shapes=[
            pltpu.SMEM(conductivity.shape, f32),
            pltpu.VMEM(rhs.shape, f32),
            pltpu.VMEM(region.shape, jnp.int32),
            pltpu.VMEM(flags.shape, jnp.int32),
            pltpu.VMEM((6, planes, rows, nz), f32),
            pltpu.VMEM((6, 4, rows, nz), f32),
            pltpu.VMEM((3, ny, nz), f32),
            pltpu.VMEM((3, planes, rows, nz), f32),
            pltpu.VMEM((3, planes, rows, nz), f32),
            pltpu.VMEM((3, planes, rows, nz), f32),
            pltpu.VMEM((4, planes, rows, nz), f32),
            pltpu.VMEM((2, 2, ny, nz), f32),
            pltpu.VMEM((2, 2, ny, nz), f32),
            pltpu.VMEM((2, 2, ny, nz), f32),
            pltpu.VMEM((2, 2, ny, nz), f32),
            pltpu.VMEM((2, 2, ny, nz), f32),
            pltpu.VMEM((2, 2, ny, nz), f32),
            pltpu.VMEM((6, ny, nz), f32),
            pltpu.VMEM((6, rows, nz), f32),
            pltpu.VMEM((8, ny, nz), f32),
            pltpu.VMEM((8, rows, nz), f32),
            *relays,
            pltpu.VMEM((320, 8, nz), f32),
            pltpu.SemaphoreType.DMA((2,)),
            pltpu.SemaphoreType.DMA((1,)),
            pltpu.SemaphoreType.DMA((9,)),
            pltpu.SemaphoreType.REGULAR((2,)),
        ],
        compiler_params=pltpu.CompilerParams(
            collective_id=0, has_side_effects=True, vmem_limit_bytes=60 * 1024 * 1024
        ),
    )(conductivity, rhs, fraction, region, flags)


def solution(mesh):
    sizes = tuple(mesh.shape[name] for name in ("gx", "gy", "gz"))
    return jax.shard_map(
        functools.partial(on_device, sizes),
        mesh=mesh,
        in_specs=(
            P(None, "gx", "gy", "gz"),
            P(),
            P(None, "gx", "gy", "gz"),
            P("gx", "gy", "gz"),
            P(None, "gx", "gy", "gz"),
        ),
        out_specs=P(None, "gx", "gy", "gz"),
        check_vma=False,
    )
```

```python
import functools
import math

import jax
import jax.numpy as jnp
from jax import lax
from jax.experimental import pallas as pl
from jax.experimental.pallas import tpu as pltpu
from jax.sharding import PartitionSpec as P

damping = 0.8
c_node = 0.8 / 7.0
MESH = pl.DeviceIdType.MESH
PAD = 2
SEG = 16


def rot(v, shift, axis):
    return pltpu.roll(v, shift % v.shape[axis], axis)


def y_up(v):
    return rot(v, -1, 0)


def y_down(v):
    return rot(v, 1, 0)


def z_up(v):
    return rot(v, -1, 1)


def z_down(v):
    return rot(v, 1, 1)


def face_zero(u1, u2):
    return (y_up(u2) - u2) - (z_up(u1) - u1)


def face_one(u0, u2, u2p):
    return (z_up(u0) - u0) - (u2p - u2)


def face_two(u0, u1, u1p):
    return (u1p - u1) - (y_up(u0) - u0)


def edges(f0, f1, f2, f1m, f2m):
    return (
        (z_down(f1) - f1) - (y_down(f2) - f2),
        (f2m - f2) - (z_down(f0) - f0),
        (y_down(f0) - f0) - (f1m - f1),
    )


def jacobi_scale(ks):
    return jnp.where(ks > 0.0, damping / (4.0 + ks), 0.0)


def next_iter(rhs, ks, scale, u, cc):
    return u + scale * (rhs - (cc + ks * u))


def masked_residual(rhs, ks, u, cc):
    return jnp.where(ks > 0.0, rhs - (cc + ks * u), 0.0)


def nodal_rhs(m0, m0m, m1, m2):
    m1m, m2m = y_down(m1), z_down(m2)
    return (
        (m0m - m0) + (m1m - m1) + (m2m - m2),
        (m0 + m0m) * 0.5,
        (m1 + m1m) * 0.5,
        (m2 + m2m) * 0.5,
    )


def nodal_step(r, rm, rp):
    around = (rm + rp) + (y_up(r) + y_down(r)) + (z_up(r) + z_down(r))
    return (1.2 * c_node) * r + (c_node * c_node) * around


def finish(rhs, ks, u, corr):
    fixed = damping * rhs
    fixed = fixed + damping * (rhs - fixed)
    return jnp.where(ks > 0.0, u + corr, fixed)


def kernel(
    sizes, nx, ny, nz, cond_hbm, rhs_hbm, frac_hbm, reg_hbm, flag_hbm, out_ref,
    cond, frac_ref, reg_ref, flag_ref,
    e, st, sw, jac, u1, u2, mm, rr, zs, zr, ds, dr, dx_out, dx_in, ends_out, ends_in, lower_out, lower_in, upper_out, upper_in,
    ya_out, ya_in, yb_out, yb_in, yc_out, yc_in, yd_out, yd_in,
    blank, load, send, recv, near,
):
    gx, gy, gz = sizes
    pos = {"gx": lax.axis_index("gx"), "gy": lax.axis_index("gy"), "gz": lax.axis_index("gz")}
    size = {"gx": gx, "gy": gy, "gz": gz}
    first, last = PAD, PAD + nx - 1
    scope = jax.named_scope

    def device(**steps):
        return {axis: lax.rem(pos[axis] + (step + size[axis]), size[axis]) for axis, step in steps.items()}

    steps = [(x, z) for z in (1, -1) for x in (0, 1, -1)]
    paired = gy == 2
    barrier = pltpu.get_barrier_semaphore()

    def greet(*devices):
        for one in devices:
            pl.semaphore_signal(barrier, inc=1, device_id=one, device_id_type=MESH)

    def on(core, **steps):
        return {**device(**steps), "gy": core}

    if paired:
        greet(on(1, gx=1), on(1, gx=-1))
        pl.when(pos["gy"] == 0)(lambda: greet(device(gy=1)))
        greet(*(on(0, gx=x, gz=z) for x, z in steps))
    else:
        greet(device(gx=1), device(gx=-1), device(gy=1), device(gy=-1), *(device(gx=x, gz=z) for x, z in steps))
        greet(*(device(gx=x, gy=y, gz=z) for x, z in steps if x for y in (1, -1)))
    own_rows = pl.ds(0, ny)
    loads = [
        pltpu.make_async_copy(src, dst, load.at[i])
        for src, dst, i in (
            (rhs_hbm, e.at[pl.ds(0, 3), pl.ds(first, nx), own_rows], 0), (reg_hbm, reg_ref, 0),
            (frac_hbm, frac_ref, 0), (flag_hbm, flag_ref, 0), (cond_hbm, cond, 1),
        )
    ]

    def tiles_of(count):
        return blank.at[pl.ds(0, count)]

    def wait_tiles(semaphore, count):
        pltpu.make_async_copy(tiles_of(count), tiles_of(count), semaphore).wait()

    with scope("load"):
        for one in loads:
            one.start()
        if paired:
            @pl.when(pos["gy"] == 1)
            def _():
                pl.semaphore_wait(barrier, 5)
                pl.semaphore_signal(near.at[0], inc=1, device_id=device(gy=1), device_id_type=MESH)
        else:
            pl.semaphore_wait(barrier, 12 + len(steps))

        loads[4].wait()
        wait_tiles(load.at[0], 10 * nx * ny // 8)

    sent_tiles = []

    def copy(group, src, dst, where, start=True):
        made = pltpu.make_async_remote_copy(
            src_ref=src, dst_ref=dst, send_sem=send.at[0], recv_sem=recv.at[group],
            device_id=where, device_id_type=MESH,
        )
        sent_tiles.append(math.prod(src.shape) // (8 * nz))
        if start:
            made.start()
        return made

    def arrived(group, count):
        wait_tiles(recv.at[group], count)

    row = lax.broadcasted_iota(jnp.int32, (8, nz), 0)
    top, bottom, halo = slice(0, 8), slice(ny - 8, ny), slice(ny, ny + 8)

    def y_start(group, places, out, into):
        for i, (ref, where) in enumerate(places):
            out[i] = jnp.where(row < 4, ref[(*where, top, slice(None))], ref[(*where, bottom, slice(None))])
        if gy == 2:
            copy(group, out, into.at[0], device(gy=1))
        else:
            copy(group, out, into.at[0], device(gy=-1))
            copy(group, out, into.at[1], device(gy=1))

    def y_finish(group, places, into):
        arrived(group, into.shape[0] * len(places))
        for i, (ref, where) in enumerate(places):
            tile = into[0, i] if gy == 2 else jnp.where(row < 4, into[0, i], into[1, i])
            ref[(*where, halo, slice(None))] = tile

    lane = lax.broadcasted_iota(jnp.int32, (ny, nz), 1)
    slot = lane // SEG
    half = nz // 2
    low_half = lane < half
    quad = (lane % SEG) // 4
    left = (lane % SEG) < 8

    def end_piece(v, j):
        return rot(v, 8 + SEG * j, 1)

    def pick(base, where, other):
        return other if base is None else jnp.where(where, other, base)

    packs = [None] * 6
    with scope("pack"):
        for x in range(nx):
            region = reg_ref[x]
            sigma = jnp.zeros((ny, nz), jnp.float32)
            for number in range(cond.shape[0]):
                sigma = jnp.where(region == number, cond[number], sigma)
            for k in range(3):
                ks = jnp.where(flag_ref[k, x] == 0, sigma * frac_ref[k, x], 0.0)
                e[3 + k, first + x, 0:ny, :] = ks
                for f, v in ((k, e[k, first + x, 0:ny, :]), (3 + k, ks)):
                    packs[f] = pick(packs[f], slot == x, end_piece(v, x))
        for side, off in ((0, 8), (1, 4)):
            tiles = [None, None]
            for f in range(6):
                tiles[f // 4] = pick(tiles[f // 4], quad == f % 4, rot(packs[f], 4 * (f % 4) - off, 1))
            for i in range(2):
                zs[side, i] = tiles[i]
            other = rot(tiles[1], half, 1)
            ds[0, side] = jnp.where(low_half, other, tiles[0])
            ds[1, side] = jnp.where(low_half, tiles[0], other)
            if side == 1:
                for i in range(2):
                    tile = jnp.where(low_half == (i == 0), other, tiles[0])
                    dx_out[i] = jnp.where(row < 4, tile[0:8], tile[ny - 8:ny])
        starts = [jacobi_scale(packs[3 + k]) * packs[k] for k in range(3)]
        moves = (
            [(f, packs[f], 1, 2 * f, 2) for f in range(6)] + [(k, starts[k], 3, 11 + k, 1) for k in (1, 2)],
            [(f, packs[f], nx - 2, 2 * f, 2) for f in range(6)] + [(k, starts[k], nx - 3, 12 + k, 1) for k in range(3)],
        )
        for side in range(2):
            tiles = [None, None]
            for f, v, at, to, wide in moves[side]:
                t, to = divmod(to, 8)
                tiles[t] = pick(tiles[t], (slot >= to) & (slot < to + wide), rot(v, SEG * (to - at), 1))
            for i in range(2):
                ends_out[side, i] = tiles[i]

    with scope("barrierwait"):
        if paired:
            @pl.when(pos["gy"] == 0)
            def _():
                pl.semaphore_wait(near.at[0], 1)

    def far_wait():
        if not paired:
            return

        @pl.when(pos["gy"] == 0)
        def _():
            pl.semaphore_wait(barrier, 2 * len(steps))
            pl.semaphore_signal(near.at[1], inc=1, device_id=device(gy=1), device_id_type=MESH)

        @pl.when(pos["gy"] == 1)
        def _():
            pl.semaphore_wait(near.at[1], 1)

    own = [(e, (f, p)) for f in range(6) for p in range(first, last + 1)]
    y_start(0, own, ya_out, ya_in)

    up, down = device(gx=1), device(gx=-1)
    ends_copies = [copy(1, ends_out.at[0], ends_in.at[0], down, False), copy(1, ends_out.at[1], ends_in.at[1], up, False)]
    raw_copies = [
        copy(2, e.at[:, first, own_rows], e.at[:, last + 1, own_rows], down, False),
        copy(3, e.at[:, last, own_rows], e.at[:, first - 1, own_rows], up, False),
    ]
    late_copies = [
        copy(4, upper_out.at[pl.ds(0, 6)], upper_in.at[pl.ds(0, 6)], down, False),
        copy(5, lower_out, lower_in.at[:, own_rows], up, False),
    ]
    last_copy = copy(9, upper_out.at[pl.ds(6, 2), own_rows], upper_in.at[pl.ds(6, 2), own_rows], down, False)
    z_copies = [copy(1, zs.at[0], zr.at[0], device(gz=-1), False), copy(1, zs.at[1], zr.at[1], device(gz=1), False)]
    corner_copies = [
        copy(1 + 9 * zside, ds.at[side, zside], dr.at[side, zside], device(gx=1 - 2 * side, gz=2 * zside - 1), False)
        for side in range(2) for zside in range(2)
    ]
    cross_copies = [
        copy(10, dx_out.at[side], dx_in.at[i, side], device(gx=1 - 2 * side, gy=2 * i - 1, gz=1), False)
        for side in range(2) for i in range(1 if paired else 2)
    ]

    def start(*copies):
        for one in copies:
            one.start()

    def start_far(zside):
        start(corner_copies[zside], corner_copies[2 + zside], z_copies[zside])

    def start_both():
        start_far(1)
        start(*cross_copies)
        start_far(0)

    down_first = (lax.rem(pos["gx"], 4) == 1) & (pos["gz"] == 0)

    def in_order(begin):
        pl.when(down_first)(lambda: begin(0, 1))
        pl.when(jnp.logical_not(down_first))(lambda: begin(1, 0))

    late_start = pos["gz"] == 0
    in_order(lambda a, b: start(ends_copies[a], ends_copies[b]))

    up_only = lax.rem(pos["gx"], 4) == 3

    def on_start():
        pl.when(down_first)(lambda: start(raw_copies[0]))
        pl.when(up_only)(lambda: start(raw_copies[1]))
        pl.when(jnp.logical_not(down_first | up_only))(lambda: start(raw_copies[1], raw_copies[0]))

    on_start()

    @pl.when(jnp.logical_not(late_start))
    def _():
        with scope("nearwait"):
            far_wait()
            start_both()


    def faces(u, p):
        v0, v1, v2 = u[0, p], u[1, p], u[2, p]
        return face_one(v0, v2, u[2, p + 1]), face_two(v0, v1, u[1, p + 1])

    def curl_sweep(u, before, lo, hi, emit, after=None):
        f1m, f2m = before
        for p in range(lo, hi):
            f1, f2 = faces(u, p) if after is None or p < hi - 1 else after
            f0 = face_zero(u[1, p], u[2, p])
            cc = edges(f0, f1, f2, f1m, f2m)
            for k in range(3):
                emit(k, p, cc[k])
            f1m, f2m = f1, f2

    def emit_second(k, p, cc):
        u2[k, p] = next_iter(e[k, p], e[3 + k, p], jac[k, p], u1[k, p], cc)

    def emit_masked(k, p, cc):
        mm[k, p] = masked_residual(e[k, p], e[3 + k, p], u2[k, p], cc)

    def emit_rest(k, p, cc):
        if k > 0 or p != first + 1:
            emit_masked(k, p, cc)

    def node_range(lo, hi):
        for p in range(lo, hi):
            r = nodal_rhs(mm[0, p], mm[0, p - 1], mm[1, p], mm[2, p])
            for q in range(4):
                rr[q, p] = r[q]

    def first_range(lo, hi):
        for p in range(lo, hi):
            for k in range(3):
                scale = jacobi_scale(e[3 + k, p])
                jac[k, p] = scale
                u1[k, p] = scale * e[k, p]

    def below(v, p):
        up0 = v[0, p]
        return (z_up(up0) - up0) + v[2, p], v[1, p] + (y_up(up0) - up0)

    with scope("y1"):
        y_finish(0, own, ya_in)
    with scope("inner"):
        first_range(first, last + 1)
        curl_sweep(u1, faces(u1, first), first + 1, last, emit_second)
        p = last - 1
        sent = (*below(u1, p), e[3, p], *below(u2, p), e[0, p] - e[3, p] * u2[0, p])
        for i, v in enumerate(sent):
            lower_out[i] = v[0:ny]
        p = first + 1
        f1, f2 = faces(u2, p)
        cc = edges(face_zero(u2[1, p], u2[2, p]), f1, f2, -u2[2, p], u2[1, p])
        m0, m1, m2 = [masked_residual(e[k, p], e[3 + k, p], u2[k, p], cc[k]) for k in range(3)]
        mm[0, p] = m0
        sent = (u1[1, p], u1[2, p], e[4, p], e[5, p], u2[1, p], u2[2, p], m0, (y_down(m1) - m1) + (z_down(m2) - m2))
        for i, v in enumerate(sent):
            upper_out[i] = v
    @pl.when(down_first)
    def _():
        start(late_copies[0], last_copy, raw_copies[1], late_copies[1])

    @pl.when(up_only)
    def _():
        start(late_copies[1], raw_copies[0], late_copies[0], last_copy)

    @pl.when(jnp.logical_not(down_first | up_only))
    def _():
        start(late_copies[1], late_copies[0], last_copy)

    with scope("inner2"):
        curl_sweep(u2, faces(u2, first + 1), first + 2, last - 1, emit_masked)
        node_range(first + 2, last - 1)

    @pl.when(late_start)
    def _():
        with scope("nearwait"):
            far_wait()
            start_both()

    def relay(name, groups, relayed, places, out, into):
        with scope(name):
            for group, count in groups:
                arrived(group, count * ny // 8)
            y_start(relayed, places, out, into)

    raw_up = [(e, (f, last + 1)) for f in range(6)]
    raw_low = [(e, (f, first - 1)) for f in range(6)]
    late_low = [(lower_in, (i,)) for i in range(6)]
    strip_tiles = [(st, (f, t)) for f in range(6) for t in range(4)]
    relay("rawup", ((2, 6),), 6, raw_up, yb_out, yb_in)

    inner = (lane >= 4) & (lane < nz - 4)

    def node_at(p, count=4):
        return [nodal_step(rr[q, p], rr[q, p - 1], rr[q, p + 1]) for q in range(count)]

    def outputs(lo, hi):
        s_next = node_at(lo)
        for p in range(lo, hi):
            s = s_next
            s_next = node_at(p + 1, 4 if p + 1 < hi else 2)
            corr = (
                (s_next[0] - s[0]) + (s[1] + s_next[1]) * 0.5,
                (y_up(s[0]) - s[0]) + (s[2] + y_up(s[2])) * 0.5,
                (z_up(s[0]) - s[0]) + (s[3] + z_up(s[3])) * 0.5,
            )
            for k in range(3):
                body = finish(e[k, p, 0:ny], e[3 + k, p, 0:ny], u2[k, p, 0:ny], corr[k][0:ny])
                ends = rot(sw[k], nz - 8 - SEG * (p - first), 1)
                out_ref[k, p - first] = jnp.where(inner, body, ends)

    lane24 = lax.broadcasted_iota(jnp.int32, (ny + 8, nz), 1)
    slot24 = lane24 // SEG
    left24 = (lane24 % SEG) < 8

    span = range(4)

    def x_up(vs):
        rs = [rot(v, -SEG, 1) for v in vs]
        return [jnp.where(lane24 < nz - SEG, rs[t], rs[t ^ 1]) for t in span]

    def x_down(vs):
        rs = [rot(v, SEG, 1) for v in vs]
        return [jnp.where(lane24 >= SEG, rs[t], rs[t ^ 1]) for t in span]

    def strip_curl(u):
        u1p, u2p = x_up(u[1]), x_up(u[2])
        f1 = [face_one(u[0][t], u[2][t], u2p[t]) for t in span]
        f2 = [face_two(u[0][t], u[1][t], u1p[t]) for t in span]
        f0 = [face_zero(u[1][t], u[2][t]) for t in span]
        f1m, f2m = x_down(f1), x_down(f2)
        out = [edges(f0[t], f1[t], f2[t], f1m[t], f2m[t]) for t in span]
        return [[out[t][k] for t in span] for k in range(3)]

    def strips():
        sr = [[st[k, t] for t in span] for k in range(3)]
        sk = [[st[3 + k, t] for t in span] for k in range(3)]
        outer = (slot24 == 3) | (slot24 == nx - 3)
        scale = [[jacobi_scale(sk[k][t]) for t in span] for k in range(3)]
        u = [[scale[k][t] * sr[k][t] for t in span] for k in range(3)]
        for k in range(3):
            u[k][1] = jnp.where(outer & left24, sr[k][1], u[k][1])
            u[k][3] = jnp.where(outer & ~left24, sr[k][3], u[k][3])
        cc = strip_curl(u)
        u = [[next_iter(sr[k][t], sk[k][t], scale[k][t], u[k][t], cc[k][t]) for t in span] for k in range(3)]
        cc = strip_curl(u)
        m = [[masked_residual(sr[k][t], sk[k][t], u[k][t], cc[k][t]) for t in span] for k in range(3)]
        m0m = x_down(m[0])
        r = [nodal_rhs(m[0][t], m0m[t], m[1][t], m[2][t]) for t in span]
        s = []
        for q in range(4):
            rq = [r[t][q] for t in span]
            rm, rp = x_down(rq), x_up(rq)
            s.append([nodal_step(rq[t], rm[t], rp[t]) if q < 2 or t % 2 == 0 else None for t in span])
        s0p, s1p = x_up(s[0]), x_up(s[1])
        results = []
        for t in (0, 2):
            s0, s1, s2, s3 = [s[q][t] for q in range(4)]
            corr = (
                (s0p[t] - s0) + (s1 + s1p[t]) * 0.5,
                (y_up(s0) - s0) + (s2 + y_up(s2)) * 0.5,
                (z_up(s0) - s0) + (s3 + z_up(s3)) * 0.5,
            )
            results.append([finish(sr[k][t], sk[k][t], u[k][t], corr[k])[0:ny] for k in range(3)])
        for k in range(3):
            sw[k] = jnp.where(left, results[0][k], results[1][k])

    def corner_of(f, plus, minus, off):
        low = low_half[0:plus.shape[0]]
        if f < 4:
            return rot(jnp.where(low, plus, minus), off - 4 * f, 1)
        return rot(jnp.where(low, minus, plus), half + off - 4 * (f - 4), 1)

    with scope("endswait"):
        arrived(1, 10 * ny // 8)
    with scope("strippack"):
        for f in range(6):
            t, to = divmod(2 * f, 8)
            piece = rot(ends_in[0, t], SEG * (1 - to), 1)
            piece = jnp.where(slot == 0, end_piece(e[f, last + 1, 0:ny, :], 0), piece)
            piece = jnp.where(slot >= nx - 2, rot(ends_in[1, t], SEG * (nx - 2 - to), 1), piece)
            if f < 3:
                piece = jnp.where(slot == 3, rot(ends_in[0, 1], SEG * (3 - (3 + f)), 1), piece)
                piece = jnp.where(slot == nx - 3, rot(ends_in[1, 1], SEG * (nx - 3 - (4 + f)), 1), piece)
            mid = packs[f]
            st[f, 0, 0:ny, :] = jnp.where(left, mid, rot(zr[0, f // 4], 8 - 4 * (f % 4), 1))
            st[f, 1, 0:ny, :] = jnp.where(left, piece, corner_of(f, dr[1, 0], dr[0, 0], 8))
            st[f, 2, 0:ny, :] = jnp.where(left, rot(zr[1, f // 4], 4 - 4 * (f % 4), 1), mid)
            st[f, 3, 0:ny, :] = piece
        y_start(8, strip_tiles, yd_out, yd_in)

    relay("latelow", ((3, 6), (5, 6)), 7, raw_low + late_low, yc_out, yc_in)
    def side_strips():
        with scope("ystrip"):
            y_finish(8, strip_tiles, yd_in)
            arrived(10, 2 * (ny // 8 + dx_in.shape[0]))
            cross = [dx_in[0, i] if paired else jnp.where(row < 4, dx_in[0, i], dx_in[1, i]) for i in range(2)]
            for f in range(6):
                st[f, 3, 0:ny, :] = jnp.where(left, corner_of(f, dr[1, 1], dr[0, 1], 4), st[f, 3, 0:ny, :])
                st[f, 3, ny:ny + 8, :] = jnp.where(left[0:8], corner_of(f, cross[1], cross[0], 4), st[f, 3, ny:ny + 8, :])
        with scope("strips"):
            strips()

    def both_sides():
        with scope("ylow"):
            y_finish(7, raw_low + late_low, yc_in)
        with scope("yup"):
            y_finish(6, raw_up, yb_in)
            arrived(4, 6 * (ny + 8) // 8)
            arrived(9, 2 * ny // 8)
        with scope("sides"):
            p = first - 1
            first_range(p, p + 1)
            curl_sweep(u1, (lower_in[0] - u1[2, p], u1[1, p] - lower_in[1]), p, first + 1, emit_second)
            f1, f2 = lower_in[3] - u2[2, p], u2[1, p] - lower_in[4]
            cc = (z_down(f1) - f1) - (y_down(f2) - f2)
            mm[0, p - 1] = jnp.where(lower_in[2] > 0.0, lower_in[5] - cc, 0.0)
            curl_sweep(u2, (f1, f2), p, first + 2, emit_rest)
            node_range(p, first + 2)
            p = last + 1
            first_range(p, p + 1)
            f1 = face_one(u1[0, p], u1[2, p], upper_in[1])
            f2 = face_two(u1[0, p], u1[1, p], upper_in[0])
            curl_sweep(u1, faces(u1, last - 1), last, p + 1, emit_second, (f1, f2))
            f1 = face_one(u2[0, p], u2[2, p], upper_in[5])
            f2 = face_two(u2[0, p], u2[1, p], upper_in[4])
            curl_sweep(u2, faces(u2, last - 2), last - 1, p + 1, emit_masked, (f1, f2))
            node_range(last - 1, p + 1)
            v0 = u2[0, p]
            q2 = jnp.where(upper_in[2] > 0.0, u2[1, p] + (y_up(v0) - v0), 0.0)
            q1 = jnp.where(upper_in[3] > 0.0, (z_up(v0) - v0) + u2[2, p], 0.0)
            m0, m0p = mm[0, p], upper_in[6]
            rr[0, p + 1] = (m0 - m0p) + (upper_in[7] + (y_down(q2) - q2) + (z_down(q1) - q1))
            rr[1, p + 1] = (m0p + m0) * 0.5
            outputs(first, last + 1)

    side_strips()
    both_sides()
    with scope("sendwait"):
        wait_tiles(send.at[0], sum(sent_tiles))


def on_device(sizes, rhs, conductivity, fraction, region, flags):
    _, nx, ny, nz = rhs.shape
    planes = nx + 2 * PAD
    rows = ny + 8
    f32 = jnp.float32
    hbm = pl.BlockSpec(memory_space=pl.ANY)
    sides = 1 if sizes[1] == 2 else 2
    relays = []
    for count in (6 * nx, 6, 12, 24):
        relays += [pltpu.VMEM((count, 8, nz), f32), pltpu.VMEM((sides, count, 8, nz), f32)]
    return pl.pallas_call(
        functools.partial(kernel, sizes, nx, ny, nz),
        out_shape=pltpu.VMEM(rhs.shape, rhs.dtype),
        in_specs=[hbm] * 5,
        out_specs=pl.BlockSpec(memory_space=pltpu.VMEM),
        scratch_shapes=[
            pltpu.SMEM(conductivity.shape, f32),
            pltpu.VMEM(rhs.shape, f32),
            pltpu.VMEM(region.shape, jnp.int32),
            pltpu.VMEM(flags.shape, jnp.int32),
            pltpu.VMEM((6, planes, rows, nz), f32),
            pltpu.VMEM((6, 4, rows, nz), f32),
            pltpu.VMEM((3, ny, nz), f32),
            pltpu.VMEM((3, planes, rows, nz), f32),
            pltpu.VMEM((3, planes, rows, nz), f32),
            pltpu.VMEM((3, planes, rows, nz), f32),
            pltpu.VMEM((3, planes, rows, nz), f32),
            pltpu.VMEM((4, planes, rows, nz), f32),
            pltpu.VMEM((2, 2, ny, nz), f32),
            pltpu.VMEM((2, 2, ny, nz), f32),
            pltpu.VMEM((2, 2, ny, nz), f32),
            pltpu.VMEM((2, 2, ny, nz), f32),
            pltpu.VMEM((2, 8, nz), f32),
            pltpu.VMEM((sides, 2, 8, nz), f32),
            pltpu.VMEM((2, 2, ny, nz), f32),
            pltpu.VMEM((2, 2, ny, nz), f32),
            pltpu.VMEM((6, ny, nz), f32),
            pltpu.VMEM((6, rows, nz), f32),
            pltpu.VMEM((8, rows, nz), f32),
            pltpu.VMEM((8, rows, nz), f32),
            *relays,
            pltpu.VMEM((320, 8, nz), f32),
            pltpu.SemaphoreType.DMA((2,)),
            pltpu.SemaphoreType.DMA((1,)),
            pltpu.SemaphoreType.DMA((11,)),
            pltpu.SemaphoreType.REGULAR((2,)),
        ],
        compiler_params=pltpu.CompilerParams(
            collective_id=0, has_side_effects=True, vmem_limit_bytes=60 * 1024 * 1024
        ),
    )(conductivity, rhs, fraction, region, flags)


def solution(mesh):
    sizes = tuple(mesh.shape[name] for name in ("gx", "gy", "gz"))
    return jax.shard_map(
        functools.partial(on_device, sizes),
        mesh=mesh,
        in_specs=(
            P(None, "gx", "gy", "gz"),
            P(),
            P(None, "gx", "gy", "gz"),
            P("gx", "gy", "gz"),
            P(None, "gx", "gy", "gz"),
        ),
        out_specs=P(None, "gx", "gy", "gz"),
        check_vma=False,
    )
```

```python
import functools
import math

import jax
import jax.numpy as jnp
from jax import lax
from jax.experimental import pallas as pl
from jax.experimental.pallas import tpu as pltpu
from jax.sharding import PartitionSpec as P

damping = 0.8
c_node = 0.8 / 7.0
MESH = pl.DeviceIdType.MESH
PAD = 2
SEG = 16


def rot(v, shift, axis):
    return pltpu.roll(v, shift % v.shape[axis], axis)


def y_up(v):
    return rot(v, -1, 0)


def y_down(v):
    return rot(v, 1, 0)


def z_up(v):
    return rot(v, -1, 1)


def z_down(v):
    return rot(v, 1, 1)


def face_zero(u1, u2):
    return (y_up(u2) - u2) - (z_up(u1) - u1)


def face_one(u0, u2, u2p):
    return (z_up(u0) - u0) - (u2p - u2)


def face_two(u0, u1, u1p):
    return (u1p - u1) - (y_up(u0) - u0)


def edges(f0, f1, f2, f1m, f2m):
    return (
        (z_down(f1) - f1) - (y_down(f2) - f2),
        (f2m - f2) - (z_down(f0) - f0),
        (y_down(f0) - f0) - (f1m - f1),
    )


def jacobi_scale(ks):
    return jnp.where(ks > 0.0, damping / (4.0 + ks), 0.0)


def next_iter(rhs, ks, scale, u, cc):
    return u + scale * (rhs - (cc + ks * u))


def masked_residual(rhs, ks, u, cc):
    return jnp.where(ks > 0.0, rhs - (cc + ks * u), 0.0)


def nodal_rhs(m0, m0m, m1, m2):
    m1m, m2m = y_down(m1), z_down(m2)
    return (
        (m0m - m0) + (m1m - m1) + (m2m - m2),
        (m0 + m0m) * 0.5,
        (m1 + m1m) * 0.5,
        (m2 + m2m) * 0.5,
    )


def nodal_step(r, rm, rp):
    around = (rm + rp) + (y_up(r) + y_down(r)) + (z_up(r) + z_down(r))
    return (1.2 * c_node) * r + (c_node * c_node) * around


def finish(rhs, ks, u, corr):
    fixed = damping * rhs
    fixed = fixed + damping * (rhs - fixed)
    return jnp.where(ks > 0.0, u + corr, fixed)


def kernel(
    sizes, nx, ny, nz, cond_hbm, rhs_hbm, frac_hbm, reg_hbm, flag_hbm, out_ref,
    cond, frac_ref, reg_ref, flag_ref,
    e, st, sw, jac, u1, u2, mm, rr, zs, zr, ds, dr, dx_out, dx_in, zx_out, zx_in, ends_out, ends_in, lower_out, lower_in, upper_out, upper_in,
    ya_out, ya_in, yb_out, yb_in, yc_out, yc_in, yd_out, yd_in, ye_out, ye_in,
    blank, load, send, recv, near,
):
    gx, gy, gz = sizes
    pos = {"gx": lax.axis_index("gx"), "gy": lax.axis_index("gy"), "gz": lax.axis_index("gz")}
    size = {"gx": gx, "gy": gy, "gz": gz}
    first, last = PAD, PAD + nx - 1
    scope = jax.named_scope

    def device(**steps):
        return {axis: lax.rem(pos[axis] + (step + size[axis]), size[axis]) for axis, step in steps.items()}

    steps = [(x, z) for z in (1, -1) for x in (0, 1, -1)]
    paired = gy == 2
    barrier = pltpu.get_barrier_semaphore()

    def greet(*devices):
        for one in devices:
            pl.semaphore_signal(barrier, inc=1, device_id=one, device_id_type=MESH)

    def on(core, **steps):
        return {**device(**steps), "gy": core}

    if paired:
        greet(on(1, gx=1), on(1, gx=-1))
        pl.when(pos["gy"] == 0)(lambda: greet(device(gy=1)))
        greet(*(on(0, gx=x, gz=z) for x, z in steps))
    else:
        greet(device(gx=1), device(gx=-1), device(gy=1), device(gy=-1), *(device(gx=x, gz=z) for x, z in steps))
        greet(*(device(gx=x, gy=y, gz=z) for x, z in steps for y in (1, -1)))
    own_rows = pl.ds(0, ny)
    loads = [
        pltpu.make_async_copy(src, dst, load.at[i])
        for src, dst, i in (
            (rhs_hbm, e.at[pl.ds(0, 3), pl.ds(first, nx), own_rows], 0), (reg_hbm, reg_ref, 0),
            (frac_hbm, frac_ref, 0), (flag_hbm, flag_ref, 0), (cond_hbm, cond, 1),
        )
    ]

    def tiles_of(count):
        return blank.at[pl.ds(0, count)]

    def wait_tiles(semaphore, count):
        pltpu.make_async_copy(tiles_of(count), tiles_of(count), semaphore).wait()

    with scope("load"):
        for one in loads:
            one.start()
        if paired:
            @pl.when(pos["gy"] == 1)
            def _():
                pl.semaphore_wait(barrier, 5)
                pl.semaphore_signal(near.at[0], inc=1, device_id=device(gy=1), device_id_type=MESH)
        else:
            pl.semaphore_wait(barrier, 4 + 3 * len(steps))

        loads[4].wait()
        wait_tiles(load.at[0], 10 * nx * ny // 8)

    sent_tiles = []

    def copy(group, src, dst, where, start=True):
        made = pltpu.make_async_remote_copy(
            src_ref=src, dst_ref=dst, send_sem=send.at[0], recv_sem=recv.at[group],
            device_id=where, device_id_type=MESH,
        )
        sent_tiles.append(math.prod(src.shape) // (8 * nz))
        if start:
            made.start()
        return made

    def arrived(group, count):
        wait_tiles(recv.at[group], count)

    row = lax.broadcasted_iota(jnp.int32, (8, nz), 0)
    top, bottom, halo = slice(0, 8), slice(ny - 8, ny), slice(ny, ny + 8)

    def y_start(group, places, out, into):
        for i, (ref, where) in enumerate(places):
            out[i] = jnp.where(row < 4, ref[(*where, top, slice(None))], ref[(*where, bottom, slice(None))])
        if gy == 2:
            copy(group, out, into.at[0], device(gy=1))
        else:
            copy(group, out, into.at[0], device(gy=-1))
            copy(group, out, into.at[1], device(gy=1))

    def y_finish(group, places, into):
        arrived(group, into.shape[0] * len(places))
        for i, (ref, where) in enumerate(places):
            tile = into[0, i] if gy == 2 else jnp.where(row < 4, into[0, i], into[1, i])
            ref[(*where, halo, slice(None))] = tile

    lane = lax.broadcasted_iota(jnp.int32, (ny, nz), 1)
    slot = lane // SEG
    half = nz // 2
    low_half = lane < half
    quad = (lane % SEG) // 4
    left = (lane % SEG) < 8

    def end_piece(v, j):
        return rot(v, 8 + SEG * j, 1)

    def pick(base, where, other):
        return other if base is None else jnp.where(where, other, base)

    packs = [None] * 6
    with scope("pack"):
        for x in range(nx):
            region = reg_ref[x]
            sigma = jnp.zeros((ny, nz), jnp.float32)
            for number in range(cond.shape[0]):
                sigma = jnp.where(region == number, cond[number], sigma)
            for k in range(3):
                ks = jnp.where(flag_ref[k, x] == 0, sigma * frac_ref[k, x], 0.0)
                e[3 + k, first + x, 0:ny, :] = ks
                for f, v in ((k, e[k, first + x, 0:ny, :]), (3 + k, ks)):
                    packs[f] = pick(packs[f], slot == x, end_piece(v, x))
        for side, off in ((0, 8), (1, 4)):
            tiles = [None, None]
            for f in range(6):
                tiles[f // 4] = pick(tiles[f // 4], quad == f % 4, rot(packs[f], 4 * (f % 4) - off, 1))
            for i in range(2):
                zs[side, i] = tiles[i]
                zx_out[side, i] = jnp.where(row < 4, tiles[i][0:8], tiles[i][ny - 8:ny])
            other = rot(tiles[1], half, 1)
            ds[0, side] = jnp.where(low_half, other, tiles[0])
            ds[1, side] = jnp.where(low_half, tiles[0], other)
            if side == 1:
                for i in range(2):
                    tile = jnp.where(low_half == (i == 0), other, tiles[0])
                    dx_out[i] = jnp.where(row < 4, tile[0:8], tile[ny - 8:ny])
        starts = [jacobi_scale(packs[3 + k]) * packs[k] for k in range(3)]
        moves = (
            [(f, packs[f], 1, 2 * f, 2) for f in range(6)] + [(k, starts[k], 3, 11 + k, 1) for k in (1, 2)],
            [(f, packs[f], nx - 2, 2 * f, 2) for f in range(6)] + [(k, starts[k], nx - 3, 12 + k, 1) for k in range(3)],
        )
        for side in range(2):
            tiles = [None, None]
            for f, v, at, to, wide in moves[side]:
                t, to = divmod(to, 8)
                tiles[t] = pick(tiles[t], (slot >= to) & (slot < to + wide), rot(v, SEG * (to - at), 1))
            for i in range(2):
                ends_out[side, i] = tiles[i]

    with scope("barrierwait"):
        if paired:
            @pl.when(pos["gy"] == 0)
            def _():
                pl.semaphore_wait(near.at[0], 1)

    def far_wait():
        if not paired:
            return

        @pl.when(pos["gy"] == 0)
        def _():
            pl.semaphore_wait(barrier, 2 * len(steps))
            pl.semaphore_signal(near.at[1], inc=1, device_id=device(gy=1), device_id_type=MESH)

        @pl.when(pos["gy"] == 1)
        def _():
            pl.semaphore_wait(near.at[1], 1)

    own = [(e, (f, p)) for f in range(6) for p in range(first, last + 1)]
    y_start(0, own, ya_out, ya_in)

    up, down = device(gx=1), device(gx=-1)
    ends_copies = [copy(1, ends_out.at[0], ends_in.at[0], down, False), copy(1, ends_out.at[1], ends_in.at[1], up, False)]
    raw_copies = [
        copy(2, e.at[:, first, own_rows], e.at[:, last + 1, own_rows], down, False),
        copy(3, e.at[:, last, own_rows], e.at[:, first - 1, own_rows], up, False),
    ]
    late_copies = [
        copy(4, upper_out.at[pl.ds(0, 6)], upper_in.at[pl.ds(0, 6)], down, False),
        copy(5, lower_out.at[:, own_rows], lower_in.at[:, own_rows], up, False),
    ]
    wide_copy = pltpu.make_async_remote_copy(
        src_ref=lower_out, dst_ref=lower_in, send_sem=send.at[0], recv_sem=recv.at[5],
        device_id=up, device_id_type=MESH,
    )
    last_copy = copy(9, upper_out.at[pl.ds(6, 2), own_rows], upper_in.at[pl.ds(6, 2), own_rows], down, False)
    z_copies = [copy(10, zs.at[i], zr.at[i], device(gz=2 * i - 1), False) for i in range(2)]
    corner_copies = [
        copy(1 + 9 * zside, ds.at[side, zside], dr.at[side, zside], device(gx=1 - 2 * side, gz=2 * zside - 1), False)
        for side in range(2) for zside in range(2)
    ]
    cross_copies = [
        copy(10, dx_out.at[side], dx_in.at[i, side], device(gx=1 - 2 * side, gy=2 * i - 1, gz=1), False)
        for side in range(2) for i in range(1 if paired else 2)
    ] + [
        copy(10, zx_out.at[side], zx_in.at[i, side], device(gy=2 * i - 1, gz=2 * side - 1), False)
        for side in range(2) for i in range(1 if paired else 2)
    ]

    def start(*copies):
        for one in copies:
            one.start()

    def start_far(zside):
        start(corner_copies[zside], corner_copies[2 + zside], z_copies[zside])

    def start_both():
        start_far(1)
        start(*cross_copies)
        start_far(0)

    down_first = (lax.rem(pos["gx"], 4) == 1) & (pos["gz"] == 0)
    wide = (lax.rem(device(gx=-1)["gx"], 4) == 1) & (pos["gz"] == 0)
    narrow = jnp.logical_not(wide)

    def in_order(begin):
        pl.when(down_first)(lambda: begin(0, 1))
        pl.when(jnp.logical_not(down_first))(lambda: begin(1, 0))

    late_start = pos["gz"] == 0
    in_order(lambda a, b: start(ends_copies[a], ends_copies[b]))

    up_only = lax.rem(pos["gx"], 4) == 3

    def on_start():
        pl.when(down_first)(lambda: start(raw_copies[0]))
        pl.when(up_only)(lambda: start(raw_copies[1]))
        pl.when(jnp.logical_not(down_first | up_only))(lambda: start(raw_copies[1], raw_copies[0]))

    on_start()

    @pl.when(jnp.logical_not(late_start))
    def _():
        with scope("nearwait"):
            far_wait()
            start_both()


    def faces(u, p):
        v0, v1, v2 = u[0, p], u[1, p], u[2, p]
        return face_one(v0, v2, u[2, p + 1]), face_two(v0, v1, u[1, p + 1])

    def curl_sweep(u, before, lo, hi, emit, after=None):
        f1m, f2m = before
        for p in range(lo, hi):
            f1, f2 = faces(u, p) if after is None or p < hi - 1 else after
            f0 = face_zero(u[1, p], u[2, p])
            cc = edges(f0, f1, f2, f1m, f2m)
            for k in range(3):
                emit(k, p, cc[k])
            f1m, f2m = f1, f2

    def emit_second(k, p, cc):
        u2[k, p] = next_iter(e[k, p], e[3 + k, p], jac[k, p], u1[k, p], cc)

    def emit_masked(k, p, cc):
        mm[k, p] = masked_residual(e[k, p], e[3 + k, p], u2[k, p], cc)

    def emit_rest(k, p, cc):
        if k > 0 or p != first + 1:
            emit_masked(k, p, cc)

    def node_range(lo, hi):
        for p in range(lo, hi):
            r = nodal_rhs(mm[0, p], mm[0, p - 1], mm[1, p], mm[2, p])
            for q in range(4):
                rr[q, p] = r[q]

    def first_range(lo, hi):
        for p in range(lo, hi):
            for k in range(3):
                scale = jacobi_scale(e[3 + k, p])
                jac[k, p] = scale
                u1[k, p] = scale * e[k, p]

    def below(v, p):
        up0 = v[0, p]
        return (z_up(up0) - up0) + v[2, p], v[1, p] + (y_up(up0) - up0)

    with scope("y1"):
        y_finish(0, own, ya_in)
    with scope("inner"):
        first_range(first, last + 1)
        curl_sweep(u1, faces(u1, first), first + 1, last, emit_second)
        p = last - 1
        sent = (*below(u1, p), e[3, p], *below(u2, p), e[0, p] - e[3, p] * u2[0, p])
        for i, v in enumerate(sent):
            lower_out[i] = v
        p = first + 1
        f1, f2 = faces(u2, p)
        cc = edges(face_zero(u2[1, p], u2[2, p]), f1, f2, -u2[2, p], u2[1, p])
        m0, m1, m2 = [masked_residual(e[k, p], e[3 + k, p], u2[k, p], cc[k]) for k in range(3)]
        mm[0, p] = m0
        sent = (u1[1, p], u1[2, p], e[4, p], e[5, p], u2[1, p], u2[2, p], m0, (y_down(m1) - m1) + (z_down(m2) - m2))
        for i, v in enumerate(sent):
            upper_out[i] = v
    @pl.when(down_first)
    def _():
        start(late_copies[0], last_copy, raw_copies[1], wide_copy)

    @pl.when(up_only)
    def _():
        start(late_copies[1], raw_copies[0], late_copies[0], last_copy)

    @pl.when(jnp.logical_not(down_first | up_only))
    def _():
        start(late_copies[1], late_copies[0], last_copy)

    with scope("inner2"):
        curl_sweep(u2, faces(u2, first + 1), first + 2, last - 1, emit_masked)
        node_range(first + 2, last - 1)

    @pl.when(late_start)
    def _():
        with scope("nearwait"):
            far_wait()
            start_both()

    def relay(name, groups, relayed, places, out, into):
        with scope(name):
            for group, count in groups:
                arrived(group, count * ny // 8)
            y_start(relayed, places, out, into)

    raw_up = [(e, (f, last + 1)) for f in range(6)]
    raw_low = [(e, (f, first - 1)) for f in range(6)]
    late_low = [(lower_in, (i,)) for i in range(6)]
    strip_tiles = [(st, (f, t)) for f in range(6) for t in range(4)]
    relay("rawup", ((2, 6),), 6, raw_up, yb_out, yb_in)

    inner = (lane >= 4) & (lane < nz - 4)

    def node_at(p, count=4):
        return [nodal_step(rr[q, p], rr[q, p - 1], rr[q, p + 1]) for q in range(count)]

    def outputs(lo, hi):
        s_next = node_at(lo)
        for p in range(lo, hi):
            s = s_next
            s_next = node_at(p + 1, 4 if p + 1 < hi else 2)
            corr = (
                (s_next[0] - s[0]) + (s[1] + s_next[1]) * 0.5,
                (y_up(s[0]) - s[0]) + (s[2] + y_up(s[2])) * 0.5,
                (z_up(s[0]) - s[0]) + (s[3] + z_up(s[3])) * 0.5,
            )
            for k in range(3):
                body = finish(e[k, p, 0:ny], e[3 + k, p, 0:ny], u2[k, p, 0:ny], corr[k][0:ny])
                ends = rot(sw[k], nz - 8 - SEG * (p - first), 1)
                out_ref[k, p - first] = jnp.where(inner, body, ends)

    lane24 = lax.broadcasted_iota(jnp.int32, (ny + 8, nz), 1)
    slot24 = lane24 // SEG
    left24 = (lane24 % SEG) < 8

    span = range(4)

    def x_up(vs):
        rs = [rot(v, -SEG, 1) for v in vs]
        return [jnp.where(lane24 < nz - SEG, rs[t], rs[t ^ 1]) for t in span]

    def x_down(vs):
        rs = [rot(v, SEG, 1) for v in vs]
        return [jnp.where(lane24 >= SEG, rs[t], rs[t ^ 1]) for t in span]

    def strip_curl(u):
        u1p, u2p = x_up(u[1]), x_up(u[2])
        f1 = [face_one(u[0][t], u[2][t], u2p[t]) for t in span]
        f2 = [face_two(u[0][t], u[1][t], u1p[t]) for t in span]
        f0 = [face_zero(u[1][t], u[2][t]) for t in span]
        f1m, f2m = x_down(f1), x_down(f2)
        out = [edges(f0[t], f1[t], f2[t], f1m[t], f2m[t]) for t in span]
        return [[out[t][k] for t in span] for k in range(3)]

    def strips():
        sr = [[st[k, t] for t in span] for k in range(3)]
        sk = [[st[3 + k, t] for t in span] for k in range(3)]
        outer = (slot24 == 3) | (slot24 == nx - 3)
        scale = [[jacobi_scale(sk[k][t]) for t in span] for k in range(3)]
        u = [[scale[k][t] * sr[k][t] for t in span] for k in range(3)]
        for k in range(3):
            u[k][1] = jnp.where(outer & left24, sr[k][1], u[k][1])
            u[k][3] = jnp.where(outer & ~left24, sr[k][3], u[k][3])
        cc = strip_curl(u)
        u = [[next_iter(sr[k][t], sk[k][t], scale[k][t], u[k][t], cc[k][t]) for t in span] for k in range(3)]
        cc = strip_curl(u)
        m = [[masked_residual(sr[k][t], sk[k][t], u[k][t], cc[k][t]) for t in span] for k in range(3)]
        m0m = x_down(m[0])
        r = [nodal_rhs(m[0][t], m0m[t], m[1][t], m[2][t]) for t in span]
        s = []
        for q in range(4):
            rq = [r[t][q] for t in span]
            rm, rp = x_down(rq), x_up(rq)
            s.append([nodal_step(rq[t], rm[t], rp[t]) if q < 2 or t % 2 == 0 else None for t in span])
        s0p, s1p = x_up(s[0]), x_up(s[1])
        results = []
        for t in (0, 2):
            s0, s1, s2, s3 = [s[q][t] for q in range(4)]
            corr = (
                (s0p[t] - s0) + (s1 + s1p[t]) * 0.5,
                (y_up(s0) - s0) + (s2 + y_up(s2)) * 0.5,
                (z_up(s0) - s0) + (s3 + z_up(s3)) * 0.5,
            )
            results.append([finish(sr[k][t], sk[k][t], u[k][t], corr[k])[0:ny] for k in range(3)])
        for k in range(3):
            sw[k] = jnp.where(left, results[0][k], results[1][k])

    def corner_of(f, plus, minus, off):
        low = low_half[0:plus.shape[0]]
        if f < 4:
            return rot(jnp.where(low, plus, minus), off - 4 * f, 1)
        return rot(jnp.where(low, minus, plus), half + off - 4 * (f - 4), 1)

    with scope("endswait"):
        arrived(1, 6 * ny // 8)
    with scope("strippack"):
        for f in range(6):
            t, to = divmod(2 * f, 8)
            piece = rot(ends_in[0, t], SEG * (1 - to), 1)
            piece = jnp.where(slot == 0, end_piece(e[f, last + 1, 0:ny, :], 0), piece)
            piece = jnp.where(slot >= nx - 2, rot(ends_in[1, t], SEG * (nx - 2 - to), 1), piece)
            if f < 3:
                piece = jnp.where(slot == 3, rot(ends_in[0, 1], SEG * (3 - (3 + f)), 1), piece)
                piece = jnp.where(slot == nx - 3, rot(ends_in[1, 1], SEG * (nx - 3 - (4 + f)), 1), piece)
            mid = packs[f]
            st[f, 0, 0:ny, :] = mid
            st[f, 1, 0:ny, :] = jnp.where(left, piece, corner_of(f, dr[1, 0], dr[0, 0], 8))
            st[f, 2, 0:ny, :] = mid
            st[f, 3, 0:ny, :] = piece
        y_start(8, strip_tiles, yd_out, yd_in)

    relay("rawlow", ((3, 6),), 7, raw_low, yc_out, yc_in)

    @pl.when(narrow)
    def _():
        relay("latelow", ((5, 6),), 11, late_low, ye_out, ye_in)

    def side_strips():
        with scope("ystrip"):
            y_finish(8, strip_tiles, yd_in)
            sides = dx_in.shape[0]
            arrived(10, 6 * (ny // 8 + sides))

            def crossed(ref, *where):
                if paired:
                    return ref[(0, *where)]
                return jnp.where(row < 4, ref[(0, *where)], ref[(1, *where)])

            for f in range(6):
                t, q = divmod(f, 4)
                for rows, above, below_z, plus, minus in (
                    (slice(0, ny), zr[0, t], zr[1, t], dr[1, 1], dr[0, 1]),
                    (halo, crossed(zx_in, 0, t), crossed(zx_in, 1, t), crossed(dx_in, 1), crossed(dx_in, 0)),
                ):
                    mine = left[0:above.shape[0]]
                    st[f, 0, rows, :] = jnp.where(mine, st[f, 0, rows, :], rot(above, 8 - 4 * q, 1))
                    st[f, 2, rows, :] = jnp.where(mine, rot(below_z, 4 - 4 * q, 1), st[f, 2, rows, :])
                    st[f, 3, rows, :] = jnp.where(mine, corner_of(f, plus, minus, 4), st[f, 3, rows, :])
        with scope("strips"):
            strips()

    def both_sides():
        with scope("ylow"):
            y_finish(7, raw_low, yc_in)
            pl.when(narrow)(lambda: y_finish(11, late_low, ye_in))
            pl.when(wide)(lambda: arrived(5, 6 * (ny + 8) // 8))
        with scope("yup"):
            y_finish(6, raw_up, yb_in)
            arrived(4, 6 * (ny + 8) // 8)
            arrived(9, 2 * ny // 8)
        with scope("sides"):
            p = first - 1
            first_range(p, p + 1)
            curl_sweep(u1, (lower_in[0] - u1[2, p], u1[1, p] - lower_in[1]), p, first + 1, emit_second)
            f1, f2 = lower_in[3] - u2[2, p], u2[1, p] - lower_in[4]
            cc = (z_down(f1) - f1) - (y_down(f2) - f2)
            mm[0, p - 1] = jnp.where(lower_in[2] > 0.0, lower_in[5] - cc, 0.0)
            curl_sweep(u2, (f1, f2), p, first + 2, emit_rest)
            node_range(p, first + 2)
            p = last + 1
            first_range(p, p + 1)
            f1 = face_one(u1[0, p], u1[2, p], upper_in[1])
            f2 = face_two(u1[0, p], u1[1, p], upper_in[0])
            curl_sweep(u1, faces(u1, last - 1), last, p + 1, emit_second, (f1, f2))
            f1 = face_one(u2[0, p], u2[2, p], upper_in[5])
            f2 = face_two(u2[0, p], u2[1, p], upper_in[4])
            curl_sweep(u2, faces(u2, last - 2), last - 1, p + 1, emit_masked, (f1, f2))
            node_range(last - 1, p + 1)
            v0 = u2[0, p]
            q2 = jnp.where(upper_in[2] > 0.0, u2[1, p] + (y_up(v0) - v0), 0.0)
            q1 = jnp.where(upper_in[3] > 0.0, (z_up(v0) - v0) + u2[2, p], 0.0)
            m0, m0p = mm[0, p], upper_in[6]
            rr[0, p + 1] = (m0 - m0p) + (upper_in[7] + (y_down(q2) - q2) + (z_down(q1) - q1))
            rr[1, p + 1] = (m0p + m0) * 0.5
            outputs(first, last + 1)

    side_strips()
    both_sides()
    with scope("sendwait"):
        total = sum(sent_tiles)
        pl.when(down_first)(lambda: wait_tiles(send.at[0], total + 6))
        pl.when(wide)(lambda: wait_tiles(send.at[0], total - 6 * dx_in.shape[0]))
        pl.when(jnp.logical_not(down_first | wide))(lambda: wait_tiles(send.at[0], total))


def on_device(sizes, rhs, conductivity, fraction, region, flags):
    _, nx, ny, nz = rhs.shape
    planes = nx + 2 * PAD
    rows = ny + 8
    f32 = jnp.float32
    hbm = pl.BlockSpec(memory_space=pl.ANY)
    sides = 1 if sizes[1] == 2 else 2
    relays = []
    for count in (6 * nx, 6, 6, 24, 6):
        relays += [pltpu.VMEM((count, 8, nz), f32), pltpu.VMEM((sides, count, 8, nz), f32)]
    return pl.pallas_call(
        functools.partial(kernel, sizes, nx, ny, nz),
        out_shape=pltpu.VMEM(rhs.shape, rhs.dtype),
        in_specs=[hbm] * 5,
        out_specs=pl.BlockSpec(memory_space=pltpu.VMEM),
        scratch_shapes=[
            pltpu.SMEM(conductivity.shape, f32),
            pltpu.VMEM(rhs.shape, f32),
            pltpu.VMEM(region.shape, jnp.int32),
            pltpu.VMEM(flags.shape, jnp.int32),
            pltpu.VMEM((6, planes, rows, nz), f32),
            pltpu.VMEM((6, 4, rows, nz), f32),
            pltpu.VMEM((3, ny, nz), f32),
            pltpu.VMEM((3, planes, rows, nz), f32),
            pltpu.VMEM((3, planes, rows, nz), f32),
            pltpu.VMEM((3, planes, rows, nz), f32),
            pltpu.VMEM((3, planes, rows, nz), f32),
            pltpu.VMEM((4, planes, rows, nz), f32),
            pltpu.VMEM((2, 2, ny, nz), f32),
            pltpu.VMEM((2, 2, ny, nz), f32),
            pltpu.VMEM((2, 2, ny, nz), f32),
            pltpu.VMEM((2, 2, ny, nz), f32),
            pltpu.VMEM((2, 8, nz), f32),
            pltpu.VMEM((sides, 2, 8, nz), f32),
            pltpu.VMEM((2, 2, 8, nz), f32),
            pltpu.VMEM((sides, 2, 2, 8, nz), f32),
            pltpu.VMEM((2, 2, ny, nz), f32),
            pltpu.VMEM((2, 2, ny, nz), f32),
            pltpu.VMEM((6, rows, nz), f32),
            pltpu.VMEM((6, rows, nz), f32),
            pltpu.VMEM((8, rows, nz), f32),
            pltpu.VMEM((8, rows, nz), f32),
            *relays,
            pltpu.VMEM((320, 8, nz), f32),
            pltpu.SemaphoreType.DMA((2,)),
            pltpu.SemaphoreType.DMA((1,)),
            pltpu.SemaphoreType.DMA((12,)),
            pltpu.SemaphoreType.REGULAR((2,)),
        ],
        compiler_params=pltpu.CompilerParams(
            collective_id=0, has_side_effects=True, vmem_limit_bytes=60 * 1024 * 1024
        ),
    )(conductivity, rhs, fraction, region, flags)


def solution(mesh):
    sizes = tuple(mesh.shape[name] for name in ("gx", "gy", "gz"))
    return jax.shard_map(
        functools.partial(on_device, sizes),
        mesh=mesh,
        in_specs=(
            P(None, "gx", "gy", "gz"),
            P(),
            P(None, "gx", "gy", "gz"),
            P("gx", "gy", "gz"),
            P(None, "gx", "gy", "gz"),
        ),
        out_specs=P(None, "gx", "gy", "gz"),
        check_vma=False,
    )
```

```python
import functools
import math

import jax
import jax.numpy as jnp
from jax import lax
from jax.experimental import pallas as pl
from jax.experimental.pallas import tpu as pltpu
from jax.sharding import PartitionSpec as P

damping = 0.8
c_node = 0.8 / 7.0
MESH = pl.DeviceIdType.MESH
PAD = 2
SEG = 16


def rot(v, shift, axis):
    return pltpu.roll(v, shift % v.shape[axis], axis)


def y_up(v):
    return rot(v, -1, 0)


def y_down(v):
    return rot(v, 1, 0)


def z_up(v):
    return rot(v, -1, 1)


def z_down(v):
    return rot(v, 1, 1)


def face_zero(u1, u2):
    return (y_up(u2) - u2) - (z_up(u1) - u1)


def face_one(u0, u2, u2p):
    return (z_up(u0) - u0) - (u2p - u2)


def face_two(u0, u1, u1p):
    return (u1p - u1) - (y_up(u0) - u0)


def edges(f0, f1, f2, f1m, f2m):
    return (
        (z_down(f1) - f1) - (y_down(f2) - f2),
        (f2m - f2) - (z_down(f0) - f0),
        (y_down(f0) - f0) - (f1m - f1),
    )


def jacobi_scale(ks):
    return jnp.where(ks > 0.0, damping / (4.0 + ks), 0.0)


def next_iter(rhs, ks, scale, u, cc):
    return u + scale * (rhs - (cc + ks * u))


def masked_residual(rhs, ks, u, cc):
    return jnp.where(ks > 0.0, rhs - (cc + ks * u), 0.0)


def nodal_rhs(m0, m0m, m1, m2):
    m1m, m2m = y_down(m1), z_down(m2)
    return (
        (m0m - m0) + (m1m - m1) + (m2m - m2),
        (m0 + m0m) * 0.5,
        (m1 + m1m) * 0.5,
        (m2 + m2m) * 0.5,
    )


def nodal_step(r, rm, rp):
    around = (rm + rp) + (y_up(r) + y_down(r)) + (z_up(r) + z_down(r))
    return (1.2 * c_node) * r + (c_node * c_node) * around


def finish(rhs, ks, u, corr):
    fixed = damping * rhs
    fixed = fixed + damping * (rhs - fixed)
    return jnp.where(ks > 0.0, u + corr, fixed)


def kernel(
    sizes, nx, ny, nz, cond_hbm, rhs_hbm, frac_hbm, reg_hbm, flag_hbm, out_ref,
    cond, frac_ref, reg_ref, flag_ref,
    e, st, sw, jac, u1, u2, mm, rr, zs, zr, ds, dr, dx_out, dx_in, zx_out, zx_in, ends_out, ends_in, lower_out, lower_in, upper_out, upper_in,
    ya_out, ya_in, yb_out, yb_in, yc_out, yc_in, yd_out, yd_in, ye_out, ye_in, yf_out, yf_in,
    blank, load, send, recv, near,
):
    gx, gy, gz = sizes
    pos = {"gx": lax.axis_index("gx"), "gy": lax.axis_index("gy"), "gz": lax.axis_index("gz")}
    size = {"gx": gx, "gy": gy, "gz": gz}
    first, last = PAD, PAD + nx - 1
    scope = jax.named_scope

    def device(**steps):
        return {axis: lax.rem(pos[axis] + (step + size[axis]), size[axis]) for axis, step in steps.items()}

    steps = [(x, z) for z in (1, -1) for x in (0, 1, -1)]
    paired = gy == 2
    barrier = pltpu.get_barrier_semaphore()

    def greet(*devices):
        for one in devices:
            pl.semaphore_signal(barrier, inc=1, device_id=one, device_id_type=MESH)

    def on(core, **steps):
        return {**device(**steps), "gy": core}

    if paired:
        greet(on(1, gx=1), on(1, gx=-1))
        pl.when(pos["gy"] == 0)(lambda: greet(device(gy=1)))
        greet(*(on(0, gx=x, gz=z) for x, z in steps))
    else:
        greet(device(gx=1), device(gx=-1), device(gy=1), device(gy=-1), *(device(gx=x, gz=z) for x, z in steps))
        greet(*(device(gx=x, gy=y, gz=z) for x, z in steps for y in (1, -1)))
    own_rows = pl.ds(0, ny)
    loads = [
        pltpu.make_async_copy(src, dst, load.at[i])
        for src, dst, i in (
            (rhs_hbm, e.at[pl.ds(0, 3), pl.ds(first, nx), own_rows], 0), (reg_hbm, reg_ref, 0),
            (frac_hbm, frac_ref, 0), (flag_hbm, flag_ref, 0), (cond_hbm, cond, 1),
        )
    ]

    def tiles_of(count):
        return blank.at[pl.ds(0, count)]

    def wait_tiles(semaphore, count):
        pltpu.make_async_copy(tiles_of(count), tiles_of(count), semaphore).wait()

    with scope("load"):
        for one in loads:
            one.start()
        loads[4].wait()
        wait_tiles(load.at[0], 10 * nx * ny // 8)

    sent_tiles = []

    def copy(group, src, dst, where, start=True):
        made = pltpu.make_async_remote_copy(
            src_ref=src, dst_ref=dst, send_sem=send.at[0], recv_sem=recv.at[group],
            device_id=where, device_id_type=MESH,
        )
        sent_tiles.append(math.prod(src.shape) // (8 * nz))
        if start:
            made.start()
        return made

    def arrived(group, count):
        wait_tiles(recv.at[group], count)

    row = lax.broadcasted_iota(jnp.int32, (8, nz), 0)
    top, bottom, halo = slice(0, 8), slice(ny - 8, ny), slice(ny, ny + 8)

    def y_start(group, places, out, into):
        for i, (ref, where) in enumerate(places):
            out[i] = jnp.where(row < 4, ref[(*where, top, slice(None))], ref[(*where, bottom, slice(None))])
        if gy == 2:
            copy(group, out, into.at[0], device(gy=1))
        else:
            copy(group, out, into.at[0], device(gy=-1))
            copy(group, out, into.at[1], device(gy=1))

    def y_finish(group, places, into):
        arrived(group, into.shape[0] * len(places))
        for i, (ref, where) in enumerate(places):
            tile = into[0, i] if gy == 2 else jnp.where(row < 4, into[0, i], into[1, i])
            ref[(*where, halo, slice(None))] = tile

    lane = lax.broadcasted_iota(jnp.int32, (ny, nz), 1)
    slot = lane // SEG
    half = nz // 2
    low_half = lane < half
    quad = (lane % SEG) // 4
    left = (lane % SEG) < 8

    def end_piece(v, j):
        return rot(v, 8 + SEG * j, 1)

    def pick(base, where, other):
        return other if base is None else jnp.where(where, other, base)

    packs = [None] * 6
    with scope("pack"):
        for x in range(nx):
            region = reg_ref[x]
            sigma = jnp.zeros((ny, nz), jnp.float32)
            for number in range(cond.shape[0]):
                sigma = jnp.where(region == number, cond[number], sigma)
            for k in range(3):
                ks = jnp.where(flag_ref[k, x] == 0, sigma * frac_ref[k, x], 0.0)
                e[3 + k, first + x, 0:ny, :] = ks
                for f, v in ((k, e[k, first + x, 0:ny, :]), (3 + k, ks)):
                    packs[f] = pick(packs[f], slot == x, end_piece(v, x))
        for side, off in ((0, 8), (1, 4)):
            tiles = [None, None]
            for f in range(6):
                tiles[f // 4] = pick(tiles[f // 4], quad == f % 4, rot(packs[f], 4 * (f % 4) - off, 1))
            for i in range(2):
                zs[side, i] = tiles[i]
                zx_out[side, i] = jnp.where(row < 4, tiles[i][0:8], tiles[i][ny - 8:ny])
            other = rot(tiles[1], half, 1)
            ds[0, side] = jnp.where(low_half, other, tiles[0])
            ds[1, side] = jnp.where(low_half, tiles[0], other)
            for i in range(2):
                tile = jnp.where(low_half == (i == 0), other, tiles[0])
                dx_out[i, side] = jnp.where(row < 4, tile[0:8], tile[ny - 8:ny])
        starts = [jacobi_scale(packs[3 + k]) * packs[k] for k in range(3)]
        moves = (
            [(packs[f], 0, 8 * (f // 2) + 3 * (f % 2), 3) for f in range(6)] + [(starts[k], 3, 5 + k, 1) for k in (1, 2)],
            [(packs[f], nx - 2, 2 * f, 2) for f in range(6)] + [(starts[k], nx - 3, 12 + k, 1) for k in range(3)],
        )
        for side in range(2):
            tiles = [None, None, None]
            for v, at, to, wide in moves[side]:
                t, to = divmod(to, 8)
                tiles[t] = pick(tiles[t], (slot >= to) & (slot < to + wide), rot(v, SEG * (to - at), 1))
            for i in range(3 - side):
                ends_out[3 * side + i] = tiles[i]

    with scope("barrierwait"):
        if paired:
            @pl.when(pos["gy"] == 1)
            def _():
                pl.semaphore_wait(barrier, 5)
                pl.semaphore_signal(near.at[0], inc=1, device_id=device(gy=1), device_id_type=MESH)

            @pl.when(pos["gy"] == 0)
            def _():
                pl.semaphore_wait(near.at[0], 1)
        else:
            pl.semaphore_wait(barrier, 4 + 3 * len(steps))

    def far_wait():
        if not paired:
            return

        @pl.when(pos["gy"] == 0)
        def _():
            pl.semaphore_wait(barrier, 2 * len(steps))
            pl.semaphore_signal(near.at[1], inc=1, device_id=device(gy=1), device_id_type=MESH)

        @pl.when(pos["gy"] == 1)
        def _():
            pl.semaphore_wait(near.at[1], 1)

    own = [(e, (f, p)) for f in range(6) for p in range(first, last + 1)]
    y_start(0, own, ya_out, ya_in)

    up, down = device(gx=1), device(gx=-1)
    ends_copies = [copy(12, ends_out.at[pl.ds(0, 3)], ends_in.at[pl.ds(0, 3)], down, False), copy(12, ends_out.at[pl.ds(3, 2)], ends_in.at[pl.ds(3, 2)], up, False)]
    raw_copies = [
        copy(2, e.at[:, first, own_rows], e.at[:, last + 1, own_rows], down, False),
        copy(3, e.at[:, last, own_rows], e.at[:, first - 1, own_rows], up, False),
    ]
    late_copies = [
        copy(4, upper_out.at[pl.ds(0, 4)], upper_in.at[pl.ds(0, 4)], down, False),
        copy(5, lower_out.at[:, own_rows], lower_in.at[:, own_rows], up, False),
    ]
    wide_copy = pltpu.make_async_remote_copy(
        src_ref=lower_out, dst_ref=lower_in, send_sem=send.at[0], recv_sem=recv.at[5],
        device_id=up, device_id_type=MESH,
    )
    thin_copies = [
        pltpu.make_async_remote_copy(
            src_ref=src, dst_ref=dst, send_sem=send.at[0], recv_sem=recv.at[4], device_id=down, device_id_type=MESH
        )
        for src, dst in (
            (upper_out.at[pl.ds(0, 4), own_rows], upper_in.at[pl.ds(0, 4), own_rows]),
            (e.at[4, first + 1, own_rows], e.at[4, last + 2, own_rows]),
        )
    ]
    last_copy = copy(9, upper_out.at[pl.ds(4, 2), own_rows], upper_in.at[pl.ds(4, 2), own_rows], down, False)
    mask_copies = [
        copy(4, e.at[4, first + 1], e.at[4, last + 2], down, False),
        copy(4, e.at[5, first + 1, own_rows], e.at[5, last + 2, own_rows], down, False),
    ]
    z_copies = [copy(10 - 9 * i, zs.at[i], zr.at[i], device(gz=2 * i - 1), False) for i in range(2)]
    corner_copies = [
        copy(10 - 9 * zside, ds.at[side, zside], dr.at[side, zside], device(gx=1 - 2 * side, gz=2 * zside - 1), False)
        for side in range(2) for zside in range(2)
    ]
    cross_copies = [
        [
            copy(10 - 9 * zside, dx_out.at[side, zside], dx_in.at[i, side, zside], device(gx=1 - 2 * side, gy=2 * i - 1, gz=2 * zside - 1), False)
            for side in range(2) for i in range(1 if paired else 2)
        ] + [
            copy(10 - 9 * zside, zx_out.at[zside], zx_in.at[i, zside], device(gy=2 * i - 1, gz=2 * zside - 1), False)
            for i in range(1 if paired else 2)
        ]
        for zside in range(2)
    ]

    def start(*copies):
        for one in copies:
            one.start()

    def start_far(zside):
        start(corner_copies[zside], corner_copies[2 + zside], z_copies[zside])

    def start_both():
        for zside in (1, 0):
            start_far(zside)
            start(*cross_copies[zside])

    down_first = (lax.rem(pos["gx"], 4) == 1) & (pos["gz"] == 0)
    wide = (lax.rem(device(gx=-1)["gx"], 4) == 1) & (pos["gz"] == 0)
    narrow = jnp.logical_not(wide)
    thin = (lax.rem(device(gx=1)["gx"], 4) == 1) & (pos["gz"] == 0)

    def in_order(begin):
        pl.when(down_first)(lambda: begin(0, 1))
        pl.when(jnp.logical_not(down_first))(lambda: begin(1, 0))

    late_start = pos["gz"] == 0
    in_order(lambda a, b: start(ends_copies[a], ends_copies[b]))

    up_only = lax.rem(pos["gx"], 4) == 3
    pl.when(jnp.logical_not(up_only))(lambda: start(raw_copies[0]))
    pl.when(jnp.logical_not(down_first))(lambda: start(raw_copies[1]))

    @pl.when(jnp.logical_not(late_start))
    def _():
        with scope("nearwait"):
            far_wait()
            start_both()


    def faces(u, p):
        v0, v1, v2 = u[0, p], u[1, p], u[2, p]
        return face_one(v0, v2, u[2, p + 1]), face_two(v0, v1, u[1, p + 1])

    def curl_sweep(u, before, lo, hi, emit, after=None):
        f1m, f2m = before
        for p in range(lo, hi):
            f1, f2 = faces(u, p) if after is None or p < hi - 1 else after
            f0 = face_zero(u[1, p], u[2, p])
            cc = edges(f0, f1, f2, f1m, f2m)
            for k in range(3):
                emit(k, p, cc[k])
            f1m, f2m = f1, f2

    def emit_second(k, p, cc):
        u2[k, p] = next_iter(e[k, p], e[3 + k, p], jac[k, p], u1[k, p], cc)

    def emit_masked(k, p, cc):
        mm[k, p] = masked_residual(e[k, p], e[3 + k, p], u2[k, p], cc)

    def emit_rest(k, p, cc):
        if k > 0 or p != first + 1:
            emit_masked(k, p, cc)

    def node_range(lo, hi):
        for p in range(lo, hi):
            r = nodal_rhs(mm[0, p], mm[0, p - 1], mm[1, p], mm[2, p])
            for q in range(4):
                rr[q, p] = r[q]

    def first_range(lo, hi):
        for p in range(lo, hi):
            for k in range(3):
                scale = jacobi_scale(e[3 + k, p])
                jac[k, p] = scale
                u1[k, p] = scale * e[k, p]

    def below(v, p):
        up0 = v[0, p]
        return (z_up(up0) - up0) + v[2, p], v[1, p] + (y_up(up0) - up0)

    with scope("y1"):
        y_finish(0, own, ya_in)
    with scope("inner"):
        first_range(first, last + 1)
        curl_sweep(u1, faces(u1, first), first + 1, last, emit_second)
        p = last - 1
        sent = (*below(u1, p), e[3, p], *below(u2, p), e[0, p] - e[3, p] * u2[0, p])
        for i, v in enumerate(sent):
            lower_out[i] = v
        p = first + 1
        f1, f2 = faces(u2, p)
        cc = edges(face_zero(u2[1, p], u2[2, p]), f1, f2, -u2[2, p], u2[1, p])
        m0, m1, m2 = [masked_residual(e[k, p], e[3 + k, p], u2[k, p], cc[k]) for k in range(3)]
        mm[0, p] = m0
        sent = (u1[1, p], u1[2, p], u2[1, p], u2[2, p], m0, (y_down(m1) - m1) + (z_down(m2) - m2))
        for i, v in enumerate(sent):
            upper_out[i] = v
    @pl.when(down_first)
    def _():
        start(mask_copies[1], *thin_copies, last_copy, raw_copies[1], wide_copy)

    @pl.when(up_only)
    def _():
        start(late_copies[1], raw_copies[0], *mask_copies, late_copies[0], last_copy)

    @pl.when(jnp.logical_not(down_first | up_only))
    def _():
        start(late_copies[1], *mask_copies, late_copies[0], last_copy)

    with scope("inner2"):
        curl_sweep(u2, faces(u2, first + 1), first + 2, last - 1, emit_masked)
        node_range(first + 2, last - 1)

    @pl.when(late_start)
    def _():
        with scope("nearwait"):
            far_wait()
            start_both()

    def relay(name, groups, relayed, places, out, into):
        with scope(name):
            for group, count in groups:
                arrived(group, count * ny // 8)
            y_start(relayed, places, out, into)

    raw_up = [(e, (f, last + 1)) for f in range(6)]
    raw_low = [(e, (f, first - 1)) for f in range(6)]
    late_low = [(lower_in, (i,)) for i in range(6)]
    strip_tiles = [(st, (f, t)) for f in range(6) for t in range(4)]

    inner = (lane >= 4) & (lane < nz - 4)

    def node_at(p, count=4):
        return [nodal_step(rr[q, p], rr[q, p - 1], rr[q, p + 1]) for q in range(count)]

    def outputs(lo, hi):
        s_next = node_at(lo)
        for p in range(lo, hi):
            s = s_next
            s_next = node_at(p + 1, 4 if p + 1 < hi else 2)
            corr = (
                (s_next[0] - s[0]) + (s[1] + s_next[1]) * 0.5,
                (y_up(s[0]) - s[0]) + (s[2] + y_up(s[2])) * 0.5,
                (z_up(s[0]) - s[0]) + (s[3] + z_up(s[3])) * 0.5,
            )
            for k in range(3):
                body = finish(e[k, p, 0:ny], e[3 + k, p, 0:ny], u2[k, p, 0:ny], corr[k][0:ny])
                ends = rot(sw[k], nz - 8 - SEG * (p - first), 1)
                out_ref[k, p - first] = jnp.where(inner, body, ends)

    lane24 = lax.broadcasted_iota(jnp.int32, (ny + 8, nz), 1)
    slot24 = lane24 // SEG
    left24 = (lane24 % SEG) < 8

    span = range(2)

    def x_up(vs):
        rs = [rot(v, -SEG, 1) for v in vs]
        return [jnp.where(lane24 < nz - SEG, rs[t], rs[t ^ 1]) for t in span]

    def x_down(vs):
        rs = [rot(v, SEG, 1) for v in vs]
        return [jnp.where(lane24 >= SEG, rs[t], rs[t ^ 1]) for t in span]

    def strip_curl(u):
        u1p, u2p = x_up(u[1]), x_up(u[2])
        f1 = [face_one(u[0][t], u[2][t], u2p[t]) for t in span]
        f2 = [face_two(u[0][t], u[1][t], u1p[t]) for t in span]
        f0 = [face_zero(u[1][t], u[2][t]) for t in span]
        f1m, f2m = x_down(f1), x_down(f2)
        out = [edges(f0[t], f1[t], f2[t], f1m[t], f2m[t]) for t in span]
        return [[out[t][k] for t in span] for k in range(3)]

    def strips(base):
        sr = [[st[k, 2 * base + t] for t in span] for k in range(3)]
        sk = [[st[3 + k, 2 * base + t] for t in span] for k in range(3)]
        outer = (slot24 == 3) | (slot24 == nx - 3)
        scale = [[jacobi_scale(sk[k][t]) for t in span] for k in range(3)]
        u = [[scale[k][t] * sr[k][t] for t in span] for k in range(3)]
        for k in range(3):
            u[k][1] = jnp.where(outer & (left24 if base == 0 else ~left24), sr[k][1], u[k][1])
        cc = strip_curl(u)
        u = [[next_iter(sr[k][t], sk[k][t], scale[k][t], u[k][t], cc[k][t]) for t in span] for k in range(3)]
        cc = strip_curl(u)
        m = [[masked_residual(sr[k][t], sk[k][t], u[k][t], cc[k][t]) for t in span] for k in range(3)]
        m0m = x_down(m[0])
        r = [nodal_rhs(m[0][t], m0m[t], m[1][t], m[2][t]) for t in span]
        s = []
        for q in range(4):
            rq = [r[t][q] for t in span]
            rm, rp = x_down(rq), x_up(rq)
            s.append([nodal_step(rq[t], rm[t], rp[t]) if q < 2 or t % 2 == 0 else None for t in span])
        s0p, s1p = x_up(s[0]), x_up(s[1])
        s0, s1, s2, s3 = [s[q][0] for q in range(4)]
        corr = (
            (s0p[0] - s0) + (s1 + s1p[0]) * 0.5,
            (y_up(s0) - s0) + (s2 + y_up(s2)) * 0.5,
            (z_up(s0) - s0) + (s3 + z_up(s3)) * 0.5,
        )
        for k in range(3):
            result = finish(sr[k][0], sk[k][0], u[k][0], corr[k])[0:ny]
            sw[k] = result if base == 0 else jnp.where(left, sw[k], result)

    def corner_of(f, plus, minus, off):
        low = low_half[0:plus.shape[0]]
        if f < 4:
            return rot(jnp.where(low, plus, minus), off - 4 * f, 1)
        return rot(jnp.where(low, minus, plus), half + off - 4 * (f - 4), 1)

    with scope("endswait"):
        arrived(12, 5 * ny // 8)
    with scope("strippack"):
        for f in range(6):
            t, to = divmod(2 * f, 8)
            piece = rot(ends_in[f // 2], SEG * (0 - 3 * (f % 2)), 1)
            piece = jnp.where(slot >= nx - 2, rot(ends_in[3 + t], SEG * (nx - 2 - to), 1), piece)
            if f < 3:
                piece = jnp.where(slot == 3, rot(ends_in[0], SEG * (3 - (5 + f)), 1), piece)
                piece = jnp.where(slot == nx - 3, rot(ends_in[4], SEG * (nx - 3 - (4 + f)), 1), piece)
            mid = packs[f]
            st[f, 0, 0:ny, :] = mid
            st[f, 1, 0:ny, :] = piece
            st[f, 2, 0:ny, :] = mid
            st[f, 3, 0:ny, :] = piece
        y_start(8, strip_tiles, yd_out, yd_in)


    def crossed(ref, *where):
        if paired:
            return ref[(0, *where)]
        return jnp.where(row < 4, ref[(0, *where)], ref[(1, *where)])

    def strip_inputs(base):
        with scope("ystrip"):
            if base == 0:
                y_finish(8, strip_tiles, yd_in)
            arrived(10 - 9 * base, 4 * (ny // 8 + dx_in.shape[0]))
            off = 8 - 4 * base
            for f in range(6):
                t, q = divmod(f, 4)
                for rows, tile, corners in (
                    (slice(0, ny), zr[base, t], [dr[i, base] for i in range(2)]),
                    (halo, crossed(zx_in, base, t), [crossed(dx_in, i, base) for i in range(2)]),
                ):
                    mine = left[0:tile.shape[0]] if base == 0 else ~left[0:tile.shape[0]]
                    for at, piece in ((2 * base, rot(tile, off - 4 * q, 1)), (2 * base + 1, corner_of(f, corners[1], corners[0], off))):
                        st[f, at, rows, :] = jnp.where(mine, st[f, at, rows, :], piece)

    late_up = [(upper_in, (i,)) for i in range(4)] + [(e, (4, last + 2))]

    def lower_inputs():
        with scope("ylow"):
            y_finish(7, raw_low, yc_in)
            pl.when(narrow)(lambda: y_finish(11, late_low, ye_in))
            pl.when(wide)(lambda: arrived(5, 6 * (ny + 8) // 8))

    def upper_inputs():
        with scope("yup"):
            y_finish(6, raw_up, yb_in)
            pl.when(jnp.logical_not(thin))(lambda: arrived(4, (5 * (ny + 8) + ny) // 8))
            pl.when(thin)(lambda: y_finish(0, late_up, yf_in))
            arrived(9, 2 * ny // 8)

    def lower_side():
        with scope("lower"):
            p = first - 1
            first_range(p, p + 1)
            curl_sweep(u1, (lower_in[0] - u1[2, p], u1[1, p] - lower_in[1]), p, first + 1, emit_second)
            f1, f2 = lower_in[3] - u2[2, p], u2[1, p] - lower_in[4]
            cc = (z_down(f1) - f1) - (y_down(f2) - f2)
            mm[0, p - 1] = jnp.where(lower_in[2] > 0.0, lower_in[5] - cc, 0.0)
            curl_sweep(u2, (f1, f2), p, first + 2, emit_rest)
            node_range(p, first + 2)

    def upper_side():
        with scope("upper"):
            p = last + 1
            first_range(p, p + 1)
            f1 = face_one(u1[0, p], u1[2, p], upper_in[1])
            f2 = face_two(u1[0, p], u1[1, p], upper_in[0])
            curl_sweep(u1, faces(u1, last - 1), last, p + 1, emit_second, (f1, f2))
            f1 = face_one(u2[0, p], u2[2, p], upper_in[3])
            f2 = face_two(u2[0, p], u2[1, p], upper_in[2])
            curl_sweep(u2, faces(u2, last - 2), last - 1, p + 1, emit_masked, (f1, f2))
            node_range(last - 1, p + 1)
            v0 = u2[0, p]
            q2 = jnp.where(e[4, p + 1] > 0.0, u2[1, p] + (y_up(v0) - v0), 0.0)
            q1 = jnp.where(e[5, p + 1] > 0.0, (z_up(v0) - v0) + u2[2, p], 0.0)
            m0, m0p = mm[0, p], upper_in[4]
            rr[0, p + 1] = (m0 - m0p) + (upper_in[5] + (y_down(q2) - q2) + (z_down(q1) - q1))
            rr[1, p + 1] = (m0p + m0) * 0.5

    def in_turn(*pieces):
        for piece in pieces:
            piece()

    def write_all():
        with scope("out"):
            outputs(first, last + 1)

    def side_strips(base):
        strip_inputs(base)
        with scope("strips"):
            strips(base)

    side_strips(0)
    relay("rawup", ((2, 6),), 6, raw_up, yb_out, yb_in)
    relay("rawlow", ((3, 6),), 7, raw_low, yc_out, yc_in)

    @pl.when(narrow)
    def _():
        relay("latelow", ((5, 6),), 11, late_low, ye_out, ye_in)

    @pl.when(thin)
    def _():
        relay("lateup", ((4, 6),), 0, late_up, yf_out, yf_in)

    side_strips(1)
    in_turn(lower_inputs, upper_inputs, lower_side, upper_side, write_all)
    with scope("sendwait"):
        sides = dx_in.shape[0]
        total = sum(sent_tiles) - 5 * sides
        pl.when(down_first)(lambda: wait_tiles(send.at[0], total + 1))
        pl.when(wide)(lambda: wait_tiles(send.at[0], total - 6 * sides))
        pl.when(thin)(lambda: wait_tiles(send.at[0], total + 5 * sides))
        pl.when(jnp.logical_not(down_first | wide | thin))(lambda: wait_tiles(send.at[0], total))


def on_device(sizes, rhs, conductivity, fraction, region, flags):
    _, nx, ny, nz = rhs.shape
    planes = nx + 2 * PAD
    rows = ny + 8
    f32 = jnp.float32
    hbm = pl.BlockSpec(memory_space=pl.ANY)
    sides = 1 if sizes[1] == 2 else 2
    relays = []
    for count in (6 * nx, 6, 6, 24, 6, 5):
        relays += [pltpu.VMEM((count, 8, nz), f32), pltpu.VMEM((sides, count, 8, nz), f32)]
    return pl.pallas_call(
        functools.partial(kernel, sizes, nx, ny, nz),
        out_shape=pltpu.VMEM(rhs.shape, rhs.dtype),
        in_specs=[hbm] * 5,
        out_specs=pl.BlockSpec(memory_space=pltpu.VMEM),
        scratch_shapes=[
            pltpu.SMEM(conductivity.shape, f32),
            pltpu.VMEM(rhs.shape, f32),
            pltpu.VMEM(region.shape, jnp.int32),
            pltpu.VMEM(flags.shape, jnp.int32),
            pltpu.VMEM((6, planes, rows, nz), f32),
            pltpu.VMEM((6, 4, rows, nz), f32),
            pltpu.VMEM((3, ny, nz), f32),
            pltpu.VMEM((3, planes, rows, nz), f32),
            pltpu.VMEM((3, planes, rows, nz), f32),
            pltpu.VMEM((3, planes, rows, nz), f32),
            pltpu.VMEM((3, planes, rows, nz), f32),
            pltpu.VMEM((4, planes, rows, nz), f32),
            pltpu.VMEM((2, 2, ny, nz), f32),
            pltpu.VMEM((2, 2, ny, nz), f32),
            pltpu.VMEM((2, 2, ny, nz), f32),
            pltpu.VMEM((2, 2, ny, nz), f32),
            pltpu.VMEM((2, 2, 8, nz), f32),
            pltpu.VMEM((sides, 2, 2, 8, nz), f32),
            pltpu.VMEM((2, 2, 8, nz), f32),
            pltpu.VMEM((sides, 2, 2, 8, nz), f32),
            pltpu.VMEM((5, ny, nz), f32),
            pltpu.VMEM((5, ny, nz), f32),
            pltpu.VMEM((6, rows, nz), f32),
            pltpu.VMEM((6, rows, nz), f32),
            pltpu.VMEM((6, rows, nz), f32),
            pltpu.VMEM((6, rows, nz), f32),
            *relays,
            pltpu.VMEM((320, 8, nz), f32),
            pltpu.SemaphoreType.DMA((2,)),
            pltpu.SemaphoreType.DMA((1,)),
            pltpu.SemaphoreType.DMA((13,)),
            pltpu.SemaphoreType.REGULAR((2,)),
        ],
        compiler_params=pltpu.CompilerParams(
            collective_id=0, has_side_effects=True, vmem_limit_bytes=60 * 1024 * 1024
        ),
    )(conductivity, rhs, fraction, region, flags)


def solution(mesh):
    sizes = tuple(mesh.shape[name] for name in ("gx", "gy", "gz"))
    return jax.shard_map(
        functools.partial(on_device, sizes),
        mesh=mesh,
        in_specs=(
            P(None, "gx", "gy", "gz"),
            P(),
            P(None, "gx", "gy", "gz"),
            P("gx", "gy", "gz"),
            P(None, "gx", "gy", "gz"),
        ),
        out_specs=P(None, "gx", "gy", "gz"),
        check_vma=False,
    )
```

```python
import functools
import math

import jax
import jax.numpy as jnp
from jax import lax
from jax.experimental import pallas as pl
from jax.experimental.pallas import tpu as pltpu
from jax.sharding import PartitionSpec as P

damping = 0.8
c_node = 0.8 / 7.0
MESH = pl.DeviceIdType.MESH
PAD = 2
SEG = 16


def rot(v, shift, axis):
    return pltpu.roll(v, shift % v.shape[axis], axis)


def y_up(v):
    return rot(v, -1, 0)


def y_down(v):
    return rot(v, 1, 0)


def z_up(v):
    return rot(v, -1, 1)


def z_down(v):
    return rot(v, 1, 1)


def face_zero(u1, u2):
    return (y_up(u2) - u2) - (z_up(u1) - u1)


def face_one(u0, u2, u2p):
    return (z_up(u0) - u0) - (u2p - u2)


def face_two(u0, u1, u1p):
    return (u1p - u1) - (y_up(u0) - u0)


def edges(f0, f1, f2, f1m, f2m):
    return (
        (z_down(f1) - f1) - (y_down(f2) - f2),
        (f2m - f2) - (z_down(f0) - f0),
        (y_down(f0) - f0) - (f1m - f1),
    )


def jacobi_scale(ks):
    return jnp.where(ks > 0.0, damping / (4.0 + ks), 0.0)


def next_iter(rhs, ks, scale, u, cc):
    return u + scale * (rhs - (cc + ks * u))


def masked_residual(rhs, ks, u, cc):
    return jnp.where(ks > 0.0, rhs - (cc + ks * u), 0.0)


def nodal_rhs(m0, m0m, m1, m2):
    m1m, m2m = y_down(m1), z_down(m2)
    return (
        (m0m - m0) + (m1m - m1) + (m2m - m2),
        (m0 + m0m) * 0.5,
        (m1 + m1m) * 0.5,
        (m2 + m2m) * 0.5,
    )


def nodal_step(r, rm, rp):
    around = (rm + rp) + (y_up(r) + y_down(r)) + (z_up(r) + z_down(r))
    return (1.2 * c_node) * r + (c_node * c_node) * around


def finish(rhs, ks, u, corr):
    fixed = damping * rhs
    fixed = fixed + damping * (rhs - fixed)
    return jnp.where(ks > 0.0, u + corr, fixed)


def kernel(
    sizes, nx, ny, nz, cond_hbm, rhs_hbm, frac_hbm, reg_hbm, flag_hbm, out_ref,
    cond, frac_ref, reg_ref, flag_ref,
    e, st, sw, jac, u1, u2, mm, rr, zs, zr, ds, dr, dx_out, dx_in, zx_out, zx_in, ends_out, ends_in, lower_out, lower_in, upper_out, upper_in,
    ya_out, ya_in, yb_out, yb_in, yc_out, yc_in, yd_out, yd_in, ye_out, ye_in, yf_out, yf_in,
    blank, load, send, recv, near,
):
    gx, gy, gz = sizes
    pos = {"gx": lax.axis_index("gx"), "gy": lax.axis_index("gy"), "gz": lax.axis_index("gz")}
    size = {"gx": gx, "gy": gy, "gz": gz}
    first, last = PAD, PAD + nx - 1
    scope = jax.named_scope

    def device(**steps):
        return {axis: lax.rem(pos[axis] + (step + size[axis]), size[axis]) for axis, step in steps.items()}

    steps = [(x, z) for z in (1, -1) for x in (0, 1, -1)]
    paired = gy == 2
    barrier = pltpu.get_barrier_semaphore()

    def greet(*devices):
        for one in devices:
            pl.semaphore_signal(barrier, inc=1, device_id=one, device_id_type=MESH)

    def on(core, **steps):
        return {**device(**steps), "gy": core}

    if paired:
        greet(on(1, gx=1), on(1, gx=-1))
        pl.when(pos["gy"] == 0)(lambda: greet(device(gy=1)))
        greet(*(on(0, gx=x, gz=z) for x, z in steps))
    else:
        greet(device(gx=1), device(gx=-1), device(gy=1), device(gy=-1), *(device(gx=x, gz=z) for x, z in steps))
        greet(*(device(gx=x, gy=y, gz=z) for x, z in steps for y in (1, -1)))
    own_rows = pl.ds(0, ny)
    loads = [
        pltpu.make_async_copy(src, dst, load.at[i])
        for src, dst, i in (
            (rhs_hbm, e.at[pl.ds(0, 3), pl.ds(first, nx), own_rows], 0), (reg_hbm, reg_ref, 0),
            (frac_hbm, frac_ref, 0), (flag_hbm, flag_ref, 0), (cond_hbm, cond, 1),
        )
    ]

    def tiles_of(count):
        return blank.at[pl.ds(0, count)]

    def wait_tiles(semaphore, count):
        pltpu.make_async_copy(tiles_of(count), tiles_of(count), semaphore).wait()

    with scope("load"):
        for one in loads:
            one.start()
        loads[4].wait()
        wait_tiles(load.at[0], 10 * nx * ny // 8)

    sent_tiles = []

    def copy(group, src, dst, where, start=True):
        made = pltpu.make_async_remote_copy(
            src_ref=src, dst_ref=dst, send_sem=send.at[0], recv_sem=recv.at[group],
            device_id=where, device_id_type=MESH,
        )
        sent_tiles.append(math.prod(src.shape) // (8 * nz))
        if start:
            made.start()
        return made

    def arrived(group, count):
        wait_tiles(recv.at[group], count)

    row = lax.broadcasted_iota(jnp.int32, (8, nz), 0)
    top, bottom, halo = slice(0, 8), slice(ny - 8, ny), slice(ny, ny + 8)

    def y_start(group, places, out, into):
        for i, (ref, where) in enumerate(places):
            out[i] = jnp.where(row < 4, ref[(*where, top, slice(None))], ref[(*where, bottom, slice(None))])
        if gy == 2:
            copy(group, out, into.at[0], device(gy=1))
        else:
            copy(group, out, into.at[0], device(gy=-1))
            copy(group, out, into.at[1], device(gy=1))

    def y_finish(group, places, into):
        arrived(group, into.shape[0] * len(places))
        for i, (ref, where) in enumerate(places):
            tile = into[0, i] if gy == 2 else jnp.where(row < 4, into[0, i], into[1, i])
            ref[(*where, halo, slice(None))] = tile

    lane = lax.broadcasted_iota(jnp.int32, (ny, nz), 1)
    slot = lane // SEG
    half = nz // 2
    low_half = lane < half
    quad = (lane % SEG) // 4
    left = (lane % SEG) < 8

    def end_piece(v, j):
        return rot(v, 8 + SEG * j, 1)

    def pick(base, where, other):
        return other if base is None else jnp.where(where, other, base)

    packs = [None] * 6
    with scope("pack"):
        for x in range(nx):
            region = reg_ref[x]
            sigma = jnp.zeros((ny, nz), jnp.float32)
            for number in range(cond.shape[0]):
                sigma = jnp.where(region == number, cond[number], sigma)
            for k in range(3):
                ks = jnp.where(flag_ref[k, x] == 0, sigma * frac_ref[k, x], 0.0)
                e[3 + k, first + x, 0:ny, :] = ks
                for f, v in ((k, e[k, first + x, 0:ny, :]), (3 + k, ks)):
                    packs[f] = pick(packs[f], slot == x, end_piece(v, x))
        for side, off in ((0, 8), (1, 4)):
            tiles = [None, None]
            for f in range(6):
                tiles[f // 4] = pick(tiles[f // 4], quad == f % 4, rot(packs[f], 4 * (f % 4) - off, 1))
            for i in range(2):
                zs[side, i] = tiles[i]
                zx_out[side, i] = jnp.where(row < 4, tiles[i][0:8], tiles[i][ny - 8:ny])
            other = rot(tiles[1], half, 1)
            ds[0, side] = jnp.where(low_half, other, tiles[0])
            ds[1, side] = jnp.where(low_half, tiles[0], other)
            for i in range(2):
                tile = jnp.where(low_half == (i == 0), other, tiles[0])
                dx_out[i, side] = jnp.where(row < 4, tile[0:8], tile[ny - 8:ny])
        starts = [jacobi_scale(packs[3 + k]) * packs[k] for k in range(3)]
        moves = (
            [(packs[f], 0, 8 * (f // 2) + 3 * (f % 2), 3) for f in range(6)] + [(starts[k], 3, 5 + k, 1) for k in (1, 2)],
            [(packs[f], nx - 2, 2 * f, 2) for f in range(6)] + [(starts[k], nx - 3, 12 + k, 1) for k in range(3)],
        )
        for side in range(2):
            tiles = [None, None, None]
            for v, at, to, wide in moves[side]:
                t, to = divmod(to, 8)
                tiles[t] = pick(tiles[t], (slot >= to) & (slot < to + wide), rot(v, SEG * (to - at), 1))
            for i in range(3 - side):
                ends_out[3 * side + i] = tiles[i]

    with scope("barrierwait"):
        if paired:
            @pl.when(pos["gy"] == 1)
            def _():
                pl.semaphore_wait(barrier, 5)
                pl.semaphore_signal(near.at[0], inc=1, device_id=device(gy=1), device_id_type=MESH)

            @pl.when(pos["gy"] == 0)
            def _():
                pl.semaphore_wait(near.at[0], 1)
        else:
            pl.semaphore_wait(barrier, 4 + 3 * len(steps))

    def far_wait():
        if not paired:
            return

        @pl.when(pos["gy"] == 0)
        def _():
            pl.semaphore_wait(barrier, 2 * len(steps))
            pl.semaphore_signal(near.at[1], inc=1, device_id=device(gy=1), device_id_type=MESH)

        @pl.when(pos["gy"] == 1)
        def _():
            pl.semaphore_wait(near.at[1], 1)

    own = [(e, (f, p)) for f in range(6) for p in range(first, last + 1)]
    y_start(0, own, ya_out, ya_in)

    up, down = device(gx=1), device(gx=-1)
    ends_copies = [copy(12, ends_out.at[pl.ds(0, 3)], ends_in.at[pl.ds(0, 3)], down, False), copy(12, ends_out.at[pl.ds(3, 2)], ends_in.at[pl.ds(3, 2)], up, False)]
    raw_copies = [
        copy(2, e.at[:, first, own_rows], e.at[:, last + 1, own_rows], down, False),
        copy(3, e.at[:, last, own_rows], e.at[:, first - 1, own_rows], up, False),
    ]
    late_copies = [
        copy(4, upper_out.at[pl.ds(0, 4)], upper_in.at[pl.ds(0, 4)], down, False),
        copy(5, lower_out.at[:, own_rows], lower_in.at[:, own_rows], up, False),
    ]
    wide_copy = pltpu.make_async_remote_copy(
        src_ref=lower_out, dst_ref=lower_in, send_sem=send.at[0], recv_sem=recv.at[5],
        device_id=up, device_id_type=MESH,
    )
    thin_copies = [
        pltpu.make_async_remote_copy(
            src_ref=src, dst_ref=dst, send_sem=send.at[0], recv_sem=recv.at[4], device_id=down, device_id_type=MESH
        )
        for src, dst in (
            (upper_out.at[pl.ds(0, 4), own_rows], upper_in.at[pl.ds(0, 4), own_rows]),
            (e.at[4, first + 1, own_rows], e.at[4, last + 2, own_rows]),
        )
    ]
    last_copy = copy(9, upper_out.at[pl.ds(4, 2), own_rows], upper_in.at[pl.ds(4, 2), own_rows], down, False)
    mask_copies = [
        copy(4, e.at[4, first + 1], e.at[4, last + 2], down, False),
        copy(4, e.at[5, first + 1, own_rows], e.at[5, last + 2, own_rows], down, False),
    ]
    z_copies = [copy(10 - 9 * i, zs.at[i], zr.at[i], device(gz=2 * i - 1), False) for i in range(2)]
    corner_copies = [
        copy(10 - 9 * zside, ds.at[side, zside], dr.at[side, zside], device(gx=1 - 2 * side, gz=2 * zside - 1), False)
        for side in range(2) for zside in range(2)
    ]
    cross_copies = [
        [
            copy(10 - 9 * zside, dx_out.at[side, zside], dx_in.at[i, side, zside], device(gx=1 - 2 * side, gy=2 * i - 1, gz=2 * zside - 1), False)
            for side in range(2) for i in range(1 if paired else 2)
        ] + [
            copy(10 - 9 * zside, zx_out.at[zside], zx_in.at[i, zside], device(gy=2 * i - 1, gz=2 * zside - 1), False)
            for i in range(1 if paired else 2)
        ]
        for zside in range(2)
    ]

    def start(*copies):
        for one in copies:
            one.start()

    def start_far(zside):
        start(corner_copies[zside], corner_copies[2 + zside], z_copies[zside])

    def start_both():
        for zside in (1, 0):
            start_far(zside)
            start(*cross_copies[zside])

    down_first = (lax.rem(pos["gx"], 4) == 1) & (pos["gz"] == 0)
    wide = (lax.rem(device(gx=-1)["gx"], 4) == 1) & (pos["gz"] == 0)
    narrow = jnp.logical_not(wide)
    thin = (lax.rem(device(gx=1)["gx"], 4) == 1) & (pos["gz"] == 0)

    def in_order(begin):
        pl.when(down_first)(lambda: begin(0, 1))
        pl.when(jnp.logical_not(down_first))(lambda: begin(1, 0))

    late_start = pos["gz"] == 0
    in_order(lambda a, b: start(ends_copies[a], ends_copies[b]))

    up_only = lax.rem(pos["gx"], 4) == 3
    pl.when(jnp.logical_not(up_only))(lambda: start(raw_copies[0]))
    pl.when(jnp.logical_not(down_first))(lambda: start(raw_copies[1]))

    @pl.when(jnp.logical_not(late_start))
    def _():
        with scope("nearwait"):
            far_wait()
            start_both()


    def faces(u, p):
        v0, v1, v2 = u[0, p], u[1, p], u[2, p]
        return face_one(v0, v2, u[2, p + 1]), face_two(v0, v1, u[1, p + 1])

    def curl_sweep(u, before, lo, hi, emit, after=None):
        f1m, f2m = before
        for p in range(lo, hi):
            f1, f2 = faces(u, p) if after is None or p < hi - 1 else after
            f0 = face_zero(u[1, p], u[2, p])
            cc = edges(f0, f1, f2, f1m, f2m)
            for k in range(3):
                emit(k, p, cc[k])
            f1m, f2m = f1, f2

    def emit_second(k, p, cc):
        u2[k, p] = next_iter(e[k, p], e[3 + k, p], jac[k, p], u1[k, p], cc)

    def emit_masked(k, p, cc):
        mm[k, p] = masked_residual(e[k, p], e[3 + k, p], u2[k, p], cc)

    def emit_rest(k, p, cc):
        if k > 0 or p != first + 1:
            emit_masked(k, p, cc)

    def node_range(lo, hi):
        for p in range(lo, hi):
            r = nodal_rhs(mm[0, p], mm[0, p - 1], mm[1, p], mm[2, p])
            for q in range(4):
                rr[q, p] = r[q]

    def first_range(lo, hi):
        for p in range(lo, hi):
            for k in range(3):
                scale = jacobi_scale(e[3 + k, p])
                jac[k, p] = scale
                u1[k, p] = scale * e[k, p]

    def below(v, p):
        up0 = v[0, p]
        return (z_up(up0) - up0) + v[2, p], v[1, p] + (y_up(up0) - up0)

    with scope("y1"):
        y_finish(0, own, ya_in)
    with scope("inner"):
        first_range(first, last + 1)
        curl_sweep(u1, faces(u1, first), first + 1, last, emit_second)
        p = last - 1
        sent = (*below(u1, p), e[3, p], *below(u2, p), e[0, p] - e[3, p] * u2[0, p])
        for i, v in enumerate(sent):
            lower_out[i] = v
        p = first + 1
        f1, f2 = faces(u2, p)
        cc = edges(face_zero(u2[1, p], u2[2, p]), f1, f2, -u2[2, p], u2[1, p])
        m0, m1, m2 = [masked_residual(e[k, p], e[3 + k, p], u2[k, p], cc[k]) for k in range(3)]
        mm[0, p] = m0
        sent = (u1[1, p], u1[2, p], u2[1, p], u2[2, p], m0, (y_down(m1) - m1) + (z_down(m2) - m2))
        for i, v in enumerate(sent):
            upper_out[i] = v
    @pl.when(down_first)
    def _():
        start(mask_copies[1], *thin_copies, last_copy, raw_copies[1], wide_copy)

    @pl.when(up_only)
    def _():
        start(late_copies[1], raw_copies[0], *mask_copies, late_copies[0], last_copy)

    @pl.when(jnp.logical_not(down_first | up_only))
    def _():
        start(late_copies[1], *mask_copies, late_copies[0], last_copy)

    with scope("inner2"):
        curl_sweep(u2, faces(u2, first + 1), first + 2, last - 1, emit_masked)
        node_range(first + 2, last - 1)

    @pl.when(late_start)
    def _():
        with scope("nearwait"):
            far_wait()
            start_both()

    def relay(name, groups, relayed, places, out, into):
        with scope(name):
            for group, count in groups:
                arrived(group, count * ny // 8)
            y_start(relayed, places, out, into)

    raw_up = [(e, (f, last + 1)) for f in range(6)]
    raw_low = [(e, (f, first - 1)) for f in range(6)]
    late_low = [(lower_in, (i,)) for i in range(6)]
    strip_tiles = [(st, (f, t)) for f in range(6) for t in range(4)]

    inner = (lane >= 4) & (lane < nz - 4)

    def node_at(p, count=4):
        return [nodal_step(rr[q, p], rr[q, p - 1], rr[q, p + 1]) for q in range(count)]

    def outputs(lo, hi):
        s_next = node_at(lo)
        for p in range(lo, hi):
            s = s_next
            s_next = node_at(p + 1, 4 if p + 1 < hi else 2)
            corr = (
                (s_next[0] - s[0]) + (s[1] + s_next[1]) * 0.5,
                (y_up(s[0]) - s[0]) + (s[2] + y_up(s[2])) * 0.5,
                (z_up(s[0]) - s[0]) + (s[3] + z_up(s[3])) * 0.5,
            )
            for k in range(3):
                body = finish(e[k, p, 0:ny], e[3 + k, p, 0:ny], u2[k, p, 0:ny], corr[k][0:ny])
                ends = rot(sw[k], nz - 8 - SEG * (p - first), 1)
                out_ref[k, p - first] = jnp.where(inner, body, ends)

    lane24 = lax.broadcasted_iota(jnp.int32, (ny + 8, nz), 1)
    slot24 = lane24 // SEG
    left24 = (lane24 % SEG) < 8

    span = range(2)

    def x_up(vs):
        rs = [rot(v, -SEG, 1) for v in vs]
        return [jnp.where(lane24 < nz - SEG, rs[t], rs[t ^ 1]) for t in span]

    def x_down(vs):
        rs = [rot(v, SEG, 1) for v in vs]
        return [jnp.where(lane24 >= SEG, rs[t], rs[t ^ 1]) for t in span]

    def strip_curl(u):
        u1p, u2p = x_up(u[1]), x_up(u[2])
        f1 = [face_one(u[0][t], u[2][t], u2p[t]) for t in span]
        f2 = [face_two(u[0][t], u[1][t], u1p[t]) for t in span]
        f0 = [face_zero(u[1][t], u[2][t]) for t in span]
        f1m, f2m = x_down(f1), x_down(f2)
        out = [edges(f0[t], f1[t], f2[t], f1m[t], f2m[t]) for t in span]
        return [[out[t][k] for t in span] for k in range(3)]

    def strips(base):
        sr = [[st[k, 2 * base + t] for t in span] for k in range(3)]
        sk = [[st[3 + k, 2 * base + t] for t in span] for k in range(3)]
        outer = (slot24 == 3) | (slot24 == nx - 3)
        scale = [[jacobi_scale(sk[k][t]) for t in span] for k in range(3)]
        u = [[scale[k][t] * sr[k][t] for t in span] for k in range(3)]
        for k in range(3):
            u[k][1] = jnp.where(outer & (left24 if base == 0 else ~left24), sr[k][1], u[k][1])
        cc = strip_curl(u)
        u = [[next_iter(sr[k][t], sk[k][t], scale[k][t], u[k][t], cc[k][t]) for t in span] for k in range(3)]
        cc = strip_curl(u)
        m = [[masked_residual(sr[k][t], sk[k][t], u[k][t], cc[k][t]) for t in span] for k in range(3)]
        m0m = x_down(m[0])
        r = [nodal_rhs(m[0][t], m0m[t], m[1][t], m[2][t]) for t in span]
        s = []
        for q in range(4):
            rq = [r[t][q] for t in span]
            rm, rp = x_down(rq), x_up(rq)
            s.append([nodal_step(rq[t], rm[t], rp[t]) if q < 2 or t % 2 == 0 else None for t in span])
        s0p, s1p = x_up(s[0]), x_up(s[1])
        s0, s1, s2, s3 = [s[q][0] for q in range(4)]
        corr = (
            (s0p[0] - s0) + (s1 + s1p[0]) * 0.5,
            (y_up(s0) - s0) + (s2 + y_up(s2)) * 0.5,
            (z_up(s0) - s0) + (s3 + z_up(s3)) * 0.5,
        )
        for k in range(3):
            result = finish(sr[k][0], sk[k][0], u[k][0], corr[k])[0:ny]
            sw[k] = result if base == 0 else jnp.where(left, sw[k], result)

    def corner_of(f, plus, minus, off):
        low = low_half[0:plus.shape[0]]
        if f < 4:
            return rot(jnp.where(low, plus, minus), off - 4 * f, 1)
        return rot(jnp.where(low, minus, plus), half + off - 4 * (f - 4), 1)

    with scope("endswait"):
        arrived(12, 5 * ny // 8)
    with scope("strippack"):
        for f in range(6):
            t, to = divmod(2 * f, 8)
            piece = rot(ends_in[f // 2], SEG * (0 - 3 * (f % 2)), 1)
            piece = jnp.where(slot >= nx - 2, rot(ends_in[3 + t], SEG * (nx - 2 - to), 1), piece)
            if f < 3:
                piece = jnp.where(slot == 3, rot(ends_in[0], SEG * (3 - (5 + f)), 1), piece)
                piece = jnp.where(slot == nx - 3, rot(ends_in[4], SEG * (nx - 3 - (4 + f)), 1), piece)
            mid = packs[f]
            st[f, 0, 0:ny, :] = mid
            st[f, 1, 0:ny, :] = piece
            st[f, 2, 0:ny, :] = mid
            st[f, 3, 0:ny, :] = piece
        y_start(8, strip_tiles, yd_out, yd_in)


    def crossed(ref, *where):
        if paired:
            return ref[(0, *where)]
        return jnp.where(row < 4, ref[(0, *where)], ref[(1, *where)])

    def strip_inputs(base):
        with scope("ystrip"):
            if base == 0:
                y_finish(8, strip_tiles, yd_in)
            arrived(10 - 9 * base, 4 * (ny // 8 + dx_in.shape[0]))
            off = 8 - 4 * base
            for f in range(6):
                t, q = divmod(f, 4)
                for rows, tile, corners in (
                    (slice(0, ny), zr[base, t], [dr[i, base] for i in range(2)]),
                    (halo, crossed(zx_in, base, t), [crossed(dx_in, i, base) for i in range(2)]),
                ):
                    mine = left[0:tile.shape[0]] if base == 0 else ~left[0:tile.shape[0]]
                    for at, piece in ((2 * base, rot(tile, off - 4 * q, 1)), (2 * base + 1, corner_of(f, corners[1], corners[0], off))):
                        st[f, at, rows, :] = jnp.where(mine, st[f, at, rows, :], piece)

    late_up = [(upper_in, (i,)) for i in range(4)] + [(e, (4, last + 2))]

    def lower_inputs():
        with scope("ylow"):
            pl.when(narrow)(lambda: y_finish(11, late_low, ye_in))
            pl.when(wide)(lambda: arrived(5, 6 * (ny + 8) // 8))

    def upper_inputs():
        with scope("yup"):
            pl.when(jnp.logical_not(thin))(lambda: arrived(4, (5 * (ny + 8) + ny) // 8))
            pl.when(thin)(lambda: y_finish(0, late_up, yf_in))
            arrived(9, 2 * ny // 8)

    def lower_side():
        with scope("lower"):
            p = first - 1
            curl_sweep(u1, (lower_in[0] - u1[2, p], u1[1, p] - lower_in[1]), p, first, emit_second)
            f1, f2 = lower_in[3] - u2[2, p], u2[1, p] - lower_in[4]
            cc = (z_down(f1) - f1) - (y_down(f2) - f2)
            mm[0, p - 1] = jnp.where(lower_in[2] > 0.0, lower_in[5] - cc, 0.0)
            curl_sweep(u2, (f1, f2), p, first + 1, emit_masked)
            node_range(p, first + 2)

    def upper_side():
        with scope("upper"):
            p = last + 1
            f1 = face_one(u1[0, p], u1[2, p], upper_in[1])
            f2 = face_two(u1[0, p], u1[1, p], upper_in[0])
            curl_sweep(u1, faces(u1, last), p, p + 1, emit_second, (f1, f2))
            f1 = face_one(u2[0, p], u2[2, p], upper_in[3])
            f2 = face_two(u2[0, p], u2[1, p], upper_in[2])
            curl_sweep(u2, faces(u2, last - 1), last, p + 1, emit_masked, (f1, f2))
            node_range(last, p + 1)
            v0 = u2[0, p]
            q2 = jnp.where(e[4, p + 1] > 0.0, u2[1, p] + (y_up(v0) - v0), 0.0)
            q1 = jnp.where(e[5, p + 1] > 0.0, (z_up(v0) - v0) + u2[2, p], 0.0)
            m0, m0p = mm[0, p], upper_in[4]
            rr[0, p + 1] = (m0 - m0p) + (upper_in[5] + (y_down(q2) - q2) + (z_down(q1) - q1))
            rr[1, p + 1] = (m0p + m0) * 0.5

    def in_turn(*pieces):
        for piece in pieces:
            piece()

    def write_all():
        with scope("out"):
            outputs(first, last + 1)

    def side_strips(base):
        strip_inputs(base)
        with scope("strips"):
            strips(base)

    def raw_relays():
        del sent_tiles[counted:]
        relay("rawup", ((2, 6),), 6, raw_up, yb_out, yb_in)
        relay("rawlow", ((3, 6),), 7, raw_low, yc_out, yc_in)

    counted = len(sent_tiles)
    strips_first = lax.rem(device(gx=1)["gx"], 4) == 3
    pl.when(jnp.logical_not(strips_first))(lambda: raw_relays())
    side_strips(0)
    pl.when(strips_first)(lambda: raw_relays())

    @pl.when(narrow)
    def _():
        relay("latelow", ((5, 6),), 11, late_low, ye_out, ye_in)

    base_tiles = sum(sent_tiles)

    @pl.when(thin)
    def _():
        relay("lateup", ((4, 6),), 0, late_up, yf_out, yf_in)

    def raw_sides():
        with scope("yraw"):
            y_finish(7, raw_low, yc_in)
            y_finish(6, raw_up, yb_in)
        with scope("rawsides"):
            first_range(first - 1, first)
            first_range(last + 1, last + 2)
            curl_sweep(u1, faces(u1, first - 1), first, first + 1, emit_second)
            curl_sweep(u1, faces(u1, last - 1), last, last + 1, emit_second)
            curl_sweep(u2, faces(u2, first), first + 1, first + 2, emit_rest)
            curl_sweep(u2, faces(u2, last - 2), last - 1, last, emit_masked)
            node_range(last - 1, last)

    pl.when(thin)(raw_sides)
    side_strips(1)
    pl.when(jnp.logical_not(thin))(raw_sides)
    in_turn(lower_inputs, upper_inputs, lower_side, upper_side, write_all)
    with scope("sendwait"):
        total = base_tiles
        sides = dx_in.shape[0]
        pl.when(down_first)(lambda: wait_tiles(send.at[0], total + 1))
        pl.when(wide)(lambda: wait_tiles(send.at[0], total - 6 * sides))
        pl.when(thin)(lambda: wait_tiles(send.at[0], total + 5 * sides))
        pl.when(jnp.logical_not(down_first | wide | thin))(lambda: wait_tiles(send.at[0], total))


def on_device(sizes, rhs, conductivity, fraction, region, flags):
    _, nx, ny, nz = rhs.shape
    planes = nx + 2 * PAD
    rows = ny + 8
    f32 = jnp.float32
    hbm = pl.BlockSpec(memory_space=pl.ANY)
    sides = 1 if sizes[1] == 2 else 2
    relays = []
    for count in (6 * nx, 6, 6, 24, 6, 5):
        relays += [pltpu.VMEM((count, 8, nz), f32), pltpu.VMEM((sides, count, 8, nz), f32)]
    return pl.pallas_call(
        functools.partial(kernel, sizes, nx, ny, nz),
        out_shape=pltpu.VMEM(rhs.shape, rhs.dtype),
        in_specs=[hbm] * 5,
        out_specs=pl.BlockSpec(memory_space=pltpu.VMEM),
        scratch_shapes=[
            pltpu.SMEM(conductivity.shape, f32),
            pltpu.VMEM(rhs.shape, f32),
            pltpu.VMEM(region.shape, jnp.int32),
            pltpu.VMEM(flags.shape, jnp.int32),
            pltpu.VMEM((6, planes, rows, nz), f32),
            pltpu.VMEM((6, 4, rows, nz), f32),
            pltpu.VMEM((3, ny, nz), f32),
            pltpu.VMEM((3, planes, rows, nz), f32),
            pltpu.VMEM((3, planes, rows, nz), f32),
            pltpu.VMEM((3, planes, rows, nz), f32),
            pltpu.VMEM((3, planes, rows, nz), f32),
            pltpu.VMEM((4, planes, rows, nz), f32),
            pltpu.VMEM((2, 2, ny, nz), f32),
            pltpu.VMEM((2, 2, ny, nz), f32),
            pltpu.VMEM((2, 2, ny, nz), f32),
            pltpu.VMEM((2, 2, ny, nz), f32),
            pltpu.VMEM((2, 2, 8, nz), f32),
            pltpu.VMEM((sides, 2, 2, 8, nz), f32),
            pltpu.VMEM((2, 2, 8, nz), f32),
            pltpu.VMEM((sides, 2, 2, 8, nz), f32),
            pltpu.VMEM((5, ny, nz), f32),
            pltpu.VMEM((5, ny, nz), f32),
            pltpu.VMEM((6, rows, nz), f32),
            pltpu.VMEM((6, rows, nz), f32),
            pltpu.VMEM((6, rows, nz), f32),
            pltpu.VMEM((6, rows, nz), f32),
            *relays,
            pltpu.VMEM((320, 8, nz), f32),
            pltpu.SemaphoreType.DMA((2,)),
            pltpu.SemaphoreType.DMA((1,)),
            pltpu.SemaphoreType.DMA((13,)),
            pltpu.SemaphoreType.REGULAR((2,)),
        ],
        compiler_params=pltpu.CompilerParams(
            collective_id=0, has_side_effects=True, vmem_limit_bytes=60 * 1024 * 1024
        ),
    )(conductivity, rhs, fraction, region, flags)


def solution(mesh):
    sizes = tuple(mesh.shape[name] for name in ("gx", "gy", "gz"))
    return jax.shard_map(
        functools.partial(on_device, sizes),
        mesh=mesh,
        in_specs=(
            P(None, "gx", "gy", "gz"),
            P(),
            P(None, "gx", "gy", "gz"),
            P("gx", "gy", "gz"),
            P(None, "gx", "gy", "gz"),
        ),
        out_specs=P(None, "gx", "gy", "gz"),
        check_vma=False,
    )
```

```python
import functools
import math

import jax
import jax.numpy as jnp
from jax import lax
from jax.experimental import pallas as pl
from jax.experimental.pallas import tpu as pltpu
from jax.sharding import PartitionSpec as P

damping = 0.8
c_node = 0.8 / 7.0
MESH = pl.DeviceIdType.MESH
PAD = 2
SEG = 16


def rot(v, shift, axis):
    return pltpu.roll(v, shift % v.shape[axis], axis)


def y_up(v):
    return rot(v, -1, 0)


def y_down(v):
    return rot(v, 1, 0)


def z_up(v):
    return rot(v, -1, 1)


def z_down(v):
    return rot(v, 1, 1)


def face_zero(u1, u2):
    return (y_up(u2) - u2) - (z_up(u1) - u1)


def face_one(u0, u2, u2p):
    return (z_up(u0) - u0) - (u2p - u2)


def face_two(u0, u1, u1p):
    return (u1p - u1) - (y_up(u0) - u0)


def edges(f0, f1, f2, f1m, f2m):
    return (
        (z_down(f1) - f1) - (y_down(f2) - f2),
        (f2m - f2) - (z_down(f0) - f0),
        (y_down(f0) - f0) - (f1m - f1),
    )


def jacobi_scale(ks):
    return jnp.where(ks > 0.0, damping / (4.0 + ks), 0.0)


def next_iter(rhs, ks, scale, u, cc):
    return u + scale * (rhs - (cc + ks * u))


def masked_residual(rhs, ks, u, cc):
    return jnp.where(ks > 0.0, rhs - (cc + ks * u), 0.0)


def nodal_rhs(m0, m0m, m1, m2):
    m1m, m2m = y_down(m1), z_down(m2)
    return (
        (m0m - m0) + (m1m - m1) + (m2m - m2),
        (m0 + m0m) * 0.5,
        (m1 + m1m) * 0.5,
        (m2 + m2m) * 0.5,
    )


def nodal_step(r, rm, rp):
    around = (rm + rp) + (y_up(r) + y_down(r)) + (z_up(r) + z_down(r))
    return (1.2 * c_node) * r + (c_node * c_node) * around


def finish(rhs, ks, u, corr):
    fixed = damping * rhs
    fixed = fixed + damping * (rhs - fixed)
    return jnp.where(ks > 0.0, u + corr, fixed)


def kernel(
    sizes, nx, ny, nz, cond_hbm, rhs_hbm, frac_hbm, reg_hbm, flag_hbm, out_ref,
    cond, frac_ref, reg_ref, flag_ref,
    e, st, sw, jac, u1, u2, mm, rr, zs, zr, ds, dr, dx_out, dx_in, zx_out, zx_in, ends_out, ends_in, lower_out, lower_in, upper_out, upper_in,
    ya_out, ya_in, yb_out, yb_in, yc_out, yc_in, yd_out, yd_in, ye_out, ye_in, yf_out, yf_in,
    blank, load, send, recv, near,
):
    gx, gy, gz = sizes
    pos = {"gx": lax.axis_index("gx"), "gy": lax.axis_index("gy"), "gz": lax.axis_index("gz")}
    size = {"gx": gx, "gy": gy, "gz": gz}
    first, last = PAD, PAD + nx - 1
    scope = jax.named_scope

    def device(**steps):
        return {axis: lax.rem(pos[axis] + (step + size[axis]), size[axis]) for axis, step in steps.items()}

    steps = [(x, z) for z in (1, -1) for x in (0, 1, -1)]
    paired = gy == 2
    barrier = pltpu.get_barrier_semaphore()

    def greet(*devices):
        for one in devices:
            pl.semaphore_signal(barrier, inc=1, device_id=one, device_id_type=MESH)

    def on(core, **steps):
        return {**device(**steps), "gy": core}

    if paired:
        greet(on(1, gx=1), on(1, gx=-1))
        greet(device(gy=1))
        greet(*(on(0, gx=x, gz=z) for x, z in steps))
    else:
        greet(device(gx=1), device(gx=-1), device(gy=1), device(gy=-1), *(device(gx=x, gz=z) for x, z in steps))
        greet(*(device(gx=x, gy=y, gz=z) for x, z in steps for y in (1, -1)))
    own_rows = pl.ds(0, ny)
    loads = [
        pltpu.make_async_copy(src, dst, load.at[i])
        for src, dst, i in (
            (cond_hbm, cond, 1), (reg_hbm, reg_ref, 0),
            *((flag_hbm.at[k], flag_ref.at[k], 0) for k in range(3)),
            *((frac_hbm.at[k], frac_ref.at[k], 0) for k in range(3)),
            *((rhs_hbm.at[k], e.at[k, pl.ds(first, nx), own_rows], 0) for k in range(3)),
        )
    ]

    def tiles_of(count):
        return blank.at[pl.ds(0, count)]

    def wait_tiles(semaphore, count):
        pltpu.make_async_copy(tiles_of(count), tiles_of(count), semaphore).wait()

    with scope("load"):
        for one in loads:
            one.start()
        loads[0].wait()
        wait_tiles(load.at[0], 10 * nx * ny // 8)

    hurry = (lax.rem(pos["gx"], 4) == 3) & (pos["gz"] == gz - 1)

    def far_collect():
        pl.semaphore_wait(barrier, 1 + 2 * len(steps))
        pl.semaphore_signal(near.at[1], inc=1, device_id=device(gy=1), device_id_type=MESH)

    if paired:
        pl.when((pos["gy"] == 0) & hurry)(lambda: far_collect())

    sent_tiles = []

    def copy(group, src, dst, where, start=True):
        made = pltpu.make_async_remote_copy(
            src_ref=src, dst_ref=dst, send_sem=send.at[0], recv_sem=recv.at[group],
            device_id=where, device_id_type=MESH,
        )
        sent_tiles.append(math.prod(src.shape) // (8 * nz))
        if start:
            made.start()
        return made

    def arrived(group, count):
        wait_tiles(recv.at[group], count)

    row = lax.broadcasted_iota(jnp.int32, (8, nz), 0)
    top, bottom, halo = slice(0, 8), slice(ny - 8, ny), slice(ny, ny + 8)

    def y_start(group, places, out, into):
        for i, (ref, where) in enumerate(places):
            out[i] = jnp.where(row < 4, ref[(*where, top, slice(None))], ref[(*where, bottom, slice(None))])
        if gy == 2:
            copy(group, out, into.at[0], device(gy=1))
        else:
            copy(group, out, into.at[0], device(gy=-1))
            copy(group, out, into.at[1], device(gy=1))

    def y_finish(group, places, into):
        arrived(group, into.shape[0] * len(places))
        for i, (ref, where) in enumerate(places):
            tile = into[0, i] if gy == 2 else jnp.where(row < 4, into[0, i], into[1, i])
            ref[(*where, halo, slice(None))] = tile

    lane = lax.broadcasted_iota(jnp.int32, (ny, nz), 1)
    slot = lane // SEG
    half = nz // 2
    low_half = lane < half
    quad = (lane % SEG) // 4
    unit = (lane % SEG) // 3
    spare = ((0, 3, 0), (1, 3, 3), (2, 3, 4), (nx - 2, 4, 0), (nx - 1, 4, 1))
    left = (lane % SEG) < 8

    def end_piece(v, j):
        return rot(v, 8 + SEG * j, 1)

    def pick(base, where, other):
        return other if base is None else jnp.where(where, other, base)

    z_copies = [copy(10 - 9 * i, zs.at[i], zr.at[i], device(gz=2 * i - 1), False) for i in range(2)]
    corner_copies = [
        copy(10 - 9 * zside, ds.at[side, zside], dr.at[side, zside], device(gx=1 - 2 * side, gz=2 * zside - 1), False)
        for side in range(2) for zside in range(2)
    ]
    cross_copies = [
        [
            copy(10 - 9 * zside, dx_out.at[zside], dx_in.at[i, side, zside], device(gx=1 - 2 * side, gy=2 * i - 1, gz=2 * zside - 1), False)
            for side in range(2) for i in range(1 if paired else 2)
        ] + [
            copy(10 - 9 * zside, zx_out.at[zside], zx_in.at[i, zside], device(gy=2 * i - 1, gz=2 * zside - 1), False)
            for i in range(1 if paired else 2)
        ]
        for zside in range(2)
    ]

    def start(*copies):
        for one in copies:
            one.start()

    def start_far(zside):
        start(corner_copies[zside], corner_copies[2 + zside], z_copies[zside])

    def start_both():
        for zside in (1, 0):
            start_far(zside)
            start(*cross_copies[zside])

    packs = [None] * 6
    with scope("pack"):
        for x in range(nx):
            region = reg_ref[x]
            sigma = jnp.zeros((ny, nz), jnp.float32)
            for number in range(cond.shape[0]):
                sigma = jnp.where(region == number, cond[number], sigma)
            for k in range(3):
                ks = jnp.where(flag_ref[k, x] == 0, sigma * frac_ref[k, x], 0.0)
                e[3 + k, first + x, 0:ny, :] = ks
                for f, v in ((k, e[k, first + x, 0:ny, :]), (3 + k, ks)):
                    packs[f] = pick(packs[f], slot == x, end_piece(v, x))
        starts = [jacobi_scale(packs[3 + k]) * packs[k] for k in range(3)]
        for side, off in ((0, 8), (1, 4)):
            tiles = [None, None]
            for f in range(6):
                tiles[f // 4] = pick(tiles[f // 4], quad == f % 4, rot(packs[f], 4 * (f % 4) - off, 1))
            for i in range(2):
                zs[side, i] = tiles[i]
                zx_out[side, i] = jnp.where(row < 4, tiles[i][0:8], tiles[i][ny - 8:ny])
            off = 8 - 3 * side
            tile = None
            for f in range(5):
                tile = pick(tile, unit == f, rot(packs[f], 3 * f - off, 1))
            for k in range(3):
                outer = (slot == nx - 3) if k == 0 else (slot == 3) | (slot == nx - 3)
                tile = pick(tile, outer & (unit == k), rot(starts[k], 3 * k - off, 1))
            for at, to, u in spare:
                tile = pick(tile, (slot == to) & (unit == u), rot(packs[5], SEG * (to - at) + 3 * u - off, 1))
            upper, lower = tile[0:ny // 2], tile[ny // 2:ny]
            ds[0, side] = jnp.where(low_half[0:ny // 2], rot(upper, half, 1), lower)
            ds[1, side] = jnp.where(low_half[0:ny // 2], upper, rot(lower, half, 1))
            dx_out[side] = jnp.where(row < 4, tile[0:8], tile[ny - 8:ny])
        if paired:
            @pl.when(hurry)
            def _():
                pl.when(pos["gy"] == 1)(lambda: pl.semaphore_wait(near.at[1], 1))
                start_both()

        moves = (
            [(packs[f], 0, 8 * (f // 2) + 3 * (f % 2), 3) for f in range(6)] + [(starts[k], 3, 5 + k, 1) for k in (1, 2)],
            [(packs[f], nx - 2, 2 * f, 2) for f in range(6)] + [(starts[k], nx - 3, 12 + k, 1) for k in range(3)],
        )
        for side in range(2):
            tiles = [None, None, None]
            for v, at, to, wide in moves[side]:
                t, to = divmod(to, 8)
                tiles[t] = pick(tiles[t], (slot >= to) & (slot < to + wide), rot(v, SEG * (to - at), 1))
            for i in range(3 - side):
                ends_out[3 * side + i] = tiles[i]

    with scope("barrierwait"):
        if paired:
            @pl.when(pos["gy"] == 1)
            def _():
                pl.semaphore_wait(barrier, 5)
                pl.semaphore_signal(near.at[0], inc=1, device_id=device(gy=1), device_id_type=MESH)

            @pl.when(pos["gy"] == 0)
            def _():
                pl.semaphore_wait(near.at[0], 1)
        else:
            pl.semaphore_wait(barrier, 4 + 3 * len(steps))

    def far_wait():
        if not paired:
            return
        pl.when(pos["gy"] == 0)(lambda: far_collect())

        @pl.when(pos["gy"] == 1)
        def _():
            pl.semaphore_wait(near.at[1], 1)

    own = [(e, (f, p)) for f in range(6) for p in range(first, last + 1)]
    y_start(0, own, ya_out, ya_in)

    up, down = device(gx=1), device(gx=-1)
    ends_copies = [copy(12, ends_out.at[pl.ds(0, 3)], ends_in.at[pl.ds(0, 3)], down, False), copy(12, ends_out.at[pl.ds(3, 2)], ends_in.at[pl.ds(3, 2)], up, False)]
    raw_copies = [
        copy(2, e.at[:, first, own_rows], e.at[:, last + 1, own_rows], down, False),
        copy(3, e.at[:, last, own_rows], e.at[:, first - 1, own_rows], up, False),
    ]
    late_copies = [
        copy(4, upper_out.at[pl.ds(0, 4)], upper_in.at[pl.ds(0, 4)], down, False),
        copy(5, lower_out.at[:, own_rows], lower_in.at[:, own_rows], up, False),
    ]
    wide_copy = pltpu.make_async_remote_copy(
        src_ref=lower_out, dst_ref=lower_in, send_sem=send.at[0], recv_sem=recv.at[5],
        device_id=up, device_id_type=MESH,
    )
    thin_copies = [
        pltpu.make_async_remote_copy(
            src_ref=src, dst_ref=dst, send_sem=send.at[0], recv_sem=recv.at[4], device_id=down, device_id_type=MESH
        )
        for src, dst in (
            (upper_out.at[pl.ds(0, 4), own_rows], upper_in.at[pl.ds(0, 4), own_rows]),
            (e.at[4, first + 1, own_rows], e.at[4, last + 2, own_rows]),
        )
    ]
    last_copy = copy(9, upper_out.at[pl.ds(4, 2), own_rows], upper_in.at[pl.ds(4, 2), own_rows], down, False)
    mask_copies = [
        copy(4, e.at[4, first + 1], e.at[4, last + 2], down, False),
        copy(4, e.at[5, first + 1, own_rows], e.at[5, last + 2, own_rows], down, False),
    ]
    down_first = (lax.rem(pos["gx"], 4) == 1) & (pos["gz"] == 0)
    wide = (lax.rem(device(gx=-1)["gx"], 4) == 1) & (pos["gz"] == 0)
    narrow = jnp.logical_not(wide)
    thin = (lax.rem(device(gx=1)["gx"], 4) == 1) & (pos["gz"] == 0)

    def in_order(begin):
        pl.when(down_first)(lambda: begin(0, 1))
        pl.when(jnp.logical_not(down_first))(lambda: begin(1, 0))

    late_start = pos["gz"] == 0
    in_order(lambda a, b: start(ends_copies[a], ends_copies[b]))

    up_only = lax.rem(pos["gx"], 4) == 3
    pl.when(jnp.logical_not(up_only))(lambda: start(raw_copies[0]))
    pl.when(jnp.logical_not(down_first))(lambda: start(raw_copies[1]))

    @pl.when(jnp.logical_not(late_start | (hurry if paired else late_start)))
    def _():
        with scope("nearwait"):
            far_wait()
            start_both()


    def faces(u, p):
        v0, v1, v2 = u[0, p], u[1, p], u[2, p]
        return face_one(v0, v2, u[2, p + 1]), face_two(v0, v1, u[1, p + 1])

    def curl_sweep(u, before, lo, hi, emit, after=None):
        f1m, f2m = before
        for p in range(lo, hi):
            f1, f2 = faces(u, p) if after is None or p < hi - 1 else after
            f0 = face_zero(u[1, p], u[2, p])
            cc = edges(f0, f1, f2, f1m, f2m)
            for k in range(3):
                emit(k, p, cc[k])
            f1m, f2m = f1, f2

    def emit_second(k, p, cc):
        u2[k, p] = next_iter(e[k, p], e[3 + k, p], jac[k, p], u1[k, p], cc)

    def emit_masked(k, p, cc):
        mm[k, p] = masked_residual(e[k, p], e[3 + k, p], u2[k, p], cc)

    def emit_rest(k, p, cc):
        if k > 0 or p != first + 1:
            emit_masked(k, p, cc)

    def node_range(lo, hi):
        for p in range(lo, hi):
            r = nodal_rhs(mm[0, p], mm[0, p - 1], mm[1, p], mm[2, p])
            for q in range(4):
                rr[q, p] = r[q]

    def first_range(lo, hi):
        for p in range(lo, hi):
            for k in range(3):
                scale = jacobi_scale(e[3 + k, p])
                jac[k, p] = scale
                u1[k, p] = scale * e[k, p]

    def below(v, p):
        up0 = v[0, p]
        return (z_up(up0) - up0) + v[2, p], v[1, p] + (y_up(up0) - up0)

    with scope("y1"):
        y_finish(0, own, ya_in)
    with scope("inner"):
        first_range(first, last + 1)
        curl_sweep(u1, faces(u1, first), first + 1, last, emit_second)
        p = last - 1
        sent = (*below(u1, p), e[3, p], *below(u2, p), e[0, p] - e[3, p] * u2[0, p])
        for i, v in enumerate(sent):
            lower_out[i] = v
        p = first + 1
        f1, f2 = faces(u2, p)
        cc = edges(face_zero(u2[1, p], u2[2, p]), f1, f2, -u2[2, p], u2[1, p])
        m0, m1, m2 = [masked_residual(e[k, p], e[3 + k, p], u2[k, p], cc[k]) for k in range(3)]
        mm[0, p] = m0
        sent = (u1[1, p], u1[2, p], u2[1, p], u2[2, p], m0, (y_down(m1) - m1) + (z_down(m2) - m2))
        for i, v in enumerate(sent):
            upper_out[i] = v
    @pl.when(down_first)
    def _():
        start(mask_copies[1], *thin_copies, last_copy, raw_copies[1], wide_copy)

    @pl.when(up_only)
    def _():
        start(late_copies[1], raw_copies[0], *mask_copies, late_copies[0], last_copy)

    @pl.when(jnp.logical_not(down_first | up_only))
    def _():
        start(late_copies[1], *mask_copies, late_copies[0], last_copy)

    with scope("inner2"):
        curl_sweep(u2, faces(u2, first + 1), first + 2, last - 1, emit_masked)
        node_range(first + 2, last - 1)

    @pl.when(late_start)
    def _():
        with scope("nearwait"):
            far_wait()
            start_both()

    def relay(name, groups, relayed, places, out, into):
        with scope(name):
            for group, count in groups:
                arrived(group, count * ny // 8)
            y_start(relayed, places, out, into)

    raw_up = [(e, (f, last + 1)) for f in range(6)]
    raw_low = [(e, (f, first - 1)) for f in range(6)]
    late_low = [(lower_in, (i,)) for i in range(6)]
    strip_tiles = [(st, (f, t)) for f in range(6) for t in range(4)]

    inner = (lane >= 4) & (lane < nz - 4)

    def node_at(p, count=4):
        return [nodal_step(rr[q, p], rr[q, p - 1], rr[q, p + 1]) for q in range(count)]

    def outputs(lo, hi):
        s_next = node_at(lo)
        for p in range(lo, hi):
            s = s_next
            s_next = node_at(p + 1, 4 if p + 1 < hi else 2)
            corr = (
                (s_next[0] - s[0]) + (s[1] + s_next[1]) * 0.5,
                (y_up(s[0]) - s[0]) + (s[2] + y_up(s[2])) * 0.5,
                (z_up(s[0]) - s[0]) + (s[3] + z_up(s[3])) * 0.5,
            )
            for k in range(3):
                body = finish(e[k, p, 0:ny], e[3 + k, p, 0:ny], u2[k, p, 0:ny], corr[k][0:ny])
                ends = rot(sw[k], nz - 8 - SEG * (p - first), 1)
                out_ref[k, p - first] = jnp.where(inner, body, ends)

    lane24 = lax.broadcasted_iota(jnp.int32, (ny + 8, nz), 1)
    slot24 = lane24 // SEG
    left24 = (lane24 % SEG) < 8

    span = range(2)

    def x_up(vs):
        rs = [rot(v, -SEG, 1) for v in vs]
        return [jnp.where(lane24 < nz - SEG, rs[t], rs[t ^ 1]) for t in span]

    def x_down(vs):
        rs = [rot(v, SEG, 1) for v in vs]
        return [jnp.where(lane24 >= SEG, rs[t], rs[t ^ 1]) for t in span]

    def strip_curl(u):
        u1p, u2p = x_up(u[1]), x_up(u[2])
        f1 = [face_one(u[0][t], u[2][t], u2p[t]) for t in span]
        f2 = [face_two(u[0][t], u[1][t], u1p[t]) for t in span]
        f0 = [face_zero(u[1][t], u[2][t]) for t in span]
        f1m, f2m = x_down(f1), x_down(f2)
        out = [edges(f0[t], f1[t], f2[t], f1m[t], f2m[t]) for t in span]
        return [[out[t][k] for t in span] for k in range(3)]

    def strips(base):
        sr = [[st[k, 2 * base + t] for t in span] for k in range(3)]
        sk = [[st[3 + k, 2 * base + t] for t in span] for k in range(3)]
        outer = (slot24 == 3) | (slot24 == nx - 3)
        scale = [[jacobi_scale(sk[k][t]) for t in span] for k in range(3)]
        u = [[scale[k][t] * sr[k][t] for t in span] for k in range(3)]
        for k in range(3):
            u[k][1] = jnp.where(outer, sr[k][1], u[k][1])
        cc = strip_curl(u)
        u = [[next_iter(sr[k][t], sk[k][t], scale[k][t], u[k][t], cc[k][t]) for t in span] for k in range(3)]
        cc = strip_curl(u)
        m = [[masked_residual(sr[k][t], sk[k][t], u[k][t], cc[k][t]) for t in span] for k in range(3)]
        m0m = x_down(m[0])
        r = [nodal_rhs(m[0][t], m0m[t], m[1][t], m[2][t]) for t in span]
        s = []
        for q in range(4):
            rq = [r[t][q] for t in span]
            rm, rp = x_down(rq), x_up(rq)
            s.append([nodal_step(rq[t], rm[t], rp[t]) if q < 2 or t % 2 == 0 else None for t in span])
        s0p, s1p = x_up(s[0]), x_up(s[1])
        s0, s1, s2, s3 = [s[q][0] for q in range(4)]
        corr = (
            (s0p[0] - s0) + (s1 + s1p[0]) * 0.5,
            (y_up(s0) - s0) + (s2 + y_up(s2)) * 0.5,
            (z_up(s0) - s0) + (s3 + z_up(s3)) * 0.5,
        )
        for k in range(3):
            result = finish(sr[k][0], sk[k][0], u[k][0], corr[k])[0:ny]
            sw[k] = result if base == 0 else jnp.where(left, sw[k], result)

    def corner_of(f, tile, off):
        if f < 5:
            return rot(tile, off - 3 * f, 1)
        piece = None
        for at, to, u in spare:
            piece = pick(piece, slot[0:tile.shape[0]] == at, rot(tile, SEG * (at - to) + off - 3 * u, 1))
        return piece

    with scope("endswait"):
        arrived(12, 5 * ny // 8)
    with scope("strippack"):
        for f in range(6):
            t, to = divmod(2 * f, 8)
            piece = rot(ends_in[f // 2], SEG * (0 - 3 * (f % 2)), 1)
            piece = jnp.where(slot >= nx - 2, rot(ends_in[3 + t], SEG * (nx - 2 - to), 1), piece)
            if f < 3:
                piece = jnp.where(slot == 3, rot(ends_in[0], SEG * (3 - (5 + f)), 1), piece)
                piece = jnp.where(slot == nx - 3, rot(ends_in[4], SEG * (nx - 3 - (4 + f)), 1), piece)
            mid = packs[f]
            st[f, 0, 0:ny, :] = mid
            st[f, 1, 0:ny, :] = piece
            st[f, 2, 0:ny, :] = mid
            st[f, 3, 0:ny, :] = piece
        y_start(8, strip_tiles, yd_out, yd_in)


    def crossed(ref, *where):
        if paired:
            return ref[(0, *where)]
        return jnp.where(row < 4, ref[(0, *where)], ref[(1, *where)])

    def strip_inputs(base):
        with scope("ystrip"):
            if base == 0:
                y_finish(8, strip_tiles, yd_in)
            arrived(10 - 9 * base, 2 * ny // 8 + 2 * (ny // 2) // 8 + 4 * dx_in.shape[0])
            off = 8 - 4 * base
            minus, plus = dr[0, base], dr[1, base]
            low = low_half[0:ny // 2]
            own_corner = jnp.concatenate(
                [jnp.where(low, plus, rot(minus, half, 1)), jnp.where(low, rot(plus, half, 1), minus)], axis=0
            )
            cross_corner = jnp.where(low_half[0:8], crossed(dx_in, 1, base), crossed(dx_in, 0, base))
            for f in range(6):
                t, q = divmod(f, 4)
                for rows, tile, corner in (
                    (slice(0, ny), zr[base, t], own_corner), (halo, crossed(zx_in, base, t), cross_corner),
                ):
                    mine = left[0:tile.shape[0]] if base == 0 else ~left[0:tile.shape[0]]
                    for at, piece in ((2 * base, rot(tile, off - 4 * q, 1)), (2 * base + 1, corner_of(f, corner, 8 - 3 * base))):
                        st[f, at, rows, :] = jnp.where(mine, st[f, at, rows, :], piece)

    late_up = [(upper_in, (i,)) for i in range(4)] + [(e, (4, last + 2))]

    def lower_inputs():
        with scope("ylow"):
            pl.when(narrow)(lambda: y_finish(11, late_low, ye_in))
            pl.when(wide)(lambda: arrived(5, 6 * (ny + 8) // 8))

    def upper_inputs():
        with scope("yup"):
            pl.when(jnp.logical_not(thin))(lambda: arrived(4, (5 * (ny + 8) + ny) // 8))
            pl.when(thin)(lambda: y_finish(0, late_up, yf_in))
            arrived(9, 2 * ny // 8)

    def lower_side():
        with scope("lower"):
            p = first - 1
            curl_sweep(u1, (lower_in[0] - u1[2, p], u1[1, p] - lower_in[1]), p, first, emit_second)
            f1, f2 = lower_in[3] - u2[2, p], u2[1, p] - lower_in[4]
            cc = (z_down(f1) - f1) - (y_down(f2) - f2)
            mm[0, p - 1] = jnp.where(lower_in[2] > 0.0, lower_in[5] - cc, 0.0)
            curl_sweep(u2, (f1, f2), p, first + 1, emit_masked)
            node_range(p, first + 2)

    def upper_side():
        with scope("upper"):
            p = last + 1
            f1 = face_one(u1[0, p], u1[2, p], upper_in[1])
            f2 = face_two(u1[0, p], u1[1, p], upper_in[0])
            curl_sweep(u1, faces(u1, last), p, p + 1, emit_second, (f1, f2))
            f1 = face_one(u2[0, p], u2[2, p], upper_in[3])
            f2 = face_two(u2[0, p], u2[1, p], upper_in[2])
            curl_sweep(u2, faces(u2, last - 1), last, p + 1, emit_masked, (f1, f2))
            node_range(last, p + 1)
            v0 = u2[0, p]
            q2 = jnp.where(e[4, p + 1] > 0.0, u2[1, p] + (y_up(v0) - v0), 0.0)
            q1 = jnp.where(e[5, p + 1] > 0.0, (z_up(v0) - v0) + u2[2, p], 0.0)
            m0, m0p = mm[0, p], upper_in[4]
            rr[0, p + 1] = (m0 - m0p) + (upper_in[5] + (y_down(q2) - q2) + (z_down(q1) - q1))
            rr[1, p + 1] = (m0p + m0) * 0.5

    def in_turn(*pieces):
        for piece in pieces:
            piece()

    def write_all():
        with scope("out"):
            outputs(first, last + 1)

    def side_strips(base):
        strip_inputs(base)
        with scope("strips"):
            strips(base)

    def raw_relays():
        del sent_tiles[counted:]
        relay("rawup", ((2, 6),), 6, raw_up, yb_out, yb_in)
        relay("rawlow", ((3, 6),), 7, raw_low, yc_out, yc_in)

    counted = len(sent_tiles)
    strips_first = lax.rem(device(gx=1)["gx"], 4) == 3
    pl.when(jnp.logical_not(strips_first))(lambda: raw_relays())
    side_strips(0)
    pl.when(strips_first)(lambda: raw_relays())

    @pl.when(narrow)
    def _():
        relay("latelow", ((5, 6),), 11, late_low, ye_out, ye_in)

    base_tiles = sum(sent_tiles)

    @pl.when(thin)
    def _():
        relay("lateup", ((4, 6),), 0, late_up, yf_out, yf_in)

    def raw_sides():
        with scope("yraw"):
            y_finish(7, raw_low, yc_in)
            y_finish(6, raw_up, yb_in)
        with scope("rawsides"):
            first_range(first - 1, first)
            first_range(last + 1, last + 2)
            curl_sweep(u1, faces(u1, first - 1), first, first + 1, emit_second)
            curl_sweep(u1, faces(u1, last - 1), last, last + 1, emit_second)
            curl_sweep(u2, faces(u2, first), first + 1, first + 2, emit_rest)
            curl_sweep(u2, faces(u2, last - 2), last - 1, last, emit_masked)
            node_range(last - 1, last)

    pl.when(thin)(raw_sides)
    side_strips(1)
    pl.when(jnp.logical_not(thin))(raw_sides)
    in_turn(lower_inputs, upper_inputs, lower_side, upper_side, write_all)
    with scope("sendwait"):
        total = base_tiles
        sides = dx_in.shape[0]
        pl.when(down_first)(lambda: wait_tiles(send.at[0], total + 1))
        pl.when(wide)(lambda: wait_tiles(send.at[0], total - 6 * sides))
        pl.when(thin)(lambda: wait_tiles(send.at[0], total + 5 * sides))
        pl.when(jnp.logical_not(down_first | wide | thin))(lambda: wait_tiles(send.at[0], total))


def on_device(sizes, rhs, conductivity, fraction, region, flags):
    _, nx, ny, nz = rhs.shape
    planes = nx + 2 * PAD
    rows = ny + 8
    f32 = jnp.float32
    hbm = pl.BlockSpec(memory_space=pl.ANY)
    sides = 1 if sizes[1] == 2 else 2
    relays = []
    for count in (6 * nx, 6, 6, 24, 6, 5):
        relays += [pltpu.VMEM((count, 8, nz), f32), pltpu.VMEM((sides, count, 8, nz), f32)]
    return pl.pallas_call(
        functools.partial(kernel, sizes, nx, ny, nz),
        out_shape=pltpu.VMEM(rhs.shape, rhs.dtype),
        in_specs=[hbm] * 5,
        out_specs=pl.BlockSpec(memory_space=pltpu.VMEM),
        scratch_shapes=[
            pltpu.SMEM(conductivity.shape, f32),
            pltpu.VMEM(rhs.shape, f32),
            pltpu.VMEM(region.shape, jnp.int32),
            pltpu.VMEM(flags.shape, jnp.int32),
            pltpu.VMEM((6, planes, rows, nz), f32),
            pltpu.VMEM((6, 4, rows, nz), f32),
            pltpu.VMEM((3, ny, nz), f32),
            pltpu.VMEM((3, planes, rows, nz), f32),
            pltpu.VMEM((3, planes, rows, nz), f32),
            pltpu.VMEM((3, planes, rows, nz), f32),
            pltpu.VMEM((3, planes, rows, nz), f32),
            pltpu.VMEM((4, planes, rows, nz), f32),
            pltpu.VMEM((2, 2, ny, nz), f32),
            pltpu.VMEM((2, 2, ny, nz), f32),
            pltpu.VMEM((2, 2, ny // 2, nz), f32),
            pltpu.VMEM((2, 2, ny // 2, nz), f32),
            pltpu.VMEM((2, 8, nz), f32),
            pltpu.VMEM((sides, 2, 2, 8, nz), f32),
            pltpu.VMEM((2, 2, 8, nz), f32),
            pltpu.VMEM((sides, 2, 2, 8, nz), f32),
            pltpu.VMEM((5, ny, nz), f32),
            pltpu.VMEM((5, ny, nz), f32),
            pltpu.VMEM((6, rows, nz), f32),
            pltpu.VMEM((6, rows, nz), f32),
            pltpu.VMEM((6, rows, nz), f32),
            pltpu.VMEM((6, rows, nz), f32),
            *relays,
            pltpu.VMEM((320, 8, nz), f32),
            pltpu.SemaphoreType.DMA((2,)),
            pltpu.SemaphoreType.DMA((1,)),
            pltpu.SemaphoreType.DMA((13,)),
            pltpu.SemaphoreType.REGULAR((2,)),
        ],
        compiler_params=pltpu.CompilerParams(
            collective_id=0, has_side_effects=True, vmem_limit_bytes=60 * 1024 * 1024
        ),
    )(conductivity, rhs, fraction, region, flags)


def solution(mesh):
    sizes = tuple(mesh.shape[name] for name in ("gx", "gy", "gz"))
    return jax.shard_map(
        functools.partial(on_device, sizes),
        mesh=mesh,
        in_specs=(
            P(None, "gx", "gy", "gz"),
            P(),
            P(None, "gx", "gy", "gz"),
            P("gx", "gy", "gz"),
            P(None, "gx", "gy", "gz"),
        ),
        out_specs=P(None, "gx", "gy", "gz"),
        check_vma=False,
    )
```

```python
import functools
import math

import jax
import jax.numpy as jnp
from jax import lax
from jax.experimental import pallas as pl
from jax.experimental.pallas import tpu as pltpu
from jax.sharding import PartitionSpec as P

damping = 0.8
c_node = 0.8 / 7.0
MESH = pl.DeviceIdType.MESH
PAD = 2
SEG = 16


def rot(v, shift, axis):
    return pltpu.roll(v, shift % v.shape[axis], axis)


def y_up(v):
    return rot(v, -1, 0)


def y_down(v):
    return rot(v, 1, 0)


def z_up(v):
    return rot(v, -1, 1)


def z_down(v):
    return rot(v, 1, 1)


def face_zero(u1, u2):
    return (y_up(u2) - u2) - (z_up(u1) - u1)


def face_one(u0, u2, u2p):
    return (z_up(u0) - u0) - (u2p - u2)


def face_two(u0, u1, u1p):
    return (u1p - u1) - (y_up(u0) - u0)


def edges(f0, f1, f2, f1m, f2m):
    return (
        (z_down(f1) - f1) - (y_down(f2) - f2),
        (f2m - f2) - (z_down(f0) - f0),
        (y_down(f0) - f0) - (f1m - f1),
    )


def jacobi_scale(ks):
    return jnp.where(ks > 0.0, damping / (4.0 + ks), 0.0)


def next_iter(rhs, ks, scale, u, cc):
    return u + scale * (rhs - (cc + ks * u))


def masked_residual(rhs, ks, u, cc):
    return jnp.where(ks > 0.0, rhs - (cc + ks * u), 0.0)


def nodal_rhs(m0, m0m, m1, m2):
    m1m, m2m = y_down(m1), z_down(m2)
    return (
        (m0m - m0) + (m1m - m1) + (m2m - m2),
        (m0 + m0m) * 0.5,
        (m1 + m1m) * 0.5,
        (m2 + m2m) * 0.5,
    )


def nodal_step(r, rm, rp):
    around = (rm + rp) + (y_up(r) + y_down(r)) + (z_up(r) + z_down(r))
    return (1.2 * c_node) * r + (c_node * c_node) * around


def finish(rhs, ks, u, corr):
    fixed = damping * rhs
    fixed = fixed + damping * (rhs - fixed)
    return jnp.where(ks > 0.0, u + corr, fixed)


def kernel(
    sizes, nx, ny, nz, cond_hbm, rhs_hbm, frac_hbm, reg_hbm, flag_hbm, out_ref,
    cond, frac_ref, reg_ref, flag_ref,
    e, st, sw, jac, u1, u2, mm, rr, zs, zr, ds, dr, dx_out, dx_in, zx_out, zx_in, ends_out, ends_in, lower_out, lower_in, upper_out, upper_in,
    ya_out, ya_in, yb_out, yb_in, yc_out, yc_in, yd_out, yd_in, ye_out, ye_in, yf_out, yf_in,
    blank, load, send, recv, near,
):
    gx, gy, gz = sizes
    pos = {"gx": lax.axis_index("gx"), "gy": lax.axis_index("gy"), "gz": lax.axis_index("gz")}
    size = {"gx": gx, "gy": gy, "gz": gz}
    first, last = PAD, PAD + nx - 1
    scope = jax.named_scope

    def device(**steps):
        return {axis: lax.rem(pos[axis] + (step + size[axis]), size[axis]) for axis, step in steps.items()}

    steps = [(x, z) for z in (1, -1) for x in (0, 1, -1)]
    paired = gy == 2
    barrier = pltpu.get_barrier_semaphore()

    def greet(*devices):
        for one in devices:
            pl.semaphore_signal(barrier, inc=1, device_id=one, device_id_type=MESH)

    def on(core, **steps):
        return {**device(**steps), "gy": core}

    if paired:
        greet(on(1, gx=1), on(1, gx=-1))
        greet(device(gy=1))
        greet(*(on(0, gx=x, gz=z) for x, z in steps))
    else:
        greet(device(gx=1), device(gx=-1), device(gy=1), device(gy=-1), *(device(gx=x, gz=z) for x, z in steps))
        greet(*(device(gx=x, gy=y, gz=z) for x, z in steps for y in (1, -1)))
    own_rows = pl.ds(0, ny)
    loads = [
        pltpu.make_async_copy(src, dst, load.at[i])
        for src, dst, i in (
            (cond_hbm, cond, 1), (reg_hbm, reg_ref, 0),
            *((flag_hbm.at[k], flag_ref.at[k], 0) for k in range(3)),
            *((frac_hbm.at[k], frac_ref.at[k], 0) for k in range(3)),
            *((rhs_hbm.at[k], e.at[k, pl.ds(first, nx), own_rows], 0) for k in range(3)),
        )
    ]

    def tiles_of(count):
        return blank.at[pl.ds(0, count)]

    def wait_tiles(semaphore, count):
        pltpu.make_async_copy(tiles_of(count), tiles_of(count), semaphore).wait()

    with scope("load"):
        for one in loads:
            one.start()
        loads[0].wait()
        wait_tiles(load.at[0], 10 * nx * ny // 8)

    hurry = (lax.rem(pos["gx"], 4) == 3) & (pos["gz"] == gz - 1)

    def far_collect():
        pl.semaphore_wait(barrier, 1 + 2 * len(steps))
        pl.semaphore_signal(near.at[1], inc=1, device_id=device(gy=1), device_id_type=MESH)

    if paired:
        pl.when((pos["gy"] == 0) & hurry)(lambda: far_collect())

    sent_tiles = []

    def copy(group, src, dst, where, start=True):
        made = pltpu.make_async_remote_copy(
            src_ref=src, dst_ref=dst, send_sem=send.at[0], recv_sem=recv.at[group],
            device_id=where, device_id_type=MESH,
        )
        sent_tiles.append(math.prod(src.shape) // (8 * nz))
        if start:
            made.start()
        return made

    def arrived(group, count):
        wait_tiles(recv.at[group], count)

    row = lax.broadcasted_iota(jnp.int32, (8, nz), 0)
    top, bottom, halo = slice(0, 8), slice(ny - 8, ny), slice(ny, ny + 8)

    def y_start(group, places, out, into):
        for i, (ref, where) in enumerate(places):
            out[i] = jnp.where(row < 4, ref[(*where, top, slice(None))], ref[(*where, bottom, slice(None))])
        if gy == 2:
            copy(group, out, into.at[0], device(gy=1))
        else:
            copy(group, out, into.at[0], device(gy=-1))
            copy(group, out, into.at[1], device(gy=1))

    def y_finish(group, places, into):
        arrived(group, into.shape[0] * len(places))
        for i, (ref, where) in enumerate(places):
            tile = into[0, i] if gy == 2 else jnp.where(row < 4, into[0, i], into[1, i])
            ref[(*where, halo, slice(None))] = tile

    lane = lax.broadcasted_iota(jnp.int32, (ny, nz), 1)
    slot = lane // SEG
    half = nz // 2
    low_half = lane < half
    quad = (lane % SEG) // 4
    unit = (lane % SEG) // 3
    fourth = ((0, 6), (3, 7))
    spare = ((0, 3, 0), (1, 3, 3), (2, 3, 4), (nx - 2, 4, 0), (nx - 1, 4, 1))
    left = (lane % SEG) < 8

    def end_piece(v, j):
        return rot(v, 8 + SEG * j, 1)

    def pick(base, where, other):
        return other if base is None else jnp.where(where, other, base)

    z_copies = [copy(10 - 9 * i, zs.at[i], zr.at[i], device(gz=2 * i - 1), False) for i in range(2)]
    corner_copies = [
        copy(10 - 9 * zside, ds.at[side, zside], dr.at[side, zside], device(gx=1 - 2 * side, gz=2 * zside - 1), False)
        for side in range(2) for zside in range(2)
    ]
    cross_copies = [
        [
            copy(10 - 9 * zside, dx_out.at[zside], dx_in.at[i, side, zside], device(gx=1 - 2 * side, gy=2 * i - 1, gz=2 * zside - 1), False)
            for side in range(2) for i in range(1 if paired else 2)
        ] + [
            copy(10 - 9 * zside, zx_out.at[zside], zx_in.at[i, zside], device(gy=2 * i - 1, gz=2 * zside - 1), False)
            for i in range(1 if paired else 2)
        ]
        for zside in range(2)
    ]

    def start(*copies):
        for one in copies:
            one.start()

    def start_far(zside):
        start(corner_copies[zside], corner_copies[2 + zside], z_copies[zside])

    def start_both():
        for zside in (1, 0):
            start_far(zside)
            start(*cross_copies[zside])

    packs = [None] * 6
    with scope("pack"):
        for x in range(nx):
            region = reg_ref[x]
            sigma = jnp.zeros((ny, nz), jnp.float32)
            for number in range(cond.shape[0]):
                sigma = jnp.where(region == number, cond[number], sigma)
            for k in range(3):
                ks = jnp.where(flag_ref[k, x] == 0, sigma * frac_ref[k, x], 0.0)
                e[3 + k, first + x, 0:ny, :] = ks
                for f, v in ((k, e[k, first + x, 0:ny, :]), (3 + k, ks)):
                    packs[f] = pick(packs[f], slot == x, end_piece(v, x))
        starts = [jacobi_scale(packs[3 + k]) * packs[k] for k in range(3)]
        for side, off in ((0, 8), (1, 4)):
            tiles = [None, None]
            for f in range(6):
                tiles[f // 4] = pick(tiles[f // 4], quad == f % 4, rot(packs[f], 4 * (f % 4) - off, 1))
            for i in range(2):
                zs[side, i] = tiles[i]
                zx_out[side, i] = jnp.where(row < 4, tiles[i][0:8], tiles[i][ny - 8:ny])
            off = 8 - 3 * side
            tile = None
            for f in range(5):
                tile = pick(tile, unit == f, rot(packs[f], 3 * f - off, 1))
            for k in range(3):
                outer = (slot == nx - 3) if k == 0 else (slot == 3) | (slot == nx - 3)
                tile = pick(tile, outer & (unit == k), rot(starts[k], 3 * k - off, 1))
            for at, to, u in spare:
                tile = pick(tile, (slot == to) & (unit == u), rot(packs[5], SEG * (to - at) + 3 * u - off, 1))
            if side == 0:
                for f, to in fourth:
                    tile = pick(tile, (slot == 4) & (lane % SEG == to), rot(packs[f], SEG * (4 - (nx - 1)) + to - 11, 1))
            upper, lower = tile[0:ny // 2], tile[ny // 2:ny]
            ds[0, side] = jnp.where(low_half[0:ny // 2], rot(upper, half, 1), lower)
            ds[1, side] = jnp.where(low_half[0:ny // 2], upper, rot(lower, half, 1))
            dx_out[side] = jnp.where(row < 4, tile[0:8], tile[ny - 8:ny])
        if paired:
            @pl.when(hurry)
            def _():
                pl.when(pos["gy"] == 1)(lambda: pl.semaphore_wait(near.at[1], 1))
                start_both()

        moves = (
            [(packs[f], 0, 8 * (f // 2) + 3 * (f % 2), 3) for f in range(6)] + [(starts[k], 3, 5 + k, 1) for k in (1, 2)],
            [(packs[f], nx - 2, 2 * f, 2) for f in range(6)] + [(starts[k], nx - 3, 12 + k, 1) for k in range(3)],
        )
        for side in range(2):
            tiles = [None, None, None]
            for v, at, to, wide in moves[side]:
                t, to = divmod(to, 8)
                tiles[t] = pick(tiles[t], (slot >= to) & (slot < to + wide), rot(v, SEG * (to - at), 1))
            for i in range(3 - side):
                ends_out[3 * side + i] = tiles[i]

    with scope("barrierwait"):
        if paired:
            @pl.when(pos["gy"] == 1)
            def _():
                pl.semaphore_wait(barrier, 5)
                pl.semaphore_signal(near.at[0], inc=1, device_id=device(gy=1), device_id_type=MESH)

            @pl.when(pos["gy"] == 0)
            def _():
                pl.semaphore_wait(near.at[0], 1)
        else:
            pl.semaphore_wait(barrier, 4 + 3 * len(steps))

    def far_wait():
        if not paired:
            return
        pl.when(pos["gy"] == 0)(lambda: far_collect())

        @pl.when(pos["gy"] == 1)
        def _():
            pl.semaphore_wait(near.at[1], 1)

    own = [(e, (f, p)) for f in range(6) for p in range(first, last + 1)]
    y_start(0, own, ya_out, ya_in)

    up, down = device(gx=1), device(gx=-1)
    ends_copies = [copy(12, ends_out.at[pl.ds(0, 3)], ends_in.at[pl.ds(0, 3)], down, False), copy(12, ends_out.at[pl.ds(3, 2)], ends_in.at[pl.ds(3, 2)], up, False)]
    raw_copies = [
        copy(2, e.at[:, first, own_rows], e.at[:, last + 1, own_rows], down, False),
        copy(3, e.at[:, last, own_rows], e.at[:, first - 1, own_rows], up, False),
    ]
    late_copies = [
        copy(4, upper_out.at[pl.ds(0, 4)], upper_in.at[pl.ds(0, 4)], down, False),
        copy(5, lower_out.at[:, own_rows], lower_in.at[:, own_rows], up, False),
    ]
    wide_copy = pltpu.make_async_remote_copy(
        src_ref=lower_out, dst_ref=lower_in, send_sem=send.at[0], recv_sem=recv.at[5],
        device_id=up, device_id_type=MESH,
    )
    thin_copies = [
        pltpu.make_async_remote_copy(
            src_ref=src, dst_ref=dst, send_sem=send.at[0], recv_sem=recv.at[4], device_id=down, device_id_type=MESH
        )
        for src, dst in (
            (upper_out.at[pl.ds(0, 4), own_rows], upper_in.at[pl.ds(0, 4), own_rows]),
            (e.at[4, first + 1, own_rows], e.at[4, last + 2, own_rows]),
        )
    ]
    last_copy = copy(9, upper_out.at[pl.ds(4, 2), own_rows], upper_in.at[pl.ds(4, 2), own_rows], down, False)
    mask_copies = [
        copy(4, e.at[4, first + 1], e.at[4, last + 2], down, False),
        copy(4, e.at[5, first + 1, own_rows], e.at[5, last + 2, own_rows], down, False),
    ]
    down_first = (lax.rem(pos["gx"], 4) == 1) & (pos["gz"] == 0)
    wide = (lax.rem(device(gx=-1)["gx"], 4) == 1) & (pos["gz"] == 0)
    narrow = jnp.logical_not(wide)
    thin = (lax.rem(device(gx=1)["gx"], 4) == 1) & (pos["gz"] == 0)

    def in_order(begin):
        pl.when(down_first)(lambda: begin(0, 1))
        pl.when(jnp.logical_not(down_first))(lambda: begin(1, 0))

    late_start = pos["gz"] == 0
    in_order(lambda a, b: start(ends_copies[a], ends_copies[b]))

    up_only = lax.rem(pos["gx"], 4) == 3
    pl.when(jnp.logical_not(up_only))(lambda: start(raw_copies[0]))
    pl.when(jnp.logical_not(down_first))(lambda: start(raw_copies[1]))

    @pl.when(jnp.logical_not(late_start | (hurry if paired else late_start)))
    def _():
        with scope("nearwait"):
            far_wait()
            start_both()


    def faces(u, p):
        v0, v1, v2 = u[0, p], u[1, p], u[2, p]
        return face_one(v0, v2, u[2, p + 1]), face_two(v0, v1, u[1, p + 1])

    def curl_sweep(u, before, lo, hi, emit, after=None):
        f1m, f2m = before
        for p in range(lo, hi):
            f1, f2 = faces(u, p) if after is None or p < hi - 1 else after
            f0 = face_zero(u[1, p], u[2, p])
            cc = edges(f0, f1, f2, f1m, f2m)
            for k in range(3):
                emit(k, p, cc[k])
            f1m, f2m = f1, f2

    def emit_second(k, p, cc):
        u2[k, p] = next_iter(e[k, p], e[3 + k, p], jac[k, p], u1[k, p], cc)

    def emit_masked(k, p, cc):
        mm[k, p] = masked_residual(e[k, p], e[3 + k, p], u2[k, p], cc)

    def emit_rest(k, p, cc):
        if k > 0 or p != first + 1:
            emit_masked(k, p, cc)

    def node_range(lo, hi):
        for p in range(lo, hi):
            r = nodal_rhs(mm[0, p], mm[0, p - 1], mm[1, p], mm[2, p])
            for q in range(4):
                rr[q, p] = r[q]

    def first_range(lo, hi):
        for p in range(lo, hi):
            for k in range(3):
                scale = jacobi_scale(e[3 + k, p])
                jac[k, p] = scale
                u1[k, p] = scale * e[k, p]

    def below(v, p):
        up0 = v[0, p]
        return (z_up(up0) - up0) + v[2, p], v[1, p] + (y_up(up0) - up0)

    with scope("y1"):
        y_finish(0, own, ya_in)
    with scope("inner"):
        first_range(first, last + 1)
        curl_sweep(u1, faces(u1, first), first + 1, last, emit_second)
        p = last - 1
        sent = (*below(u1, p), e[3, p], *below(u2, p), e[0, p] - e[3, p] * u2[0, p])
        for i, v in enumerate(sent):
            lower_out[i] = v
        p = first + 1
        f1, f2 = faces(u2, p)
        cc = edges(face_zero(u2[1, p], u2[2, p]), f1, f2, -u2[2, p], u2[1, p])
        m0, m1, m2 = [masked_residual(e[k, p], e[3 + k, p], u2[k, p], cc[k]) for k in range(3)]
        mm[0, p] = m0
        sent = (u1[1, p], u1[2, p], u2[1, p], u2[2, p], m0, (y_down(m1) - m1) + (z_down(m2) - m2))
        for i, v in enumerate(sent):
            upper_out[i] = v
    @pl.when(down_first)
    def _():
        start(mask_copies[1], *thin_copies, last_copy, raw_copies[1], wide_copy)

    @pl.when(up_only)
    def _():
        start(late_copies[1], raw_copies[0], *mask_copies, late_copies[0], last_copy)

    @pl.when(jnp.logical_not(down_first | up_only))
    def _():
        start(late_copies[1], *mask_copies, late_copies[0], last_copy)

    with scope("inner2"):
        curl_sweep(u2, faces(u2, first + 1), first + 2, last - 1, emit_masked)
        node_range(first + 2, last - 1)

    @pl.when(late_start)
    def _():
        with scope("nearwait"):
            far_wait()
            start_both()

    def relay(name, groups, relayed, places, out, into):
        with scope(name):
            for group, count in groups:
                arrived(group, count * ny // 8)
            y_start(relayed, places, out, into)

    raw_up = [(e, (f, last + 1)) for f in range(6)]
    raw_low = [(e, (f, first - 1)) for f in range(6)]
    late_low = [(lower_in, (i,)) for i in range(6)]
    strip_tiles = [(st, (f, t)) for f in range(6) for t in range(4)]

    inner = (lane >= 4) & (lane < nz - 4)

    def node_at(p, count=4):
        return [nodal_step(rr[q, p], rr[q, p - 1], rr[q, p + 1]) for q in range(count)]

    def outputs(lo, hi):
        s_next = node_at(lo)
        for p in range(lo, hi):
            s = s_next
            s_next = node_at(p + 1, 4 if p + 1 < hi else 2)
            corr = (
                (s_next[0] - s[0]) + (s[1] + s_next[1]) * 0.5,
                (y_up(s[0]) - s[0]) + (s[2] + y_up(s[2])) * 0.5,
                (z_up(s[0]) - s[0]) + (s[3] + z_up(s[3])) * 0.5,
            )
            for k in range(3):
                body = finish(e[k, p, 0:ny], e[3 + k, p, 0:ny], u2[k, p, 0:ny], corr[k][0:ny])
                ends = rot(sw[k], nz - 8 - SEG * (p - first), 1)
                out_ref[k, p - first] = jnp.where(inner, body, ends)

    lane24 = lax.broadcasted_iota(jnp.int32, (ny + 8, nz), 1)
    slot24 = lane24 // SEG
    left24 = (lane24 % SEG) < 8

    span = range(2)

    def x_up(vs):
        rs = [rot(v, -SEG, 1) for v in vs]
        return [jnp.where(lane24 < nz - SEG, rs[t], rs[t ^ 1]) for t in span]

    def x_down(vs):
        rs = [rot(v, SEG, 1) for v in vs]
        return [jnp.where(lane24 >= SEG, rs[t], rs[t ^ 1]) for t in span]

    def strip_curl(u):
        u1p, u2p = x_up(u[1]), x_up(u[2])
        f1 = [face_one(u[0][t], u[2][t], u2p[t]) for t in span]
        f2 = [face_two(u[0][t], u[1][t], u1p[t]) for t in span]
        f0 = [face_zero(u[1][t], u[2][t]) for t in span]
        f1m, f2m = x_down(f1), x_down(f2)
        out = [edges(f0[t], f1[t], f2[t], f1m[t], f2m[t]) for t in span]
        return [[out[t][k] for t in span] for k in range(3)]

    def strips(base):
        sr = [[st[k, 2 * base + t] for t in span] for k in range(3)]
        sk = [[st[3 + k, 2 * base + t] for t in span] for k in range(3)]
        outer = (slot24 == 3) | (slot24 == nx - 3)
        scale = [[jacobi_scale(sk[k][t]) for t in span] for k in range(3)]
        u = [[scale[k][t] * sr[k][t] for t in span] for k in range(3)]
        for k in range(3):
            u[k][1] = jnp.where(outer, sr[k][1], u[k][1])
        cc = strip_curl(u)
        u = [[next_iter(sr[k][t], sk[k][t], scale[k][t], u[k][t], cc[k][t]) for t in span] for k in range(3)]
        cc = strip_curl(u)
        m = [[masked_residual(sr[k][t], sk[k][t], u[k][t], cc[k][t]) for t in span] for k in range(3)]
        m0m = x_down(m[0])
        r = [nodal_rhs(m[0][t], m0m[t], m[1][t], m[2][t]) for t in span]
        s = []
        for q in range(4):
            rq = [r[t][q] for t in span]
            rm, rp = x_down(rq), x_up(rq)
            s.append([nodal_step(rq[t], rm[t], rp[t]) if q < 2 or t % 2 == 0 else None for t in span])
        s0p, s1p = x_up(s[0]), x_up(s[1])
        s0, s1, s2, s3 = [s[q][0] for q in range(4)]
        corr = (
            (s0p[0] - s0) + (s1 + s1p[0]) * 0.5,
            (y_up(s0) - s0) + (s2 + y_up(s2)) * 0.5,
            (z_up(s0) - s0) + (s3 + z_up(s3)) * 0.5,
        )
        for k in range(3):
            result = finish(sr[k][0], sk[k][0], u[k][0], corr[k])[0:ny]
            sw[k] = result if base == 0 else jnp.where(left, sw[k], result)

    def corner_of(f, tile, off):
        if f < 5:
            piece = rot(tile, off - 3 * f, 1)
            for k, to in fourth:
                if off == 8 and k == f:
                    at = ((slot == nx - 1) & (lane % SEG == 11))[0:tile.shape[0]]
                    piece = jnp.where(at, rot(tile, SEG * (nx - 1 - 4) + 11 - to, 1), piece)
            return piece
        piece = None
        for at, to, u in spare:
            piece = pick(piece, slot[0:tile.shape[0]] == at, rot(tile, SEG * (at - to) + off - 3 * u, 1))
        return piece

    with scope("endswait"):
        arrived(12, 5 * ny // 8)
    with scope("strippack"):
        for f in range(6):
            t, to = divmod(2 * f, 8)
            piece = rot(ends_in[f // 2], SEG * (0 - 3 * (f % 2)), 1)
            piece = jnp.where(slot >= nx - 2, rot(ends_in[3 + t], SEG * (nx - 2 - to), 1), piece)
            if f < 3:
                piece = jnp.where(slot == 3, rot(ends_in[0], SEG * (3 - (5 + f)), 1), piece)
                piece = jnp.where(slot == nx - 3, rot(ends_in[4], SEG * (nx - 3 - (4 + f)), 1), piece)
            mid = packs[f]
            st[f, 0, 0:ny, :] = mid
            st[f, 1, 0:ny, :] = piece
            st[f, 2, 0:ny, :] = mid
            st[f, 3, 0:ny, :] = piece
        y_start(8, strip_tiles, yd_out, yd_in)


    def crossed(ref, *where):
        if paired:
            return ref[(0, *where)]
        return jnp.where(row < 4, ref[(0, *where)], ref[(1, *where)])

    def strip_inputs(base):
        with scope("ystrip"):
            if base == 0:
                y_finish(8, strip_tiles, yd_in)
            arrived(10 - 9 * base, 2 * ny // 8 + 2 * (ny // 2) // 8 + 4 * dx_in.shape[0])
            off = 8 - 4 * base
            minus, plus = dr[0, base], dr[1, base]
            low = low_half[0:ny // 2]
            own_corner = jnp.concatenate(
                [jnp.where(low, plus, rot(minus, half, 1)), jnp.where(low, rot(plus, half, 1), minus)], axis=0
            )
            cross_corner = jnp.where(low_half[0:8], crossed(dx_in, 1, base), crossed(dx_in, 0, base))
            for f in range(6):
                t, q = divmod(f, 4)
                for rows, tile, corner in (
                    (slice(0, ny), zr[base, t], own_corner), (halo, crossed(zx_in, base, t), cross_corner),
                ):
                    mine = left[0:tile.shape[0]] if base == 0 else ~left[0:tile.shape[0]]
                    for at, piece in ((2 * base, rot(tile, off - 4 * q, 1)), (2 * base + 1, corner_of(f, corner, 8 - 3 * base))):
                        st[f, at, rows, :] = jnp.where(mine, st[f, at, rows, :], piece)

    late_up = [(upper_in, (i,)) for i in range(4)] + [(e, (4, last + 2))]

    def lower_inputs():
        with scope("ylow"):
            pl.when(narrow)(lambda: y_finish(11, late_low, ye_in))
            pl.when(wide)(lambda: arrived(5, 6 * (ny + 8) // 8))

    def upper_inputs():
        with scope("yup"):
            pl.when(jnp.logical_not(thin))(lambda: arrived(4, (5 * (ny + 8) + ny) // 8))
            pl.when(thin)(lambda: y_finish(0, late_up, yf_in))
            arrived(9, 2 * ny // 8)

    def lower_side():
        with scope("lower"):
            p = first - 1
            curl_sweep(u1, (lower_in[0] - u1[2, p], u1[1, p] - lower_in[1]), p, first, emit_second)
            f1, f2 = lower_in[3] - u2[2, p], u2[1, p] - lower_in[4]
            cc = (z_down(f1) - f1) - (y_down(f2) - f2)
            mm[0, p - 1] = jnp.where(lower_in[2] > 0.0, lower_in[5] - cc, 0.0)
            curl_sweep(u2, (f1, f2), p, first + 1, emit_masked)
            node_range(p, first + 2)

    def upper_side():
        with scope("upper"):
            p = last + 1
            f1 = face_one(u1[0, p], u1[2, p], upper_in[1])
            f2 = face_two(u1[0, p], u1[1, p], upper_in[0])
            curl_sweep(u1, faces(u1, last), p, p + 1, emit_second, (f1, f2))
            f1 = face_one(u2[0, p], u2[2, p], upper_in[3])
            f2 = face_two(u2[0, p], u2[1, p], upper_in[2])
            curl_sweep(u2, faces(u2, last - 1), last, p + 1, emit_masked, (f1, f2))
            node_range(last, p + 1)
            v0 = u2[0, p]
            q2 = jnp.where(e[4, p + 1] > 0.0, u2[1, p] + (y_up(v0) - v0), 0.0)
            q1 = jnp.where(e[5, p + 1] > 0.0, (z_up(v0) - v0) + u2[2, p], 0.0)
            m0, m0p = mm[0, p], upper_in[4]
            rr[0, p + 1] = (m0 - m0p) + (upper_in[5] + (y_down(q2) - q2) + (z_down(q1) - q1))
            rr[1, p + 1] = (m0p + m0) * 0.5

    def in_turn(*pieces):
        for piece in pieces:
            piece()

    def write_all():
        with scope("out"):
            outputs(first, last + 1)

    def side_strips(base):
        strip_inputs(base)
        with scope("strips"):
            strips(base)

    def raw_relays():
        del sent_tiles[counted:]
        relay("rawup", ((2, 6),), 6, raw_up, yb_out, yb_in)
        relay("rawlow", ((3, 6),), 7, raw_low, yc_out, yc_in)

    counted = len(sent_tiles)
    strips_first = lax.rem(device(gx=1)["gx"], 4) == 3
    pl.when(jnp.logical_not(strips_first))(lambda: raw_relays())
    side_strips(0)
    pl.when(strips_first)(lambda: raw_relays())

    @pl.when(narrow)
    def _():
        relay("latelow", ((5, 6),), 11, late_low, ye_out, ye_in)

    base_tiles = sum(sent_tiles)

    @pl.when(thin)
    def _():
        relay("lateup", ((4, 6),), 0, late_up, yf_out, yf_in)

    def raw_sides():
        with scope("yraw"):
            y_finish(7, raw_low, yc_in)
            y_finish(6, raw_up, yb_in)
        with scope("rawsides"):
            first_range(first - 1, first)
            first_range(last + 1, last + 2)
            curl_sweep(u1, faces(u1, first - 1), first, first + 1, emit_second)
            curl_sweep(u1, faces(u1, last - 1), last, last + 1, emit_second)
            curl_sweep(u2, faces(u2, first), first + 1, first + 2, emit_rest)
            curl_sweep(u2, faces(u2, last - 2), last - 1, last, emit_masked)
            node_range(last - 1, last)

    pl.when(thin)(raw_sides)
    side_strips(1)
    pl.when(jnp.logical_not(thin))(raw_sides)
    in_turn(lower_inputs, upper_inputs, lower_side, upper_side, write_all)
    with scope("sendwait"):
        total = base_tiles
        sides = dx_in.shape[0]
        pl.when(down_first)(lambda: wait_tiles(send.at[0], total + 1))
        pl.when(wide)(lambda: wait_tiles(send.at[0], total - 6 * sides))
        pl.when(thin)(lambda: wait_tiles(send.at[0], total + 5 * sides))
        pl.when(jnp.logical_not(down_first | wide | thin))(lambda: wait_tiles(send.at[0], total))


def on_device(sizes, rhs, conductivity, fraction, region, flags):
    _, nx, ny, nz = rhs.shape
    planes = nx + 2 * PAD
    rows = ny + 8
    f32 = jnp.float32
    hbm = pl.BlockSpec(memory_space=pl.ANY)
    sides = 1 if sizes[1] == 2 else 2
    relays = []
    for count in (6 * nx, 6, 6, 24, 6, 5):
        relays += [pltpu.VMEM((count, 8, nz), f32), pltpu.VMEM((sides, count, 8, nz), f32)]
    return pl.pallas_call(
        functools.partial(kernel, sizes, nx, ny, nz),
        out_shape=pltpu.VMEM(rhs.shape, rhs.dtype),
        in_specs=[hbm] * 5,
        out_specs=pl.BlockSpec(memory_space=pltpu.VMEM),
        scratch_shapes=[
            pltpu.SMEM(conductivity.shape, f32),
            pltpu.VMEM(rhs.shape, f32),
            pltpu.VMEM(region.shape, jnp.int32),
            pltpu.VMEM(flags.shape, jnp.int32),
            pltpu.VMEM((6, planes, rows, nz), f32),
            pltpu.VMEM((6, 4, rows, nz), f32),
            pltpu.VMEM((3, ny, nz), f32),
            pltpu.VMEM((3, planes, rows, nz), f32),
            pltpu.VMEM((3, planes, rows, nz), f32),
            pltpu.VMEM((3, planes, rows, nz), f32),
            pltpu.VMEM((3, planes, rows, nz), f32),
            pltpu.VMEM((4, planes, rows, nz), f32),
            pltpu.VMEM((2, 2, ny, nz), f32),
            pltpu.VMEM((2, 2, ny, nz), f32),
            pltpu.VMEM((2, 2, ny // 2, nz), f32),
            pltpu.VMEM((2, 2, ny // 2, nz), f32),
            pltpu.VMEM((2, 8, nz), f32),
            pltpu.VMEM((sides, 2, 2, 8, nz), f32),
            pltpu.VMEM((2, 2, 8, nz), f32),
            pltpu.VMEM((sides, 2, 2, 8, nz), f32),
            pltpu.VMEM((5, ny, nz), f32),
            pltpu.VMEM((5, ny, nz), f32),
            pltpu.VMEM((6, rows, nz), f32),
            pltpu.VMEM((6, rows, nz), f32),
            pltpu.VMEM((6, rows, nz), f32),
            pltpu.VMEM((6, rows, nz), f32),
            *relays,
            pltpu.VMEM((320, 8, nz), f32),
            pltpu.SemaphoreType.DMA((2,)),
            pltpu.SemaphoreType.DMA((1,)),
            pltpu.SemaphoreType.DMA((13,)),
            pltpu.SemaphoreType.REGULAR((2,)),
        ],
        compiler_params=pltpu.CompilerParams(
            collective_id=0, has_side_effects=True, vmem_limit_bytes=60 * 1024 * 1024
        ),
    )(conductivity, rhs, fraction, region, flags)


def solution(mesh):
    sizes = tuple(mesh.shape[name] for name in ("gx", "gy", "gz"))
    return jax.shard_map(
        functools.partial(on_device, sizes),
        mesh=mesh,
        in_specs=(
            P(None, "gx", "gy", "gz"),
            P(),
            P(None, "gx", "gy", "gz"),
            P("gx", "gy", "gz"),
            P(None, "gx", "gy", "gz"),
        ),
        out_specs=P(None, "gx", "gy", "gz"),
        check_vma=False,
    )
```

```python
import functools
import math

import jax
import jax.numpy as jnp
from jax import lax
from jax.experimental import pallas as pl
from jax.experimental.pallas import tpu as pltpu
from jax.sharding import PartitionSpec as P

damping = 0.8
c_node = 0.8 / 7.0
MESH = pl.DeviceIdType.MESH
PAD = 2
SEG = 16


def rot(v, shift, axis):
    return pltpu.roll(v, shift % v.shape[axis], axis)


def y_up(v):
    return rot(v, -1, 0)


def y_down(v):
    return rot(v, 1, 0)


def z_up(v):
    return rot(v, -1, 1)


def z_down(v):
    return rot(v, 1, 1)


def face_zero(u1, u2):
    return (y_up(u2) - u2) - (z_up(u1) - u1)


def face_one(u0, u2, u2p):
    return (z_up(u0) - u0) - (u2p - u2)


def face_two(u0, u1, u1p):
    return (u1p - u1) - (y_up(u0) - u0)


def edges(f0, f1, f2, f1m, f2m):
    return (
        (z_down(f1) - f1) - (y_down(f2) - f2),
        (f2m - f2) - (z_down(f0) - f0),
        (y_down(f0) - f0) - (f1m - f1),
    )


def jacobi_scale(ks):
    return jnp.where(ks > 0.0, damping / (4.0 + ks), 0.0)


def next_iter(rhs, ks, scale, u, cc):
    return u + scale * (rhs - (cc + ks * u))


def masked_residual(rhs, ks, u, cc):
    return jnp.where(ks > 0.0, rhs - (cc + ks * u), 0.0)


def nodal_rhs(m0, m0m, m1, m2):
    m1m, m2m = y_down(m1), z_down(m2)
    return (
        (m0m - m0) + (m1m - m1) + (m2m - m2),
        (m0 + m0m) * 0.5,
        (m1 + m1m) * 0.5,
        (m2 + m2m) * 0.5,
    )


def nodal_step(r, rm, rp):
    around = (rm + rp) + (y_up(r) + y_down(r)) + (z_up(r) + z_down(r))
    return (1.2 * c_node) * r + (c_node * c_node) * around


def finish(rhs, ks, u, corr):
    fixed = damping * rhs
    fixed = fixed + damping * (rhs - fixed)
    return jnp.where(ks > 0.0, u + corr, fixed)


def kernel(
    sizes, nx, ny, nz, cond_hbm, rhs_hbm, frac_hbm, reg_hbm, flag_hbm, out_ref,
    cond, frac_ref, reg_ref, flag_ref,
    e, st, sw, jac, u1, u2, mm, rr, zs, zr, ds, dr, dx_out, dx_in, zx_out, zx_in, ends_out, ends_in, lower_out, lower_in, upper_out, upper_in,
    ya_out, ya_in, yb_out, yb_in, yc_out, yc_in, yd_out, yd_in, ye_out, ye_in, yf_out, yf_in,
    blank, load, send, recv, near,
):
    gx, gy, gz = sizes
    pos = {"gx": lax.axis_index("gx"), "gy": lax.axis_index("gy"), "gz": lax.axis_index("gz")}
    size = {"gx": gx, "gy": gy, "gz": gz}
    first, last = PAD, PAD + nx - 1
    scope = jax.named_scope

    def device(**steps):
        return {axis: lax.rem(pos[axis] + (step + size[axis]), size[axis]) for axis, step in steps.items()}

    steps = [(x, z) for z in (1, -1) for x in (0, 1, -1)]
    paired = gy == 2
    barrier = pltpu.get_barrier_semaphore()

    def greet(*devices):
        for one in devices:
            pl.semaphore_signal(barrier, inc=1, device_id=one, device_id_type=MESH)

    def on(core, **steps):
        return {**device(**steps), "gy": core}

    if paired:
        greet(on(1, gx=1), on(1, gx=-1))
        greet(device(gy=1))
        greet(*(on(0, gx=x, gz=z) for x, z in steps))
    else:
        greet(device(gx=1), device(gx=-1), device(gy=1), device(gy=-1), *(device(gx=x, gz=z) for x, z in steps))
        greet(*(device(gx=x, gy=y, gz=z) for x, z in steps for y in (1, -1)))
    own_rows = pl.ds(0, ny)
    loads = [
        pltpu.make_async_copy(src, dst, load.at[i])
        for src, dst, i in (
            (cond_hbm, cond, 1), (reg_hbm, reg_ref, 0),
            *((flag_hbm.at[k], flag_ref.at[k], 0) for k in range(3)),
            *((frac_hbm.at[k], frac_ref.at[k], 0) for k in range(3)),
            *((rhs_hbm.at[k], e.at[k, pl.ds(first, nx), own_rows], 0) for k in range(3)),
        )
    ]

    def tiles_of(count):
        return blank.at[pl.ds(0, count)]

    def wait_tiles(semaphore, count):
        pltpu.make_async_copy(tiles_of(count), tiles_of(count), semaphore).wait()

    with scope("load"):
        for one in loads:
            one.start()
        loads[0].wait()
        wait_tiles(load.at[0], 10 * nx * ny // 8)

    hurry = (lax.rem(pos["gx"], 4) == 3) & (pos["gz"] == gz - 1)

    def far_collect():
        pl.semaphore_wait(barrier, 1 + 2 * len(steps))
        pl.semaphore_signal(near.at[1], inc=1, device_id=device(gy=1), device_id_type=MESH)

    if paired:
        pl.when((pos["gy"] == 0) & hurry)(lambda: far_collect())

    sent_tiles = []

    def copy(group, src, dst, where, start=True):
        made = pltpu.make_async_remote_copy(
            src_ref=src, dst_ref=dst, send_sem=send.at[0], recv_sem=recv.at[group],
            device_id=where, device_id_type=MESH,
        )
        sent_tiles.append(math.prod(src.shape) // (8 * nz))
        if start:
            made.start()
        return made

    def arrived(group, count):
        wait_tiles(recv.at[group], count)

    row = lax.broadcasted_iota(jnp.int32, (8, nz), 0)
    top, bottom, halo = slice(0, 8), slice(ny - 8, ny), slice(ny, ny + 8)

    def y_start(group, places, out, into):
        for i, (ref, where) in enumerate(places):
            out[i] = jnp.where(row < 4, ref[(*where, top, slice(None))], ref[(*where, bottom, slice(None))])
        if gy == 2:
            copy(group, out, into.at[0], device(gy=1))
        else:
            copy(group, out, into.at[0], device(gy=-1))
            copy(group, out, into.at[1], device(gy=1))

    def y_finish(group, places, into):
        arrived(group, into.shape[0] * len(places))
        for i, (ref, where) in enumerate(places):
            tile = into[0, i] if gy == 2 else jnp.where(row < 4, into[0, i], into[1, i])
            ref[(*where, halo, slice(None))] = tile

    lane = lax.broadcasted_iota(jnp.int32, (ny, nz), 1)
    slot = lane // SEG
    half = nz // 2
    low_half = lane < half
    quad = (lane % SEG) // 4
    unit = (lane % SEG) // 3
    fourth = ((0, 6), (3, 7))
    spare = ((0, 3, 0), (1, 3, 3), (2, 3, 4), (nx - 2, 4, 0), (nx - 1, 4, 1))
    left = (lane % SEG) < 8

    def end_piece(v, j):
        return rot(v, 8 + SEG * j, 1)

    def pick(base, where, other):
        return other if base is None else jnp.where(where, other, base)

    z_copies = [copy(10 - 9 * i, zs.at[i], zr.at[i], device(gz=2 * i - 1), False) for i in range(2)]
    corner_copies = [
        copy(10 - 9 * zside, ds.at[side, zside], dr.at[side, zside], device(gx=1 - 2 * side, gz=2 * zside - 1), False)
        for side in range(2) for zside in range(2)
    ]
    cross_copies = [
        [
            copy(10 - 9 * zside, dx_out.at[zside], dx_in.at[i, side, zside], device(gx=1 - 2 * side, gy=2 * i - 1, gz=2 * zside - 1), False)
            for side in range(2) for i in range(1 if paired else 2)
        ] + [
            copy(10 - 9 * zside, zx_out.at[zside], zx_in.at[i, zside], device(gy=2 * i - 1, gz=2 * zside - 1), False)
            for i in range(1 if paired else 2)
        ]
        for zside in range(2)
    ]

    def start(*copies):
        for one in copies:
            one.start()

    def start_far(zside):
        start(corner_copies[zside], corner_copies[2 + zside], z_copies[zside])

    def start_both():
        for zside in (1, 0):
            start_far(zside)
            start(*cross_copies[zside])

    packs = [None] * 6
    with scope("pack"):
        for x in range(nx):
            region = reg_ref[x]
            sigma = jnp.zeros((ny, nz), jnp.float32)
            for number in range(cond.shape[0]):
                sigma = jnp.where(region == number, cond[number], sigma)
            for k in range(3):
                ks = jnp.where(flag_ref[k, x] == 0, sigma * frac_ref[k, x], 0.0)
                e[3 + k, first + x, 0:ny, :] = ks
                for f, v in ((k, e[k, first + x, 0:ny, :]), (3 + k, ks)):
                    packs[f] = pick(packs[f], slot == x, end_piece(v, x))
        starts = [jacobi_scale(packs[3 + k]) * packs[k] for k in range(3)]
        for side, off in ((0, 8), (1, 4)):
            tiles = [None, None]
            for f in range(6):
                tiles[f // 4] = pick(tiles[f // 4], quad == f % 4, rot(packs[f], 4 * (f % 4) - off, 1))
            for i in range(2):
                zs[side, i] = tiles[i]
                zx_out[side, i] = jnp.where(row < 4, tiles[i][0:8], tiles[i][ny - 8:ny])
            off = 8 - 3 * side
            tile = None
            for f in range(5):
                tile = pick(tile, unit == f, rot(packs[f], 3 * f - off, 1))
            for k in range(3):
                outer = (slot == nx - 3) if k == 0 else (slot == 3) | (slot == nx - 3)
                tile = pick(tile, outer & (unit == k), rot(starts[k], 3 * k - off, 1))
            for at, to, u in spare:
                tile = pick(tile, (slot == to) & (unit == u), rot(packs[5], SEG * (to - at) + 3 * u - off, 1))
            if side == 0:
                for f, to in fourth:
                    tile = pick(tile, (slot == 4) & (lane % SEG == to), rot(packs[f], SEG * (4 - (nx - 1)) + to - 11, 1))
            upper, lower = tile[0:ny // 2], tile[ny // 2:ny]
            ds[0, side] = jnp.where(low_half[0:ny // 2], rot(upper, half, 1), lower)
            ds[1, side] = jnp.where(low_half[0:ny // 2], upper, rot(lower, half, 1))
            dx_out[side] = jnp.where(row < 4, tile[0:8], tile[ny - 8:ny])
        if paired:
            @pl.when(hurry)
            def _():
                pl.when(pos["gy"] == 1)(lambda: pl.semaphore_wait(near.at[1], 1))
                start_both()

        moves = (
            [(packs[f], 0, 8 * (f // 2) + 3 * (f % 2), 3) for f in range(6)] + [(starts[k], 3, 5 + k, 1) for k in (1, 2)],
            [(packs[f], nx - 2, 2 * f, 2) for f in range(6)] + [(starts[k], nx - 3, 12 + k, 1) for k in range(3)],
        )
        for side in range(2):
            tiles = [None, None, None]
            for v, at, to, wide in moves[side]:
                t, to = divmod(to, 8)
                tiles[t] = pick(tiles[t], (slot >= to) & (slot < to + wide), rot(v, SEG * (to - at), 1))
            for i in range(3 - side):
                ends_out[3 * side + i] = tiles[i]

    with scope("barrierwait"):
        if paired:
            @pl.when(pos["gy"] == 1)
            def _():
                pl.semaphore_wait(barrier, 5)
                pl.semaphore_signal(near.at[0], inc=1, device_id=device(gy=1), device_id_type=MESH)

            @pl.when(pos["gy"] == 0)
            def _():
                pl.semaphore_wait(near.at[0], 1)
        else:
            pl.semaphore_wait(barrier, 4 + 3 * len(steps))

    def far_wait():
        if not paired:
            return
        pl.when(pos["gy"] == 0)(lambda: far_collect())

        @pl.when(pos["gy"] == 1)
        def _():
            pl.semaphore_wait(near.at[1], 1)

    own = [(e, (f, p)) for f in range(6) for p in range(first, last + 1)]
    y_start(0, own, ya_out, ya_in)

    up, down = device(gx=1), device(gx=-1)
    ends_copies = [copy(12, ends_out.at[pl.ds(0, 3)], ends_in.at[pl.ds(0, 3)], down, False), copy(12, ends_out.at[pl.ds(3, 2)], ends_in.at[pl.ds(3, 2)], up, False)]
    raw_copies = [
        copy(2, e.at[:, first, own_rows], e.at[:, last + 1, own_rows], down, False),
        copy(3, e.at[:, last, own_rows], e.at[:, first - 1, own_rows], up, False),
    ]
    late_copies = [
        copy(4, upper_out.at[pl.ds(0, 4)], upper_in.at[pl.ds(0, 4)], down, False),
        copy(5, lower_out.at[:, own_rows], lower_in.at[:, own_rows], up, False),
    ]
    wide_copy = pltpu.make_async_remote_copy(
        src_ref=lower_out, dst_ref=lower_in, send_sem=send.at[0], recv_sem=recv.at[5],
        device_id=up, device_id_type=MESH,
    )
    thin_copies = [
        pltpu.make_async_remote_copy(
            src_ref=src, dst_ref=dst, send_sem=send.at[0], recv_sem=recv.at[4], device_id=down, device_id_type=MESH
        )
        for src, dst in (
            (upper_out.at[pl.ds(0, 4), own_rows], upper_in.at[pl.ds(0, 4), own_rows]),
            (e.at[4, first + 1, own_rows], e.at[4, last + 2, own_rows]),
        )
    ]
    last_copy = copy(9, upper_out.at[pl.ds(4, 2), own_rows], upper_in.at[pl.ds(4, 2), own_rows], down, False)
    mask_copies = [
        copy(4, e.at[4, first + 1], e.at[4, last + 2], down, False),
        copy(4, e.at[5, first + 1, own_rows], e.at[5, last + 2, own_rows], down, False),
    ]
    uneven = (pos["gz"] == 0) & (pos["gx"] >= gx % 4 * gx)
    down_first = (lax.rem(pos["gx"], 4) == 1) & uneven
    wide = (lax.rem(device(gx=-1)["gx"], 4) == 1) & uneven
    narrow = jnp.logical_not(wide)
    thin = (lax.rem(device(gx=1)["gx"], 4) == 1) & uneven

    def in_order(begin):
        pl.when(down_first)(lambda: begin(0, 1))
        pl.when(jnp.logical_not(down_first))(lambda: begin(1, 0))

    late_start = pos["gz"] == 0
    in_order(lambda a, b: start(ends_copies[a], ends_copies[b]))

    up_only = lax.rem(pos["gx"], 4) == 3
    pl.when(jnp.logical_not(up_only))(lambda: start(raw_copies[0]))
    pl.when(jnp.logical_not(down_first))(lambda: start(raw_copies[1]))

    @pl.when(jnp.logical_not(late_start | (hurry if paired else late_start)))
    def _():
        with scope("nearwait"):
            far_wait()
            start_both()


    def faces(u, p):
        v0, v1, v2 = u[0, p], u[1, p], u[2, p]
        return face_one(v0, v2, u[2, p + 1]), face_two(v0, v1, u[1, p + 1])

    def curl_sweep(u, before, lo, hi, emit, after=None):
        f1m, f2m = before
        for p in range(lo, hi):
            f1, f2 = faces(u, p) if after is None or p < hi - 1 else after
            f0 = face_zero(u[1, p], u[2, p])
            cc = edges(f0, f1, f2, f1m, f2m)
            for k in range(3):
                emit(k, p, cc[k])
            f1m, f2m = f1, f2

    def emit_second(k, p, cc):
        u2[k, p] = next_iter(e[k, p], e[3 + k, p], jac[k, p], u1[k, p], cc)

    def emit_masked(k, p, cc):
        mm[k, p] = masked_residual(e[k, p], e[3 + k, p], u2[k, p], cc)

    def emit_rest(k, p, cc):
        if k > 0 or p != first + 1:
            emit_masked(k, p, cc)

    def node_range(lo, hi):
        for p in range(lo, hi):
            r = nodal_rhs(mm[0, p], mm[0, p - 1], mm[1, p], mm[2, p])
            for q in range(4):
                rr[q, p] = r[q]

    def first_range(lo, hi):
        for p in range(lo, hi):
            for k in range(3):
                scale = jacobi_scale(e[3 + k, p])
                jac[k, p] = scale
                u1[k, p] = scale * e[k, p]

    def below(v, p):
        up0 = v[0, p]
        return (z_up(up0) - up0) + v[2, p], v[1, p] + (y_up(up0) - up0)

    with scope("y1"):
        y_finish(0, own, ya_in)
    with scope("inner"):
        first_range(first, last + 1)
        curl_sweep(u1, faces(u1, first), first + 1, last, emit_second)
        p = last - 1
        sent = (*below(u1, p), e[3, p], *below(u2, p), e[0, p] - e[3, p] * u2[0, p])
        for i, v in enumerate(sent):
            lower_out[i] = v
        p = first + 1
        f1, f2 = faces(u2, p)
        cc = edges(face_zero(u2[1, p], u2[2, p]), f1, f2, -u2[2, p], u2[1, p])
        m0, m1, m2 = [masked_residual(e[k, p], e[3 + k, p], u2[k, p], cc[k]) for k in range(3)]
        mm[0, p] = m0
        sent = (u1[1, p], u1[2, p], u2[1, p], u2[2, p], m0, (y_down(m1) - m1) + (z_down(m2) - m2))
        for i, v in enumerate(sent):
            upper_out[i] = v
    @pl.when(down_first)
    def _():
        start(mask_copies[1], *thin_copies, last_copy, raw_copies[1], wide_copy)

    @pl.when(up_only)
    def _():
        start(late_copies[1], raw_copies[0], *mask_copies, late_copies[0], last_copy)

    @pl.when(jnp.logical_not(down_first | up_only))
    def _():
        start(late_copies[1], *mask_copies, late_copies[0], last_copy)

    with scope("inner2"):
        curl_sweep(u2, faces(u2, first + 1), first + 2, last - 1, emit_masked)
        node_range(first + 2, last - 1)

    @pl.when(late_start)
    def _():
        with scope("nearwait"):
            far_wait()
            start_both()

    def relay(name, groups, relayed, places, out, into):
        with scope(name):
            for group, count in groups:
                arrived(group, count * ny // 8)
            y_start(relayed, places, out, into)

    raw_up = [(e, (f, last + 1)) for f in range(6)]
    raw_low = [(e, (f, first - 1)) for f in range(6)]
    late_low = [(lower_in, (i,)) for i in range(6)]
    strip_tiles = [(st, (f, t)) for f in range(6) for t in range(4)]

    inner = (lane >= 4) & (lane < nz - 4)

    def node_at(p, count=4):
        return [nodal_step(rr[q, p], rr[q, p - 1], rr[q, p + 1]) for q in range(count)]

    def outputs(lo, hi):
        s_next = node_at(lo)
        for p in range(lo, hi):
            s = s_next
            s_next = node_at(p + 1, 4 if p + 1 < hi else 2)
            corr = (
                (s_next[0] - s[0]) + (s[1] + s_next[1]) * 0.5,
                (y_up(s[0]) - s[0]) + (s[2] + y_up(s[2])) * 0.5,
                (z_up(s[0]) - s[0]) + (s[3] + z_up(s[3])) * 0.5,
            )
            for k in range(3):
                body = finish(e[k, p, 0:ny], e[3 + k, p, 0:ny], u2[k, p, 0:ny], corr[k][0:ny])
                ends = rot(sw[k], nz - 8 - SEG * (p - first), 1)
                out_ref[k, p - first] = jnp.where(inner, body, ends)

    lane24 = lax.broadcasted_iota(jnp.int32, (ny + 8, nz), 1)
    slot24 = lane24 // SEG
    left24 = (lane24 % SEG) < 8

    span = range(2)

    def x_up(vs):
        rs = [rot(v, -SEG, 1) for v in vs]
        return [jnp.where(lane24 < nz - SEG, rs[t], rs[t ^ 1]) for t in span]

    def x_down(vs):
        rs = [rot(v, SEG, 1) for v in vs]
        return [jnp.where(lane24 >= SEG, rs[t], rs[t ^ 1]) for t in span]

    def strip_curl(u):
        u1p, u2p = x_up(u[1]), x_up(u[2])
        f1 = [face_one(u[0][t], u[2][t], u2p[t]) for t in span]
        f2 = [face_two(u[0][t], u[1][t], u1p[t]) for t in span]
        f0 = [face_zero(u[1][t], u[2][t]) for t in span]
        f1m, f2m = x_down(f1), x_down(f2)
        out = [edges(f0[t], f1[t], f2[t], f1m[t], f2m[t]) for t in span]
        return [[out[t][k] for t in span] for k in range(3)]

    def strips(base):
        sr = [[st[k, 2 * base + t] for t in span] for k in range(3)]
        sk = [[st[3 + k, 2 * base + t] for t in span] for k in range(3)]
        outer = (slot24 == 3) | (slot24 == nx - 3)
        scale = [[jacobi_scale(sk[k][t]) for t in span] for k in range(3)]
        u = [[scale[k][t] * sr[k][t] for t in span] for k in range(3)]
        for k in range(3):
            u[k][1] = jnp.where(outer, sr[k][1], u[k][1])
        cc = strip_curl(u)
        u = [[next_iter(sr[k][t], sk[k][t], scale[k][t], u[k][t], cc[k][t]) for t in span] for k in range(3)]
        cc = strip_curl(u)
        m = [[masked_residual(sr[k][t], sk[k][t], u[k][t], cc[k][t]) for t in span] for k in range(3)]
        m0m = x_down(m[0])
        r = [nodal_rhs(m[0][t], m0m[t], m[1][t], m[2][t]) for t in span]
        s = []
        for q in range(4):
            rq = [r[t][q] for t in span]
            rm, rp = x_down(rq), x_up(rq)
            s.append([nodal_step(rq[t], rm[t], rp[t]) if q < 2 or t % 2 == 0 else None for t in span])
        s0p, s1p = x_up(s[0]), x_up(s[1])
        s0, s1, s2, s3 = [s[q][0] for q in range(4)]
        corr = (
            (s0p[0] - s0) + (s1 + s1p[0]) * 0.5,
            (y_up(s0) - s0) + (s2 + y_up(s2)) * 0.5,
            (z_up(s0) - s0) + (s3 + z_up(s3)) * 0.5,
        )
        for k in range(3):
            result = finish(sr[k][0], sk[k][0], u[k][0], corr[k])[0:ny]
            sw[k] = result if base == 0 else jnp.where(left, sw[k], result)

    def corner_of(f, tile, off):
        if f < 5:
            piece = rot(tile, off - 3 * f, 1)
            for k, to in fourth:
                if off == 8 and k == f:
                    at = ((slot == nx - 1) & (lane % SEG == 11))[0:tile.shape[0]]
                    piece = jnp.where(at, rot(tile, SEG * (nx - 1 - 4) + 11 - to, 1), piece)
            return piece
        piece = None
        for at, to, u in spare:
            piece = pick(piece, slot[0:tile.shape[0]] == at, rot(tile, SEG * (at - to) + off - 3 * u, 1))
        return piece

    with scope("endswait"):
        arrived(12, 5 * ny // 8)
    with scope("strippack"):
        for f in range(6):
            t, to = divmod(2 * f, 8)
            piece = rot(ends_in[f // 2], SEG * (0 - 3 * (f % 2)), 1)
            piece = jnp.where(slot >= nx - 2, rot(ends_in[3 + t], SEG * (nx - 2 - to), 1), piece)
            if f < 3:
                piece = jnp.where(slot == 3, rot(ends_in[0], SEG * (3 - (5 + f)), 1), piece)
                piece = jnp.where(slot == nx - 3, rot(ends_in[4], SEG * (nx - 3 - (4 + f)), 1), piece)
            mid = packs[f]
            st[f, 0, 0:ny, :] = mid
            st[f, 1, 0:ny, :] = piece
            st[f, 2, 0:ny, :] = mid
            st[f, 3, 0:ny, :] = piece
        y_start(8, strip_tiles, yd_out, yd_in)


    def crossed(ref, *where):
        if paired:
            return ref[(0, *where)]
        return jnp.where(row < 4, ref[(0, *where)], ref[(1, *where)])

    def strip_inputs(base):
        with scope("ystrip"):
            if base == 0:
                y_finish(8, strip_tiles, yd_in)
            arrived(10 - 9 * base, 2 * ny // 8 + 2 * (ny // 2) // 8 + 4 * dx_in.shape[0])
            off = 8 - 4 * base
            minus, plus = dr[0, base], dr[1, base]
            low = low_half[0:ny // 2]
            own_corner = jnp.concatenate(
                [jnp.where(low, plus, rot(minus, half, 1)), jnp.where(low, rot(plus, half, 1), minus)], axis=0
            )
            cross_corner = jnp.where(low_half[0:8], crossed(dx_in, 1, base), crossed(dx_in, 0, base))
            for f in range(6):
                t, q = divmod(f, 4)
                for rows, tile, corner in (
                    (slice(0, ny), zr[base, t], own_corner), (halo, crossed(zx_in, base, t), cross_corner),
                ):
                    mine = left[0:tile.shape[0]] if base == 0 else ~left[0:tile.shape[0]]
                    for at, piece in ((2 * base, rot(tile, off - 4 * q, 1)), (2 * base + 1, corner_of(f, corner, 8 - 3 * base))):
                        st[f, at, rows, :] = jnp.where(mine, st[f, at, rows, :], piece)

    late_up = [(upper_in, (i,)) for i in range(4)] + [(e, (4, last + 2))]

    def lower_inputs():
        with scope("ylow"):
            pl.when(narrow)(lambda: y_finish(11, late_low, ye_in))
            pl.when(wide)(lambda: arrived(5, 6 * (ny + 8) // 8))

    def upper_inputs():
        with scope("yup"):
            pl.when(jnp.logical_not(thin))(lambda: arrived(4, (5 * (ny + 8) + ny) // 8))
            pl.when(thin)(lambda: y_finish(0, late_up, yf_in))
            arrived(9, 2 * ny // 8)

    def lower_side():
        with scope("lower"):
            p = first - 1
            curl_sweep(u1, (lower_in[0] - u1[2, p], u1[1, p] - lower_in[1]), p, first, emit_second)
            f1, f2 = lower_in[3] - u2[2, p], u2[1, p] - lower_in[4]
            cc = (z_down(f1) - f1) - (y_down(f2) - f2)
            mm[0, p - 1] = jnp.where(lower_in[2] > 0.0, lower_in[5] - cc, 0.0)
            curl_sweep(u2, (f1, f2), p, first + 1, emit_masked)
            node_range(p, first + 2)

    def upper_side():
        with scope("upper"):
            p = last + 1
            f1 = face_one(u1[0, p], u1[2, p], upper_in[1])
            f2 = face_two(u1[0, p], u1[1, p], upper_in[0])
            curl_sweep(u1, faces(u1, last), p, p + 1, emit_second, (f1, f2))
            f1 = face_one(u2[0, p], u2[2, p], upper_in[3])
            f2 = face_two(u2[0, p], u2[1, p], upper_in[2])
            curl_sweep(u2, faces(u2, last - 1), last, p + 1, emit_masked, (f1, f2))
            node_range(last, p + 1)
            v0 = u2[0, p]
            q2 = jnp.where(e[4, p + 1] > 0.0, u2[1, p] + (y_up(v0) - v0), 0.0)
            q1 = jnp.where(e[5, p + 1] > 0.0, (z_up(v0) - v0) + u2[2, p], 0.0)
            m0, m0p = mm[0, p], upper_in[4]
            rr[0, p + 1] = (m0 - m0p) + (upper_in[5] + (y_down(q2) - q2) + (z_down(q1) - q1))
            rr[1, p + 1] = (m0p + m0) * 0.5

    def in_turn(*pieces):
        for piece in pieces:
            piece()

    def write_all():
        with scope("out"):
            outputs(first, last + 1)

    def side_strips(base):
        strip_inputs(base)
        with scope("strips"):
            strips(base)

    def raw_relays():
        del sent_tiles[counted:]
        relay("rawup", ((2, 6),), 6, raw_up, yb_out, yb_in)
        relay("rawlow", ((3, 6),), 7, raw_low, yc_out, yc_in)

    counted = len(sent_tiles)
    strips_first = lax.rem(device(gx=1)["gx"], 4) == 3
    pl.when(jnp.logical_not(strips_first))(lambda: raw_relays())
    side_strips(0)
    pl.when(strips_first)(lambda: raw_relays())

    @pl.when(narrow)
    def _():
        relay("latelow", ((5, 6),), 11, late_low, ye_out, ye_in)

    base_tiles = sum(sent_tiles)

    @pl.when(thin)
    def _():
        relay("lateup", ((4, 6),), 0, late_up, yf_out, yf_in)

    def raw_sides():
        with scope("yraw"):
            y_finish(7, raw_low, yc_in)
            y_finish(6, raw_up, yb_in)
        with scope("rawsides"):
            first_range(first - 1, first)
            first_range(last + 1, last + 2)
            curl_sweep(u1, faces(u1, first - 1), first, first + 1, emit_second)
            curl_sweep(u1, faces(u1, last - 1), last, last + 1, emit_second)
            curl_sweep(u2, faces(u2, first), first + 1, first + 2, emit_rest)
            curl_sweep(u2, faces(u2, last - 2), last - 1, last, emit_masked)
            node_range(last - 1, last)

    pl.when(thin)(raw_sides)
    side_strips(1)
    pl.when(jnp.logical_not(thin))(raw_sides)
    in_turn(lower_inputs, upper_inputs, lower_side, upper_side, write_all)
    with scope("sendwait"):
        total = base_tiles
        sides = dx_in.shape[0]
        pl.when(down_first)(lambda: wait_tiles(send.at[0], total + 1))
        pl.when(wide)(lambda: wait_tiles(send.at[0], total - 6 * sides))
        pl.when(thin)(lambda: wait_tiles(send.at[0], total + 5 * sides))
        pl.when(jnp.logical_not(down_first | wide | thin))(lambda: wait_tiles(send.at[0], total))


def on_device(sizes, rhs, conductivity, fraction, region, flags):
    _, nx, ny, nz = rhs.shape
    planes = nx + 2 * PAD
    rows = ny + 8
    f32 = jnp.float32
    hbm = pl.BlockSpec(memory_space=pl.ANY)
    sides = 1 if sizes[1] == 2 else 2
    relays = []
    for count in (6 * nx, 6, 6, 24, 6, 5):
        relays += [pltpu.VMEM((count, 8, nz), f32), pltpu.VMEM((sides, count, 8, nz), f32)]
    return pl.pallas_call(
        functools.partial(kernel, sizes, nx, ny, nz),
        out_shape=pltpu.VMEM(rhs.shape, rhs.dtype),
        in_specs=[hbm] * 5,
        out_specs=pl.BlockSpec(memory_space=pltpu.VMEM),
        scratch_shapes=[
            pltpu.SMEM(conductivity.shape, f32),
            pltpu.VMEM(rhs.shape, f32),
            pltpu.VMEM(region.shape, jnp.int32),
            pltpu.VMEM(flags.shape, jnp.int32),
            pltpu.VMEM((6, planes, rows, nz), f32),
            pltpu.VMEM((6, 4, rows, nz), f32),
            pltpu.VMEM((3, ny, nz), f32),
            pltpu.VMEM((3, planes, rows, nz), f32),
            pltpu.VMEM((3, planes, rows, nz), f32),
            pltpu.VMEM((3, planes, rows, nz), f32),
            pltpu.VMEM((3, planes, rows, nz), f32),
            pltpu.VMEM((4, planes, rows, nz), f32),
            pltpu.VMEM((2, 2, ny, nz), f32),
            pltpu.VMEM((2, 2, ny, nz), f32),
            pltpu.VMEM((2, 2, ny // 2, nz), f32),
            pltpu.VMEM((2, 2, ny // 2, nz), f32),
            pltpu.VMEM((2, 8, nz), f32),
            pltpu.VMEM((sides, 2, 2, 8, nz), f32),
            pltpu.VMEM((2, 2, 8, nz), f32),
            pltpu.VMEM((sides, 2, 2, 8, nz), f32),
            pltpu.VMEM((5, ny, nz), f32),
            pltpu.VMEM((5, ny, nz), f32),
            pltpu.VMEM((6, rows, nz), f32),
            pltpu.VMEM((6, rows, nz), f32),
            pltpu.VMEM((6, rows, nz), f32),
            pltpu.VMEM((6, rows, nz), f32),
            *relays,
            pltpu.VMEM((320, 8, nz), f32),
            pltpu.SemaphoreType.DMA((2,)),
            pltpu.SemaphoreType.DMA((1,)),
            pltpu.SemaphoreType.DMA((13,)),
            pltpu.SemaphoreType.REGULAR((2,)),
        ],
        compiler_params=pltpu.CompilerParams(
            collective_id=0, has_side_effects=True, vmem_limit_bytes=60 * 1024 * 1024
        ),
    )(conductivity, rhs, fraction, region, flags)


def solution(mesh):
    sizes = tuple(mesh.shape[name] for name in ("gx", "gy", "gz"))
    return jax.shard_map(
        functools.partial(on_device, sizes),
        mesh=mesh,
        in_specs=(
            P(None, "gx", "gy", "gz"),
            P(),
            P(None, "gx", "gy", "gz"),
            P("gx", "gy", "gz"),
            P(None, "gx", "gy", "gz"),
        ),
        out_specs=P(None, "gx", "gy", "gz"),
        check_vma=False,
    )
```

```python
import functools
import math

import jax
import jax.numpy as jnp
from jax import lax
from jax.experimental import pallas as pl
from jax.experimental.pallas import tpu as pltpu
from jax.sharding import PartitionSpec as P

damping = 0.8
c_node = 0.8 / 7.0
MESH = pl.DeviceIdType.MESH
PAD = 2
SEG = 16


def rot(v, shift, axis):
    return pltpu.roll(v, shift % v.shape[axis], axis)


def y_up(v):
    return rot(v, -1, 0)


def y_down(v):
    return rot(v, 1, 0)


def z_up(v):
    return rot(v, -1, 1)


def z_down(v):
    return rot(v, 1, 1)


def face_zero(u1, u2):
    return (y_up(u2) - u2) - (z_up(u1) - u1)


def face_one(u0, u2, u2p):
    return (z_up(u0) - u0) - (u2p - u2)


def face_two(u0, u1, u1p):
    return (u1p - u1) - (y_up(u0) - u0)


def edges(f0, f1, f2, f1m, f2m):
    return (
        (z_down(f1) - f1) - (y_down(f2) - f2),
        (f2m - f2) - (z_down(f0) - f0),
        (y_down(f0) - f0) - (f1m - f1),
    )


def jacobi_scale(ks):
    return jnp.where(ks > 0.0, damping / (4.0 + ks), 0.0)


def next_iter(rhs, ks, scale, u, cc):
    return u + scale * (rhs - (cc + ks * u))


def masked_residual(rhs, ks, u, cc):
    return jnp.where(ks > 0.0, rhs - (cc + ks * u), 0.0)


def nodal_rhs(m0, m0m, m1, m2):
    m1m, m2m = y_down(m1), z_down(m2)
    return (
        (m0m - m0) + (m1m - m1) + (m2m - m2),
        (m0 + m0m) * 0.5,
        (m1 + m1m) * 0.5,
        (m2 + m2m) * 0.5,
    )


def nodal_step(r, rm, rp):
    around = (rm + rp) + (y_up(r) + y_down(r)) + (z_up(r) + z_down(r))
    return (1.2 * c_node) * r + (c_node * c_node) * around


def finish(rhs, ks, u, corr):
    fixed = damping * rhs
    fixed = fixed + damping * (rhs - fixed)
    return jnp.where(ks > 0.0, u + corr, fixed)


def kernel(
    sizes, nx, ny, nz, cond_hbm, rhs_hbm, frac_hbm, reg_hbm, flag_hbm, out_ref,
    cond, frac_ref, reg_ref, flag_ref,
    e, st, sw, jac, u1, u2, mm, rr, zs, zr, ds, dr, dx_out, dx_in, zx_out, zx_in, ends_out, ends_in, lower_out, lower_in, upper_out, upper_in,
    ya_out, ya_in, yb_out, yb_in, yc_out, yc_in, yd_out, yd_in, ye_out, ye_in, yf_out, yf_in,
    blank, load, send, recv, near,
):
    gx, gy, gz = sizes
    pos = {"gx": lax.axis_index("gx"), "gy": lax.axis_index("gy"), "gz": lax.axis_index("gz")}
    size = {"gx": gx, "gy": gy, "gz": gz}
    first, last = PAD, PAD + nx - 1
    scope = jax.named_scope

    def device(**steps):
        return {axis: lax.rem(pos[axis] + (step + size[axis]), size[axis]) for axis, step in steps.items()}

    steps = [(x, z) for z in (1, -1) for x in (0, 1, -1)]
    paired = gy == 2
    barrier = pltpu.get_barrier_semaphore()

    def greet(*devices):
        for one in devices:
            pl.semaphore_signal(barrier, inc=1, device_id=one, device_id_type=MESH)

    def on(core, **steps):
        return {**device(**steps), "gy": core}

    if paired:
        greet(on(1, gx=1), on(1, gx=-1))
        greet(device(gy=1))
        greet(*(on(0, gx=x, gz=z) for x, z in steps))
    else:
        greet(device(gx=1), device(gx=-1), device(gy=1), device(gy=-1), *(device(gx=x, gz=z) for x, z in steps))
        greet(*(device(gx=x, gy=y, gz=z) for x, z in steps for y in (1, -1)))
    own_rows = pl.ds(0, ny)
    loads = [
        pltpu.make_async_copy(src, dst, load.at[i])
        for src, dst, i in (
            (cond_hbm, cond, 1), (reg_hbm, reg_ref, 0),
            *((flag_hbm.at[k], flag_ref.at[k], 0) for k in range(3)),
            *((frac_hbm.at[k], frac_ref.at[k], 0) for k in range(3)),
            *((rhs_hbm.at[k], e.at[k, pl.ds(first, nx), own_rows], 0) for k in range(3)),
        )
    ]

    def tiles_of(count):
        return blank.at[pl.ds(0, count)]

    def wait_tiles(semaphore, count):
        pltpu.make_async_copy(tiles_of(count), tiles_of(count), semaphore).wait()

    with scope("load"):
        for one in loads:
            one.start()
        loads[0].wait()
        wait_tiles(load.at[0], 10 * nx * ny // 8)

    hurry = (lax.rem(pos["gx"], 4) == 3) & (pos["gz"] == gz - 1)

    def far_collect():
        pl.semaphore_wait(barrier, 1 + 2 * len(steps))
        pl.semaphore_signal(near.at[1], inc=1, device_id=device(gy=1), device_id_type=MESH)

    if paired:
        pl.when((pos["gy"] == 0) & hurry)(lambda: far_collect())

    sent_tiles = []

    def copy(group, src, dst, where, start=True):
        made = pltpu.make_async_remote_copy(
            src_ref=src, dst_ref=dst, send_sem=send.at[0], recv_sem=recv.at[group],
            device_id=where, device_id_type=MESH,
        )
        sent_tiles.append(math.prod(src.shape) // (8 * nz))
        if start:
            made.start()
        return made

    def arrived(group, count):
        wait_tiles(recv.at[group], count)

    row = lax.broadcasted_iota(jnp.int32, (8, nz), 0)
    top, bottom, halo = slice(0, 8), slice(ny - 8, ny), slice(ny, ny + 8)

    def y_start(group, places, out, into):
        for i, (ref, where) in enumerate(places):
            out[i] = jnp.where(row < 4, ref[(*where, top, slice(None))], ref[(*where, bottom, slice(None))])
        if gy == 2:
            copy(group, out, into.at[0], device(gy=1))
        else:
            copy(group, out, into.at[0], device(gy=-1))
            copy(group, out, into.at[1], device(gy=1))

    def y_finish(group, places, into):
        arrived(group, into.shape[0] * len(places))
        for i, (ref, where) in enumerate(places):
            tile = into[0, i] if gy == 2 else jnp.where(row < 4, into[0, i], into[1, i])
            ref[(*where, halo, slice(None))] = tile

    lane = lax.broadcasted_iota(jnp.int32, (ny, nz), 1)
    slot = lane // SEG
    half = nz // 2
    low_half = lane < half
    quad = (lane % SEG) // 4
    unit = (lane % SEG) // 3
    fourth = ((0, 6), (3, 7))
    spare = ((0, 3, 0), (1, 3, 3), (2, 3, 4), (nx - 2, 4, 0), (nx - 1, 4, 1))
    left = (lane % SEG) < 8

    def end_piece(v, j):
        return rot(v, 8 + SEG * j, 1)

    def pick(base, where, other):
        return other if base is None else jnp.where(where, other, base)

    z_copies = [copy(10 - 9 * i, zs.at[i], zr.at[i], device(gz=2 * i - 1), False) for i in range(2)]
    corner_copies = [
        copy(10 - 9 * zside, ds.at[side, zside], dr.at[side, zside], device(gx=1 - 2 * side, gz=2 * zside - 1), False)
        for side in range(2) for zside in range(2)
    ]
    cross_copies = [
        [
            copy(10 - 9 * zside, dx_out.at[zside], dx_in.at[i, side, zside], device(gx=1 - 2 * side, gy=2 * i - 1, gz=2 * zside - 1), False)
            for side in range(2) for i in range(1 if paired else 2)
        ] + [
            copy(10 - 9 * zside, zx_out.at[zside], zx_in.at[i, zside], device(gy=2 * i - 1, gz=2 * zside - 1), False)
            for i in range(1 if paired else 2)
        ]
        for zside in range(2)
    ]

    def start(*copies):
        for one in copies:
            one.start()

    def start_far(zside):
        start(corner_copies[zside], corner_copies[2 + zside], z_copies[zside])

    def start_both():
        for zside in (1, 0):
            start_far(zside)
            start(*cross_copies[zside])

    packs = [None] * 6
    with scope("pack"):
        for x in range(nx):
            region = reg_ref[x]
            sigma = jnp.zeros((ny, nz), jnp.float32)
            for number in range(cond.shape[0]):
                sigma = jnp.where(region == number, cond[number], sigma)
            for k in range(3):
                ks = jnp.where(flag_ref[k, x] == 0, sigma * frac_ref[k, x], 0.0)
                e[3 + k, first + x, 0:ny, :] = ks
                for f, v in ((k, e[k, first + x, 0:ny, :]), (3 + k, ks)):
                    packs[f] = pick(packs[f], slot == x, end_piece(v, x))
        starts = [jacobi_scale(packs[3 + k]) * packs[k] for k in range(3)]
        for side, off in ((1, 4), (0, 8)):
            tiles = [None, None]
            for f in range(6):
                tiles[f // 4] = pick(tiles[f // 4], quad == f % 4, rot(packs[f], 4 * (f % 4) - off, 1))
            for i in range(2):
                zs[side, i] = tiles[i]
                zx_out[side, i] = jnp.where(row < 4, tiles[i][0:8], tiles[i][ny - 8:ny])
            off = 8 - 3 * side
            tile = None
            for f in range(5):
                tile = pick(tile, unit == f, rot(packs[f], 3 * f - off, 1))
            for k in range(3):
                outer = (slot == nx - 3) if k == 0 else (slot == 3) | (slot == nx - 3)
                tile = pick(tile, outer & (unit == k), rot(starts[k], 3 * k - off, 1))
            for at, to, u in spare:
                tile = pick(tile, (slot == to) & (unit == u), rot(packs[5], SEG * (to - at) + 3 * u - off, 1))
            if side == 0:
                for f, to in fourth:
                    tile = pick(tile, (slot == 4) & (lane % SEG == to), rot(packs[f], SEG * (4 - (nx - 1)) + to - 11, 1))
            upper, lower = tile[0:ny // 2], tile[ny // 2:ny]
            ds[0, side] = jnp.where(low_half[0:ny // 2], rot(upper, half, 1), lower)
            ds[1, side] = jnp.where(low_half[0:ny // 2], upper, rot(lower, half, 1))
            dx_out[side] = jnp.where(row < 4, tile[0:8], tile[ny - 8:ny])
            if paired:
                @pl.when(hurry)
                def _():
                    if side == 1:
                        pl.when(pos["gy"] == 1)(lambda: pl.semaphore_wait(near.at[1], 1))
                    start_far(side)
                    start(*cross_copies[side])

        moves = (
            [(packs[f], 0, 8 * (f // 2) + 3 * (f % 2), 3) for f in range(6)] + [(starts[k], 3, 5 + k, 1) for k in (1, 2)],
            [(packs[f], nx - 2, 2 * f, 2) for f in range(6)] + [(starts[k], nx - 3, 12 + k, 1) for k in range(3)],
        )
        for side in range(2):
            tiles = [None, None, None]
            for v, at, to, wide in moves[side]:
                t, to = divmod(to, 8)
                tiles[t] = pick(tiles[t], (slot >= to) & (slot < to + wide), rot(v, SEG * (to - at), 1))
            for i in range(3 - side):
                ends_out[3 * side + i] = tiles[i]

    with scope("barrierwait"):
        if paired:
            @pl.when(pos["gy"] == 1)
            def _():
                pl.semaphore_wait(barrier, 5)
                pl.semaphore_signal(near.at[0], inc=1, device_id=device(gy=1), device_id_type=MESH)

            @pl.when(pos["gy"] == 0)
            def _():
                pl.semaphore_wait(near.at[0], 1)
        else:
            pl.semaphore_wait(barrier, 4 + 3 * len(steps))

    def far_wait():
        if not paired:
            return
        pl.when(pos["gy"] == 0)(lambda: far_collect())

        @pl.when(pos["gy"] == 1)
        def _():
            pl.semaphore_wait(near.at[1], 1)

    own = [(e, (f, p)) for f in range(6) for p in range(first, last + 1)]
    y_start(0, own, ya_out, ya_in)

    up, down = device(gx=1), device(gx=-1)
    ends_copies = [copy(12, ends_out.at[pl.ds(0, 3)], ends_in.at[pl.ds(0, 3)], down, False), copy(12, ends_out.at[pl.ds(3, 2)], ends_in.at[pl.ds(3, 2)], up, False)]
    raw_copies = [
        copy(2, e.at[:, first, own_rows], e.at[:, last + 1, own_rows], down, False),
        copy(3, e.at[:, last, own_rows], e.at[:, first - 1, own_rows], up, False),
    ]
    late_copies = [
        copy(4, upper_out.at[pl.ds(0, 4)], upper_in.at[pl.ds(0, 4)], down, False),
        copy(5, lower_out.at[:, own_rows], lower_in.at[:, own_rows], up, False),
    ]
    wide_copy = pltpu.make_async_remote_copy(
        src_ref=lower_out, dst_ref=lower_in, send_sem=send.at[0], recv_sem=recv.at[5],
        device_id=up, device_id_type=MESH,
    )
    thin_copies = [
        pltpu.make_async_remote_copy(
            src_ref=src, dst_ref=dst, send_sem=send.at[0], recv_sem=recv.at[4], device_id=down, device_id_type=MESH
        )
        for src, dst in (
            (upper_out.at[pl.ds(0, 4), own_rows], upper_in.at[pl.ds(0, 4), own_rows]),
            (e.at[4, first + 1, own_rows], e.at[4, last + 2, own_rows]),
        )
    ]
    last_copy = copy(9, upper_out.at[pl.ds(4, 2), own_rows], upper_in.at[pl.ds(4, 2), own_rows], down, False)
    mask_copies = [
        copy(4, e.at[4, first + 1], e.at[4, last + 2], down, False),
        copy(4, e.at[5, first + 1, own_rows], e.at[5, last + 2, own_rows], down, False),
    ]
    uneven = (pos["gz"] == 0) & (pos["gx"] >= gx % 4 * gx)
    down_first = (lax.rem(pos["gx"], 4) == 1) & uneven
    wide = (lax.rem(device(gx=-1)["gx"], 4) == 1) & uneven
    narrow = jnp.logical_not(wide)
    thin = (lax.rem(device(gx=1)["gx"], 4) == 1) & uneven

    def in_order(begin):
        pl.when(down_first)(lambda: begin(0, 1))
        pl.when(jnp.logical_not(down_first))(lambda: begin(1, 0))

    late_start = pos["gz"] == 0
    in_order(lambda a, b: start(ends_copies[a], ends_copies[b]))

    up_only = lax.rem(pos["gx"], 4) == 3
    pl.when(jnp.logical_not(up_only))(lambda: start(raw_copies[0]))
    pl.when(jnp.logical_not(down_first))(lambda: start(raw_copies[1]))

    @pl.when(jnp.logical_not(late_start | (hurry if paired else late_start)))
    def _():
        with scope("nearwait"):
            far_wait()
            start_both()


    def faces(u, p):
        v0, v1, v2 = u[0, p], u[1, p], u[2, p]
        return face_one(v0, v2, u[2, p + 1]), face_two(v0, v1, u[1, p + 1])

    def curl_sweep(u, before, lo, hi, emit, after=None):
        f1m, f2m = before
        for p in range(lo, hi):
            f1, f2 = faces(u, p) if after is None or p < hi - 1 else after
            f0 = face_zero(u[1, p], u[2, p])
            cc = edges(f0, f1, f2, f1m, f2m)
            for k in range(3):
                emit(k, p, cc[k])
            f1m, f2m = f1, f2

    def emit_second(k, p, cc):
        u2[k, p] = next_iter(e[k, p], e[3 + k, p], jac[k, p], u1[k, p], cc)

    def emit_masked(k, p, cc):
        mm[k, p] = masked_residual(e[k, p], e[3 + k, p], u2[k, p], cc)

    def emit_rest(k, p, cc):
        if k > 0 or p != first + 1:
            emit_masked(k, p, cc)

    def node_range(lo, hi):
        for p in range(lo, hi):
            r = nodal_rhs(mm[0, p], mm[0, p - 1], mm[1, p], mm[2, p])
            for q in range(4):
                rr[q, p] = r[q]

    def first_range(lo, hi):
        for p in range(lo, hi):
            for k in range(3):
                scale = jacobi_scale(e[3 + k, p])
                jac[k, p] = scale
                u1[k, p] = scale * e[k, p]

    def below(v, p):
        up0 = v[0, p]
        return (z_up(up0) - up0) + v[2, p], v[1, p] + (y_up(up0) - up0)

    with scope("y1"):
        y_finish(0, own, ya_in)
    with scope("inner"):
        first_range(first, last + 1)
        curl_sweep(u1, faces(u1, first), first + 1, last, emit_second)
        p = last - 1
        sent = (*below(u1, p), e[3, p], *below(u2, p), e[0, p] - e[3, p] * u2[0, p])
        for i, v in enumerate(sent):
            lower_out[i] = v
        p = first + 1
        f1, f2 = faces(u2, p)
        cc = edges(face_zero(u2[1, p], u2[2, p]), f1, f2, -u2[2, p], u2[1, p])
        m0, m1, m2 = [masked_residual(e[k, p], e[3 + k, p], u2[k, p], cc[k]) for k in range(3)]
        mm[0, p] = m0
        sent = (u1[1, p], u1[2, p], u2[1, p], u2[2, p], m0, (y_down(m1) - m1) + (z_down(m2) - m2))
        for i, v in enumerate(sent):
            upper_out[i] = v
    @pl.when(down_first)
    def _():
        start(mask_copies[1], *thin_copies, last_copy, raw_copies[1], wide_copy)

    @pl.when(up_only)
    def _():
        start(late_copies[1], raw_copies[0], *mask_copies, late_copies[0], last_copy)

    @pl.when(jnp.logical_not(down_first | up_only))
    def _():
        start(late_copies[1], *mask_copies, late_copies[0], last_copy)

    with scope("inner2"):
        curl_sweep(u2, faces(u2, first + 1), first + 2, last - 1, emit_masked)
        node_range(first + 2, last - 1)

    @pl.when(late_start)
    def _():
        with scope("nearwait"):
            far_wait()
            start_both()

    def relay(name, groups, relayed, places, out, into):
        with scope(name):
            for group, count in groups:
                arrived(group, count * ny // 8)
            y_start(relayed, places, out, into)

    raw_up = [(e, (f, last + 1)) for f in range(6)]
    raw_low = [(e, (f, first - 1)) for f in range(6)]
    late_low = [(lower_in, (i,)) for i in range(6)]
    strip_tiles = [(st, (f, t)) for f in range(6) for t in range(4)]

    inner = (lane >= 4) & (lane < nz - 4)

    def node_at(p, count=4):
        return [nodal_step(rr[q, p], rr[q, p - 1], rr[q, p + 1]) for q in range(count)]

    def outputs(lo, hi):
        s_next = node_at(lo)
        for p in range(lo, hi):
            s = s_next
            s_next = node_at(p + 1, 4 if p + 1 < hi else 2)
            corr = (
                (s_next[0] - s[0]) + (s[1] + s_next[1]) * 0.5,
                (y_up(s[0]) - s[0]) + (s[2] + y_up(s[2])) * 0.5,
                (z_up(s[0]) - s[0]) + (s[3] + z_up(s[3])) * 0.5,
            )
            for k in range(3):
                body = finish(e[k, p, 0:ny], e[3 + k, p, 0:ny], u2[k, p, 0:ny], corr[k][0:ny])
                ends = rot(sw[k], nz - 8 - SEG * (p - first), 1)
                out_ref[k, p - first] = jnp.where(inner, body, ends)

    lane24 = lax.broadcasted_iota(jnp.int32, (ny + 8, nz), 1)
    slot24 = lane24 // SEG
    left24 = (lane24 % SEG) < 8

    span = range(2)

    def x_up(vs):
        rs = [rot(v, -SEG, 1) for v in vs]
        return [jnp.where(lane24 < nz - SEG, rs[t], rs[t ^ 1]) for t in span]

    def x_down(vs):
        rs = [rot(v, SEG, 1) for v in vs]
        return [jnp.where(lane24 >= SEG, rs[t], rs[t ^ 1]) for t in span]

    def strip_curl(u):
        u1p, u2p = x_up(u[1]), x_up(u[2])
        f1 = [face_one(u[0][t], u[2][t], u2p[t]) for t in span]
        f2 = [face_two(u[0][t], u[1][t], u1p[t]) for t in span]
        f0 = [face_zero(u[1][t], u[2][t]) for t in span]
        f1m, f2m = x_down(f1), x_down(f2)
        out = [edges(f0[t], f1[t], f2[t], f1m[t], f2m[t]) for t in span]
        return [[out[t][k] for t in span] for k in range(3)]

    def strips(base):
        sr = [[st[k, 2 * base + t] for t in span] for k in range(3)]
        sk = [[st[3 + k, 2 * base + t] for t in span] for k in range(3)]
        outer = (slot24 == 3) | (slot24 == nx - 3)
        scale = [[jacobi_scale(sk[k][t]) for t in span] for k in range(3)]
        u = [[scale[k][t] * sr[k][t] for t in span] for k in range(3)]
        for k in range(3):
            u[k][1] = jnp.where(outer, sr[k][1], u[k][1])
        cc = strip_curl(u)
        u = [[next_iter(sr[k][t], sk[k][t], scale[k][t], u[k][t], cc[k][t]) for t in span] for k in range(3)]
        cc = strip_curl(u)
        m = [[masked_residual(sr[k][t], sk[k][t], u[k][t], cc[k][t]) for t in span] for k in range(3)]
        m0m = x_down(m[0])
        r = [nodal_rhs(m[0][t], m0m[t], m[1][t], m[2][t]) for t in span]
        s = []
        for q in range(4):
            rq = [r[t][q] for t in span]
            rm, rp = x_down(rq), x_up(rq)
            s.append([nodal_step(rq[t], rm[t], rp[t]) if q < 2 or t % 2 == 0 else None for t in span])
        s0p, s1p = x_up(s[0]), x_up(s[1])
        s0, s1, s2, s3 = [s[q][0] for q in range(4)]
        corr = (
            (s0p[0] - s0) + (s1 + s1p[0]) * 0.5,
            (y_up(s0) - s0) + (s2 + y_up(s2)) * 0.5,
            (z_up(s0) - s0) + (s3 + z_up(s3)) * 0.5,
        )
        for k in range(3):
            result = finish(sr[k][0], sk[k][0], u[k][0], corr[k])[0:ny]
            sw[k] = result if base == 0 else jnp.where(left, sw[k], result)

    def corner_of(f, tile, off):
        if f < 5:
            piece = rot(tile, off - 3 * f, 1)
            for k, to in fourth:
                if off == 8 and k == f:
                    at = ((slot == nx - 1) & (lane % SEG == 11))[0:tile.shape[0]]
                    piece = jnp.where(at, rot(tile, SEG * (nx - 1 - 4) + 11 - to, 1), piece)
            return piece
        piece = None
        for at, to, u in spare:
            piece = pick(piece, slot[0:tile.shape[0]] == at, rot(tile, SEG * (at - to) + off - 3 * u, 1))
        return piece

    with scope("endswait"):
        arrived(12, 5 * ny // 8)
    with scope("strippack"):
        for f in range(6):
            t, to = divmod(2 * f, 8)
            piece = rot(ends_in[f // 2], SEG * (0 - 3 * (f % 2)), 1)
            piece = jnp.where(slot >= nx - 2, rot(ends_in[3 + t], SEG * (nx - 2 - to), 1), piece)
            if f < 3:
                piece = jnp.where(slot == 3, rot(ends_in[0], SEG * (3 - (5 + f)), 1), piece)
                piece = jnp.where(slot == nx - 3, rot(ends_in[4], SEG * (nx - 3 - (4 + f)), 1), piece)
            mid = packs[f]
            st[f, 0, 0:ny, :] = mid
            st[f, 1, 0:ny, :] = piece
            st[f, 2, 0:ny, :] = mid
            st[f, 3, 0:ny, :] = piece
        y_start(8, strip_tiles, yd_out, yd_in)


    def crossed(ref, *where):
        if paired:
            return ref[(0, *where)]
        return jnp.where(row < 4, ref[(0, *where)], ref[(1, *where)])

    def strip_inputs(base):
        with scope("ystrip"):
            if base == 0:
                y_finish(8, strip_tiles, yd_in)
            arrived(10 - 9 * base, 2 * ny // 8 + 2 * (ny // 2) // 8 + 4 * dx_in.shape[0])
            off = 8 - 4 * base
            minus, plus = dr[0, base], dr[1, base]
            low = low_half[0:ny // 2]
            own_corner = jnp.concatenate(
                [jnp.where(low, plus, rot(minus, half, 1)), jnp.where(low, rot(plus, half, 1), minus)], axis=0
            )
            cross_corner = jnp.where(low_half[0:8], crossed(dx_in, 1, base), crossed(dx_in, 0, base))
            for f in range(6):
                t, q = divmod(f, 4)
                for rows, tile, corner in (
                    (slice(0, ny), zr[base, t], own_corner), (halo, crossed(zx_in, base, t), cross_corner),
                ):
                    mine = left[0:tile.shape[0]] if base == 0 else ~left[0:tile.shape[0]]
                    for at, piece in ((2 * base, rot(tile, off - 4 * q, 1)), (2 * base + 1, corner_of(f, corner, 8 - 3 * base))):
                        st[f, at, rows, :] = jnp.where(mine, st[f, at, rows, :], piece)

    late_up = [(upper_in, (i,)) for i in range(4)] + [(e, (4, last + 2))]

    def lower_inputs():
        with scope("ylow"):
            pl.when(narrow)(lambda: y_finish(11, late_low, ye_in))
            pl.when(wide)(lambda: arrived(5, 6 * (ny + 8) // 8))

    def upper_inputs():
        with scope("yup"):
            pl.when(jnp.logical_not(thin))(lambda: arrived(4, (5 * (ny + 8) + ny) // 8))
            pl.when(thin)(lambda: y_finish(0, late_up, yf_in))
            arrived(9, 2 * ny // 8)

    def lower_side():
        with scope("lower"):
            p = first - 1
            curl_sweep(u1, (lower_in[0] - u1[2, p], u1[1, p] - lower_in[1]), p, first, emit_second)
            f1, f2 = lower_in[3] - u2[2, p], u2[1, p] - lower_in[4]
            cc = (z_down(f1) - f1) - (y_down(f2) - f2)
            mm[0, p - 1] = jnp.where(lower_in[2] > 0.0, lower_in[5] - cc, 0.0)
            curl_sweep(u2, (f1, f2), p, first + 1, emit_masked)
            node_range(p, first + 2)

    def upper_side():
        with scope("upper"):
            p = last + 1
            f1 = face_one(u1[0, p], u1[2, p], upper_in[1])
            f2 = face_two(u1[0, p], u1[1, p], upper_in[0])
            curl_sweep(u1, faces(u1, last), p, p + 1, emit_second, (f1, f2))
            f1 = face_one(u2[0, p], u2[2, p], upper_in[3])
            f2 = face_two(u2[0, p], u2[1, p], upper_in[2])
            curl_sweep(u2, faces(u2, last - 1), last, p + 1, emit_masked, (f1, f2))
            node_range(last, p + 1)
            v0 = u2[0, p]
            q2 = jnp.where(e[4, p + 1] > 0.0, u2[1, p] + (y_up(v0) - v0), 0.0)
            q1 = jnp.where(e[5, p + 1] > 0.0, (z_up(v0) - v0) + u2[2, p], 0.0)
            m0, m0p = mm[0, p], upper_in[4]
            rr[0, p + 1] = (m0 - m0p) + (upper_in[5] + (y_down(q2) - q2) + (z_down(q1) - q1))
            rr[1, p + 1] = (m0p + m0) * 0.5

    def in_turn(*pieces):
        for piece in pieces:
            piece()

    def write_all():
        with scope("out"):
            outputs(first, last + 1)

    def side_strips(base):
        strip_inputs(base)
        with scope("strips"):
            strips(base)

    def raw_relays():
        del sent_tiles[counted:]
        relay("rawup", ((2, 6),), 6, raw_up, yb_out, yb_in)
        relay("rawlow", ((3, 6),), 7, raw_low, yc_out, yc_in)

    counted = len(sent_tiles)
    strips_first = lax.rem(device(gx=1)["gx"], 4) == 3
    pl.when(jnp.logical_not(strips_first))(lambda: raw_relays())
    side_strips(0)
    pl.when(strips_first)(lambda: raw_relays())

    @pl.when(narrow)
    def _():
        relay("latelow", ((5, 6),), 11, late_low, ye_out, ye_in)

    base_tiles = sum(sent_tiles)

    @pl.when(thin)
    def _():
        relay("lateup", ((4, 6),), 0, late_up, yf_out, yf_in)

    def raw_sides():
        with scope("yraw"):
            y_finish(7, raw_low, yc_in)
            y_finish(6, raw_up, yb_in)
        with scope("rawsides"):
            first_range(first - 1, first)
            first_range(last + 1, last + 2)
            curl_sweep(u1, faces(u1, first - 1), first, first + 1, emit_second)
            curl_sweep(u1, faces(u1, last - 1), last, last + 1, emit_second)
            curl_sweep(u2, faces(u2, first), first + 1, first + 2, emit_rest)
            curl_sweep(u2, faces(u2, last - 2), last - 1, last, emit_masked)
            node_range(last - 1, last)

    pl.when(thin)(raw_sides)
    side_strips(1)
    pl.when(jnp.logical_not(thin))(raw_sides)
    in_turn(lower_inputs, upper_inputs, lower_side, upper_side, write_all)
    with scope("sendwait"):
        total = base_tiles
        sides = dx_in.shape[0]
        pl.when(down_first)(lambda: wait_tiles(send.at[0], total + 1))
        pl.when(wide)(lambda: wait_tiles(send.at[0], total - 6 * sides))
        pl.when(thin)(lambda: wait_tiles(send.at[0], total + 5 * sides))
        pl.when(jnp.logical_not(down_first | wide | thin))(lambda: wait_tiles(send.at[0], total))


def on_device(sizes, rhs, conductivity, fraction, region, flags):
    _, nx, ny, nz = rhs.shape
    planes = nx + 2 * PAD
    rows = ny + 8
    f32 = jnp.float32
    hbm = pl.BlockSpec(memory_space=pl.ANY)
    sides = 1 if sizes[1] == 2 else 2
    relays = []
    for count in (6 * nx, 6, 6, 24, 6, 5):
        relays += [pltpu.VMEM((count, 8, nz), f32), pltpu.VMEM((sides, count, 8, nz), f32)]
    return pl.pallas_call(
        functools.partial(kernel, sizes, nx, ny, nz),
        out_shape=pltpu.VMEM(rhs.shape, rhs.dtype),
        in_specs=[hbm] * 5,
        out_specs=pl.BlockSpec(memory_space=pltpu.VMEM),
        scratch_shapes=[
            pltpu.SMEM(conductivity.shape, f32),
            pltpu.VMEM(rhs.shape, f32),
            pltpu.VMEM(region.shape, jnp.int32),
            pltpu.VMEM(flags.shape, jnp.int32),
            pltpu.VMEM((6, planes, rows, nz), f32),
            pltpu.VMEM((6, 4, rows, nz), f32),
            pltpu.VMEM((3, ny, nz), f32),
            pltpu.VMEM((3, planes, rows, nz), f32),
            pltpu.VMEM((3, planes, rows, nz), f32),
            pltpu.VMEM((3, planes, rows, nz), f32),
            pltpu.VMEM((3, planes, rows, nz), f32),
            pltpu.VMEM((4, planes, rows, nz), f32),
            pltpu.VMEM((2, 2, ny, nz), f32),
            pltpu.VMEM((2, 2, ny, nz), f32),
            pltpu.VMEM((2, 2, ny // 2, nz), f32),
            pltpu.VMEM((2, 2, ny // 2, nz), f32),
            pltpu.VMEM((2, 8, nz), f32),
            pltpu.VMEM((sides, 2, 2, 8, nz), f32),
            pltpu.VMEM((2, 2, 8, nz), f32),
            pltpu.VMEM((sides, 2, 2, 8, nz), f32),
            pltpu.VMEM((5, ny, nz), f32),
            pltpu.VMEM((5, ny, nz), f32),
            pltpu.VMEM((6, rows, nz), f32),
            pltpu.VMEM((6, rows, nz), f32),
            pltpu.VMEM((6, rows, nz), f32),
            pltpu.VMEM((6, rows, nz), f32),
            *relays,
            pltpu.VMEM((320, 8, nz), f32),
            pltpu.SemaphoreType.DMA((2,)),
            pltpu.SemaphoreType.DMA((1,)),
            pltpu.SemaphoreType.DMA((13,)),
            pltpu.SemaphoreType.REGULAR((2,)),
        ],
        compiler_params=pltpu.CompilerParams(
            collective_id=0, has_side_effects=True, vmem_limit_bytes=60 * 1024 * 1024
        ),
    )(conductivity, rhs, fraction, region, flags)


def solution(mesh):
    sizes = tuple(mesh.shape[name] for name in ("gx", "gy", "gz"))
    return jax.shard_map(
        functools.partial(on_device, sizes),
        mesh=mesh,
        in_specs=(
            P(None, "gx", "gy", "gz"),
            P(),
            P(None, "gx", "gy", "gz"),
            P("gx", "gy", "gz"),
            P(None, "gx", "gy", "gz"),
        ),
        out_specs=P(None, "gx", "gy", "gz"),
        check_vma=False,
    )
```

```python
import functools
import math

import jax
import jax.numpy as jnp
from jax import lax
from jax.experimental import pallas as pl
from jax.experimental.pallas import tpu as pltpu
from jax.sharding import PartitionSpec as P

damping = 0.8
c_node = 0.8 / 7.0
MESH = pl.DeviceIdType.MESH
PAD = 2
SEG = 16


def rot(v, shift, axis):
    return pltpu.roll(v, shift % v.shape[axis], axis)


def y_up(v):
    return rot(v, -1, 0)


def y_down(v):
    return rot(v, 1, 0)


def z_up(v):
    return rot(v, -1, 1)


def z_down(v):
    return rot(v, 1, 1)


def face_zero(u1, u2):
    return (y_up(u2) - u2) - (z_up(u1) - u1)


def face_one(u0, u2, u2p):
    return (z_up(u0) - u0) - (u2p - u2)


def face_two(u0, u1, u1p):
    return (u1p - u1) - (y_up(u0) - u0)


def edges(f0, f1, f2, f1m, f2m):
    return (
        (z_down(f1) - f1) - (y_down(f2) - f2),
        (f2m - f2) - (z_down(f0) - f0),
        (y_down(f0) - f0) - (f1m - f1),
    )


def jacobi_scale(ks):
    return jnp.where(ks > 0.0, damping / (4.0 + ks), 0.0)


def next_iter(rhs, ks, scale, u, cc):
    return u + scale * (rhs - (cc + ks * u))


def masked_residual(rhs, ks, u, cc):
    return jnp.where(ks > 0.0, rhs - (cc + ks * u), 0.0)


def nodal_rhs(m0, m0m, m1, m2):
    m1m, m2m = y_down(m1), z_down(m2)
    return (
        (m0m - m0) + (m1m - m1) + (m2m - m2),
        (m0 + m0m) * 0.5,
        (m1 + m1m) * 0.5,
        (m2 + m2m) * 0.5,
    )


def nodal_step(r, rm, rp):
    around = (rm + rp) + (y_up(r) + y_down(r)) + (z_up(r) + z_down(r))
    return (1.2 * c_node) * r + (c_node * c_node) * around


def finish(rhs, ks, u, corr):
    fixed = damping * rhs
    fixed = fixed + damping * (rhs - fixed)
    return jnp.where(ks > 0.0, u + corr, fixed)


def kernel(
    sizes, nx, ny, nz, cond_hbm, rhs_hbm, frac_hbm, reg_hbm, flag_hbm, out_ref,
    cond, frac_ref, reg_ref, flag_ref,
    e, st, sw, jac, u1, u2, mm, rr, zs, zr, ds, dr, dx_out, dx_in, zx_out, zx_in, ends_out, ends_in, lower_out, lower_in, upper_out, upper_in,
    ya_out, ya_in, yb_out, yb_in, yc_out, yc_in, yd_out, yd_in, ye_out, ye_in, yf_out, yf_in,
    blank, load, send, recv, near,
):
    gx, gy, gz = sizes
    pos = {"gx": lax.axis_index("gx"), "gy": lax.axis_index("gy"), "gz": lax.axis_index("gz")}
    size = {"gx": gx, "gy": gy, "gz": gz}
    first, last = PAD, PAD + nx - 1
    scope = jax.named_scope

    def device(**steps):
        return {axis: lax.rem(pos[axis] + (step + size[axis]), size[axis]) for axis, step in steps.items()}

    steps = [(x, z) for z in (1, -1) for x in (0, 1, -1)]
    paired = gy == 2
    barrier = pltpu.get_barrier_semaphore()

    def greet(*devices):
        for one in devices:
            pl.semaphore_signal(barrier, inc=1, device_id=one, device_id_type=MESH)

    def on(core, **steps):
        return {**device(**steps), "gy": core}

    if paired:
        greet(on(1, gx=1), on(1, gx=-1))
        greet(device(gy=1))
        greet(*(on(0, gx=x, gz=z) for x, z in steps))
    else:
        greet(device(gx=1), device(gx=-1), device(gy=1), device(gy=-1), *(device(gx=x, gz=z) for x, z in steps))
        greet(*(device(gx=x, gy=y, gz=z) for x, z in steps for y in (1, -1)))
    own_rows = pl.ds(0, ny)
    loads = [
        pltpu.make_async_copy(src, dst, load.at[i])
        for src, dst, i in (
            (cond_hbm, cond, 1), (reg_hbm, reg_ref, 0),
            *((flag_hbm.at[k], flag_ref.at[k], 0) for k in range(3)),
            *((frac_hbm.at[k], frac_ref.at[k], 0) for k in range(3)),
            *((rhs_hbm.at[k], e.at[k, pl.ds(first, nx), own_rows], 0) for k in range(3)),
        )
    ]

    def tiles_of(count):
        return blank.at[pl.ds(0, count)]

    def wait_tiles(semaphore, count):
        pltpu.make_async_copy(tiles_of(count), tiles_of(count), semaphore).wait()

    with scope("load"):
        for one in loads:
            one.start()
        loads[0].wait()
        wait_tiles(load.at[0], 10 * nx * ny // 8)

    hurry = (lax.rem(pos["gx"], 4) == 3) & (pos["gz"] == gz - 1)

    def far_collect():
        pl.semaphore_wait(barrier, 1 + 2 * len(steps))
        pl.semaphore_signal(near.at[1], inc=1, device_id=device(gy=1), device_id_type=MESH)

    if paired:
        pl.when((pos["gy"] == 0) & hurry)(lambda: far_collect())

    sent_tiles = []

    def copy(group, src, dst, where, start=True):
        made = pltpu.make_async_remote_copy(
            src_ref=src, dst_ref=dst, send_sem=send.at[0], recv_sem=recv.at[group],
            device_id=where, device_id_type=MESH,
        )
        sent_tiles.append(math.prod(src.shape) // (8 * nz))
        if start:
            made.start()
        return made

    def arrived(group, count):
        wait_tiles(recv.at[group], count)

    row = lax.broadcasted_iota(jnp.int32, (8, nz), 0)
    top, bottom, halo = slice(0, 8), slice(ny - 8, ny), slice(ny, ny + 8)

    def y_start(group, places, out, into):
        for i, (ref, where) in enumerate(places):
            out[i] = jnp.where(row < 4, ref[(*where, top, slice(None))], ref[(*where, bottom, slice(None))])
        if gy == 2:
            copy(group, out, into.at[0], device(gy=1))
        else:
            copy(group, out, into.at[0], device(gy=-1))
            copy(group, out, into.at[1], device(gy=1))

    def y_finish(group, places, into):
        arrived(group, into.shape[0] * len(places))
        for i, (ref, where) in enumerate(places):
            tile = into[0, i] if gy == 2 else jnp.where(row < 4, into[0, i], into[1, i])
            ref[(*where, halo, slice(None))] = tile

    lane = lax.broadcasted_iota(jnp.int32, (ny, nz), 1)
    slot = lane // SEG
    half = nz // 2
    low_half = lane < half
    quad = (lane % SEG) // 4
    unit = (lane % SEG) // 3
    fourth = ((0, 6), (3, 7))
    spare = ((0, 3, 0), (1, 3, 3), (2, 3, 4), (nx - 2, 4, 0), (nx - 1, 4, 1))
    left = (lane % SEG) < 8

    def end_piece(v, j):
        return rot(v, 8 + SEG * j, 1)

    def pick(base, where, other):
        return other if base is None else jnp.where(where, other, base)

    z_copies = [copy(10 - 9 * i, zs.at[i], zr.at[i], device(gz=2 * i - 1), False) for i in range(2)]
    corner_copies = [
        copy(10 - 9 * zside, ds.at[side, zside], dr.at[side, zside], device(gx=1 - 2 * side, gz=2 * zside - 1), False)
        for side in range(2) for zside in range(2)
    ]
    cross_copies = [
        [
            copy(10 - 9 * zside, dx_out.at[zside], dx_in.at[i, side, zside], device(gx=1 - 2 * side, gy=2 * i - 1, gz=2 * zside - 1), False)
            for side in range(2) for i in range(1 if paired else 2)
        ] + [
            copy(10 - 9 * zside, zx_out.at[zside], zx_in.at[i, zside], device(gy=2 * i - 1, gz=2 * zside - 1), False)
            for i in range(1 if paired else 2)
        ]
        for zside in range(2)
    ]

    def start(*copies):
        for one in copies:
            one.start()

    def start_far(zside):
        start(corner_copies[zside], corner_copies[2 + zside], z_copies[zside])

    def start_both():
        for zside in (1, 0):
            start_far(zside)
            start(*cross_copies[zside])

    packs = [None] * 6
    with scope("pack"):
        for x in range(nx):
            region = reg_ref[x]
            sigma = jnp.zeros((ny, nz), jnp.float32)
            for number in range(cond.shape[0]):
                sigma = jnp.where(region == number, cond[number], sigma)
            for k in range(3):
                ks = jnp.where(flag_ref[k, x] == 0, sigma * frac_ref[k, x], 0.0)
                e[3 + k, first + x, 0:ny, :] = ks
                for f, v in ((k, e[k, first + x, 0:ny, :]), (3 + k, ks)):
                    packs[f] = pick(packs[f], slot == x, end_piece(v, x))
        starts = [jacobi_scale(packs[3 + k]) * packs[k] for k in range(3)]
        for side, off in ((0, 8), (1, 4)):
            tiles = [None, None]
            for f in range(6):
                tiles[f // 4] = pick(tiles[f // 4], quad == f % 4, rot(packs[f], 4 * (f % 4) - off, 1))
            for i in range(2):
                zs[side, i] = tiles[i]
                zx_out[side, i] = jnp.where(row < 4, tiles[i][0:8], tiles[i][ny - 8:ny])
            off = 8 - 3 * side
            tile = None
            for f in range(5):
                tile = pick(tile, unit == f, rot(packs[f], 3 * f - off, 1))
            for k in range(3):
                outer = (slot == nx - 3) if k == 0 else (slot == 3) | (slot == nx - 3)
                tile = pick(tile, outer & (unit == k), rot(starts[k], 3 * k - off, 1))
            for at, to, u in spare:
                tile = pick(tile, (slot == to) & (unit == u), rot(packs[5], SEG * (to - at) + 3 * u - off, 1))
            if side == 0:
                for f, to in fourth:
                    tile = pick(tile, (slot == 4) & (lane % SEG == to), rot(packs[f], SEG * (4 - (nx - 1)) + to - 11, 1))
            upper, lower = tile[0:ny // 2], tile[ny // 2:ny]
            ds[0, side] = jnp.where(low_half[0:ny // 2], rot(upper, half, 1), lower)
            ds[1, side] = jnp.where(low_half[0:ny // 2], upper, rot(lower, half, 1))
            dx_out[side] = jnp.where(row < 4, tile[0:8], tile[ny - 8:ny])
        if paired:
            @pl.when(hurry)
            def _():
                pl.when(pos["gy"] == 1)(lambda: pl.semaphore_wait(near.at[1], 1))
                start_both()

        moves = (
            [(packs[f], 0, 8 * (f // 2) + 3 * (f % 2), 3) for f in range(6)] + [(starts[k], 3, 5 + k, 1) for k in (1, 2)],
            [(packs[f], nx - 2, 2 * f, 2) for f in range(6)] + [(starts[k], nx - 3, 12 + k, 1) for k in range(3)],
        )
        for side in range(2):
            tiles = [None, None, None]
            for v, at, to, wide in moves[side]:
                t, to = divmod(to, 8)
                tiles[t] = pick(tiles[t], (slot >= to) & (slot < to + wide), rot(v, SEG * (to - at), 1))
            for i in range(3 - side):
                ends_out[3 * side + i] = tiles[i]

    with scope("barrierwait"):
        if paired:
            @pl.when(pos["gy"] == 1)
            def _():
                pl.semaphore_wait(barrier, 5)
                pl.semaphore_signal(near.at[0], inc=1, device_id=device(gy=1), device_id_type=MESH)

            @pl.when(pos["gy"] == 0)
            def _():
                pl.semaphore_wait(near.at[0], 1)
        else:
            pl.semaphore_wait(barrier, 4 + 3 * len(steps))

    def far_wait():
        if not paired:
            return
        pl.when(pos["gy"] == 0)(lambda: far_collect())

        @pl.when(pos["gy"] == 1)
        def _():
            pl.semaphore_wait(near.at[1], 1)

    own = [(e, (f, p)) for f in range(6) for p in range(first, last + 1)]
    y_start(0, own, ya_out, ya_in)

    up, down = device(gx=1), device(gx=-1)
    ends_copies = [copy(9, ends_out.at[pl.ds(0, 3)], ends_in.at[pl.ds(0, 3)], down, False), copy(9, ends_out.at[pl.ds(3, 2)], ends_in.at[pl.ds(3, 2)], up, False)]
    raw_copies = [
        copy(2, e.at[:, first, own_rows], e.at[:, last + 1, own_rows], down, False),
        copy(3, e.at[:, last, own_rows], e.at[:, first - 1, own_rows], up, False),
    ]
    late_copies = [
        copy(4, upper_out.at[pl.ds(0, 4)], upper_in.at[pl.ds(0, 4)], down, False),
        copy(5, lower_out.at[:, own_rows], lower_in.at[:, own_rows], up, False),
    ]
    wide_copy = pltpu.make_async_remote_copy(
        src_ref=lower_out, dst_ref=lower_in, send_sem=send.at[0], recv_sem=recv.at[5],
        device_id=up, device_id_type=MESH,
    )
    thin_copies = [
        pltpu.make_async_remote_copy(
            src_ref=src, dst_ref=dst, send_sem=send.at[0], recv_sem=recv.at[4], device_id=down, device_id_type=MESH
        )
        for src, dst in (
            (upper_out.at[pl.ds(0, 4), own_rows], upper_in.at[pl.ds(0, 4), own_rows]),
            (e.at[4, first + 1, own_rows], e.at[4, last + 2, own_rows]),
        )
    ]
    last_copy = copy(4, upper_out.at[pl.ds(4, 2), own_rows], upper_in.at[pl.ds(4, 2), own_rows], down, False)
    mask_copies = [
        copy(4, e.at[4, first + 1], e.at[4, last + 2], down, False),
        copy(4, e.at[5, first + 1, own_rows], e.at[5, last + 2, own_rows], down, False),
    ]
    uneven = (pos["gz"] == 0) & (pos["gx"] >= gx % 4 * gx)
    down_first = (lax.rem(pos["gx"], 4) == 1) & uneven
    wide = (lax.rem(device(gx=-1)["gx"], 4) == 1) & uneven
    narrow = jnp.logical_not(wide)
    thin = (lax.rem(device(gx=1)["gx"], 4) == 1) & uneven

    def in_order(begin):
        pl.when(down_first)(lambda: begin(0, 1))
        pl.when(jnp.logical_not(down_first))(lambda: begin(1, 0))

    late_start = pos["gz"] == 0
    in_order(lambda a, b: start(ends_copies[a], ends_copies[b]))

    up_only = lax.rem(pos["gx"], 4) == 3
    pl.when(jnp.logical_not(up_only))(lambda: start(raw_copies[0]))
    pl.when(jnp.logical_not(down_first))(lambda: start(raw_copies[1]))

    @pl.when(jnp.logical_not(late_start | (hurry if paired else late_start)))
    def _():
        with scope("nearwait"):
            far_wait()
            start_both()


    def faces(u, p):
        v0, v1, v2 = u[0, p], u[1, p], u[2, p]
        return face_one(v0, v2, u[2, p + 1]), face_two(v0, v1, u[1, p + 1])

    def curl_sweep(u, before, lo, hi, emit, after=None):
        f1m, f2m = before
        for p in range(lo, hi):
            f1, f2 = faces(u, p) if after is None or p < hi - 1 else after
            f0 = face_zero(u[1, p], u[2, p])
            cc = edges(f0, f1, f2, f1m, f2m)
            for k in range(3):
                emit(k, p, cc[k])
            f1m, f2m = f1, f2

    def emit_second(k, p, cc):
        u2[k, p] = next_iter(e[k, p], e[3 + k, p], jac[k, p], u1[k, p], cc)

    def emit_masked(k, p, cc):
        mm[k, p] = masked_residual(e[k, p], e[3 + k, p], u2[k, p], cc)

    def emit_rest(k, p, cc):
        if k > 0 or p != first + 1:
            emit_masked(k, p, cc)

    def node_range(lo, hi):
        for p in range(lo, hi):
            r = nodal_rhs(mm[0, p], mm[0, p - 1], mm[1, p], mm[2, p])
            for q in range(4):
                rr[q, p] = r[q]

    def first_range(lo, hi):
        for p in range(lo, hi):
            for k in range(3):
                scale = jacobi_scale(e[3 + k, p])
                jac[k, p] = scale
                u1[k, p] = scale * e[k, p]

    def below(v, p):
        up0 = v[0, p]
        return (z_up(up0) - up0) + v[2, p], v[1, p] + (y_up(up0) - up0)

    with scope("y1"):
        y_finish(0, own, ya_in)
    with scope("inner"):
        first_range(first, last + 1)
        curl_sweep(u1, faces(u1, first), first + 1, last, emit_second)
        p = last - 1
        sent = (*below(u1, p), e[3, p], *below(u2, p), e[0, p] - e[3, p] * u2[0, p])
        for i, v in enumerate(sent):
            lower_out[i] = v
        p = first + 1
        f1, f2 = faces(u2, p)
        cc = edges(face_zero(u2[1, p], u2[2, p]), f1, f2, -u2[2, p], u2[1, p])
        m0, m1, m2 = [masked_residual(e[k, p], e[3 + k, p], u2[k, p], cc[k]) for k in range(3)]
        mm[0, p] = m0
        sent = (u1[1, p], u1[2, p], u2[1, p], u2[2, p], m0, (y_down(m1) - m1) + (z_down(m2) - m2))
        for i, v in enumerate(sent):
            upper_out[i] = v
    @pl.when(down_first)
    def _():
        start(mask_copies[1], *thin_copies, last_copy, raw_copies[1], wide_copy)

    @pl.when(up_only)
    def _():
        start(late_copies[1], raw_copies[0], *mask_copies, late_copies[0], last_copy)

    @pl.when(jnp.logical_not(down_first | up_only))
    def _():
        start(late_copies[1], *mask_copies, late_copies[0], last_copy)

    with scope("inner2"):
        curl_sweep(u2, faces(u2, first + 1), first + 2, last - 1, emit_masked)
        node_range(first + 2, last - 1)

    @pl.when(late_start)
    def _():
        with scope("nearwait"):
            far_wait()
            start_both()

    def relay(name, groups, relayed, places, out, into):
        with scope(name):
            for group, count in groups:
                arrived(group, count * ny // 8)
            y_start(relayed, places, out, into)

    raw_up = [(e, (f, last + 1)) for f in range(6)]
    raw_low = [(e, (f, first - 1)) for f in range(6)]
    late_low = [(lower_in, (i,)) for i in range(6)]
    strip_tiles = [(st, (f, t)) for f in range(6) for t in range(4)]

    inner = (lane >= 4) & (lane < nz - 4)

    def node_at(p, count=4):
        return [nodal_step(rr[q, p], rr[q, p - 1], rr[q, p + 1]) for q in range(count)]

    def outputs(lo, hi):
        s_next = node_at(lo)
        for p in range(lo, hi):
            s = s_next
            s_next = node_at(p + 1, 4 if p + 1 < hi else 2)
            corr = (
                (s_next[0] - s[0]) + (s[1] + s_next[1]) * 0.5,
                (y_up(s[0]) - s[0]) + (s[2] + y_up(s[2])) * 0.5,
                (z_up(s[0]) - s[0]) + (s[3] + z_up(s[3])) * 0.5,
            )
            for k in range(3):
                body = finish(e[k, p, 0:ny], e[3 + k, p, 0:ny], u2[k, p, 0:ny], corr[k][0:ny])
                ends = rot(sw[k], nz - 8 - SEG * (p - first), 1)
                out_ref[k, p - first] = jnp.where(inner, body, ends)

    lane24 = lax.broadcasted_iota(jnp.int32, (ny + 8, nz), 1)
    slot24 = lane24 // SEG
    left24 = (lane24 % SEG) < 8

    span = range(2)

    def x_up(vs):
        rs = [rot(v, -SEG, 1) for v in vs]
        return [jnp.where(lane24 < nz - SEG, rs[t], rs[t ^ 1]) for t in span]

    def x_down(vs):
        rs = [rot(v, SEG, 1) for v in vs]
        return [jnp.where(lane24 >= SEG, rs[t], rs[t ^ 1]) for t in span]

    def strip_curl(u):
        u1p, u2p = x_up(u[1]), x_up(u[2])
        f1 = [face_one(u[0][t], u[2][t], u2p[t]) for t in span]
        f2 = [face_two(u[0][t], u[1][t], u1p[t]) for t in span]
        f0 = [face_zero(u[1][t], u[2][t]) for t in span]
        f1m, f2m = x_down(f1), x_down(f2)
        out = [edges(f0[t], f1[t], f2[t], f1m[t], f2m[t]) for t in span]
        return [[out[t][k] for t in span] for k in range(3)]

    def strips(base):
        sr = [[st[k, 2 * base + t] for t in span] for k in range(3)]
        sk = [[st[3 + k, 2 * base + t] for t in span] for k in range(3)]
        outer = (slot24 == 3) | (slot24 == nx - 3)
        scale = [[jacobi_scale(sk[k][t]) for t in span] for k in range(3)]
        u = [[scale[k][t] * sr[k][t] for t in span] for k in range(3)]
        for k in range(3):
            u[k][1] = jnp.where(outer, sr[k][1], u[k][1])
        cc = strip_curl(u)
        u = [[next_iter(sr[k][t], sk[k][t], scale[k][t], u[k][t], cc[k][t]) for t in span] for k in range(3)]
        cc = strip_curl(u)
        m = [[masked_residual(sr[k][t], sk[k][t], u[k][t], cc[k][t]) for t in span] for k in range(3)]
        m0m = x_down(m[0])
        r = [nodal_rhs(m[0][t], m0m[t], m[1][t], m[2][t]) for t in span]
        s = []
        for q in range(4):
            rq = [r[t][q] for t in span]
            rm, rp = x_down(rq), x_up(rq)
            s.append([nodal_step(rq[t], rm[t], rp[t]) if q < 2 or t % 2 == 0 else None for t in span])
        s0p, s1p = x_up(s[0]), x_up(s[1])
        s0, s1, s2, s3 = [s[q][0] for q in range(4)]
        corr = (
            (s0p[0] - s0) + (s1 + s1p[0]) * 0.5,
            (y_up(s0) - s0) + (s2 + y_up(s2)) * 0.5,
            (z_up(s0) - s0) + (s3 + z_up(s3)) * 0.5,
        )
        for k in range(3):
            result = finish(sr[k][0], sk[k][0], u[k][0], corr[k])[0:ny]
            sw[k] = result if base == 0 else jnp.where(left, sw[k], result)

    def corner_of(f, tile, off):
        if f < 5:
            piece = rot(tile, off - 3 * f, 1)
            for k, to in fourth:
                if off == 8 and k == f:
                    at = ((slot == nx - 1) & (lane % SEG == 11))[0:tile.shape[0]]
                    piece = jnp.where(at, rot(tile, SEG * (nx - 1 - 4) + 11 - to, 1), piece)
            return piece
        piece = None
        for at, to, u in spare:
            piece = pick(piece, slot[0:tile.shape[0]] == at, rot(tile, SEG * (at - to) + off - 3 * u, 1))
        return piece

    with scope("endswait"):
        arrived(9, 5 * ny // 8)
    with scope("strippack"):
        for f in range(6):
            t, to = divmod(2 * f, 8)
            piece = rot(ends_in[f // 2], SEG * (0 - 3 * (f % 2)), 1)
            piece = jnp.where(slot >= nx - 2, rot(ends_in[3 + t], SEG * (nx - 2 - to), 1), piece)
            if f < 3:
                piece = jnp.where(slot == 3, rot(ends_in[0], SEG * (3 - (5 + f)), 1), piece)
                piece = jnp.where(slot == nx - 3, rot(ends_in[4], SEG * (nx - 3 - (4 + f)), 1), piece)
            mid = packs[f]
            st[f, 0, 0:ny, :] = mid
            st[f, 1, 0:ny, :] = piece
            st[f, 2, 0:ny, :] = mid
            st[f, 3, 0:ny, :] = piece
        y_start(8, strip_tiles, yd_out, yd_in)


    def crossed(ref, *where):
        if paired:
            return ref[(0, *where)]
        return jnp.where(row < 4, ref[(0, *where)], ref[(1, *where)])

    def strip_inputs(base):
        with scope("ystrip"):
            if base == 0:
                y_finish(8, strip_tiles, yd_in)
            arrived(10 - 9 * base, 2 * ny // 8 + 2 * (ny // 2) // 8 + 4 * dx_in.shape[0])
            off = 8 - 4 * base
            minus, plus = dr[0, base], dr[1, base]
            low = low_half[0:ny // 2]
            own_corner = jnp.concatenate(
                [jnp.where(low, plus, rot(minus, half, 1)), jnp.where(low, rot(plus, half, 1), minus)], axis=0
            )
            cross_corner = jnp.where(low_half[0:8], crossed(dx_in, 1, base), crossed(dx_in, 0, base))
            for f in range(6):
                t, q = divmod(f, 4)
                for rows, tile, corner in (
                    (slice(0, ny), zr[base, t], own_corner), (halo, crossed(zx_in, base, t), cross_corner),
                ):
                    mine = left[0:tile.shape[0]] if base == 0 else ~left[0:tile.shape[0]]
                    for at, piece in ((2 * base, rot(tile, off - 4 * q, 1)), (2 * base + 1, corner_of(f, corner, 8 - 3 * base))):
                        st[f, at, rows, :] = jnp.where(mine, st[f, at, rows, :], piece)

    late_up = [(upper_in, (i,)) for i in range(4)] + [(e, (4, last + 2))]

    def lower_inputs():
        with scope("ylow"):
            pl.when(narrow)(lambda: y_finish(11, late_low, ye_in))
            pl.when(wide)(lambda: arrived(5, 6 * (ny + 8) // 8))

    def upper_inputs():
        with scope("yup"):
            pl.when(jnp.logical_not(thin))(lambda: arrived(4, (5 * (ny + 8) + 3 * ny) // 8))
            pl.when(thin)(lambda: y_finish(0, late_up, yf_in))

    def lower_side():
        with scope("lower"):
            p = first - 1
            curl_sweep(u1, (lower_in[0] - u1[2, p], u1[1, p] - lower_in[1]), p, first, emit_second)
            f1, f2 = lower_in[3] - u2[2, p], u2[1, p] - lower_in[4]
            cc = (z_down(f1) - f1) - (y_down(f2) - f2)
            mm[0, p - 1] = jnp.where(lower_in[2] > 0.0, lower_in[5] - cc, 0.0)
            curl_sweep(u2, (f1, f2), p, first + 1, emit_masked)
            node_range(p, first + 2)

    def upper_side():
        with scope("upper"):
            p = last + 1
            f1 = face_one(u1[0, p], u1[2, p], upper_in[1])
            f2 = face_two(u1[0, p], u1[1, p], upper_in[0])
            curl_sweep(u1, faces(u1, last), p, p + 1, emit_second, (f1, f2))
            f1 = face_one(u2[0, p], u2[2, p], upper_in[3])
            f2 = face_two(u2[0, p], u2[1, p], upper_in[2])
            curl_sweep(u2, faces(u2, last - 1), last, p + 1, emit_masked, (f1, f2))
            node_range(last, p + 1)
            v0 = u2[0, p]
            q2 = jnp.where(e[4, p + 1] > 0.0, u2[1, p] + (y_up(v0) - v0), 0.0)
            q1 = jnp.where(e[5, p + 1] > 0.0, (z_up(v0) - v0) + u2[2, p], 0.0)
            m0, m0p = mm[0, p], upper_in[4]
            rr[0, p + 1] = (m0 - m0p) + (upper_in[5] + (y_down(q2) - q2) + (z_down(q1) - q1))
            rr[1, p + 1] = (m0p + m0) * 0.5

    def in_turn(*pieces):
        for piece in pieces:
            piece()

    def write_all():
        with scope("out"):
            outputs(first, last + 1)

    def side_strips(base):
        strip_inputs(base)
        with scope("strips"):
            strips(base)

    def raw_relays():
        del sent_tiles[counted:]
        relay("rawup", ((2, 6),), 6, raw_up, yb_out, yb_in)
        relay("rawlow", ((3, 6),), 7, raw_low, yc_out, yc_in)

    counted = len(sent_tiles)
    strips_first = lax.rem(device(gx=1)["gx"], 4) == 3
    pl.when(jnp.logical_not(strips_first))(lambda: raw_relays())
    side_strips(0)
    pl.when(strips_first)(lambda: raw_relays())

    @pl.when(narrow)
    def _():
        relay("latelow", ((5, 6),), 11, late_low, ye_out, ye_in)

    base_tiles = sum(sent_tiles)

    @pl.when(thin)
    def _():
        relay("lateup", ((4, 8),), 0, late_up, yf_out, yf_in)

    def raw_sides():
        with scope("yraw"):
            y_finish(7, raw_low, yc_in)
            y_finish(6, raw_up, yb_in)
        with scope("rawsides"):
            first_range(first - 1, first)
            first_range(last + 1, last + 2)
            curl_sweep(u1, faces(u1, first - 1), first, first + 1, emit_second)
            curl_sweep(u1, faces(u1, last - 1), last, last + 1, emit_second)
            curl_sweep(u2, faces(u2, first), first + 1, first + 2, emit_rest)
            curl_sweep(u2, faces(u2, last - 2), last - 1, last, emit_masked)
            node_range(last - 1, last)

    pl.when(thin)(raw_sides)
    side_strips(1)
    pl.when(jnp.logical_not(thin))(raw_sides)
    in_turn(lower_inputs, upper_inputs, lower_side, upper_side, write_all)
    with scope("sendwait"):
        total = base_tiles
        sides = dx_in.shape[0]
        pl.when(down_first)(lambda: wait_tiles(send.at[0], total + 1))
        pl.when(wide)(lambda: wait_tiles(send.at[0], total - 6 * sides))
        pl.when(thin)(lambda: wait_tiles(send.at[0], total + 5 * sides))
        pl.when(jnp.logical_not(down_first | wide | thin))(lambda: wait_tiles(send.at[0], total))


def on_device(sizes, rhs, conductivity, fraction, region, flags):
    _, nx, ny, nz = rhs.shape
    planes = nx + 2 * PAD
    rows = ny + 8
    f32 = jnp.float32
    hbm = pl.BlockSpec(memory_space=pl.ANY)
    sides = 1 if sizes[1] == 2 else 2
    relays = []
    for count in (6 * nx, 6, 6, 24, 6, 5):
        relays += [pltpu.VMEM((count, 8, nz), f32), pltpu.VMEM((sides, count, 8, nz), f32)]
    return pl.pallas_call(
        functools.partial(kernel, sizes, nx, ny, nz),
        out_shape=pltpu.VMEM(rhs.shape, rhs.dtype),
        in_specs=[hbm] * 5,
        out_specs=pl.BlockSpec(memory_space=pltpu.VMEM),
        scratch_shapes=[
            pltpu.SMEM(conductivity.shape, f32),
            pltpu.VMEM(rhs.shape, f32),
            pltpu.VMEM(region.shape, jnp.int32),
            pltpu.VMEM(flags.shape, jnp.int32),
            pltpu.VMEM((6, planes, rows, nz), f32),
            pltpu.VMEM((6, 4, rows, nz), f32),
            pltpu.VMEM((3, ny, nz), f32),
            pltpu.VMEM((3, planes, rows, nz), f32),
            pltpu.VMEM((3, planes, rows, nz), f32),
            pltpu.VMEM((3, planes, rows, nz), f32),
            pltpu.VMEM((3, planes, rows, nz), f32),
            pltpu.VMEM((4, planes, rows, nz), f32),
            pltpu.VMEM((2, 2, ny, nz), f32),
            pltpu.VMEM((2, 2, ny, nz), f32),
            pltpu.VMEM((2, 2, ny // 2, nz), f32),
            pltpu.VMEM((2, 2, ny // 2, nz), f32),
            pltpu.VMEM((2, 8, nz), f32),
            pltpu.VMEM((sides, 2, 2, 8, nz), f32),
            pltpu.VMEM((2, 2, 8, nz), f32),
            pltpu.VMEM((sides, 2, 2, 8, nz), f32),
            pltpu.VMEM((5, ny, nz), f32),
            pltpu.VMEM((5, ny, nz), f32),
            pltpu.VMEM((6, rows, nz), f32),
            pltpu.VMEM((6, rows, nz), f32),
            pltpu.VMEM((6, rows, nz), f32),
            pltpu.VMEM((6, rows, nz), f32),
            *relays,
            pltpu.VMEM((320, 8, nz), f32),
            pltpu.SemaphoreType.DMA((2,)),
            pltpu.SemaphoreType.DMA((1,)),
            pltpu.SemaphoreType.DMA((12,)),
            pltpu.SemaphoreType.REGULAR((2,)),
        ],
        compiler_params=pltpu.CompilerParams(
            collective_id=0, has_side_effects=True, vmem_limit_bytes=60 * 1024 * 1024
        ),
    )(conductivity, rhs, fraction, region, flags)


def solution(mesh):
    sizes = tuple(mesh.shape[name] for name in ("gx", "gy", "gz"))
    return jax.shard_map(
        functools.partial(on_device, sizes),
        mesh=mesh,
        in_specs=(
            P(None, "gx", "gy", "gz"),
            P(),
            P(None, "gx", "gy", "gz"),
            P("gx", "gy", "gz"),
            P(None, "gx", "gy", "gz"),
        ),
        out_specs=P(None, "gx", "gy", "gz"),
        check_vma=False,
    )
```
